32 devices in a mesh: rep: 2 (over y), shard: 16 (over z, x, core).
Axes of the slice: x: 2, y: 2, z: 4, core: 2. Of those that a mesh axis runs over, the one named last changes fastest.
Arguments:
- tokens: bfloat16 [2, 3072, 768], P('rep', 'shard'), may hold values from -6 to 6
- segments: int32 [2, 3072], P('rep', 'shard'), may hold values from 0 to 16, never falling along the last dimension, each value on 1 to 2304 neighbouring positions
- padding: int32 [2, 3072], P('rep', 'shard'), may hold values from 0 to 1, as said below
- query_weight: float32 [768, 768], P('shard'), may hold values from -0.21875 to 0.21875
- key_weight: float32 [768, 768], P('shard'), may hold values from -0.21875 to 0.21875
- value_weight: float32 [768, 768], P('shard'), may hold values from -0.21875 to 0.21875
- query_bias: float32 [768], P('shard'), may hold values from -3 to 3
- value_bias: float32 [768], P('shard'), may hold values from -3 to 3
- out_weight: float32 [768, 768], P('shard'), may hold values from -0.875 to 0.875
- out_bias: float32 [768], P('shard'), may hold values from -3 to 3
- middle_gain: float32 [768], P('shard'), may hold values from 0.5 to 1.5
- middle_shift: float32 [768], P('shard'), may hold values from -3 to 3
- up_weight: float32 [768, 3072], P('shard'), may hold values from -0.21875 to 0.21875
- up_bias: float32 [3072], P('shard'), may hold values from -3 to 3
- down_weight: float32 [3072, 768], P('shard'), may hold values from -0.109375 to 0.109375
- down_bias: float32 [768], P('shard'), may hold values from -3 to 3
- final_gain: float32 [768], P('shard'), may hold values from 0.5 to 1.5
- final_shift: float32 [768], P('shard'), may hold values from -3 to 3
- cotangent: bfloat16 [2, 3072, 768], P('rep', 'shard'), may hold values from -6 to 6
Outputs:
- output: bfloat16 [2, 3072, 768], P('rep', 'shard')
- grad_tokens: bfloat16 [2, 3072, 768], P('rep', 'shard')
- grad_query_weight: float32 [768, 768], P('shard')
- grad_key_weight: float32 [768, 768], P('shard')
- grad_value_weight: float32 [768, 768], P('shard')
- grad_query_bias: float32 [768], P('shard')
- grad_value_bias: float32 [768], P('shard')
- grad_out_weight: float32 [768, 768], P('shard')
- grad_out_bias: float32 [768], P('shard')
- grad_middle_gain: float32 [768], P('shard')
- grad_middle_shift: float32 [768], P('shard')
- grad_up_weight: float32 [768, 3072], P('shard')
- grad_up_bias: float32 [3072], P('shard')
- grad_down_weight: float32 [3072, 768], P('shard')
- grad_down_bias: float32 [768], P('shard')
- grad_final_gain: float32 [768], P('shard')
- grad_final_shift: float32 [768], P('shard')
The draws below stay inside these ranges and needn't reach their ends.
Inputs may be any that keep to these rules, and one draw needn't show every extreme that they name: `segments`: within each sequence the numbers never fall; every document has 1 to 2304 tokens and one has exactly 2304. Each sequence ends with a run of at least one padding token and has no other padding.
All inputs are finite; a program needn't handle non-finite values.
Results may differ from the reference program's by a relative error of at most 0.024.
Values may be sent and summed in bfloat16 or wider, within the bound.
A program may use at most 256 MiB of HBM per device.

```python
import math
import jax
import jax.numpy as jnp
import numpy as np
from jax import lax

D = 768
HEADS = 12
HEAD_DIM = 64
FF = 3072
TOK_DEV = 192
SEQ_LEN = 3072
SEQS = 2
DOCS = 17
LONGEST = 2304


def draw_padding(key, part):
    pad_length = jax.random.randint(key, (SEQS, 1), 1, TOK_DEV + 1)
    places = jnp.arange(SEQ_LEN, dtype=jnp.int32)[None, :]
    return (places < SEQ_LEN - pad_length).astype(jnp.int32)


def block_scale(own_key, shape, cuts, least, top_value):
    factor_of, own = 1.0, jax.random.fold_in(own_key, 6)
    for dim, shards_of in cuts:
        heights = jnp.exp(jax.random.uniform(jax.random.fold_in(own, dim), (shards_of,), jnp.float32, least / len(cuts), top_value / len(cuts)))
        factor_of = factor_of * jnp.repeat(heights, shape[dim] // shards_of).reshape([-1 if axis == dim else 1 for axis in range(len(shape))])
    return factor_of


def profile(amount, total, limit, slope):
    portions = [(1 << 20) // math.isqrt(rank ** slope) + 1 for rank in range(2, amount + 1)]
    surplus, counts = total - limit - (amount - 1), [1] * (amount - 1)
    while surplus > 0:
        free = [i for i in range(amount - 1) if counts[i] < limit]
        mass, left = sum([portions[i] for i in free]), surplus
        for i in free:
            extra = min(limit - counts[i], max(1, left * portions[i] // mass), surplus)
            counts[i] = counts[i] + extra
            surplus = surplus - extra
    return np.array([limit] + counts)


def ragged_sizes(key, number_of, total, reach, lean):
    if number_of == 2:
        one = jax.random.randint(key, (), max(1, total - reach), min(reach, total - 1) + 1)
        return jnp.stack([one, total - one])
    lengths = jnp.asarray(profile(number_of, total, reach, lean), jnp.int32)
    couples = (number_of - 1) // 2
    donor, receiver = lengths[1:1 + 2 * couples:2], lengths[2:2 + 2 * couples:2]
    margin = jnp.minimum(donor - 1, reach - receiver)
    moved = jax.random.randint(jax.random.fold_in(key, 1), (couples,), 0, 1 << 20) % (margin + 1)
    lengths = lengths.at[1:1 + 2 * couples:2].set(donor - moved).at[2:2 + 2 * couples:2].set(receiver + moved)
    return lengths[jax.random.permutation(jax.random.fold_in(key, 2), number_of)]


def centred(stream_key, dims, width, reach, cuts=(), held_as=jnp.bfloat16):
    entries = jax.random.normal(stream_key, dims, jnp.float32) * width
    if len(cuts) > 0:
        entries = block_scale(stream_key, dims, cuts, -0.22, 0.18) * entries
    return jnp.clip(entries, min=-reach, max=reach).astype(held_as)


def setup_inputs(seed: int = 0) -> dict:
    seeds = jax.random.split(jax.random.key(seed), 20)
    return {
        "tokens": centred(seeds[0], (SEQS, SEQ_LEN, D), 1.0, 6.0, ((0, 2), (1, 16))),
        "segments": jax.vmap(lambda own: jnp.searchsorted(jnp.cumsum(ragged_sizes(own, DOCS, SEQ_LEN, LONGEST, 2)), jnp.arange(SEQ_LEN), side="right"))(jax.random.split(seeds[1], SEQS)).reshape((SEQS, SEQ_LEN)).astype(jnp.int32),
        "padding": draw_padding(jax.random.fold_in(seeds[19], 71), 0),
        "query_weight": centred(seeds[3], (D, D), D ** -0.5, 0.21875, ((0, 16),), jnp.float32),
        "key_weight": centred(seeds[4], (D, D), D ** -0.5, 0.21875, ((0, 16),), jnp.float32),
        "value_weight": centred(seeds[5], (D, D), D ** -0.5, 0.21875, ((0, 16),), jnp.float32),
        "query_bias": centred(seeds[6], (D,), 0.5, 3.0, ((0, 16),), jnp.float32),
        "value_bias": centred(seeds[7], (D,), 0.5, 3.0, ((0, 16),), jnp.float32),
        "out_weight": centred(seeds[8], (D, D), (D // 16) ** -0.5, 0.875, ((0, 16),), jnp.float32),
        "out_bias": centred(seeds[9], (D,), 0.5, 3.0, ((0, 16),), jnp.float32),
        "middle_gain": jnp.clip(1.0 + 0.1 * jax.random.normal(seeds[10], (D,), jnp.float32), 0.5, 1.5),
        "middle_shift": centred(seeds[11], (D,), 0.5, 3.0, ((0, 16),), jnp.float32),
        "up_weight": centred(seeds[12], (D, FF), D ** -0.5, 0.21875, ((0, 16),), jnp.float32),
        "up_bias": centred(seeds[13], (FF,), 0.5, 3.0, ((0, 16),), jnp.float32),
        "down_weight": centred(seeds[14], (FF, D), FF ** -0.5, 0.109375, ((0, 16),), jnp.float32),
        "down_bias": centred(seeds[15], (D,), 0.5, 3.0, ((0, 16),), jnp.float32),
        "final_gain": jnp.clip(1.0 + 0.1 * jax.random.normal(seeds[16], (D,), jnp.float32), 0.5, 1.5),
        "final_shift": centred(seeds[17], (D,), 0.5, 3.0, ((0, 16),), jnp.float32),
        "cotangent": centred(seeds[18], (SEQS, SEQ_LEN, D), 1.0, 6.0, ((0, 2), (1, 16))),
    }


highest = lax.Precision.HIGHEST
epsilon = 1e-12
very_low = -1e+30

@jax.custom_vjp
def low(v):
    return lax.optimization_barrier(v.astype(jnp.bfloat16)).astype(jnp.float32)

@jax.custom_vjp
def low_back(v):
    return v

def low_keep(v):
    return (low(v), None)

def low_pass(kept, grad):
    return (grad,)

def back_keep(v):
    return (v, None)

def back_low(kept, grad):
    return (low(grad),)
low.defvjp(low_keep, low_pass)
low_back.defvjp(back_keep, back_low)

def product(left, right):
    return jnp.dot(left, right, precision=highest, preferred_element_type=jnp.float32)

def both_ways(value):
    return low(low_back(value))

def layer_norm(value, gain, shift):
    center = value - lax.optimization_barrier(jnp.mean(value, axis=-1, keepdims=True))
    spread = lax.optimization_barrier(jnp.mean(center * center, axis=-1, keepdims=True))
    return center * lax.rsqrt(spread + epsilon) * gain + shift

def attention(queries, key_rows, value_rows, codes):
    length = 512 if SEQ_LEN % 512 == 0 else SEQ_LEN
    number = SEQ_LEN // length

    def one_block(inputs):
        query_block, query_codes = inputs
        scores = low_back(jnp.einsum('qhd,khd->hqk', query_block, key_rows, precision=highest) * 0.125)
        allowed = (query_codes[:, None] == codes[None, :])[None]
        masked = jnp.where(allowed, scores, very_low)
        largest = lax.optimization_barrier(jnp.max(masked, axis=2, keepdims=True))
        total = lax.optimization_barrier(jnp.sum(jnp.where(allowed, jnp.exp(masked - largest), 0.0), axis=2, keepdims=True))
        log_total = largest + jnp.log(total)
        chances = low(jnp.where(allowed, jnp.exp(masked - log_total), 0.0))
        return jnp.einsum('hqk,khd->qhd', chances, value_rows, precision=highest)
    blocks = lax.map(jax.checkpoint(one_block), (queries.reshape(number, length, HEADS, HEAD_DIM), codes.reshape(number, length)))
    return blocks.reshape(SEQ_LEN, HEADS * HEAD_DIM)

def one_sequence(params, inputs, codes):
    w_query, w_key, w_value, b_query, b_value, w_out, b_out, gain_mid, shift_mid, w_up, b_up, w_down, b_down, gain_end, shift_end = params
    queries = both_ways(product(inputs, w_query) + b_query)
    key_rows = both_ways(product(inputs, w_key))
    value_rows = both_ways(product(inputs, w_value) + b_value)
    context = attention(queries.reshape(SEQ_LEN, HEADS, HEAD_DIM), key_rows.reshape(SEQ_LEN, HEADS, HEAD_DIM), value_rows.reshape(SEQ_LEN, HEADS, HEAD_DIM), codes)
    context = both_ways(context)
    branch = low_back(product(context, w_out) + b_out)
    middle = layer_norm(inputs + branch, gain_mid, shift_mid)
    hidden = low_back(product(low(middle), w_up) + b_up)
    active = low(jax.nn.gelu(hidden, approximate=False))
    feed = low_back(product(active, w_down) + b_down)
    return layer_norm(middle + feed, gain_end, shift_end)

def forward(inputs, params, codes):
    rounded = tuple((low(item) for item in params))

    def per_sequence(pair):
        return one_sequence(rounded, pair[0], pair[1])
    return lax.map(per_sequence, (inputs, codes))

def reference(tokens, segments, padding, query_weight, key_weight, value_weight, query_bias, value_bias, out_weight, out_bias, middle_gain, middle_shift, up_weight, up_bias, down_weight, down_bias, final_gain, final_shift, cotangent):
    codes = (2 * segments + padding).astype(jnp.int32)
    params = (query_weight, key_weight, value_weight, query_bias, value_bias, out_weight, out_bias, middle_gain, middle_shift, up_weight, up_bias, down_weight, down_bias, final_gain, final_shift)
    inputs = tokens.astype(jnp.float32)

    def whole(value, weights):
        return forward(value, weights, codes)
    result, pullback = jax.vjp(whole, inputs, params)
    grad_inputs, grads = pullback(cotangent.astype(jnp.float32))
    return (result.astype(jnp.bfloat16), grad_inputs.astype(jnp.bfloat16), grads[0], grads[1], grads[2], grads[3], grads[4], grads[5], grads[6], grads[7], grads[8], grads[9], grads[10], grads[11], grads[12], grads[13], grads[14])
```

```python
import functools

import jax
import jax.numpy as jnp
from jax import lax
from jax.experimental import pallas as pl
from jax.experimental.pallas import tpu as pltpu
from jax.sharding import PartitionSpec as P

D = 768
HEADS = 12
HEAD_DIM = 64
PLANE = 4
GROUP_HEADS = HEADS // PLANE
GROUP_DIM = GROUP_HEADS * HEAD_DIM
FF = 3072
GROUP_FF = FF // PLANE

epsilon = 1e-12
very_low = -1e30
root_half = 0.7071067811865476
inv_root_tau = 0.3989422804014327
bf16 = jnp.bfloat16
f32 = jnp.float32
MESH = pl.DeviceIdType.MESH
VMEM_SPEC = pl.BlockSpec(memory_space=pltpu.VMEM)
ANY_SPEC = pl.BlockSpec(memory_space=pl.ANY)
VMEM_BYTES = 60000 * 1024


def struct(shape, dtype=bf16):
    return jax.ShapeDtypeStruct(shape, dtype)


def comm_call(body, name, ident, inputs, out_shapes, out_specs, scratch):
    return pl.pallas_call(
        body,
        name=name,
        out_shape=out_shapes,
        in_specs=[VMEM_SPEC] * len(inputs),
        out_specs=out_specs,
        scratch_shapes=scratch,
        compiler_params=pltpu.CompilerParams(
            collective_id=ident, has_side_effects=True, vmem_limit_bytes=VMEM_BYTES
        ),
    )(*inputs)


def greet(peers):
    barrier = pltpu.get_barrier_semaphore()
    for peer in peers:
        pl.semaphore_signal(barrier, inc=1, device_id=peer, device_id_type=MESH)
    pl.semaphore_wait(barrier, len(peers))


def remote(src, dst, send_sem, recv_sem, peer):
    return pltpu.make_async_remote_copy(
        src_ref=src,
        dst_ref=dst,
        send_sem=send_sem,
        recv_sem=recv_sem,
        device_id=peer,
        device_id_type=MESH,
    )


def plane_peer(me, mask):
    group = lax.rem(me, PLANE)
    core = lax.rem(group, 2)
    column = lax.div(group, 2)
    if mask & 1:
        core = 1 - core
    if mask & 2:
        column = 1 - column
    return me - group + 2 * column + core


def plane_slot(me, mask):
    return lax.rem(plane_peer(me, mask), PLANE)


def plane_gather(value, ident):
    rows, cols = value.shape

    def body(x_ref, out_ref, send, recv, local):
        me = lax.axis_index("shard")
        peers = [{"shard": plane_peer(me, mask)} for mask in (1, 2)]
        greet(peers)
        mine, far = lax.rem(me, PLANE), plane_slot(me, 2)
        own = pltpu.make_async_copy(x_ref, out_ref.at[mine], local)
        own.start()
        across = remote(x_ref, out_ref.at[mine], send.at[0], recv.at[0], peers[1])
        across.start()
        beside = remote(x_ref, out_ref.at[mine], send.at[1], recv.at[1], peers[0])
        beside.start()
        across.wait_recv()
        relay = remote(out_ref.at[far], out_ref.at[far], send.at[2], recv.at[2], peers[0])
        relay.start()
        beside.wait_recv()
        relay.wait_recv()
        across.wait_send()
        beside.wait_send()
        relay.wait_send()
        own.wait()

    return comm_call(
        body,
        "plane_gather",
        ident,
        [value],
        struct((PLANE, rows, cols), value.dtype),
        VMEM_SPEC,
        [
            pltpu.SemaphoreType.DMA((3,)),
            pltpu.SemaphoreType.DMA((3,)),
            pltpu.SemaphoreType.DMA,
        ],
    )


def plane_sum(parts, ident):
    _, rows, cols = parts.shape

    def body(p_ref, out_ref, near, held, far_in, send, recv):
        me = lax.axis_index("shard")
        peers = [{"shard": plane_peer(me, mask)} for mask in (1, 2)]
        greet(peers)
        first = remote(
            p_ref.at[plane_slot(me, 3)], near.at[0], send.at[0], recv.at[0], peers[0]
        )
        first.start()
        second = remote(
            p_ref.at[plane_slot(me, 1)], near.at[1], send.at[1], recv.at[1], peers[0]
        )
        second.start()
        first.wait_recv()
        held[...] = (p_ref[plane_slot(me, 2)].astype(f32) + near[0].astype(f32)).astype(bf16)
        third = remote(held, far_in, send.at[2], recv.at[2], peers[1])
        third.start()
        second.wait_recv()
        out_ref[...] = p_ref[lax.rem(me, PLANE)].astype(f32) + near[1].astype(f32)
        third.wait_recv()
        out_ref[...] += far_in[...].astype(f32)
        first.wait_send()
        second.wait_send()
        third.wait_send()

    return comm_call(
        body,
        "plane_sum",
        ident,
        [parts],
        struct((rows, cols), f32),
        VMEM_SPEC,
        [
            pltpu.VMEM((2, rows, cols), bf16),
            pltpu.VMEM((rows, cols), bf16),
            pltpu.VMEM((rows, cols), bf16),
            pltpu.SemaphoreType.DMA((3,)),
            pltpu.SemaphoreType.DMA((3,)),
        ],
    )


def others(me, count):
    return [{"shard": lax.rem(me + step, count)} for step in range(1, count)]


def gather_weights(count, tokens, qkv, up, out_w, down, small, ident):
    planes = count // PLANE
    rows = qkv.shape[1]
    block = down.shape[0]

    def body(x_ref, qkv_ref, up_ref, wo_ref, down_ref, small_ref, *rest):
        x_out, qkv_out, up_out, wo_out, down_out, small_out = rest[:6]
        send, recv, local, send_wo, recv_wo = rest[6:]
        me = lax.axis_index("shard")
        group, plane = lax.rem(me, PLANE), lax.div(me, PLANE)
        greet(others(me, count))
        owns = [
            (x_ref, x_out.at[group]),
            (qkv_ref.at[group], qkv_out.at[me]),
            (up_ref.at[group], up_out.at[me]),
            (down_ref, down_out.at[plane]),
            (small_ref, small_out.at[me]),
        ]
        started = []
        for index, (src, dst) in enumerate(owns):
            copy = pltpu.make_async_copy(src, dst, local.at[index])
            copy.start()
            started.append(copy)
        sent = []

        def push(src, dst, peer):
            index = len(sent)
            copy = remote(src, dst, send.at[index], recv.at[index], {"shard": peer})
            copy.start()
            sent.append(copy)

        for mask in (2, 1, 3):
            push(x_ref, x_out.at[group], plane_peer(me, mask))
        for src, dst in ((small_ref, small_out), (qkv_ref, qkv_out), (up_ref, up_out)):
            for step in range(1, count):
                peer = lax.rem(me + step, count)
                piece = src if src is small_ref else src.at[lax.rem(peer, PLANE)]
                push(piece, dst.at[me], peer)
        for step in range(1, planes):
            push(down_ref, down_out.at[plane], lax.rem(me + PLANE * step, count))
        target, place = lax.div(me, planes), lax.rem(me, planes)

        def wo_copy(source, index):
            peer = PLANE * index + target
            return peer, remote(
                wo_ref, wo_out.at[place], send_wo.at[index], recv_wo.at[source], {"shard": peer}
            )

        for index in range(planes):
            peer, copy = wo_copy(place, index)
            pl.when(peer != me)(copy.start)
        keep = pltpu.make_async_copy(wo_ref, wo_out.at[place], local.at[5])
        pl.when(target == group)(keep.start)
        for copy in sent:
            copy.wait_recv()
        for index in range(planes):
            pl.when(group * planes + index != me)(wo_copy(index, index)[1].wait_recv)
        for index in range(planes):
            peer, copy = wo_copy(place, index)
            pl.when(peer != me)(copy.wait_send)
        pl.when(target == group)(keep.wait)
        for copy in sent:
            copy.wait_send()
        for copy in started:
            copy.wait()

    total = 3 + 3 * (count - 1) + planes - 1
    return comm_call(
        body,
        "gather_weights",
        ident,
        [tokens, qkv, up, out_w, down, small],
        [
            struct((PLANE,) + tokens.shape),
            struct((count, rows, qkv.shape[2])),
            struct((count, rows, up.shape[2])),
            struct((planes,) + out_w.shape),
            struct((planes, block, D)),
            struct((count,) + small.shape),
        ],
        [ANY_SPEC] * 6,
        [
            pltpu.SemaphoreType.DMA((total,)),
            pltpu.SemaphoreType.DMA((total,)),
            pltpu.SemaphoreType.DMA((6,)),
            pltpu.SemaphoreType.DMA((planes,)),
            pltpu.SemaphoreType.DMA((planes,)),
        ],
    )


def gather_planes(count, value, ident):
    planes = count // PLANE

    def body(x_ref, out_ref, send, recv, local):
        me = lax.axis_index("shard")
        plane = lax.div(me, PLANE)
        peers = [{"shard": lax.rem(me + PLANE * s, count)} for s in range(1, planes)]
        greet(peers)
        own = pltpu.make_async_copy(x_ref, out_ref.at[plane], local)
        own.start()
        sent = []
        for index, peer in enumerate(peers):
            copy = remote(x_ref, out_ref.at[plane], send.at[index], recv.at[index], peer)
            copy.start()
            sent.append(copy)
        for copy in sent:
            copy.wait_recv()
        for copy in sent:
            copy.wait_send()
        own.wait()

    return comm_call(
        body,
        "gather_planes",
        ident,
        [value],
        struct((planes,) + value.shape),
        ANY_SPEC,
        [
            pltpu.SemaphoreType.DMA((planes,)),
            pltpu.SemaphoreType.DMA((planes,)),
            pltpu.SemaphoreType.DMA,
        ],
    )


def sum_planes(count, parts, ident):
    planes, rows, cols = parts.shape

    def body(p_ref, out_ref, held, send, recv):
        me = lax.axis_index("shard")
        plane = lax.div(me, PLANE)
        peers = [lax.rem(me + PLANE * s, count) for s in range(1, planes)]
        greet([{"shard": peer} for peer in peers])
        sent = []
        for index, peer in enumerate(peers):
            copy = remote(
                p_ref.at[lax.div(peer, PLANE)],
                held.at[index],
                send.at[index],
                recv.at[index],
                {"shard": peer},
            )
            copy.start()
            sent.append(copy)
        for copy in sent:
            copy.wait_recv()
        total = p_ref[plane].astype(f32)
        for index in range(planes - 1):
            total = total + held[index].astype(f32)
        out_ref[...] = total.astype(bf16)
        for copy in sent:
            copy.wait_send()

    return comm_call(
        body,
        "sum_planes",
        ident,
        [parts],
        struct((rows, cols)),
        VMEM_SPEC,
        [
            pltpu.VMEM((planes - 1, rows, cols), bf16),
            pltpu.SemaphoreType.DMA((planes,)),
            pltpu.SemaphoreType.DMA((planes,)),
        ],
    )


def reduce_grads(count, copies, qkv, up, out_w, down, small, ident):
    planes = count // PLANE
    rows = qkv.shape[1]
    block = down.shape[1]
    arrays = [qkv, up, out_w, small]

    def body(qkv_ref, up_ref, wo_ref, small_ref, down_ref, *rest):
        outs, (qkv_in, up_in, wo_in, small_in, down_in) = rest[:5], rest[5:10]
        halves, gets = rest[10:15], rest[15:20]
        send, recv, send_rep, recv_rep, send_wo, recv_wo = rest[20:]
        me = lax.axis_index("shard")
        rep = lax.axis_index("rep")
        plane = lax.div(me, PLANE)
        across = [{"rep": lax.rem(rep + step, copies)} for step in range(1, copies)]
        greet(others(me, count) + across)
        sent = []

        def push(src, dst, peer):
            index = len(sent)
            copy = remote(src, dst, send.at[index], recv.at[index], {"shard": peer})
            copy.start()
            sent.append(copy)

        pairs = [(qkv_ref, qkv_in), (up_ref, up_in), (small_ref, small_in)]
        group = lax.rem(me, PLANE)
        target, place = lax.div(me, planes), lax.rem(me, planes)
        for src, held in pairs:
            for step in range(1, count):
                peer = lax.rem(me + step, count)
                push(src.at[peer], held.at[me], peer)
        for step in range(1, planes):
            peer = lax.rem(me + PLANE * step, count)
            push(down_ref.at[lax.div(peer, PLANE)], down_in.at[plane], peer)
        for src, held in pairs:
            held[me] = src[me]
        down_in[plane] = down_ref[plane]

        def wo_copy(source, index):
            peer = group * planes + index
            return peer, remote(
                wo_ref.at[index],
                wo_in.at[plane],
                send_wo.at[index],
                recv_wo.at[source],
                {"shard": peer},
            )

        for index in range(planes):
            peer, copy = wo_copy(plane, index)
            pl.when(peer != me)(copy.start)

        @pl.when(target == group)
        def _():
            wo_in[plane] = wo_ref[place]

        for copy in sent:
            copy.wait_recv()
        for index in range(planes):
            pl.when(PLANE * index + target != me)(wo_copy(index, index)[1].wait_recv)
        for index in range(planes):
            peer, copy = wo_copy(plane, index)
            pl.when(peer != me)(copy.wait_send)
        for half, held in zip(halves[:2], (qkv_in, up_in)):
            for lane in range(PLANE):
                total = held[lane].astype(f32)
                for other in range(1, planes):
                    total = total + held[other * PLANE + lane].astype(f32)
                half[lane] = total.astype(bf16)
        for half, held, number in (
            (halves[2], wo_in, planes),
            (halves[3], small_in, count),
            (halves[4], down_in, planes),
        ):
            total = held[0].astype(f32)
            for other in range(1, number):
                total = total + held[other].astype(f32)
            half[...] = total.astype(bf16)
        passed = []
        for index, peer in enumerate(across):
            for place, (half, got) in enumerate(zip(halves, gets)):
                copy = remote(
                    half,
                    got.at[index],
                    send_rep.at[5 * index + place],
                    recv_rep.at[5 * index + place],
                    peer,
                )
                copy.start()
                passed.append(copy)
        for copy in passed:
            copy.wait_recv()
        for out, half, got in zip(outs, halves, gets):
            total = half[...].astype(f32)
            for index in range(copies - 1):
                total = total + got[index].astype(f32)
            out[...] = total
        for copy in sent + passed:
            copy.wait_send()

    totals = 3 * (count - 1) + planes - 1
    shapes = [
        (PLANE, rows, qkv.shape[2]),
        (PLANE, rows, up.shape[2]),
        (rows, D),
        small.shape[1:],
        (block, D),
    ]
    return comm_call(
        body,
        "reduce_grads",
        ident,
        arrays + [down],
        [struct(shape, f32) for shape in shapes],
        [VMEM_SPEC] * 5,
        [pltpu.VMEM(item.shape, bf16) for item in arrays + [down]]
        + [pltpu.VMEM(shape, bf16) for shape in shapes]
        + [pltpu.VMEM((copies - 1,) + shape, bf16) for shape in shapes]
        + [
            pltpu.SemaphoreType.DMA((totals,)),
            pltpu.SemaphoreType.DMA((totals,)),
            pltpu.SemaphoreType.DMA((5 * (copies - 1),)),
            pltpu.SemaphoreType.DMA((5 * (copies - 1),)),
            pltpu.SemaphoreType.DMA((planes,)),
            pltpu.SemaphoreType.DMA((planes,)),
        ],
    )


def norm_forward(value, gain, shift):
    center = value - jnp.mean(value, axis=-1, keepdims=True)
    spread = jnp.mean(center * center, axis=-1, keepdims=True)
    scale = lax.rsqrt(spread + epsilon)
    normal = center * scale
    return (normal * gain + shift, normal, scale)


def norm_backward(upstream, normal, scale, gain):
    inner = upstream * gain
    return scale * (
        inner
        - jnp.mean(inner, axis=-1, keepdims=True)
        - normal * jnp.mean(inner * normal, axis=-1, keepdims=True)
    )


def gelu_slope(hidden):
    return 0.5 * (1.0 + lax.erf(hidden * root_half)) + hidden * inv_root_tau * jnp.exp(
        -0.5 * hidden * hidden
    )


def dot(left, right):
    return jnp.dot(left, right, preferred_element_type=f32)


def dot_left(left, right):
    return lax.dot_general(left, right, (((0,), (0,)), ((), ())), preferred_element_type=f32)


def dot_right(left, right):
    return lax.dot_general(left, right, (((1,), (1,)), ((), ())), preferred_element_type=f32)


def heads_of(value):
    return value.reshape(value.shape[0], GROUP_HEADS, HEAD_DIM).transpose(1, 0, 2)


def flat_of(value):
    return value.transpose(1, 0, 2).reshape(value.shape[1], GROUP_DIM)


def attend_forward(queries, keys, values, own_codes, all_codes):
    def step(carried, pieces):
        top, total, summed = carried
        key_rows, value_rows, key_codes = pieces
        raw = jnp.einsum("hqd,khd->hqk", queries, key_rows, preferred_element_type=f32) * 0.125
        allowed = (own_codes[:, None] == key_codes[None, :])[None]
        masked = jnp.where(allowed, raw, very_low)
        new_top = jnp.maximum(top, jnp.max(masked, axis=2))
        rescale = jnp.exp(top - new_top)
        weights = jnp.where(allowed, jnp.exp(masked - new_top[:, :, None]), 0.0)
        added = jnp.einsum(
            "hqk,khd->hqd", weights.astype(bf16), value_rows, preferred_element_type=f32
        )
        return (
            new_top,
            total * rescale + jnp.sum(weights, axis=2),
            summed * rescale[:, :, None] + added,
        ), None

    rows = queries.shape[1]
    start = (
        jnp.full((GROUP_HEADS, rows), very_low, f32),
        jnp.zeros((GROUP_HEADS, rows), f32),
        jnp.zeros((GROUP_HEADS, rows, HEAD_DIM), f32),
    )
    (top, total, summed), _ = lax.scan(step, start, (keys, values, all_codes))
    return summed / total[:, :, None], top + jnp.log(total)


def attend_backward(queries, keys, values, own_codes, all_codes, logs, delta, upstream):
    def step(carried, pieces):
        key_rows, value_rows, key_codes = pieces
        raw = jnp.einsum("hqd,khd->hqk", queries, key_rows, preferred_element_type=f32) * 0.125
        allowed = (own_codes[:, None] == key_codes[None, :])[None]
        chances = jnp.where(allowed, jnp.exp(raw - logs[:, :, None]), 0.0)
        d_chance = jnp.einsum("hqd,khd->hqk", upstream, value_rows, preferred_element_type=f32)
        d_score = (chances * (d_chance - delta[:, :, None])).astype(bf16)
        carried = carried + jnp.einsum(
            "hqk,khd->hqd", d_score, key_rows, preferred_element_type=f32
        )
        d_key = jnp.einsum("hqk,hqd->khd", d_score, queries, preferred_element_type=f32) * 0.125
        d_value = jnp.einsum(
            "hqk,hqd->khd", chances.astype(bf16), upstream, preferred_element_type=f32
        )
        size = key_rows.shape[0]
        return carried, jnp.concatenate(
            [d_key.reshape(size, GROUP_DIM), d_value.reshape(size, GROUP_DIM)], axis=1
        ).astype(bf16)

    start = jnp.zeros(queries.shape, f32)
    d_query, d_pair = lax.scan(step, start, (keys, values, all_codes))
    return d_query * 0.125, d_pair


def shards(count, copies, *arrays):
    (
        tokens,
        segments,
        padding,
        query_weight,
        key_weight,
        value_weight,
        query_bias,
        value_bias,
        out_weight,
        out_bias,
        middle_gain,
        middle_shift,
        up_weight,
        up_bias,
        down_weight,
        down_bias,
        final_gain,
        final_shift,
        cotangent,
    ) = arrays
    planes = count // PLANE
    rows = query_weight.shape[0]
    block = down_weight.shape[0]
    x_own = tokens[0]
    here = x_own.shape[0]
    wide = PLANE * here
    me = lax.axis_index("shard")
    group = lax.rem(me, PLANE)
    qkv_send = jnp.concatenate(
        [
            item.astype(bf16).reshape(rows, PLANE, GROUP_DIM)
            for item in (query_weight, key_weight, value_weight)
        ],
        axis=2,
    ).transpose(1, 0, 2)
    up_send = (
        up_weight.astype(bf16)
        .reshape(rows, planes, PLANE, block)
        .transpose(2, 0, 1, 3)
        .reshape(PLANE, rows, GROUP_FF)
    )
    codes = (2 * segments[0] + padding[0]).astype(f32)
    lanes = 128 * ((max(here, block) + 127) // 128)

    def padded(value):
        return jnp.pad(value.astype(f32), (0, lanes - value.shape[0]))

    vectors = [
        query_bias,
        value_bias,
        out_bias,
        middle_gain,
        middle_shift,
        down_bias,
        final_gain,
        final_shift,
        up_bias,
        codes,
    ]
    small_send = jnp.pad(
        jnp.stack([padded(item) for item in vectors]), ((0, 6), (0, 0))
    ).astype(bf16)
    x_all, qkv_all, up_all, wo_all, down_all, small = gather_weights(
        count,
        x_own,
        qkv_send,
        up_send,
        out_weight.astype(bf16),
        down_weight.astype(bf16),
        small_send,
        0,
    )
    x_plane = x_all.reshape(wide, D)
    w_qkv = qkv_all.reshape(D, 3 * GROUP_DIM)
    w_up = up_all.reshape(D, GROUP_FF)
    w_out = wo_all.reshape(GROUP_DIM, D)
    w_down = down_all.reshape(GROUP_FF, D)
    small = small.astype(f32)
    spread = [small[:, index, :rows].reshape(D) for index in range(8)]
    b_query, b_value, b_out, gain_mid, shift_mid, b_down, gain_end, shift_end = spread
    b_up = lax.dynamic_index_in_dim(
        small[:, 8, :block].reshape(planes, PLANE, block), group, 1, keepdims=False
    ).reshape(GROUP_FF)
    all_codes = small[:, 9, :here].reshape(planes, wide)
    own_codes = lax.dynamic_index_in_dim(all_codes, lax.div(me, PLANE), 0, keepdims=False)

    def group_part(value):
        return lax.dynamic_slice(value, (group * GROUP_DIM,), (GROUP_DIM,))

    qkv_bias = jnp.concatenate(
        [group_part(b_query), jnp.zeros((GROUP_DIM,), f32), group_part(b_value)]
    )
    qkv = (dot(x_plane, w_qkv) + qkv_bias).astype(bf16)
    pairs = gather_planes(count, qkv[:, GROUP_DIM:], 1)
    queries = heads_of(qkv[:, :GROUP_DIM])
    keys = pairs[:, :, :GROUP_DIM].reshape(planes, wide, GROUP_HEADS, HEAD_DIM)
    values = pairs[:, :, GROUP_DIM:].reshape(planes, wide, GROUP_HEADS, HEAD_DIM)
    context_heads, logs = attend_forward(queries, keys, values, own_codes, all_codes)
    context_low = flat_of(context_heads).astype(bf16)

    def split(value):
        return value.reshape(PLANE, here, D)

    branch = plane_sum(split(dot(context_low, w_out).astype(bf16)), 2) + b_out
    middle, normal_mid, scale_mid = norm_forward(x_own.astype(f32) + branch, gain_mid, shift_mid)
    middle_plane = plane_gather(middle.astype(bf16), 3).reshape(wide, D)
    hidden = dot(middle_plane, w_up) + b_up
    active_low = jax.nn.gelu(hidden, approximate=False).astype(bf16)
    feed = plane_sum(split(dot(active_low, w_down).astype(bf16)), 4) + b_down
    result, normal_end, scale_end = norm_forward(middle + feed, gain_end, shift_end)
    output = result.astype(bf16)[None]
    upstream = cotangent[0].astype(f32)
    d_second = norm_backward(upstream, normal_end, scale_end, gain_end)
    feed_low = d_second.astype(bf16)
    feed_plane = plane_gather(feed_low, 5).reshape(wide, D)
    grad_down = dot_left(active_low, feed_plane).astype(bf16)
    up_low = (dot_right(feed_plane, w_down) * gelu_slope(hidden)).astype(bf16)
    grad_up = dot_left(middle_plane, up_low).astype(bf16)
    d_middle = plane_sum(split(dot_right(up_low, w_up).astype(bf16)), 6) + d_second
    d_first = norm_backward(d_middle, normal_mid, scale_mid, gain_mid)
    branch_low = d_first.astype(bf16)
    branch_plane = plane_gather(branch_low, 7).reshape(wide, D)
    grad_out = dot_left(context_low, branch_plane).astype(bf16)
    d_context = heads_of(dot_right(branch_plane, w_out).astype(bf16))
    delta = jnp.sum(d_context.astype(f32) * context_heads, axis=2)
    d_query, d_pair = attend_backward(
        queries, keys, values, own_codes, all_codes, logs, delta, d_context
    )
    pair_low = sum_planes(count, d_pair, 8)
    mixer_low = jnp.concatenate([flat_of(d_query).astype(bf16), pair_low], axis=1)
    grad_qkv = dot_left(x_plane, mixer_low).astype(bf16)
    grad_input = plane_sum(split(dot_right(mixer_low, w_qkv).astype(bf16)), 9)
    grad_tokens = (grad_input + d_first).astype(bf16)[None]
    mixer_sums = jnp.sum(mixer_low.astype(f32), axis=0)

    def from_group(value):
        return lax.dynamic_update_slice(jnp.zeros((D,), f32), value, (group * GROUP_DIM,))

    sums = [
        from_group(mixer_sums[:GROUP_DIM]),
        from_group(mixer_sums[2 * GROUP_DIM :]),
        jnp.sum(branch_low.astype(f32), axis=0),
        jnp.sum(d_middle * normal_mid, axis=0),
        jnp.sum(d_middle, axis=0),
        jnp.sum(feed_low.astype(f32), axis=0),
        jnp.sum(upstream * normal_end, axis=0),
        jnp.sum(upstream, axis=0),
    ]
    own_lane = (jnp.arange(PLANE) == group).astype(f32)
    up_sums = jnp.sum(up_low.astype(f32), axis=0).reshape(planes, 1, block)
    up_sums = (up_sums * own_lane[None, :, None]).reshape(count, 1, block)
    sums = jnp.stack([item.reshape(count, rows) for item in sums], axis=1)
    small_grads = jnp.concatenate(
        [
            jnp.pad(sums, ((0, 0), (0, 0), (0, lanes - rows))),
            jnp.pad(up_sums, ((0, 0), (0, 7), (0, lanes - block))),
        ],
        axis=1,
    ).astype(bf16)
    qkv_total, up_total, out_total, small_total, down_total = reduce_grads(
        count,
        copies,
        grad_qkv.reshape(count, rows, 3 * GROUP_DIM),
        grad_up.reshape(count, rows, GROUP_FF),
        grad_out.reshape(planes, rows, D),
        grad_down.reshape(planes, block, D),
        small_grads,
        10,
    )

    def joined(value):
        return value.transpose(1, 0, 2).reshape(rows, D)

    up_grad = (
        up_total.reshape(PLANE, rows, planes, block).transpose(1, 2, 0, 3).reshape(rows, FF)
    )
    return (
        output,
        grad_tokens,
        joined(qkv_total[:, :, :GROUP_DIM]),
        joined(qkv_total[:, :, GROUP_DIM : 2 * GROUP_DIM]),
        joined(qkv_total[:, :, 2 * GROUP_DIM :]),
        small_total[0, :rows],
        small_total[1, :rows],
        out_total,
        small_total[2, :rows],
        small_total[3, :rows],
        small_total[4, :rows],
        up_grad,
        small_total[8, :block],
        down_total,
        small_total[5, :rows],
        small_total[6, :rows],
        small_total[7, :rows],
    )


def solution(mesh):
    sheet, line = P("shard", None), P("shard")
    batch = P("rep", "shard", None)
    in_specs = (batch, P("rep", "shard"), P("rep", "shard"), sheet, sheet, sheet, line, line)
    in_specs += (sheet, line, line, line, sheet, line, sheet, line, line, line, batch)
    out_specs = (batch, batch, sheet, sheet, sheet, line, line, sheet, line, line, line)
    out_specs += (sheet, line, sheet, line, line, line)
    body = functools.partial(shards, mesh.shape["shard"], mesh.shape["rep"])
    return jax.shard_map(
        body, mesh=mesh, in_specs=in_specs, out_specs=out_specs, check_vma=False
    )
```

```python
import functools

import jax
import jax.numpy as jnp
from jax import lax
from jax.experimental import pallas as pl
from jax.experimental.pallas import tpu as pltpu
from jax.sharding import PartitionSpec as P

D = 768
HEADS = 12
HEAD_DIM = 64
PLANE = 4
GROUP_HEADS = HEADS // PLANE
GROUP_DIM = GROUP_HEADS * HEAD_DIM
FF = 3072
GROUP_FF = FF // PLANE

epsilon = 1e-12
very_low = -1e30
root_half = 0.7071067811865476
inv_root_tau = 0.3989422804014327
bf16 = jnp.bfloat16
f32 = jnp.float32
MESH = pl.DeviceIdType.MESH
VMEM_SPEC = pl.BlockSpec(memory_space=pltpu.VMEM)
ANY_SPEC = pl.BlockSpec(memory_space=pl.ANY)
VMEM_BYTES = 60000 * 1024


def struct(shape, dtype=bf16):
    return jax.ShapeDtypeStruct(shape, dtype)


def comm_call(body, name, ident, inputs, out_shapes, out_specs, scratch):
    return pl.pallas_call(
        body,
        name=name,
        out_shape=out_shapes,
        in_specs=[VMEM_SPEC] * len(inputs),
        out_specs=out_specs,
        scratch_shapes=scratch,
        compiler_params=pltpu.CompilerParams(
            collective_id=ident, has_side_effects=True, vmem_limit_bytes=VMEM_BYTES
        ),
    )(*inputs)


def greet(peers):
    barrier = pltpu.get_barrier_semaphore()
    for peer in peers:
        pl.semaphore_signal(barrier, inc=1, device_id=peer, device_id_type=MESH)
    pl.semaphore_wait(barrier, len(peers))


def remote(src, dst, send_sem, recv_sem, peer):
    return pltpu.make_async_remote_copy(
        src_ref=src,
        dst_ref=dst,
        send_sem=send_sem,
        recv_sem=recv_sem,
        device_id=peer,
        device_id_type=MESH,
    )


def plane_peer(me, mask):
    group = lax.rem(me, PLANE)
    core = lax.rem(group, 2)
    column = lax.div(group, 2)
    if mask & 1:
        core = 1 - core
    if mask & 2:
        column = 1 - column
    return me - group + 2 * column + core


def plane_slot(me, mask):
    return lax.rem(plane_peer(me, mask), PLANE)


def plane_gather(value, ident):
    rows, cols = value.shape

    def body(x_ref, out_ref, send, recv, local):
        me = lax.axis_index("shard")
        peers = [{"shard": plane_peer(me, mask)} for mask in (1, 2)]
        greet(peers)
        mine, far = lax.rem(me, PLANE), plane_slot(me, 2)
        own = pltpu.make_async_copy(x_ref, out_ref.at[mine], local)
        own.start()
        across = remote(x_ref, out_ref.at[mine], send.at[0], recv.at[0], peers[1])
        across.start()
        beside = remote(x_ref, out_ref.at[mine], send.at[1], recv.at[1], peers[0])
        beside.start()
        across.wait_recv()
        relay = remote(out_ref.at[far], out_ref.at[far], send.at[2], recv.at[2], peers[0])
        relay.start()
        beside.wait_recv()
        relay.wait_recv()
        across.wait_send()
        beside.wait_send()
        relay.wait_send()
        own.wait()

    return comm_call(
        body,
        "plane_gather",
        ident,
        [value],
        struct((PLANE, rows, cols), value.dtype),
        VMEM_SPEC,
        [
            pltpu.SemaphoreType.DMA((3,)),
            pltpu.SemaphoreType.DMA((3,)),
            pltpu.SemaphoreType.DMA,
        ],
    )


def plane_sum(parts, ident):
    _, rows, cols = parts.shape

    def body(p_ref, out_ref, near, held, far_in, send, recv):
        me = lax.axis_index("shard")
        peers = [{"shard": plane_peer(me, mask)} for mask in (1, 2)]
        greet(peers)
        first = remote(
            p_ref.at[plane_slot(me, 3)], near.at[0], send.at[0], recv.at[0], peers[0]
        )
        first.start()
        second = remote(
            p_ref.at[plane_slot(me, 1)], near.at[1], send.at[1], recv.at[1], peers[0]
        )
        second.start()
        first.wait_recv()
        held[...] = (p_ref[plane_slot(me, 2)].astype(f32) + near[0].astype(f32)).astype(bf16)
        third = remote(held, far_in, send.at[2], recv.at[2], peers[1])
        third.start()
        second.wait_recv()
        out_ref[...] = p_ref[lax.rem(me, PLANE)].astype(f32) + near[1].astype(f32)
        third.wait_recv()
        out_ref[...] += far_in[...].astype(f32)
        first.wait_send()
        second.wait_send()
        third.wait_send()

    return comm_call(
        body,
        "plane_sum",
        ident,
        [parts],
        struct((rows, cols), f32),
        VMEM_SPEC,
        [
            pltpu.VMEM((2, rows, cols), bf16),
            pltpu.VMEM((rows, cols), bf16),
            pltpu.VMEM((rows, cols), bf16),
            pltpu.SemaphoreType.DMA((3,)),
            pltpu.SemaphoreType.DMA((3,)),
        ],
    )


def others(me, count):
    return [{"shard": lax.rem(me + step, count)} for step in range(1, count)]


def gather_weights(count, copies, tokens, qkv, up, out_w, down, small, ident):
    planes = count // PLANE
    rows = qkv.shape[1]
    block = down.shape[0]

    def body(x_ref, qkv_ref, up_ref, wo_ref, down_ref, small_ref, *rest):
        x_out, qkv_out, up_out, wo_out, down_out, small_out = rest[:6]
        send, recv, local, send_wo, recv_wo, send_unit, recv_unit = rest[6:]
        me = lax.axis_index("shard")
        group, plane = lax.rem(me, PLANE), lax.div(me, PLANE)
        across = [
            {"rep": lax.rem(lax.axis_index("rep") + step, copies)} for step in range(1, copies)
        ]
        greet(others(me, count) + across)
        owns = [
            (x_ref, x_out.at[group]),
            (qkv_ref.at[group], qkv_out.at[me]),
            (up_ref.at[group], up_out.at[me]),
            (down_ref, down_out.at[plane]),
            (small_ref, small_out.at[me]),
        ]
        started = []
        for index, (src, dst) in enumerate(owns):
            copy = pltpu.make_async_copy(src, dst, local.at[index])
            copy.start()
            started.append(copy)
        sent = []

        def push(src, dst, peer):
            index = len(sent)
            copy = remote(src, dst, send.at[index], recv.at[index], {"shard": peer})
            copy.start()
            sent.append(copy)

        for mask in (2, 1, 3):
            push(x_ref, x_out.at[group], plane_peer(me, mask))
        for step in range(1, count):
            push(small_ref, small_out.at[me], lax.rem(me + step, count))
        rep = lax.axis_index("rep")
        split = copies == 2
        units = []
        for step in range(planes):
            for lane in range(PLANE):
                if step or lane:
                    units.append((qkv_ref, qkv_out, step, lane))
        for step in range(planes):
            for lane in range(PLANE):
                if step or lane:
                    units.append((up_ref, up_out, step, lane))
            if step:
                units.append((down_ref, down_out, step, 0))

        def unit_copy(index):
            src, dst, step, lane = units[index]
            goal = lax.rem(plane + step, planes)
            goal_group = lax.rem(group + lane, PLANE)
            piece, slot = (src, plane) if src is down_ref else (src.at[goal_group], me)
            return remote(
                piece,
                dst.at[slot],
                send_unit.at[index],
                recv_unit.at[index],
                {"shard": goal * PLANE + goal_group},
            )

        def unit_relay(index):
            src, dst, step, lane = units[index]
            origin = lax.rem(plane + planes - step, planes)
            origin_group = lax.rem(group + PLANE - lane, PLANE)
            slot = origin if src is down_ref else origin * PLANE + origin_group
            return remote(
                dst.at[slot],
                dst.at[slot],
                send_unit.at[index],
                recv_unit.at[index],
                {"rep": lax.rem(rep + 1, copies)},
            )

        def carried(index, mine):
            step = units[index][2]
            if not split or step == 0:
                return None
            return (rep == step % 2) if mine else (rep != step % 2)

        def guarded(test, action):
            if test is None:
                action()
            else:
                pl.when(test)(action)

        for index in range(len(units)):
            guarded(carried(index, True), unit_copy(index).start)
        target, place = lax.div(me, planes), lax.rem(me, planes)

        def wo_copy(source, index):
            peer = PLANE * index + target
            return peer, remote(
                wo_ref, wo_out.at[place], send_wo.at[index], recv_wo.at[source], {"shard": peer}
            )

        for index in range(planes):
            peer, copy = wo_copy(place, index)
            pl.when(peer != me)(copy.start)
        keep = pltpu.make_async_copy(wo_ref, wo_out.at[place], local.at[5])
        pl.when(target == group)(keep.start)
        for index, (_, _, step, _) in enumerate(units):
            if split and step:

                @pl.when(rep == step % 2)
                def _(index=index):
                    unit_relay(index).wait_recv()
                    unit_copy(index).wait_send()
                    unit_relay(index).start()

            else:
                unit_copy(index).wait_recv()
                unit_copy(index).wait_send()
        for index, (_, _, step, _) in enumerate(units):
            if split and step:
                pl.when(rep != step % 2)(unit_relay(index).wait_recv)
                pl.when(rep == step % 2)(unit_relay(index).wait_send)
        for copy in sent:
            copy.wait_recv()
        for index in range(planes):
            pl.when(group * planes + index != me)(wo_copy(index, index)[1].wait_recv)
        for index in range(planes):
            peer, copy = wo_copy(place, index)
            pl.when(peer != me)(copy.wait_send)
        pl.when(target == group)(keep.wait)
        for copy in sent:
            copy.wait_send()
        for copy in started:
            copy.wait()

    total = 3 + count - 1
    number = 2 * (count - 1) + planes - 1
    return comm_call(
        body,
        "gather_weights",
        ident,
        [tokens, qkv, up, out_w, down, small],
        [
            struct((PLANE,) + tokens.shape),
            struct((count, rows, qkv.shape[2])),
            struct((count, rows, up.shape[2])),
            struct((planes,) + out_w.shape),
            struct((planes, block, D)),
            struct((count,) + small.shape),
        ],
        [ANY_SPEC] * 6,
        [
            pltpu.SemaphoreType.DMA((total,)),
            pltpu.SemaphoreType.DMA((total,)),
            pltpu.SemaphoreType.DMA((6,)),
            pltpu.SemaphoreType.DMA((planes,)),
            pltpu.SemaphoreType.DMA((planes,)),
            pltpu.SemaphoreType.DMA((number,)),
            pltpu.SemaphoreType.DMA((number,)),
        ],
    )


def gather_planes(count, value, ident):
    planes = count // PLANE

    def body(x_ref, out_ref, send, recv, local):
        me = lax.axis_index("shard")
        plane = lax.div(me, PLANE)
        greet([{"shard": lax.rem(me + PLANE * s, count)} for s in range(1, planes)])
        own = pltpu.make_async_copy(x_ref, out_ref.at[plane], local)
        own.start()

        def hop(way, source, src):
            peer = me + PLANE if way == 0 else me - PLANE
            return remote(
                src,
                out_ref.at[source],
                send.at[way, source],
                recv.at[way, source],
                {"shard": lax.rem(peer + count, count)},
            )

        @pl.when(plane < planes - 1)
        def _():
            hop(0, plane, x_ref).start()

        @pl.when(plane > 0)
        def _():
            hop(1, plane, x_ref).start()

        for step in range(1, planes):
            for way, source in ((0, plane - step), (1, plane + step)):
                onward = plane < planes - 1 if way == 0 else plane > 0

                @pl.when((source >= 0) & (source < planes))
                def _(way=way, source=source, onward=onward):
                    copy = hop(way, source, out_ref.at[source])
                    copy.wait_recv()
                    pl.when(onward)(copy.start)

        @pl.when(plane < planes - 1)
        def _():
            hop(0, plane, x_ref).wait_send()

        @pl.when(plane > 0)
        def _():
            hop(1, plane, x_ref).wait_send()

        for step in range(1, planes):
            for way, source in ((0, plane - step), (1, plane + step)):
                onward = plane < planes - 1 if way == 0 else plane > 0

                @pl.when((source >= 0) & (source < planes) & onward)
                def _(way=way, source=source):
                    hop(way, source, out_ref.at[source]).wait_send()

        own.wait()

    return comm_call(
        body,
        "gather_planes",
        ident,
        [value],
        struct((planes,) + value.shape),
        ANY_SPEC,
        [
            pltpu.SemaphoreType.DMA((2, planes)),
            pltpu.SemaphoreType.DMA((2, planes)),
            pltpu.SemaphoreType.DMA,
        ],
    )


def sum_planes(count, parts, ident):
    planes, rows, cols = parts.shape

    def body(p_ref, out_ref, held, staged, send, recv):
        me = lax.axis_index("shard")
        plane = lax.div(me, PLANE)
        greet([{"shard": lax.rem(me + PLANE * s, count)} for s in range(1, planes)])

        def hop(way, goal, src):
            peer = me + PLANE if way == 0 else me - PLANE
            return remote(
                src,
                held.at[way, goal],
                send.at[goal],
                recv.at[way, goal],
                {"shard": lax.rem(peer + count, count)},
            )

        for step in range(planes - 1):
            for way, goal in ((0, planes - 1 - step), (1, step)):
                ahead = goal > plane if way == 0 else goal < plane
                first = plane == 0 if way == 0 else plane == planes - 1

                @pl.when(ahead & first)
                def _(way=way, goal=goal):
                    hop(way, goal, p_ref.at[goal]).start()

                @pl.when(ahead & jnp.logical_not(first))
                def _(way=way, goal=goal):
                    copy = hop(way, goal, staged.at[goal])
                    copy.wait_recv()
                    total = p_ref[goal].astype(f32) + held[way, goal].astype(f32)
                    staged[goal] = total.astype(bf16)
                    copy.start()

        out_ref[...] = p_ref[plane]

        @pl.when(plane > 0)
        def _():
            hop(0, plane, staged.at[plane]).wait_recv()
            out_ref[...] = (out_ref[...].astype(f32) + held[0, plane].astype(f32)).astype(bf16)

        @pl.when(plane < planes - 1)
        def _():
            hop(1, plane, staged.at[plane]).wait_recv()
            out_ref[...] = (out_ref[...].astype(f32) + held[1, plane].astype(f32)).astype(bf16)

        for goal in range(planes):

            @pl.when(goal != plane)
            def _(goal=goal):
                hop(0, goal, staged.at[goal]).wait_send()

    return comm_call(
        body,
        "sum_planes",
        ident,
        [parts],
        struct((rows, cols)),
        VMEM_SPEC,
        [
            pltpu.VMEM((2, planes, rows, cols), bf16),
            pltpu.VMEM((planes, rows, cols), bf16),
            pltpu.SemaphoreType.DMA((planes,)),
            pltpu.SemaphoreType.DMA((2, planes)),
        ],
    )


def reduce_grads(count, copies, qkv, up, out_w, down, small, ident):
    planes = count // PLANE
    rows = qkv.shape[1]
    block = down.shape[1]
    arrays = [qkv, up, out_w, small]

    def body(qkv_ref, up_ref, wo_ref, small_ref, down_ref, *rest):
        outs, (qkv_in, up_in, wo_in, small_in, down_in) = rest[:5], rest[5:10]
        halves, gets = rest[10:15], rest[15:20]
        send, recv, send_rep, recv_rep, send_wo, recv_wo = rest[20:]
        me = lax.axis_index("shard")
        rep = lax.axis_index("rep")
        plane = lax.div(me, PLANE)
        across = [{"rep": lax.rem(rep + step, copies)} for step in range(1, copies)]
        greet(others(me, count) + across)
        sent = []

        def push(src, dst, peer):
            index = len(sent)
            copy = remote(src, dst, send.at[index], recv.at[index], {"shard": peer})
            copy.start()
            sent.append(copy)

        pairs = [(qkv_ref, qkv_in), (up_ref, up_in), (small_ref, small_in)]
        group = lax.rem(me, PLANE)
        target, place = lax.div(me, planes), lax.rem(me, planes)
        for src, held in pairs:
            for step in range(1, count):
                peer = lax.rem(me + step, count)
                push(src.at[peer], held.at[me], peer)
        for step in range(1, planes):
            peer = lax.rem(me + PLANE * step, count)
            push(down_ref.at[lax.div(peer, PLANE)], down_in.at[plane], peer)
        for src, held in pairs:
            held[me] = src[me]
        down_in[plane] = down_ref[plane]

        def wo_copy(source, index):
            peer = group * planes + index
            return peer, remote(
                wo_ref.at[index],
                wo_in.at[plane],
                send_wo.at[index],
                recv_wo.at[source],
                {"shard": peer},
            )

        for index in range(planes):
            peer, copy = wo_copy(plane, index)
            pl.when(peer != me)(copy.start)

        @pl.when(target == group)
        def _():
            wo_in[plane] = wo_ref[place]

        for copy in sent:
            copy.wait_recv()
        for index in range(planes):
            pl.when(PLANE * index + target != me)(wo_copy(index, index)[1].wait_recv)
        for index in range(planes):
            peer, copy = wo_copy(plane, index)
            pl.when(peer != me)(copy.wait_send)
        for half, held in zip(halves[:2], (qkv_in, up_in)):
            for lane in range(PLANE):
                total = held[lane].astype(f32)
                for other in range(1, planes):
                    total = total + held[other * PLANE + lane].astype(f32)
                half[lane] = total.astype(bf16)
        for half, held, number in (
            (halves[2], wo_in, planes),
            (halves[3], small_in, count),
            (halves[4], down_in, planes),
        ):
            total = held[0].astype(f32)
            for other in range(1, number):
                total = total + held[other].astype(f32)
            half[...] = total.astype(bf16)
        passed = []
        for index, peer in enumerate(across):
            for place, (half, got) in enumerate(zip(halves, gets)):
                copy = remote(
                    half,
                    got.at[index],
                    send_rep.at[5 * index + place],
                    recv_rep.at[5 * index + place],
                    peer,
                )
                copy.start()
                passed.append(copy)
        for copy in passed:
            copy.wait_recv()
        for out, half, got in zip(outs, halves, gets):
            total = half[...].astype(f32)
            for index in range(copies - 1):
                total = total + got[index].astype(f32)
            out[...] = total
        for copy in sent + passed:
            copy.wait_send()

    totals = 3 * (count - 1) + planes - 1
    shapes = [
        (PLANE, rows, qkv.shape[2]),
        (PLANE, rows, up.shape[2]),
        (rows, D),
        small.shape[1:],
        (block, D),
    ]
    return comm_call(
        body,
        "reduce_grads",
        ident,
        arrays + [down],
        [struct(shape, f32) for shape in shapes],
        [VMEM_SPEC] * 5,
        [pltpu.VMEM(item.shape, bf16) for item in arrays + [down]]
        + [pltpu.VMEM(shape, bf16) for shape in shapes]
        + [pltpu.VMEM((copies - 1,) + shape, bf16) for shape in shapes]
        + [
            pltpu.SemaphoreType.DMA((totals,)),
            pltpu.SemaphoreType.DMA((totals,)),
            pltpu.SemaphoreType.DMA((5 * (copies - 1),)),
            pltpu.SemaphoreType.DMA((5 * (copies - 1),)),
            pltpu.SemaphoreType.DMA((planes,)),
            pltpu.SemaphoreType.DMA((planes,)),
        ],
    )


def norm_forward(value, gain, shift):
    center = value - jnp.mean(value, axis=-1, keepdims=True)
    spread = jnp.mean(center * center, axis=-1, keepdims=True)
    scale = lax.rsqrt(spread + epsilon)
    normal = center * scale
    return (normal * gain + shift, normal, scale)


def norm_backward(upstream, normal, scale, gain):
    inner = upstream * gain
    return scale * (
        inner
        - jnp.mean(inner, axis=-1, keepdims=True)
        - normal * jnp.mean(inner * normal, axis=-1, keepdims=True)
    )


def gelu_slope(hidden):
    return 0.5 * (1.0 + lax.erf(hidden * root_half)) + hidden * inv_root_tau * jnp.exp(
        -0.5 * hidden * hidden
    )


def dot(left, right):
    return jnp.dot(left, right, preferred_element_type=f32)


def dot_left(left, right):
    return lax.dot_general(left, right, (((0,), (0,)), ((), ())), preferred_element_type=f32)


def dot_right(left, right):
    return lax.dot_general(left, right, (((1,), (1,)), ((), ())), preferred_element_type=f32)


def heads_of(value):
    return value.reshape(value.shape[0], GROUP_HEADS, HEAD_DIM).transpose(1, 0, 2)


def flat_of(value):
    return value.transpose(1, 0, 2).reshape(value.shape[1], GROUP_DIM)


def attend_forward(queries, keys, values, own_codes, all_codes):
    def step(carried, pieces):
        top, total, summed = carried
        key_rows, value_rows, key_codes = pieces
        raw = jnp.einsum("hqd,khd->hqk", queries, key_rows, preferred_element_type=f32) * 0.125
        allowed = (own_codes[:, None] == key_codes[None, :])[None]
        masked = jnp.where(allowed, raw, very_low)
        new_top = jnp.maximum(top, jnp.max(masked, axis=2))
        rescale = jnp.exp(top - new_top)
        weights = jnp.where(allowed, jnp.exp(masked - new_top[:, :, None]), 0.0)
        added = jnp.einsum(
            "hqk,khd->hqd", weights.astype(bf16), value_rows, preferred_element_type=f32
        )
        return (
            new_top,
            total * rescale + jnp.sum(weights, axis=2),
            summed * rescale[:, :, None] + added,
        ), None

    rows = queries.shape[1]
    start = (
        jnp.full((GROUP_HEADS, rows), very_low, f32),
        jnp.zeros((GROUP_HEADS, rows), f32),
        jnp.zeros((GROUP_HEADS, rows, HEAD_DIM), f32),
    )
    (top, total, summed), _ = lax.scan(step, start, (keys, values, all_codes))
    return summed / total[:, :, None], top + jnp.log(total)


def attend_backward(queries, keys, values, own_codes, all_codes, logs, delta, upstream):
    def step(carried, pieces):
        key_rows, value_rows, key_codes = pieces
        raw = jnp.einsum("hqd,khd->hqk", queries, key_rows, preferred_element_type=f32) * 0.125
        allowed = (own_codes[:, None] == key_codes[None, :])[None]
        chances = jnp.where(allowed, jnp.exp(raw - logs[:, :, None]), 0.0)
        d_chance = jnp.einsum("hqd,khd->hqk", upstream, value_rows, preferred_element_type=f32)
        d_score = (chances * (d_chance - delta[:, :, None])).astype(bf16)
        carried = carried + jnp.einsum(
            "hqk,khd->hqd", d_score, key_rows, preferred_element_type=f32
        )
        d_key = jnp.einsum("hqk,hqd->khd", d_score, queries, preferred_element_type=f32) * 0.125
        d_value = jnp.einsum(
            "hqk,hqd->khd", chances.astype(bf16), upstream, preferred_element_type=f32
        )
        size = key_rows.shape[0]
        return carried, jnp.concatenate(
            [d_key.reshape(size, GROUP_DIM), d_value.reshape(size, GROUP_DIM)], axis=1
        ).astype(bf16)

    start = jnp.zeros(queries.shape, f32)
    d_query, d_pair = lax.scan(step, start, (keys, values, all_codes))
    return d_query * 0.125, d_pair


def shards(count, copies, *arrays):
    (
        tokens,
        segments,
        padding,
        query_weight,
        key_weight,
        value_weight,
        query_bias,
        value_bias,
        out_weight,
        out_bias,
        middle_gain,
        middle_shift,
        up_weight,
        up_bias,
        down_weight,
        down_bias,
        final_gain,
        final_shift,
        cotangent,
    ) = arrays
    planes = count // PLANE
    rows = query_weight.shape[0]
    block = down_weight.shape[0]
    x_own = tokens[0]
    here = x_own.shape[0]
    wide = PLANE * here
    me = lax.axis_index("shard")
    group = lax.rem(me, PLANE)
    qkv_send = jnp.concatenate(
        [
            item.astype(bf16).reshape(rows, PLANE, GROUP_DIM)
            for item in (query_weight, key_weight, value_weight)
        ],
        axis=2,
    ).transpose(1, 0, 2)
    up_send = (
        up_weight.astype(bf16)
        .reshape(rows, planes, PLANE, block)
        .transpose(2, 0, 1, 3)
        .reshape(PLANE, rows, GROUP_FF)
    )
    codes = (2 * segments[0] + padding[0]).astype(f32)
    lanes = 128 * ((max(here, block) + 127) // 128)

    def padded(value):
        return jnp.pad(value.astype(f32), (0, lanes - value.shape[0]))

    vectors = [
        query_bias,
        value_bias,
        out_bias,
        middle_gain,
        middle_shift,
        down_bias,
        final_gain,
        final_shift,
        up_bias,
        codes,
    ]
    small_send = jnp.pad(
        jnp.stack([padded(item) for item in vectors]), ((0, 6), (0, 0))
    ).astype(bf16)
    x_all, qkv_all, up_all, wo_all, down_all, small = gather_weights(
        count,
        copies,
        x_own,
        qkv_send,
        up_send,
        out_weight.astype(bf16),
        down_weight.astype(bf16),
        small_send,
        0,
    )
    x_plane = x_all.reshape(wide, D)
    w_qkv = qkv_all.reshape(D, 3 * GROUP_DIM)
    w_up = up_all.reshape(D, GROUP_FF)
    w_out = wo_all.reshape(GROUP_DIM, D)
    w_down = down_all.reshape(GROUP_FF, D)
    small = small.astype(f32)
    spread = [small[:, index, :rows].reshape(D) for index in range(8)]
    b_query, b_value, b_out, gain_mid, shift_mid, b_down, gain_end, shift_end = spread
    b_up = lax.dynamic_index_in_dim(
        small[:, 8, :block].reshape(planes, PLANE, block), group, 1, keepdims=False
    ).reshape(GROUP_FF)
    all_codes = small[:, 9, :here].reshape(planes, wide)
    own_codes = lax.dynamic_index_in_dim(all_codes, lax.div(me, PLANE), 0, keepdims=False)

    def group_part(value):
        return lax.dynamic_slice(value, (group * GROUP_DIM,), (GROUP_DIM,))

    qkv_bias = jnp.concatenate(
        [group_part(b_query), jnp.zeros((GROUP_DIM,), f32), group_part(b_value)]
    )
    qkv = (dot(x_plane, w_qkv) + qkv_bias).astype(bf16)
    pairs = gather_planes(count, qkv[:, GROUP_DIM:], 1)
    queries = heads_of(qkv[:, :GROUP_DIM])
    keys = pairs[:, :, :GROUP_DIM].reshape(planes, wide, GROUP_HEADS, HEAD_DIM)
    values = pairs[:, :, GROUP_DIM:].reshape(planes, wide, GROUP_HEADS, HEAD_DIM)
    context_heads, logs = attend_forward(queries, keys, values, own_codes, all_codes)
    context_low = flat_of(context_heads).astype(bf16)

    def split(value):
        return value.reshape(PLANE, here, D)

    branch = plane_sum(split(dot(context_low, w_out).astype(bf16)), 2) + b_out
    middle, normal_mid, scale_mid = norm_forward(x_own.astype(f32) + branch, gain_mid, shift_mid)
    middle_plane = plane_gather(middle.astype(bf16), 3).reshape(wide, D)
    hidden = dot(middle_plane, w_up) + b_up
    active_low = jax.nn.gelu(hidden, approximate=False).astype(bf16)
    feed = plane_sum(split(dot(active_low, w_down).astype(bf16)), 4) + b_down
    result, normal_end, scale_end = norm_forward(middle + feed, gain_end, shift_end)
    output = result.astype(bf16)[None]
    upstream = cotangent[0].astype(f32)
    d_second = norm_backward(upstream, normal_end, scale_end, gain_end)
    feed_low = d_second.astype(bf16)
    feed_plane = plane_gather(feed_low, 5).reshape(wide, D)
    grad_down = dot_left(active_low, feed_plane).astype(bf16)
    up_low = (dot_right(feed_plane, w_down) * gelu_slope(hidden)).astype(bf16)
    grad_up = dot_left(middle_plane, up_low).astype(bf16)
    d_middle = plane_sum(split(dot_right(up_low, w_up).astype(bf16)), 6) + d_second
    d_first = norm_backward(d_middle, normal_mid, scale_mid, gain_mid)
    branch_low = d_first.astype(bf16)
    branch_plane = plane_gather(branch_low, 7).reshape(wide, D)
    grad_out = dot_left(context_low, branch_plane).astype(bf16)
    d_context = heads_of(dot_right(branch_plane, w_out).astype(bf16))
    delta = jnp.sum(d_context.astype(f32) * context_heads, axis=2)
    d_query, d_pair = attend_backward(
        queries, keys, values, own_codes, all_codes, logs, delta, d_context
    )
    pair_low = sum_planes(count, d_pair, 8)
    mixer_low = jnp.concatenate([flat_of(d_query).astype(bf16), pair_low], axis=1)
    grad_qkv = dot_left(x_plane, mixer_low).astype(bf16)
    grad_input = plane_sum(split(dot_right(mixer_low, w_qkv).astype(bf16)), 9)
    grad_tokens = (grad_input + d_first).astype(bf16)[None]
    mixer_sums = jnp.sum(mixer_low.astype(f32), axis=0)

    def from_group(value):
        return lax.dynamic_update_slice(jnp.zeros((D,), f32), value, (group * GROUP_DIM,))

    sums = [
        from_group(mixer_sums[:GROUP_DIM]),
        from_group(mixer_sums[2 * GROUP_DIM :]),
        jnp.sum(branch_low.astype(f32), axis=0),
        jnp.sum(d_middle * normal_mid, axis=0),
        jnp.sum(d_middle, axis=0),
        jnp.sum(feed_low.astype(f32), axis=0),
        jnp.sum(upstream * normal_end, axis=0),
        jnp.sum(upstream, axis=0),
    ]
    own_lane = (jnp.arange(PLANE) == group).astype(f32)
    up_sums = jnp.sum(up_low.astype(f32), axis=0).reshape(planes, 1, block)
    up_sums = (up_sums * own_lane[None, :, None]).reshape(count, 1, block)
    sums = jnp.stack([item.reshape(count, rows) for item in sums], axis=1)
    small_grads = jnp.concatenate(
        [
            jnp.pad(sums, ((0, 0), (0, 0), (0, lanes - rows))),
            jnp.pad(up_sums, ((0, 0), (0, 7), (0, lanes - block))),
        ],
        axis=1,
    ).astype(bf16)
    qkv_total, up_total, out_total, small_total, down_total = reduce_grads(
        count,
        copies,
        grad_qkv.reshape(count, rows, 3 * GROUP_DIM),
        grad_up.reshape(count, rows, GROUP_FF),
        grad_out.reshape(planes, rows, D),
        grad_down.reshape(planes, block, D),
        small_grads,
        10,
    )

    def joined(value):
        return value.transpose(1, 0, 2).reshape(rows, D)

    up_grad = (
        up_total.reshape(PLANE, rows, planes, block).transpose(1, 2, 0, 3).reshape(rows, FF)
    )
    return (
        output,
        grad_tokens,
        joined(qkv_total[:, :, :GROUP_DIM]),
        joined(qkv_total[:, :, GROUP_DIM : 2 * GROUP_DIM]),
        joined(qkv_total[:, :, 2 * GROUP_DIM :]),
        small_total[0, :rows],
        small_total[1, :rows],
        out_total,
        small_total[2, :rows],
        small_total[3, :rows],
        small_total[4, :rows],
        up_grad,
        small_total[8, :block],
        down_total,
        small_total[5, :rows],
        small_total[6, :rows],
        small_total[7, :rows],
    )


def solution(mesh):
    sheet, line = P("shard", None), P("shard")
    batch = P("rep", "shard", None)
    in_specs = (batch, P("rep", "shard"), P("rep", "shard"), sheet, sheet, sheet, line, line)
    in_specs += (sheet, line, line, line, sheet, line, sheet, line, line, line, batch)
    out_specs = (batch, batch, sheet, sheet, sheet, line, line, sheet, line, line, line)
    out_specs += (sheet, line, sheet, line, line, line)
    body = functools.partial(shards, mesh.shape["shard"], mesh.shape["rep"])
    return jax.shard_map(
        body, mesh=mesh, in_specs=in_specs, out_specs=out_specs, check_vma=False
    )
```

```python
import functools

import jax
import jax.numpy as jnp
from jax import lax
from jax.experimental import pallas as pl
from jax.experimental.pallas import tpu as pltpu
from jax.sharding import PartitionSpec as P

D = 768
HEADS = 12
HEAD_DIM = 64
PLANE = 4
GROUP_HEADS = HEADS // PLANE
GROUP_DIM = GROUP_HEADS * HEAD_DIM
FF = 3072
GROUP_FF = FF // PLANE

epsilon = 1e-12
very_low = -1e30
root_half = 0.7071067811865476
inv_root_tau = 0.3989422804014327
bf16 = jnp.bfloat16
f32 = jnp.float32
MESH = pl.DeviceIdType.MESH
VMEM_SPEC = pl.BlockSpec(memory_space=pltpu.VMEM)
ANY_SPEC = pl.BlockSpec(memory_space=pl.ANY)
VMEM_BYTES = 60000 * 1024
MODEL_BYTES = 100_000_000


def struct(shape, dtype=bf16):
    return jax.ShapeDtypeStruct(shape, dtype)


def comm_call(body, name, ident, inputs, out_shapes, out_specs, scratch):
    return pl.pallas_call(
        body,
        name=name,
        out_shape=out_shapes,
        in_specs=[VMEM_SPEC] * len(inputs),
        out_specs=out_specs,
        scratch_shapes=scratch,
        cost_estimate=pl.CostEstimate(flops=0, bytes_accessed=MODEL_BYTES, transcendentals=0),
        compiler_params=pltpu.CompilerParams(
            collective_id=ident, has_side_effects=True, vmem_limit_bytes=VMEM_BYTES
        ),
    )(*inputs)


def greet(peers):
    barrier = pltpu.get_barrier_semaphore()
    for peer in peers:
        pl.semaphore_signal(barrier, inc=1, device_id=peer, device_id_type=MESH)
    pl.semaphore_wait(barrier, len(peers))


def remote(src, dst, send_sem, recv_sem, peer):
    return pltpu.make_async_remote_copy(
        src_ref=src,
        dst_ref=dst,
        send_sem=send_sem,
        recv_sem=recv_sem,
        device_id=peer,
        device_id_type=MESH,
    )


def plane_peer(me, mask):
    group = lax.rem(me, PLANE)
    core = lax.rem(group, 2)
    column = lax.div(group, 2)
    if mask & 1:
        core = 1 - core
    if mask & 2:
        column = 1 - column
    return me - group + 2 * column + core


def plane_slot(me, mask):
    return lax.rem(plane_peer(me, mask), PLANE)


def plane_gather(value, ident):
    rows, cols = value.shape

    def body(x_ref, out_ref, send, recv, local):
        me = lax.axis_index("shard")
        peers = [{"shard": plane_peer(me, mask)} for mask in (1, 2)]
        greet(peers)
        mine, far = lax.rem(me, PLANE), plane_slot(me, 2)
        own = pltpu.make_async_copy(x_ref, out_ref.at[mine], local)
        own.start()
        across = remote(x_ref, out_ref.at[mine], send.at[0], recv.at[0], peers[1])
        across.start()
        beside = remote(x_ref, out_ref.at[mine], send.at[1], recv.at[1], peers[0])
        beside.start()
        across.wait_recv()
        relay = remote(out_ref.at[far], out_ref.at[far], send.at[2], recv.at[2], peers[0])
        relay.start()
        beside.wait_recv()
        relay.wait_recv()
        across.wait_send()
        beside.wait_send()
        relay.wait_send()
        own.wait()

    return comm_call(
        body,
        "plane_gather",
        ident,
        [value],
        struct((PLANE, rows, cols), value.dtype),
        VMEM_SPEC,
        [
            pltpu.SemaphoreType.DMA((3,)),
            pltpu.SemaphoreType.DMA((3,)),
            pltpu.SemaphoreType.DMA,
        ],
    )


def plane_sum(parts, ident):
    _, rows, cols = parts.shape

    def body(p_ref, out_ref, near, held, far_in, send, recv):
        me = lax.axis_index("shard")
        peers = [{"shard": plane_peer(me, mask)} for mask in (1, 2)]
        greet(peers)
        first = remote(
            p_ref.at[plane_slot(me, 3)], near.at[0], send.at[0], recv.at[0], peers[0]
        )
        first.start()
        second = remote(
            p_ref.at[plane_slot(me, 1)], near.at[1], send.at[1], recv.at[1], peers[0]
        )
        second.start()
        first.wait_recv()
        held[...] = (p_ref[plane_slot(me, 2)].astype(f32) + near[0].astype(f32)).astype(bf16)
        third = remote(held, far_in, send.at[2], recv.at[2], peers[1])
        third.start()
        second.wait_recv()
        out_ref[...] = p_ref[lax.rem(me, PLANE)].astype(f32) + near[1].astype(f32)
        third.wait_recv()
        out_ref[...] += far_in[...].astype(f32)
        first.wait_send()
        second.wait_send()
        third.wait_send()

    return comm_call(
        body,
        "plane_sum",
        ident,
        [parts],
        struct((rows, cols), f32),
        VMEM_SPEC,
        [
            pltpu.VMEM((2, rows, cols), bf16),
            pltpu.VMEM((rows, cols), bf16),
            pltpu.VMEM((rows, cols), bf16),
            pltpu.SemaphoreType.DMA((3,)),
            pltpu.SemaphoreType.DMA((3,)),
        ],
    )


def others(me, count):
    return [{"shard": lax.rem(me + step, count)} for step in range(1, count)]


def gather_weights(count, copies, tokens, qkv, up, out_w, small, ident):
    planes = count // PLANE
    rows = qkv.shape[1]

    def body(x_ref, qkv_ref, up_ref, wo_ref, small_ref, *rest):
        x_out, qkv_out, up_out, wo_out, small_out = rest[:5]
        send, recv, local, send_wo, recv_wo, send_unit, recv_unit = rest[5:]
        me = lax.axis_index("shard")
        group, plane = lax.rem(me, PLANE), lax.div(me, PLANE)
        across = [
            {"rep": lax.rem(lax.axis_index("rep") + step, copies)} for step in range(1, copies)
        ]
        greet(others(me, count) + across)
        owns = [
            (x_ref, x_out.at[group]),
            (qkv_ref.at[group], qkv_out.at[me]),
            (up_ref.at[group], up_out.at[group]),
            (small_ref, small_out.at[me]),
        ]
        started = []
        for index, (src, dst) in enumerate(owns):
            copy = pltpu.make_async_copy(src, dst, local.at[index])
            copy.start()
            started.append(copy)
        sent = []

        def push(src, dst, peer):
            index = len(sent)
            copy = remote(src, dst, send.at[index], recv.at[index], {"shard": peer})
            copy.start()
            sent.append(copy)

        for mask in (2, 1, 3):
            push(x_ref, x_out.at[group], plane_peer(me, mask))
        for step in range(1, count):
            push(small_ref, small_out.at[me], lax.rem(me + step, count))
        rep = lax.axis_index("rep")
        split = copies == 2
        units = []
        for step in range(planes):
            for lane in range(PLANE):
                if step or lane:
                    units.append((qkv_ref, qkv_out, step, lane))
        for lane in range(1, PLANE):
            units.append((up_ref, up_out, 0, lane))

        def unit_copy(index):
            src, dst, step, lane = units[index]
            goal = lax.rem(plane + step, planes)
            goal_group = lax.rem(group + lane, PLANE)
            slot = group if src is up_ref else me
            return remote(
                src.at[goal_group],
                dst.at[slot],
                send_unit.at[index],
                recv_unit.at[index],
                {"shard": goal * PLANE + goal_group},
            )

        def unit_relay(index):
            src, dst, step, lane = units[index]
            origin = lax.rem(plane + planes - step, planes)
            origin_group = lax.rem(group + PLANE - lane, PLANE)
            slot = origin_group if src is up_ref else origin * PLANE + origin_group
            return remote(
                dst.at[slot],
                dst.at[slot],
                send_unit.at[index],
                recv_unit.at[index],
                {"rep": lax.rem(rep + 1, copies)},
            )

        def carried(index, mine):
            step = units[index][2]
            if not split or step == 0:
                return None
            return (rep == step % 2) if mine else (rep != step % 2)

        def guarded(test, action):
            if test is None:
                action()
            else:
                pl.when(test)(action)

        for index in range(len(units)):
            guarded(carried(index, True), unit_copy(index).start)
        target, place = lax.div(me, planes), lax.rem(me, planes)

        def wo_copy(source, index):
            peer = PLANE * index + target
            return peer, remote(
                wo_ref, wo_out.at[place], send_wo.at[index], recv_wo.at[source], {"shard": peer}
            )

        for index in range(planes):
            peer, copy = wo_copy(place, index)
            pl.when(peer != me)(copy.start)
        keep = pltpu.make_async_copy(wo_ref, wo_out.at[place], local.at[5])
        pl.when(target == group)(keep.start)
        for index, (_, _, step, _) in enumerate(units):
            if split and step:

                @pl.when(rep == step % 2)
                def _(index=index):
                    unit_relay(index).wait_recv()
                    unit_copy(index).wait_send()
                    unit_relay(index).start()

            else:
                unit_copy(index).wait_recv()
                unit_copy(index).wait_send()
        for index, (_, _, step, _) in enumerate(units):
            if split and step:
                pl.when(rep != step % 2)(unit_relay(index).wait_recv)
                pl.when(rep == step % 2)(unit_relay(index).wait_send)
        for copy in sent:
            copy.wait_recv()
        for index in range(planes):
            pl.when(group * planes + index != me)(wo_copy(index, index)[1].wait_recv)
        for index in range(planes):
            peer, copy = wo_copy(place, index)
            pl.when(peer != me)(copy.wait_send)
        pl.when(target == group)(keep.wait)
        for copy in sent:
            copy.wait_send()
        for copy in started:
            copy.wait()

    total = 3 + count - 1
    number = count - 1 + PLANE - 1
    return comm_call(
        body,
        "gather_weights",
        ident,
        [tokens, qkv, up, out_w, small],
        [
            struct((PLANE,) + tokens.shape),
            struct((count, rows, qkv.shape[2])),
            struct((PLANE, rows, up.shape[2])),
            struct((planes,) + out_w.shape),
            struct((count,) + small.shape),
        ],
        [ANY_SPEC] * 5,
        [
            pltpu.SemaphoreType.DMA((total,)),
            pltpu.SemaphoreType.DMA((total,)),
            pltpu.SemaphoreType.DMA((6,)),
            pltpu.SemaphoreType.DMA((planes,)),
            pltpu.SemaphoreType.DMA((planes,)),
            pltpu.SemaphoreType.DMA((number,)),
            pltpu.SemaphoreType.DMA((number,)),
        ],
    )


def gather_planes(count, value, ident):
    planes = count // PLANE

    def body(x_ref, out_ref, send, recv, local):
        me = lax.axis_index("shard")
        plane = lax.div(me, PLANE)
        greet([{"shard": lax.rem(me + PLANE * s, count)} for s in range(1, planes)])
        own = pltpu.make_async_copy(x_ref, out_ref.at[plane], local)
        own.start()

        def hop(way, source, src):
            peer = me + PLANE if way == 0 else me - PLANE
            return remote(
                src,
                out_ref.at[source],
                send.at[way, source],
                recv.at[way, source],
                {"shard": lax.rem(peer + count, count)},
            )

        @pl.when(plane < planes - 1)
        def _():
            hop(0, plane, x_ref).start()

        @pl.when(plane > 0)
        def _():
            hop(1, plane, x_ref).start()

        for step in range(1, planes):
            for way, source in ((0, plane - step), (1, plane + step)):
                onward = plane < planes - 1 if way == 0 else plane > 0

                @pl.when((source >= 0) & (source < planes))
                def _(way=way, source=source, onward=onward):
                    copy = hop(way, source, out_ref.at[source])
                    copy.wait_recv()
                    pl.when(onward)(copy.start)

        @pl.when(plane < planes - 1)
        def _():
            hop(0, plane, x_ref).wait_send()

        @pl.when(plane > 0)
        def _():
            hop(1, plane, x_ref).wait_send()

        for step in range(1, planes):
            for way, source in ((0, plane - step), (1, plane + step)):
                onward = plane < planes - 1 if way == 0 else plane > 0

                @pl.when((source >= 0) & (source < planes) & onward)
                def _(way=way, source=source):
                    hop(way, source, out_ref.at[source]).wait_send()

        own.wait()

    return comm_call(
        body,
        "gather_planes",
        ident,
        [value],
        struct((planes,) + value.shape),
        ANY_SPEC,
        [
            pltpu.SemaphoreType.DMA((2, planes)),
            pltpu.SemaphoreType.DMA((2, planes)),
            pltpu.SemaphoreType.DMA,
        ],
    )


def sum_planes(count, parts, ident):
    planes, rows, cols = parts.shape

    def body(p_ref, out_ref, held, staged, send, recv):
        me = lax.axis_index("shard")
        plane = lax.div(me, PLANE)
        greet([{"shard": lax.rem(me + PLANE * s, count)} for s in range(1, planes)])

        def hop(way, goal, src):
            peer = me + PLANE if way == 0 else me - PLANE
            return remote(
                src,
                held.at[way, goal],
                send.at[goal],
                recv.at[way, goal],
                {"shard": lax.rem(peer + count, count)},
            )

        for step in range(planes - 1):
            for way, goal in ((0, planes - 1 - step), (1, step)):
                ahead = goal > plane if way == 0 else goal < plane
                first = plane == 0 if way == 0 else plane == planes - 1

                @pl.when(ahead & first)
                def _(way=way, goal=goal):
                    hop(way, goal, p_ref.at[goal]).start()

                @pl.when(ahead & jnp.logical_not(first))
                def _(way=way, goal=goal):
                    copy = hop(way, goal, staged.at[goal])
                    copy.wait_recv()
                    total = p_ref[goal].astype(f32) + held[way, goal].astype(f32)
                    staged[goal] = total.astype(bf16)
                    copy.start()

        out_ref[...] = p_ref[plane]

        @pl.when(plane > 0)
        def _():
            hop(0, plane, staged.at[plane]).wait_recv()
            out_ref[...] = (out_ref[...].astype(f32) + held[0, plane].astype(f32)).astype(bf16)

        @pl.when(plane < planes - 1)
        def _():
            hop(1, plane, staged.at[plane]).wait_recv()
            out_ref[...] = (out_ref[...].astype(f32) + held[1, plane].astype(f32)).astype(bf16)

        for goal in range(planes):

            @pl.when(goal != plane)
            def _(goal=goal):
                hop(0, goal, staged.at[goal]).wait_send()

    return comm_call(
        body,
        "sum_planes",
        ident,
        [parts],
        struct((rows, cols)),
        VMEM_SPEC,
        [
            pltpu.VMEM((2, planes, rows, cols), bf16),
            pltpu.VMEM((planes, rows, cols), bf16),
            pltpu.SemaphoreType.DMA((planes,)),
            pltpu.SemaphoreType.DMA((2, planes)),
        ],
    )


def reduce_grads(count, copies, qkv, up, out_w, down, small, ident):
    planes = count // PLANE
    rows = qkv.shape[1]
    block = down.shape[0]
    arrays = [qkv, up, out_w, small]

    def body(qkv_ref, up_ref, wo_ref, small_ref, down_ref, *rest):
        outs, (qkv_in, up_in, wo_in, small_in) = rest[:5], rest[5:9]
        halves, gets = [rest[9], up_in, rest[10], rest[11], down_ref], rest[12:17]
        send, recv, send_rep, recv_rep, send_wo, recv_wo = rest[17:]
        me = lax.axis_index("shard")
        rep = lax.axis_index("rep")
        plane = lax.div(me, PLANE)
        across = [{"rep": lax.rem(rep + step, copies)} for step in range(1, copies)]
        greet(others(me, count) + across)
        sent = []

        def push(src, dst, peer):
            index = len(sent)
            copy = remote(src, dst, send.at[index], recv.at[index], {"shard": peer})
            copy.start()
            sent.append(copy)

        pairs = [(qkv_ref, qkv_in), (small_ref, small_in)]
        group = lax.rem(me, PLANE)
        target, place = lax.div(me, planes), lax.rem(me, planes)
        for src, held in pairs:
            for step in range(1, count):
                peer = lax.rem(me + step, count)
                push(src.at[peer], held.at[me], peer)
        for lane in range(1, PLANE):
            goal = lax.rem(group + lane, PLANE)
            push(up_ref.at[goal], up_in.at[group], plane * PLANE + goal)
        up_in[group] = up_ref[group]
        for src, held in pairs:
            held[me] = src[me]

        def wo_copy(source, index):
            peer = group * planes + index
            return peer, remote(
                wo_ref.at[index],
                wo_in.at[plane],
                send_wo.at[index],
                recv_wo.at[source],
                {"shard": peer},
            )

        for index in range(planes):
            peer, copy = wo_copy(plane, index)
            pl.when(peer != me)(copy.start)

        @pl.when(target == group)
        def _():
            wo_in[plane] = wo_ref[place]

        for copy in sent:
            copy.wait_recv()
        for index in range(planes):
            pl.when(PLANE * index + target != me)(wo_copy(index, index)[1].wait_recv)
        for index in range(planes):
            peer, copy = wo_copy(plane, index)
            pl.when(peer != me)(copy.wait_send)
        for half, held in zip(halves[:1], (qkv_in,)):
            for lane in range(PLANE):
                total = held[lane].astype(f32)
                for other in range(1, planes):
                    total = total + held[other * PLANE + lane].astype(f32)
                half[lane] = total.astype(bf16)
        for half, held, number in (
            (halves[2], wo_in, planes),
            (halves[3], small_in, count),
        ):
            total = held[0].astype(f32)
            for other in range(1, number):
                total = total + held[other].astype(f32)
            half[...] = total.astype(bf16)
        passed = []
        for index, peer in enumerate(across):
            for place, (half, got) in enumerate(zip(halves, gets)):
                copy = remote(
                    half,
                    got.at[index],
                    send_rep.at[5 * index + place],
                    recv_rep.at[5 * index + place],
                    peer,
                )
                copy.start()
                passed.append(copy)
        for copy in passed:
            copy.wait_recv()
        for out, half, got in zip(outs, halves, gets):
            total = half[...].astype(f32)
            for index in range(copies - 1):
                total = total + got[index].astype(f32)
            out[...] = total
        for copy in sent + passed:
            copy.wait_send()

    totals = 2 * (count - 1) + PLANE - 1
    shapes = [
        (PLANE, rows, qkv.shape[2]),
        (PLANE, rows, up.shape[2]),
        (rows, D),
        small.shape[1:],
        (block, D),
    ]
    return comm_call(
        body,
        "reduce_grads",
        ident,
        arrays + [down],
        [struct(shape, f32) for shape in shapes],
        [VMEM_SPEC] * 5,
        [pltpu.VMEM(item.shape, bf16) for item in arrays]
        + [pltpu.VMEM(shapes[index], bf16) for index in (0, 2, 3)]
        + [pltpu.VMEM((copies - 1,) + shape, bf16) for shape in shapes]
        + [
            pltpu.SemaphoreType.DMA((totals,)),
            pltpu.SemaphoreType.DMA((totals,)),
            pltpu.SemaphoreType.DMA((5 * (copies - 1),)),
            pltpu.SemaphoreType.DMA((5 * (copies - 1),)),
            pltpu.SemaphoreType.DMA((planes,)),
            pltpu.SemaphoreType.DMA((planes,)),
        ],
    )


def norm_forward(value, gain, shift):
    center = value - jnp.mean(value, axis=-1, keepdims=True)
    spread = jnp.mean(center * center, axis=-1, keepdims=True)
    scale = lax.rsqrt(spread + epsilon)
    normal = center * scale
    return (normal * gain + shift, normal, scale)


def norm_backward(upstream, normal, scale, gain):
    inner = upstream * gain
    return scale * (
        inner
        - jnp.mean(inner, axis=-1, keepdims=True)
        - normal * jnp.mean(inner * normal, axis=-1, keepdims=True)
    )


def gelu_slope(hidden):
    return 0.5 * (1.0 + lax.erf(hidden * root_half)) + hidden * inv_root_tau * jnp.exp(
        -0.5 * hidden * hidden
    )


def dot(left, right):
    return jnp.dot(left, right, preferred_element_type=f32)


def dot_left(left, right):
    return lax.dot_general(left, right, (((0,), (0,)), ((), ())), preferred_element_type=f32)


def dot_right(left, right):
    return lax.dot_general(left, right, (((1,), (1,)), ((), ())), preferred_element_type=f32)


def heads_of(value):
    return value.reshape(value.shape[0], GROUP_HEADS, HEAD_DIM).transpose(1, 0, 2)


def flat_of(value):
    return value.transpose(1, 0, 2).reshape(value.shape[1], GROUP_DIM)


def attend_forward(queries, keys, values, own_codes, all_codes):
    def step(carried, pieces):
        top, total, summed = carried
        key_rows, value_rows, key_codes = pieces
        raw = jnp.einsum("hqd,khd->hqk", queries, key_rows, preferred_element_type=f32) * 0.125
        allowed = (own_codes[:, None] == key_codes[None, :])[None]
        masked = jnp.where(allowed, raw, very_low)
        new_top = jnp.maximum(top, jnp.max(masked, axis=2))
        rescale = jnp.exp(top - new_top)
        weights = jnp.where(allowed, jnp.exp(masked - new_top[:, :, None]), 0.0)
        added = jnp.einsum(
            "hqk,khd->hqd", weights.astype(bf16), value_rows, preferred_element_type=f32
        )
        return (
            new_top,
            total * rescale + jnp.sum(weights, axis=2),
            summed * rescale[:, :, None] + added,
        ), None

    rows = queries.shape[1]
    start = (
        jnp.full((GROUP_HEADS, rows), very_low, f32),
        jnp.zeros((GROUP_HEADS, rows), f32),
        jnp.zeros((GROUP_HEADS, rows, HEAD_DIM), f32),
    )
    (top, total, summed), _ = lax.scan(step, start, (keys, values, all_codes))
    return summed / total[:, :, None], top + jnp.log(total)


def attend_backward(queries, keys, values, own_codes, all_codes, logs, delta, upstream):
    def step(carried, pieces):
        key_rows, value_rows, key_codes = pieces
        raw = jnp.einsum("hqd,khd->hqk", queries, key_rows, preferred_element_type=f32) * 0.125
        allowed = (own_codes[:, None] == key_codes[None, :])[None]
        chances = jnp.where(allowed, jnp.exp(raw - logs[:, :, None]), 0.0)
        d_chance = jnp.einsum("hqd,khd->hqk", upstream, value_rows, preferred_element_type=f32)
        d_score = (chances * (d_chance - delta[:, :, None])).astype(bf16)
        carried = carried + jnp.einsum(
            "hqk,khd->hqd", d_score, key_rows, preferred_element_type=f32
        )
        d_key = jnp.einsum("hqk,hqd->khd", d_score, queries, preferred_element_type=f32) * 0.125
        d_value = jnp.einsum(
            "hqk,hqd->khd", chances.astype(bf16), upstream, preferred_element_type=f32
        )
        size = key_rows.shape[0]
        return carried, jnp.concatenate(
            [d_key.reshape(size, GROUP_DIM), d_value.reshape(size, GROUP_DIM)], axis=1
        ).astype(bf16)

    start = jnp.zeros(queries.shape, f32)
    d_query, d_pair = lax.scan(step, start, (keys, values, all_codes))
    return d_query * 0.125, d_pair


def shards(count, copies, *arrays):
    (
        tokens,
        segments,
        padding,
        query_weight,
        key_weight,
        value_weight,
        query_bias,
        value_bias,
        out_weight,
        out_bias,
        middle_gain,
        middle_shift,
        up_weight,
        up_bias,
        down_weight,
        down_bias,
        final_gain,
        final_shift,
        cotangent,
    ) = arrays
    planes = count // PLANE
    rows = query_weight.shape[0]
    block = down_weight.shape[0]
    x_own = tokens[0]
    here = x_own.shape[0]
    wide = PLANE * here
    me = lax.axis_index("shard")
    group = lax.rem(me, PLANE)
    qkv_send = jnp.concatenate(
        [
            item.astype(bf16).reshape(rows, PLANE, GROUP_DIM)
            for item in (query_weight, key_weight, value_weight)
        ],
        axis=2,
    ).transpose(1, 0, 2)
    up_send = (
        up_weight.astype(bf16)
        .reshape(rows, planes, PLANE, block)
        .transpose(2, 0, 1, 3)
        .reshape(PLANE, rows, GROUP_FF)
    )
    codes = (2 * segments[0] + padding[0]).astype(f32)
    lanes = 128 * ((max(here, block) + 127) // 128)

    def padded(value):
        return jnp.pad(value.astype(f32), (0, lanes - value.shape[0]))

    vectors = [
        query_bias,
        value_bias,
        out_bias,
        middle_gain,
        middle_shift,
        down_bias,
        final_gain,
        final_shift,
        up_bias,
        codes,
    ]
    small_send = jnp.pad(
        jnp.stack([padded(item) for item in vectors]), ((0, 6), (0, 0))
    ).astype(bf16)
    x_all, qkv_all, up_all, wo_all, small = gather_weights(
        count,
        copies,
        x_own,
        qkv_send,
        up_send,
        out_weight.astype(bf16),
        small_send,
        0,
    )
    x_plane = x_all.reshape(wide, D)
    w_qkv = qkv_all.reshape(D, 3 * GROUP_DIM)
    lines = [[start + PLANE * step for step in range(planes)] for start in range(PLANE)]
    strip = jnp.concatenate([up_all.reshape(PLANE * rows, D), down_weight.astype(bf16)], axis=0)
    strips = lax.all_gather(strip, "shard", axis_index_groups=lines, axis=0)
    w_up = strips[:, : PLANE * rows].reshape(D, GROUP_FF)
    w_out = wo_all.reshape(GROUP_DIM, D)
    w_down = strips[:, PLANE * rows :].reshape(GROUP_FF, D)
    small = small.astype(f32)
    spread = [small[:, index, :rows].reshape(D) for index in range(8)]
    b_query, b_value, b_out, gain_mid, shift_mid, b_down, gain_end, shift_end = spread
    b_up = lax.dynamic_index_in_dim(
        small[:, 8, :block].reshape(planes, PLANE, block), group, 1, keepdims=False
    ).reshape(GROUP_FF)
    all_codes = small[:, 9, :here].reshape(planes, wide)
    own_codes = lax.dynamic_index_in_dim(all_codes, lax.div(me, PLANE), 0, keepdims=False)

    def group_part(value):
        return lax.dynamic_slice(value, (group * GROUP_DIM,), (GROUP_DIM,))

    qkv_bias = jnp.concatenate(
        [group_part(b_query), jnp.zeros((GROUP_DIM,), f32), group_part(b_value)]
    )
    qkv = (dot(x_plane, w_qkv) + qkv_bias).astype(bf16)
    pairs = gather_planes(count, qkv[:, GROUP_DIM:], 1)
    queries = heads_of(qkv[:, :GROUP_DIM])
    keys = pairs[:, :, :GROUP_DIM].reshape(planes, wide, GROUP_HEADS, HEAD_DIM)
    values = pairs[:, :, GROUP_DIM:].reshape(planes, wide, GROUP_HEADS, HEAD_DIM)
    context_heads, logs = attend_forward(queries, keys, values, own_codes, all_codes)
    context_low = flat_of(context_heads).astype(bf16)

    def split(value):
        return value.reshape(PLANE, here, D)

    branch = plane_sum(split(dot(context_low, w_out).astype(bf16)), 2) + b_out
    middle, normal_mid, scale_mid = norm_forward(x_own.astype(f32) + branch, gain_mid, shift_mid)
    middle_plane = plane_gather(middle.astype(bf16), 3).reshape(wide, D)
    hidden = dot(middle_plane, w_up) + b_up
    active_low = jax.nn.gelu(hidden, approximate=False).astype(bf16)
    feed = plane_sum(split(dot(active_low, w_down).astype(bf16)), 4) + b_down
    result, normal_end, scale_end = norm_forward(middle + feed, gain_end, shift_end)
    output = result.astype(bf16)[None]
    upstream = cotangent[0].astype(f32)
    d_second = norm_backward(upstream, normal_end, scale_end, gain_end)
    feed_low = d_second.astype(bf16)
    feed_plane = plane_gather(feed_low, 5).reshape(wide, D)
    grad_down = dot_left(active_low, feed_plane).astype(bf16)
    up_low = (dot_right(feed_plane, w_down) * gelu_slope(hidden)).astype(bf16)
    grad_up = dot_left(middle_plane, up_low).astype(bf16)
    strip_grads = lax.psum_scatter(
        jnp.concatenate(
            [
                grad_up.reshape(planes, PLANE * rows, GROUP_FF),
                grad_down.reshape(planes, block, D),
            ],
            axis=1,
        ),
        "shard",
        axis_index_groups=lines,
        scatter_dimension=0,
    )
    d_middle = plane_sum(split(dot_right(up_low, w_up).astype(bf16)), 6) + d_second
    d_first = norm_backward(d_middle, normal_mid, scale_mid, gain_mid)
    branch_low = d_first.astype(bf16)
    branch_plane = plane_gather(branch_low, 7).reshape(wide, D)
    grad_out = dot_left(context_low, branch_plane).astype(bf16)
    d_context = heads_of(dot_right(branch_plane, w_out).astype(bf16))
    delta = jnp.sum(d_context.astype(f32) * context_heads, axis=2)
    d_query, d_pair = attend_backward(
        queries, keys, values, own_codes, all_codes, logs, delta, d_context
    )
    pair_low = sum_planes(count, d_pair, 8)
    mixer_low = jnp.concatenate([flat_of(d_query).astype(bf16), pair_low], axis=1)
    grad_qkv = dot_left(x_plane, mixer_low).astype(bf16)
    grad_input = plane_sum(split(dot_right(mixer_low, w_qkv).astype(bf16)), 9)
    grad_tokens = (grad_input + d_first).astype(bf16)[None]
    mixer_sums = jnp.sum(mixer_low.astype(f32), axis=0)

    def from_group(value):
        return lax.dynamic_update_slice(jnp.zeros((D,), f32), value, (group * GROUP_DIM,))

    sums = [
        from_group(mixer_sums[:GROUP_DIM]),
        from_group(mixer_sums[2 * GROUP_DIM :]),
        jnp.sum(branch_low.astype(f32), axis=0),
        jnp.sum(d_middle * normal_mid, axis=0),
        jnp.sum(d_middle, axis=0),
        jnp.sum(feed_low.astype(f32), axis=0),
        jnp.sum(upstream * normal_end, axis=0),
        jnp.sum(upstream, axis=0),
    ]
    own_lane = (jnp.arange(PLANE) == group).astype(f32)
    up_sums = jnp.sum(up_low.astype(f32), axis=0).reshape(planes, 1, block)
    up_sums = (up_sums * own_lane[None, :, None]).reshape(count, 1, block)
    sums = jnp.stack([item.reshape(count, rows) for item in sums], axis=1)
    small_grads = jnp.concatenate(
        [
            jnp.pad(sums, ((0, 0), (0, 0), (0, lanes - rows))),
            jnp.pad(up_sums, ((0, 0), (0, 7), (0, lanes - block))),
        ],
        axis=1,
    ).astype(bf16)
    qkv_total, up_total, out_total, small_total, down_total = reduce_grads(
        count,
        copies,
        grad_qkv.reshape(count, rows, 3 * GROUP_DIM),
        strip_grads[: PLANE * rows].reshape(PLANE, rows, GROUP_FF),
        grad_out.reshape(planes, rows, D),
        strip_grads[PLANE * rows :],
        small_grads,
        10,
    )

    def joined(value):
        return value.transpose(1, 0, 2).reshape(rows, D)

    up_grad = (
        up_total.reshape(PLANE, rows, planes, block).transpose(1, 2, 0, 3).reshape(rows, FF)
    )
    return (
        output,
        grad_tokens,
        joined(qkv_total[:, :, :GROUP_DIM]),
        joined(qkv_total[:, :, GROUP_DIM : 2 * GROUP_DIM]),
        joined(qkv_total[:, :, 2 * GROUP_DIM :]),
        small_total[0, :rows],
        small_total[1, :rows],
        out_total,
        small_total[2, :rows],
        small_total[3, :rows],
        small_total[4, :rows],
        up_grad,
        small_total[8, :block],
        down_total,
        small_total[5, :rows],
        small_total[6, :rows],
        small_total[7, :rows],
    )


def solution(mesh):
    sheet, line = P("shard", None), P("shard")
    batch = P("rep", "shard", None)
    in_specs = (batch, P("rep", "shard"), P("rep", "shard"), sheet, sheet, sheet, line, line)
    in_specs += (sheet, line, line, line, sheet, line, sheet, line, line, line, batch)
    out_specs = (batch, batch, sheet, sheet, sheet, line, line, sheet, line, line, line)
    out_specs += (sheet, line, sheet, line, line, line)
    body = functools.partial(shards, mesh.shape["shard"], mesh.shape["rep"])
    return jax.shard_map(
        body, mesh=mesh, in_specs=in_specs, out_specs=out_specs, check_vma=False
    )
```

```python
import functools

import jax
import jax.numpy as jnp
from jax import lax
from jax.experimental import pallas as pl
from jax.experimental.pallas import tpu as pltpu
from jax.sharding import PartitionSpec as P

D = 768
HEADS = 12
HEAD_DIM = 64
PLANE = 4
GROUP_HEADS = HEADS // PLANE
GROUP_DIM = GROUP_HEADS * HEAD_DIM
FF = 3072
GROUP_FF = FF // PLANE

epsilon = 1e-12
very_low = -1e30
root_half = 0.7071067811865476
inv_root_tau = 0.3989422804014327
bf16 = jnp.bfloat16
f32 = jnp.float32
MESH = pl.DeviceIdType.MESH
VMEM_SPEC = pl.BlockSpec(memory_space=pltpu.VMEM)
ANY_SPEC = pl.BlockSpec(memory_space=pl.ANY)
VMEM_BYTES = 60000 * 1024
MODEL_BYTES = 100_000_000


def struct(shape, dtype=bf16):
    return jax.ShapeDtypeStruct(shape, dtype)


def comm_call(body, name, ident, inputs, out_shapes, out_specs, scratch):
    return pl.pallas_call(
        body,
        name=name,
        out_shape=out_shapes,
        in_specs=[VMEM_SPEC] * len(inputs),
        out_specs=out_specs,
        scratch_shapes=scratch,
        cost_estimate=pl.CostEstimate(flops=0, bytes_accessed=MODEL_BYTES, transcendentals=0),
        compiler_params=pltpu.CompilerParams(
            collective_id=ident, has_side_effects=True, vmem_limit_bytes=VMEM_BYTES
        ),
    )(*inputs)


def greet(peers):
    barrier = pltpu.get_barrier_semaphore()
    for peer in peers:
        pl.semaphore_signal(barrier, inc=1, device_id=peer, device_id_type=MESH)
    pl.semaphore_wait(barrier, len(peers))


def remote(src, dst, send_sem, recv_sem, peer):
    return pltpu.make_async_remote_copy(
        src_ref=src,
        dst_ref=dst,
        send_sem=send_sem,
        recv_sem=recv_sem,
        device_id=peer,
        device_id_type=MESH,
    )


def plane_peer(me, mask):
    group = lax.rem(me, PLANE)
    core = lax.rem(group, 2)
    column = lax.div(group, 2)
    if mask & 1:
        core = 1 - core
    if mask & 2:
        column = 1 - column
    return me - group + 2 * column + core


def plane_slot(me, mask):
    return lax.rem(plane_peer(me, mask), PLANE)


def plane_gather(value, ident):
    rows, cols = value.shape

    def body(x_ref, out_ref, send, recv, local):
        me = lax.axis_index("shard")
        peers = [{"shard": plane_peer(me, mask)} for mask in (1, 2)]
        greet(peers)
        mine, far = lax.rem(me, PLANE), plane_slot(me, 2)
        own = pltpu.make_async_copy(x_ref, out_ref.at[mine], local)
        own.start()
        across = remote(x_ref, out_ref.at[mine], send.at[0], recv.at[0], peers[1])
        across.start()
        beside = remote(x_ref, out_ref.at[mine], send.at[1], recv.at[1], peers[0])
        beside.start()
        across.wait_recv()
        relay = remote(out_ref.at[far], out_ref.at[far], send.at[2], recv.at[2], peers[0])
        relay.start()
        beside.wait_recv()
        relay.wait_recv()
        across.wait_send()
        beside.wait_send()
        relay.wait_send()
        own.wait()

    return comm_call(
        body,
        "plane_gather",
        ident,
        [value],
        struct((PLANE, rows, cols), value.dtype),
        VMEM_SPEC,
        [
            pltpu.SemaphoreType.DMA((3,)),
            pltpu.SemaphoreType.DMA((3,)),
            pltpu.SemaphoreType.DMA,
        ],
    )


def plane_sum(parts, ident):
    _, rows, cols = parts.shape

    def body(p_ref, out_ref, near, held, far_in, send, recv):
        me = lax.axis_index("shard")
        peers = [{"shard": plane_peer(me, mask)} for mask in (1, 2)]
        greet(peers)
        first = remote(
            p_ref.at[plane_slot(me, 3)], near.at[0], send.at[0], recv.at[0], peers[0]
        )
        first.start()
        second = remote(
            p_ref.at[plane_slot(me, 1)], near.at[1], send.at[1], recv.at[1], peers[0]
        )
        second.start()
        first.wait_recv()
        held[...] = (p_ref[plane_slot(me, 2)].astype(f32) + near[0].astype(f32)).astype(bf16)
        third = remote(held, far_in, send.at[2], recv.at[2], peers[1])
        third.start()
        second.wait_recv()
        out_ref[...] = p_ref[lax.rem(me, PLANE)].astype(f32) + near[1].astype(f32)
        third.wait_recv()
        out_ref[...] += far_in[...].astype(f32)
        first.wait_send()
        second.wait_send()
        third.wait_send()

    return comm_call(
        body,
        "plane_sum",
        ident,
        [parts],
        struct((rows, cols), f32),
        VMEM_SPEC,
        [
            pltpu.VMEM((2, rows, cols), bf16),
            pltpu.VMEM((rows, cols), bf16),
            pltpu.VMEM((rows, cols), bf16),
            pltpu.SemaphoreType.DMA((3,)),
            pltpu.SemaphoreType.DMA((3,)),
        ],
    )


def others(me, count):
    return [{"shard": lax.rem(me + step, count)} for step in range(1, count)]


def gather_weights(count, copies, tokens, qkv, up, out_w, small, ident):
    planes = count // PLANE
    rows = qkv.shape[1]

    def body(x_ref, qkv_ref, up_ref, wo_ref, small_ref, *rest):
        x_out, qkv_out, up_out, wo_out, small_out = rest[:5]
        send, recv, local, send_wo, recv_wo, send_unit, recv_unit = rest[5:]
        me = lax.axis_index("shard")
        group, plane = lax.rem(me, PLANE), lax.div(me, PLANE)
        across = [
            {"rep": lax.rem(lax.axis_index("rep") + step, copies)} for step in range(1, copies)
        ]
        greet(others(me, count) + across)
        owns = [
            (x_ref, x_out.at[group]),
            (qkv_ref.at[group], qkv_out.at[me]),
            (up_ref.at[group], up_out.at[group]),
            (small_ref, small_out.at[me]),
        ]
        started = []
        for index, (src, dst) in enumerate(owns):
            copy = pltpu.make_async_copy(src, dst, local.at[index])
            copy.start()
            started.append(copy)
        sent = []

        def push(src, dst, peer):
            index = len(sent)
            copy = remote(src, dst, send.at[index], recv.at[index], {"shard": peer})
            copy.start()
            sent.append(copy)

        for mask in (2, 1):
            push(x_ref, x_out.at[group], plane_peer(me, mask))
        far = plane_slot(me, 2)
        x_relay = remote(
            x_out.at[far], x_out.at[far], send.at[2], recv.at[2], {"shard": plane_peer(me, 1)}
        )
        sent.append(x_relay)
        for step in range(1, count):
            push(small_ref, small_out.at[me], lax.rem(me + step, count))
        rep = lax.axis_index("rep")
        split = copies == 2
        units = []
        for step in range(planes):
            for lane in range(PLANE):
                if step or lane:
                    units.append((qkv_ref, qkv_out, step, lane))
        for lane in range(1, PLANE):
            units.append((up_ref, up_out, 0, lane))

        def unit_copy(index):
            src, dst, step, lane = units[index]
            goal = lax.rem(plane + step, planes)
            goal_group = lax.rem(group + lane, PLANE)
            slot = group if src is up_ref else me
            return remote(
                src.at[goal_group],
                dst.at[slot],
                send_unit.at[index],
                recv_unit.at[index],
                {"shard": goal * PLANE + goal_group},
            )

        def unit_relay(index):
            src, dst, step, lane = units[index]
            origin = lax.rem(plane + planes - step, planes)
            origin_group = lax.rem(group + PLANE - lane, PLANE)
            slot = origin_group if src is up_ref else origin * PLANE + origin_group
            return remote(
                dst.at[slot],
                dst.at[slot],
                send_unit.at[index],
                recv_unit.at[index],
                {"rep": lax.rem(rep + 1, copies)},
            )

        def carried(index, mine):
            step = units[index][2]
            if not split or step == 0:
                return None
            return (rep == step % 2) if mine else (rep != step % 2)

        def guarded(test, action):
            if test is None:
                action()
            else:
                pl.when(test)(action)

        for index in range(len(units)):
            guarded(carried(index, True), unit_copy(index).start)
        target, place = lax.div(me, planes), lax.rem(me, planes)

        def wo_copy(source, index):
            peer = PLANE * index + target
            return peer, remote(
                wo_ref, wo_out.at[place], send_wo.at[index], recv_wo.at[source], {"shard": peer}
            )

        for index in range(planes):
            peer, copy = wo_copy(place, index)
            pl.when(peer != me)(copy.start)
        keep = pltpu.make_async_copy(wo_ref, wo_out.at[place], local.at[5])
        pl.when(target == group)(keep.start)
        sent[0].wait_recv()
        x_relay.start()
        for index, (_, _, step, _) in enumerate(units):
            if split and step:

                @pl.when(rep == step % 2)
                def _(index=index):
                    unit_relay(index).wait_recv()
                    unit_copy(index).wait_send()
                    unit_relay(index).start()

            else:
                unit_copy(index).wait_recv()
                unit_copy(index).wait_send()
        for index, (_, _, step, _) in enumerate(units):
            if split and step:
                pl.when(rep != step % 2)(unit_relay(index).wait_recv)
                pl.when(rep == step % 2)(unit_relay(index).wait_send)
        for copy in sent[1:]:
            copy.wait_recv()
        for index in range(planes):
            pl.when(group * planes + index != me)(wo_copy(index, index)[1].wait_recv)
        for index in range(planes):
            peer, copy = wo_copy(place, index)
            pl.when(peer != me)(copy.wait_send)
        pl.when(target == group)(keep.wait)
        for copy in sent:
            copy.wait_send()
        for copy in started:
            copy.wait()

    total = 3 + count - 1
    number = count - 1 + PLANE - 1
    return comm_call(
        body,
        "gather_weights",
        ident,
        [tokens, qkv, up, out_w, small],
        [
            struct((PLANE,) + tokens.shape),
            struct((count, rows, qkv.shape[2])),
            struct((PLANE, rows, up.shape[2])),
            struct((planes,) + out_w.shape),
            struct((count,) + small.shape),
        ],
        [ANY_SPEC] * 5,
        [
            pltpu.SemaphoreType.DMA((total,)),
            pltpu.SemaphoreType.DMA((total,)),
            pltpu.SemaphoreType.DMA((6,)),
            pltpu.SemaphoreType.DMA((planes,)),
            pltpu.SemaphoreType.DMA((planes,)),
            pltpu.SemaphoreType.DMA((number,)),
            pltpu.SemaphoreType.DMA((number,)),
        ],
    )


def gather_planes(count, value, ident):
    planes = count // PLANE

    def body(x_ref, out_ref, send, recv, local):
        me = lax.axis_index("shard")
        plane = lax.div(me, PLANE)
        greet([{"shard": lax.rem(me + PLANE * s, count)} for s in range(1, planes)])
        own = pltpu.make_async_copy(x_ref, out_ref.at[plane], local)
        own.start()

        def hop(way, source, src):
            peer = me + PLANE if way == 0 else me - PLANE
            return remote(
                src,
                out_ref.at[source],
                send.at[way, source],
                recv.at[way, source],
                {"shard": lax.rem(peer + count, count)},
            )

        @pl.when(plane < planes - 1)
        def _():
            hop(0, plane, x_ref).start()

        @pl.when(plane > 0)
        def _():
            hop(1, plane, x_ref).start()

        for step in range(1, planes):
            for way, source in ((0, plane - step), (1, plane + step)):
                onward = plane < planes - 1 if way == 0 else plane > 0

                @pl.when((source >= 0) & (source < planes))
                def _(way=way, source=source, onward=onward):
                    copy = hop(way, source, out_ref.at[source])
                    copy.wait_recv()
                    pl.when(onward)(copy.start)

        @pl.when(plane < planes - 1)
        def _():
            hop(0, plane, x_ref).wait_send()

        @pl.when(plane > 0)
        def _():
            hop(1, plane, x_ref).wait_send()

        for step in range(1, planes):
            for way, source in ((0, plane - step), (1, plane + step)):
                onward = plane < planes - 1 if way == 0 else plane > 0

                @pl.when((source >= 0) & (source < planes) & onward)
                def _(way=way, source=source):
                    hop(way, source, out_ref.at[source]).wait_send()

        own.wait()

    return comm_call(
        body,
        "gather_planes",
        ident,
        [value],
        struct((planes,) + value.shape),
        ANY_SPEC,
        [
            pltpu.SemaphoreType.DMA((2, planes)),
            pltpu.SemaphoreType.DMA((2, planes)),
            pltpu.SemaphoreType.DMA,
        ],
    )


def sum_planes(count, parts, ident):
    planes, rows, cols = parts.shape

    def body(p_ref, out_ref, held, staged, send, recv):
        me = lax.axis_index("shard")
        plane = lax.div(me, PLANE)
        greet([{"shard": lax.rem(me + PLANE * s, count)} for s in range(1, planes)])

        def hop(way, goal, src):
            peer = me + PLANE if way == 0 else me - PLANE
            return remote(
                src,
                held.at[way, goal],
                send.at[goal],
                recv.at[way, goal],
                {"shard": lax.rem(peer + count, count)},
            )

        for step in range(planes - 1):
            for way, goal in ((0, planes - 1 - step), (1, step)):
                ahead = goal > plane if way == 0 else goal < plane
                first = plane == 0 if way == 0 else plane == planes - 1

                @pl.when(ahead & first)
                def _(way=way, goal=goal):
                    hop(way, goal, p_ref.at[goal]).start()

                @pl.when(ahead & jnp.logical_not(first))
                def _(way=way, goal=goal):
                    copy = hop(way, goal, staged.at[goal])
                    copy.wait_recv()
                    total = p_ref[goal].astype(f32) + held[way, goal].astype(f32)
                    staged[goal] = total.astype(bf16)
                    copy.start()

        out_ref[...] = p_ref[plane]

        @pl.when(plane > 0)
        def _():
            hop(0, plane, staged.at[plane]).wait_recv()
            out_ref[...] = (out_ref[...].astype(f32) + held[0, plane].astype(f32)).astype(bf16)

        @pl.when(plane < planes - 1)
        def _():
            hop(1, plane, staged.at[plane]).wait_recv()
            out_ref[...] = (out_ref[...].astype(f32) + held[1, plane].astype(f32)).astype(bf16)

        for goal in range(planes):

            @pl.when(goal != plane)
            def _(goal=goal):
                hop(0, goal, staged.at[goal]).wait_send()

    return comm_call(
        body,
        "sum_planes",
        ident,
        [parts],
        struct((rows, cols)),
        VMEM_SPEC,
        [
            pltpu.VMEM((2, planes, rows, cols), bf16),
            pltpu.VMEM((planes, rows, cols), bf16),
            pltpu.SemaphoreType.DMA((planes,)),
            pltpu.SemaphoreType.DMA((2, planes)),
        ],
    )


def reduce_grads(count, copies, qkv, up, out_w, down, small, ident):
    planes = count // PLANE
    rows = qkv.shape[1]
    block = down.shape[0]
    arrays = [qkv, up, out_w, small]

    def body(qkv_ref, up_ref, wo_ref, small_ref, down_ref, *rest):
        outs, (qkv_in, up_in, wo_in, small_in) = rest[:5], rest[5:9]
        halves, gets = [rest[9], up_in, rest[10], rest[11], down_ref], rest[12:17]
        send, recv, send_rep, recv_rep, send_wo, recv_wo = rest[17:]
        me = lax.axis_index("shard")
        rep = lax.axis_index("rep")
        plane = lax.div(me, PLANE)
        across = [{"rep": lax.rem(rep + step, copies)} for step in range(1, copies)]
        greet(others(me, count) + across)
        sent = []

        def push(src, dst, peer):
            index = len(sent)
            copy = remote(src, dst, send.at[index], recv.at[index], {"shard": peer})
            copy.start()
            sent.append(copy)

        pairs = [(qkv_ref, qkv_in), (small_ref, small_in)]
        passed = []

        def exchange(*places):
            for index, peer in enumerate(across):
                for place in places:
                    copy = remote(
                        halves[place],
                        gets[place].at[index],
                        send_rep.at[5 * index + place],
                        recv_rep.at[5 * index + place],
                        peer,
                    )
                    copy.start()
                    passed.append(copy)

        exchange(4)
        group = lax.rem(me, PLANE)
        target, place = lax.div(me, planes), lax.rem(me, planes)
        for lane in range(1, PLANE):
            goal = lax.rem(group + lane, PLANE)
            push(up_ref.at[goal], up_in.at[group], plane * PLANE + goal)
        up_in[group] = up_ref[group]
        for src, held in pairs:
            for step in range(1, count):
                peer = lax.rem(me + step, count)
                push(src.at[peer], held.at[me], peer)
        for src, held in pairs:
            held[me] = src[me]

        def wo_copy(source, index):
            peer = group * planes + index
            return peer, remote(
                wo_ref.at[index],
                wo_in.at[plane],
                send_wo.at[index],
                recv_wo.at[source],
                {"shard": peer},
            )

        for index in range(planes):
            peer, copy = wo_copy(plane, index)
            pl.when(peer != me)(copy.start)

        @pl.when(target == group)
        def _():
            wo_in[plane] = wo_ref[place]

        for copy in sent[: PLANE - 1]:
            copy.wait_recv()
        exchange(1)
        for index in range(planes):
            pl.when(PLANE * index + target != me)(wo_copy(index, index)[1].wait_recv)
        for index in range(planes):
            peer, copy = wo_copy(plane, index)
            pl.when(peer != me)(copy.wait_send)
        total = wo_in[0].astype(f32)
        for other in range(1, planes):
            total = total + wo_in[other].astype(f32)
        halves[2][...] = total.astype(bf16)
        exchange(2)
        for copy in sent[PLANE - 1 :]:
            copy.wait_recv()
        for half, held in zip(halves[:1], (qkv_in,)):
            for lane in range(PLANE):
                total = held[lane].astype(f32)
                for other in range(1, planes):
                    total = total + held[other * PLANE + lane].astype(f32)
                half[lane] = total.astype(bf16)
        for half, held, number in (
            (halves[3], small_in, count),
        ):
            total = held[0].astype(f32)
            for other in range(1, number):
                total = total + held[other].astype(f32)
            half[...] = total.astype(bf16)
        exchange(0, 3)
        for copy in passed:
            copy.wait_recv()
        for out, half, got in zip(outs, halves, gets):
            total = half[...].astype(f32)
            for index in range(copies - 1):
                total = total + got[index].astype(f32)
            out[...] = total
        for copy in sent + passed:
            copy.wait_send()

    totals = 2 * (count - 1) + PLANE - 1
    shapes = [
        (PLANE, rows, qkv.shape[2]),
        (PLANE, rows, up.shape[2]),
        (rows, D),
        small.shape[1:],
        (block, D),
    ]
    return comm_call(
        body,
        "reduce_grads",
        ident,
        arrays + [down],
        [struct(shape, f32) for shape in shapes],
        [VMEM_SPEC] * 5,
        [pltpu.VMEM(item.shape, bf16) for item in arrays]
        + [pltpu.VMEM(shapes[index], bf16) for index in (0, 2, 3)]
        + [pltpu.VMEM((copies - 1,) + shape, bf16) for shape in shapes]
        + [
            pltpu.SemaphoreType.DMA((totals,)),
            pltpu.SemaphoreType.DMA((totals,)),
            pltpu.SemaphoreType.DMA((5 * (copies - 1),)),
            pltpu.SemaphoreType.DMA((5 * (copies - 1),)),
            pltpu.SemaphoreType.DMA((planes,)),
            pltpu.SemaphoreType.DMA((planes,)),
        ],
    )


def norm_forward(value, gain, shift):
    center = value - jnp.mean(value, axis=-1, keepdims=True)
    spread = jnp.mean(center * center, axis=-1, keepdims=True)
    scale = lax.rsqrt(spread + epsilon)
    normal = center * scale
    return (normal * gain + shift, normal, scale)


def norm_backward(upstream, normal, scale, gain):
    inner = upstream * gain
    return scale * (
        inner
        - jnp.mean(inner, axis=-1, keepdims=True)
        - normal * jnp.mean(inner * normal, axis=-1, keepdims=True)
    )


def gelu_slope(hidden):
    return 0.5 * (1.0 + lax.erf(hidden * root_half)) + hidden * inv_root_tau * jnp.exp(
        -0.5 * hidden * hidden
    )


def dot(left, right):
    return jnp.dot(left, right, preferred_element_type=f32)


def dot_left(left, right):
    return lax.dot_general(left, right, (((0,), (0,)), ((), ())), preferred_element_type=f32)


def dot_right(left, right):
    return lax.dot_general(left, right, (((1,), (1,)), ((), ())), preferred_element_type=f32)


def heads_of(value):
    return value.reshape(value.shape[0], GROUP_HEADS, HEAD_DIM).transpose(1, 0, 2)


def flat_of(value):
    return value.transpose(1, 0, 2).reshape(value.shape[1], GROUP_DIM)


def attend_forward(queries, keys, values, own_codes, all_codes):
    def step(carried, pieces):
        top, total, summed = carried
        key_rows, value_rows, key_codes = pieces
        raw = jnp.einsum("hqd,khd->hqk", queries, key_rows, preferred_element_type=f32) * 0.125
        allowed = (own_codes[:, None] == key_codes[None, :])[None]
        masked = jnp.where(allowed, raw, very_low)
        new_top = jnp.maximum(top, jnp.max(masked, axis=2))
        rescale = jnp.exp(top - new_top)
        weights = jnp.where(allowed, jnp.exp(masked - new_top[:, :, None]), 0.0)
        added = jnp.einsum(
            "hqk,khd->hqd", weights.astype(bf16), value_rows, preferred_element_type=f32
        )
        return (
            new_top,
            total * rescale + jnp.sum(weights, axis=2),
            summed * rescale[:, :, None] + added,
        ), None

    rows = queries.shape[1]
    start = (
        jnp.full((GROUP_HEADS, rows), very_low, f32),
        jnp.zeros((GROUP_HEADS, rows), f32),
        jnp.zeros((GROUP_HEADS, rows, HEAD_DIM), f32),
    )
    (top, total, summed), _ = lax.scan(step, start, (keys, values, all_codes))
    return summed / total[:, :, None], top + jnp.log(total)


def attend_backward(queries, keys, values, own_codes, all_codes, logs, delta, upstream):
    def step(carried, pieces):
        key_rows, value_rows, key_codes = pieces
        raw = jnp.einsum("hqd,khd->hqk", queries, key_rows, preferred_element_type=f32) * 0.125
        allowed = (own_codes[:, None] == key_codes[None, :])[None]
        chances = jnp.where(allowed, jnp.exp(raw - logs[:, :, None]), 0.0)
        d_chance = jnp.einsum("hqd,khd->hqk", upstream, value_rows, preferred_element_type=f32)
        d_score = (chances * (d_chance - delta[:, :, None])).astype(bf16)
        carried = carried + jnp.einsum(
            "hqk,khd->hqd", d_score, key_rows, preferred_element_type=f32
        )
        d_key = jnp.einsum("hqk,hqd->khd", d_score, queries, preferred_element_type=f32) * 0.125
        d_value = jnp.einsum(
            "hqk,hqd->khd", chances.astype(bf16), upstream, preferred_element_type=f32
        )
        size = key_rows.shape[0]
        return carried, jnp.concatenate(
            [d_key.reshape(size, GROUP_DIM), d_value.reshape(size, GROUP_DIM)], axis=1
        ).astype(bf16)

    start = jnp.zeros(queries.shape, f32)
    d_query, d_pair = lax.scan(step, start, (keys, values, all_codes))
    return d_query * 0.125, d_pair


def shards(count, copies, *arrays):
    (
        tokens,
        segments,
        padding,
        query_weight,
        key_weight,
        value_weight,
        query_bias,
        value_bias,
        out_weight,
        out_bias,
        middle_gain,
        middle_shift,
        up_weight,
        up_bias,
        down_weight,
        down_bias,
        final_gain,
        final_shift,
        cotangent,
    ) = arrays
    planes = count // PLANE
    rows = query_weight.shape[0]
    block = down_weight.shape[0]
    x_own = tokens[0]
    here = x_own.shape[0]
    wide = PLANE * here
    me = lax.axis_index("shard")
    group = lax.rem(me, PLANE)
    qkv_send = jnp.concatenate(
        [
            item.astype(bf16).reshape(rows, PLANE, GROUP_DIM)
            for item in (query_weight, key_weight, value_weight)
        ],
        axis=2,
    ).transpose(1, 0, 2)
    up_send = (
        up_weight.astype(bf16)
        .reshape(rows, planes, PLANE, block)
        .transpose(2, 0, 1, 3)
        .reshape(PLANE, rows, GROUP_FF)
    )
    codes = (2 * segments[0] + padding[0]).astype(f32)
    lanes = 128 * ((max(here, block) + 127) // 128)

    def padded(value):
        return jnp.pad(value.astype(f32), (0, lanes - value.shape[0]))

    vectors = [
        query_bias,
        value_bias,
        out_bias,
        middle_gain,
        middle_shift,
        down_bias,
        final_gain,
        final_shift,
        up_bias,
        codes,
    ]
    small_send = jnp.pad(
        jnp.stack([padded(item) for item in vectors]), ((0, 6), (0, 0))
    ).astype(bf16)
    x_all, qkv_all, up_all, wo_all, small = gather_weights(
        count,
        copies,
        x_own,
        qkv_send,
        up_send,
        out_weight.astype(bf16),
        small_send,
        0,
    )
    x_plane = x_all.reshape(wide, D)
    w_qkv = qkv_all.reshape(D, 3 * GROUP_DIM)
    lines = [[start + PLANE * step for step in range(planes)] for start in range(PLANE)]
    strip = jnp.concatenate([up_all.reshape(PLANE * rows, D), down_weight.astype(bf16)], axis=0)
    w_out = wo_all.reshape(GROUP_DIM, D)
    small = small.astype(f32)
    spread = [small[:, index, :rows].reshape(D) for index in range(8)]
    b_query, b_value, b_out, gain_mid, shift_mid, b_down, gain_end, shift_end = spread
    b_up = lax.dynamic_index_in_dim(
        small[:, 8, :block].reshape(planes, PLANE, block), group, 1, keepdims=False
    ).reshape(GROUP_FF)
    all_codes = small[:, 9, :here].reshape(planes, wide)
    own_codes = lax.dynamic_index_in_dim(all_codes, lax.div(me, PLANE), 0, keepdims=False)

    def group_part(value):
        return lax.dynamic_slice(value, (group * GROUP_DIM,), (GROUP_DIM,))

    qkv_bias = jnp.concatenate(
        [group_part(b_query), jnp.zeros((GROUP_DIM,), f32), group_part(b_value)]
    )
    qkv = (dot(x_plane, w_qkv) + qkv_bias).astype(bf16)
    pairs = gather_planes(count, qkv[:, GROUP_DIM:], 1)
    strip, pairs = lax.optimization_barrier((strip, pairs))
    strips = lax.all_gather(strip, "shard", axis_index_groups=lines, axis=0)
    w_up = strips[:, : PLANE * rows].reshape(D, GROUP_FF)
    w_down = strips[:, PLANE * rows :].reshape(GROUP_FF, D)
    queries = heads_of(qkv[:, :GROUP_DIM])
    keys = pairs[:, :, :GROUP_DIM].reshape(planes, wide, GROUP_HEADS, HEAD_DIM)
    values = pairs[:, :, GROUP_DIM:].reshape(planes, wide, GROUP_HEADS, HEAD_DIM)
    context_heads, logs = attend_forward(queries, keys, values, own_codes, all_codes)
    context_low = flat_of(context_heads).astype(bf16)

    def split(value):
        return value.reshape(PLANE, here, D)

    branch = plane_sum(split(dot(context_low, w_out).astype(bf16)), 2) + b_out
    middle, normal_mid, scale_mid = norm_forward(x_own.astype(f32) + branch, gain_mid, shift_mid)
    middle_plane = plane_gather(middle.astype(bf16), 3).reshape(wide, D)
    hidden = dot(middle_plane, w_up) + b_up
    active_low = jax.nn.gelu(hidden, approximate=False).astype(bf16)
    feed = plane_sum(split(dot(active_low, w_down).astype(bf16)), 4) + b_down
    result, normal_end, scale_end = norm_forward(middle + feed, gain_end, shift_end)
    output = result.astype(bf16)[None]
    upstream = cotangent[0].astype(f32)
    d_second = norm_backward(upstream, normal_end, scale_end, gain_end)
    feed_low = d_second.astype(bf16)
    feed_plane = plane_gather(feed_low, 5).reshape(wide, D)
    grad_down = dot_left(active_low, feed_plane).astype(bf16)
    up_low = (dot_right(feed_plane, w_down) * gelu_slope(hidden)).astype(bf16)
    grad_up = dot_left(middle_plane, up_low).astype(bf16)
    strip_grads = lax.psum_scatter(
        jnp.concatenate(
            [
                grad_up.reshape(planes, PLANE * rows, GROUP_FF),
                grad_down.reshape(planes, block, D),
            ],
            axis=1,
        ),
        "shard",
        axis_index_groups=lines,
        scatter_dimension=0,
    )
    d_middle = plane_sum(split(dot_right(up_low, w_up).astype(bf16)), 6) + d_second
    d_first = norm_backward(d_middle, normal_mid, scale_mid, gain_mid)
    branch_low = d_first.astype(bf16)
    branch_plane = plane_gather(branch_low, 7).reshape(wide, D)
    grad_out = dot_left(context_low, branch_plane).astype(bf16)
    d_context = heads_of(dot_right(branch_plane, w_out).astype(bf16))
    delta = jnp.sum(d_context.astype(f32) * context_heads, axis=2)
    d_query, d_pair = attend_backward(
        queries, keys, values, own_codes, all_codes, logs, delta, d_context
    )
    pair_low = sum_planes(count, d_pair, 8)
    mixer_low = jnp.concatenate([flat_of(d_query).astype(bf16), pair_low], axis=1)
    grad_qkv = dot_left(x_plane, mixer_low).astype(bf16)
    grad_input = plane_sum(split(dot_right(mixer_low, w_qkv).astype(bf16)), 9)
    grad_tokens = (grad_input + d_first).astype(bf16)[None]
    mixer_sums = jnp.sum(mixer_low.astype(f32), axis=0)

    def from_group(value):
        return lax.dynamic_update_slice(jnp.zeros((D,), f32), value, (group * GROUP_DIM,))

    sums = [
        from_group(mixer_sums[:GROUP_DIM]),
        from_group(mixer_sums[2 * GROUP_DIM :]),
        jnp.sum(branch_low.astype(f32), axis=0),
        jnp.sum(d_middle * normal_mid, axis=0),
        jnp.sum(d_middle, axis=0),
        jnp.sum(feed_low.astype(f32), axis=0),
        jnp.sum(upstream * normal_end, axis=0),
        jnp.sum(upstream, axis=0),
    ]
    own_lane = (jnp.arange(PLANE) == group).astype(f32)
    up_sums = jnp.sum(up_low.astype(f32), axis=0).reshape(planes, 1, block)
    up_sums = (up_sums * own_lane[None, :, None]).reshape(count, 1, block)
    sums = jnp.stack([item.reshape(count, rows) for item in sums], axis=1)
    small_grads = jnp.concatenate(
        [
            jnp.pad(sums, ((0, 0), (0, 0), (0, lanes - rows))),
            jnp.pad(up_sums, ((0, 0), (0, 7), (0, lanes - block))),
        ],
        axis=1,
    ).astype(bf16)
    qkv_total, up_total, out_total, small_total, down_total = reduce_grads(
        count,
        copies,
        grad_qkv.reshape(count, rows, 3 * GROUP_DIM),
        strip_grads[: PLANE * rows].reshape(PLANE, rows, GROUP_FF),
        grad_out.reshape(planes, rows, D),
        strip_grads[PLANE * rows :],
        small_grads,
        10,
    )

    def joined(value):
        return value.transpose(1, 0, 2).reshape(rows, D)

    up_grad = (
        up_total.reshape(PLANE, rows, planes, block).transpose(1, 2, 0, 3).reshape(rows, FF)
    )
    return (
        output,
        grad_tokens,
        joined(qkv_total[:, :, :GROUP_DIM]),
        joined(qkv_total[:, :, GROUP_DIM : 2 * GROUP_DIM]),
        joined(qkv_total[:, :, 2 * GROUP_DIM :]),
        small_total[0, :rows],
        small_total[1, :rows],
        out_total,
        small_total[2, :rows],
        small_total[3, :rows],
        small_total[4, :rows],
        up_grad,
        small_total[8, :block],
        down_total,
        small_total[5, :rows],
        small_total[6, :rows],
        small_total[7, :rows],
    )


def solution(mesh):
    sheet, line = P("shard", None), P("shard")
    batch = P("rep", "shard", None)
    in_specs = (batch, P("rep", "shard"), P("rep", "shard"), sheet, sheet, sheet, line, line)
    in_specs += (sheet, line, line, line, sheet, line, sheet, line, line, line, batch)
    out_specs = (batch, batch, sheet, sheet, sheet, line, line, sheet, line, line, line)
    out_specs += (sheet, line, sheet, line, line, line)
    body = functools.partial(shards, mesh.shape["shard"], mesh.shape["rep"])
    return jax.shard_map(
        body, mesh=mesh, in_specs=in_specs, out_specs=out_specs, check_vma=False
    )
```

```python
import functools

import jax
import jax.numpy as jnp
from jax import lax
from jax.experimental import pallas as pl
from jax.experimental.pallas import tpu as pltpu
from jax.sharding import PartitionSpec as P

D = 768
HEADS = 12
HEAD_DIM = 64
PLANE = 4
GROUP_HEADS = HEADS // PLANE
GROUP_DIM = GROUP_HEADS * HEAD_DIM
FF = 3072
GROUP_FF = FF // PLANE

epsilon = 1e-12
very_low = -1e30
root_half = 0.7071067811865476
inv_root_tau = 0.3989422804014327
bf16 = jnp.bfloat16
f32 = jnp.float32
MESH = pl.DeviceIdType.MESH
VMEM_SPEC = pl.BlockSpec(memory_space=pltpu.VMEM)
ANY_SPEC = pl.BlockSpec(memory_space=pl.ANY)
VMEM_BYTES = 60000 * 1024
MODEL_BYTES = 100_000_000


def struct(shape, dtype=bf16):
    return jax.ShapeDtypeStruct(shape, dtype)


def comm_call(body, name, ident, inputs, out_shapes, out_specs, scratch):
    return pl.pallas_call(
        body,
        name=name,
        out_shape=out_shapes,
        in_specs=[VMEM_SPEC] * len(inputs),
        out_specs=out_specs,
        scratch_shapes=scratch,
        cost_estimate=pl.CostEstimate(flops=0, bytes_accessed=MODEL_BYTES, transcendentals=0),
        compiler_params=pltpu.CompilerParams(
            collective_id=ident, has_side_effects=True, vmem_limit_bytes=VMEM_BYTES
        ),
    )(*inputs)


def greet(peers):
    barrier = pltpu.get_barrier_semaphore()
    for peer in peers:
        pl.semaphore_signal(barrier, inc=1, device_id=peer, device_id_type=MESH)
    pl.semaphore_wait(barrier, len(peers))


def remote(src, dst, send_sem, recv_sem, peer):
    return pltpu.make_async_remote_copy(
        src_ref=src,
        dst_ref=dst,
        send_sem=send_sem,
        recv_sem=recv_sem,
        device_id=peer,
        device_id_type=MESH,
    )


def plane_peer(me, mask):
    group = lax.rem(me, PLANE)
    core = lax.rem(group, 2)
    column = lax.div(group, 2)
    if mask & 1:
        core = 1 - core
    if mask & 2:
        column = 1 - column
    return me - group + 2 * column + core


def plane_slot(me, mask):
    return lax.rem(plane_peer(me, mask), PLANE)


def plane_step(parts, pieces, vectors, action, out_types, ident):
    _, rows, cols = parts.shape
    chunks = 3 if rows % 48 == 0 else 1
    size = rows // chunks
    many, few = len(pieces), len(out_types)

    def body(p_ref, *rest):
        piece_refs, vector_ref = rest[:many], rest[many]
        all_ref, sums_ref = rest[many + 1 : many + 3]
        out_refs = rest[many + 3 : many + 3 + few]
        near, held, far_in, low, send, recv = rest[many + 3 + few :]
        me = lax.axis_index("shard")
        beside, across = [{"shard": plane_peer(me, mask)} for mask in (1, 2)]
        mine, far = lax.rem(me, PLANE), plane_slot(me, 2)
        greet([beside, across])
        spans = [pl.ds(size * index, size) for index in range(chunks)]

        def copy(kind, index):
            span = spans[index]
            table = {
                0: lambda: (p_ref.at[plane_slot(me, 3), span], near.at[0, span], beside),
                1: lambda: (p_ref.at[plane_slot(me, 1), span], near.at[1, span], beside),
                2: lambda: (held.at[span], far_in.at[span], across),
                3: lambda: (low.at[span], all_ref.at[mine, span], across),
                4: lambda: (low.at[span], all_ref.at[mine, span], beside),
                5: lambda: (all_ref.at[far, span], all_ref.at[far, span], beside),
            }
            src, dst, peer = table[kind]()
            return remote(src, dst, send.at[kind, index], recv.at[kind, index], peer)

        for index in range(chunks):
            copy(0, index).start()
        for index in range(chunks):
            copy(1, index).start()
        for index in range(chunks):
            span = spans[index]
            copy(0, index).wait_recv()
            total = p_ref[plane_slot(me, 2), span].astype(f32) + near[0, span].astype(f32)
            held[span] = total.astype(bf16)
            copy(2, index).start()
        lines = [vector_ref[index : index + 1] for index in range(len(vectors))]
        sums = None
        for index in range(chunks):
            span = spans[index]
            copy(1, index).wait_recv()
            copy(2, index).wait_recv()
            total = p_ref[mine, span].astype(f32) + near[1, span].astype(f32)
            total = total + far_in[span].astype(f32)
            result, outs, terms = action(
                total, [item[span].astype(f32) for item in piece_refs], lines
            )
            low[span] = result
            copy(3, index).start()
            copy(4, index).start()
            for ref, value in zip(out_refs, outs):
                ref[span] = value.astype(ref.dtype)
            all_ref[mine, span] = result
            terms = [jnp.sum(item, axis=0, keepdims=True) for item in terms]
            sums = terms if sums is None else [x + y for x, y in zip(sums, terms)]
        sums_ref[...] = jnp.zeros(sums_ref.shape, f32)
        for place, value in enumerate(sums):
            sums_ref[place : place + 1] = value
        for index in range(chunks):
            copy(3, index).wait_recv()
            copy(5, index).start()
        for index in range(chunks):
            copy(4, index).wait_recv()
            copy(5, index).wait_recv()
        for index in range(chunks):
            for kind in range(6):
                copy(kind, index).wait_send()

    stack = jnp.stack(vectors)
    shape = (rows, cols)
    return comm_call(
        body,
        "plane_step",
        ident,
        [parts] + list(pieces) + [stack],
        [struct((PLANE, rows, cols)), struct((8, cols), f32)]
        + [struct(shape, item) for item in out_types],
        [VMEM_SPEC] * (2 + few),
        [
            pltpu.VMEM((2, rows, cols), bf16),
            pltpu.VMEM(shape, bf16),
            pltpu.VMEM(shape, bf16),
            pltpu.VMEM(shape, bf16),
            pltpu.SemaphoreType.DMA((6, chunks)),
            pltpu.SemaphoreType.DMA((6, chunks)),
        ],
    )


def others(me, count):
    return [{"shard": lax.rem(me + step, count)} for step in range(1, count)]


def gather_weights(count, copies, tokens, qkv, up, out_w, small, ident):
    planes = count // PLANE
    rows = qkv.shape[1]

    def body(x_ref, qkv_ref, up_ref, wo_ref, small_ref, *rest):
        x_out, qkv_out, up_out, wo_out, small_out = rest[:5]
        send, recv, local, send_wo, recv_wo, send_unit, recv_unit = rest[5:]
        me = lax.axis_index("shard")
        group, plane = lax.rem(me, PLANE), lax.div(me, PLANE)
        across = [
            {"rep": lax.rem(lax.axis_index("rep") + step, copies)} for step in range(1, copies)
        ]
        greet(others(me, count) + across)
        owns = [
            (x_ref, x_out.at[group]),
            (qkv_ref.at[group], qkv_out.at[me]),
            (up_ref.at[group], up_out.at[group]),
            (small_ref, small_out.at[me]),
        ]
        started = []
        for index, (src, dst) in enumerate(owns):
            copy = pltpu.make_async_copy(src, dst, local.at[index])
            copy.start()
            started.append(copy)
        sent = []

        def push(src, dst, peer):
            index = len(sent)
            copy = remote(src, dst, send.at[index], recv.at[index], {"shard": peer})
            copy.start()
            sent.append(copy)

        for mask in (2, 1):
            push(x_ref, x_out.at[group], plane_peer(me, mask))
        far = plane_slot(me, 2)
        x_relay = remote(
            x_out.at[far], x_out.at[far], send.at[2], recv.at[2], {"shard": plane_peer(me, 1)}
        )
        sent.append(x_relay)
        for step in range(1, count):
            push(small_ref, small_out.at[me], lax.rem(me + step, count))
        rep = lax.axis_index("rep")
        split = copies == 2
        units = []
        for step in range(planes):
            for lane in range(PLANE):
                if step or lane:
                    units.append((qkv_ref, qkv_out, step, lane))
        for lane in range(1, PLANE):
            units.append((up_ref, up_out, 0, lane))

        def unit_copy(index):
            src, dst, step, lane = units[index]
            goal = lax.rem(plane + step, planes)
            goal_group = lax.rem(group + lane, PLANE)
            slot = group if src is up_ref else me
            return remote(
                src.at[goal_group],
                dst.at[slot],
                send_unit.at[index],
                recv_unit.at[index],
                {"shard": goal * PLANE + goal_group},
            )

        def unit_relay(index):
            src, dst, step, lane = units[index]
            origin = lax.rem(plane + planes - step, planes)
            origin_group = lax.rem(group + PLANE - lane, PLANE)
            slot = origin_group if src is up_ref else origin * PLANE + origin_group
            return remote(
                dst.at[slot],
                dst.at[slot],
                send_unit.at[index],
                recv_unit.at[index],
                {"rep": lax.rem(rep + 1, copies)},
            )

        def carried(index, mine):
            step = units[index][2]
            if not split or step == 0:
                return None
            return (rep == step % 2) if mine else (rep != step % 2)

        def guarded(test, action):
            if test is None:
                action()
            else:
                pl.when(test)(action)

        for index in range(len(units)):
            guarded(carried(index, True), unit_copy(index).start)
        target, place = lax.div(me, planes), lax.rem(me, planes)

        def wo_copy(source, index):
            peer = PLANE * index + target
            return peer, remote(
                wo_ref, wo_out.at[place], send_wo.at[index], recv_wo.at[source], {"shard": peer}
            )

        for index in range(planes):
            peer, copy = wo_copy(place, index)
            pl.when(peer != me)(copy.start)
        keep = pltpu.make_async_copy(wo_ref, wo_out.at[place], local.at[5])
        pl.when(target == group)(keep.start)
        sent[0].wait_recv()
        x_relay.start()
        for index, (_, _, step, _) in enumerate(units):
            if split and step:

                @pl.when(rep == step % 2)
                def _(index=index):
                    unit_relay(index).wait_recv()
                    unit_copy(index).wait_send()
                    unit_relay(index).start()

            else:
                unit_copy(index).wait_recv()
                unit_copy(index).wait_send()
        for index, (_, _, step, _) in enumerate(units):
            if split and step:
                pl.when(rep != step % 2)(unit_relay(index).wait_recv)
                pl.when(rep == step % 2)(unit_relay(index).wait_send)
        for copy in sent[1:]:
            copy.wait_recv()
        for index in range(planes):
            pl.when(group * planes + index != me)(wo_copy(index, index)[1].wait_recv)
        for index in range(planes):
            peer, copy = wo_copy(place, index)
            pl.when(peer != me)(copy.wait_send)
        pl.when(target == group)(keep.wait)
        for copy in sent:
            copy.wait_send()
        for copy in started:
            copy.wait()

    total = 3 + count - 1
    number = count - 1 + PLANE - 1
    return comm_call(
        body,
        "gather_weights",
        ident,
        [tokens, qkv, up, out_w, small],
        [
            struct((PLANE,) + tokens.shape),
            struct((count, rows, qkv.shape[2])),
            struct((PLANE, rows, up.shape[2])),
            struct((planes,) + out_w.shape),
            struct((count,) + small.shape),
        ],
        [ANY_SPEC] * 5,
        [
            pltpu.SemaphoreType.DMA((total,)),
            pltpu.SemaphoreType.DMA((total,)),
            pltpu.SemaphoreType.DMA((6,)),
            pltpu.SemaphoreType.DMA((planes,)),
            pltpu.SemaphoreType.DMA((planes,)),
            pltpu.SemaphoreType.DMA((number,)),
            pltpu.SemaphoreType.DMA((number,)),
        ],
    )


def gather_planes(count, value, ident):
    planes = count // PLANE

    def body(x_ref, out_ref, send, recv, local):
        me = lax.axis_index("shard")
        plane = lax.div(me, PLANE)
        greet([{"shard": lax.rem(me + PLANE * s, count)} for s in range(1, planes)])
        own = pltpu.make_async_copy(x_ref, out_ref.at[plane], local)
        own.start()

        def hop(way, source, src):
            peer = me + PLANE if way == 0 else me - PLANE
            return remote(
                src,
                out_ref.at[source],
                send.at[way, source],
                recv.at[way, source],
                {"shard": lax.rem(peer + count, count)},
            )

        @pl.when(plane < planes - 1)
        def _():
            hop(0, plane, x_ref).start()

        @pl.when(plane > 0)
        def _():
            hop(1, plane, x_ref).start()

        for step in range(1, planes):
            for way, source in ((0, plane - step), (1, plane + step)):
                onward = plane < planes - 1 if way == 0 else plane > 0

                @pl.when((source >= 0) & (source < planes))
                def _(way=way, source=source, onward=onward):
                    copy = hop(way, source, out_ref.at[source])
                    copy.wait_recv()
                    pl.when(onward)(copy.start)

        @pl.when(plane < planes - 1)
        def _():
            hop(0, plane, x_ref).wait_send()

        @pl.when(plane > 0)
        def _():
            hop(1, plane, x_ref).wait_send()

        for step in range(1, planes):
            for way, source in ((0, plane - step), (1, plane + step)):
                onward = plane < planes - 1 if way == 0 else plane > 0

                @pl.when((source >= 0) & (source < planes) & onward)
                def _(way=way, source=source):
                    hop(way, source, out_ref.at[source]).wait_send()

        own.wait()

    return comm_call(
        body,
        "gather_planes",
        ident,
        [value],
        struct((planes,) + value.shape),
        ANY_SPEC,
        [
            pltpu.SemaphoreType.DMA((2, planes)),
            pltpu.SemaphoreType.DMA((2, planes)),
            pltpu.SemaphoreType.DMA,
        ],
    )


def sum_planes(count, parts, ident):
    planes, rows, cols = parts.shape

    def body(p_ref, out_ref, held, staged, send, recv):
        me = lax.axis_index("shard")
        plane = lax.div(me, PLANE)
        greet([{"shard": lax.rem(me + PLANE * s, count)} for s in range(1, planes)])

        def hop(way, goal, src):
            peer = me + PLANE if way == 0 else me - PLANE
            return remote(
                src,
                held.at[way, goal],
                send.at[goal],
                recv.at[way, goal],
                {"shard": lax.rem(peer + count, count)},
            )

        for step in range(planes - 1):
            for way, goal in ((0, planes - 1 - step), (1, step)):
                ahead = goal > plane if way == 0 else goal < plane
                first = plane == 0 if way == 0 else plane == planes - 1

                @pl.when(ahead & first)
                def _(way=way, goal=goal):
                    hop(way, goal, p_ref.at[goal]).start()

                @pl.when(ahead & jnp.logical_not(first))
                def _(way=way, goal=goal):
                    copy = hop(way, goal, staged.at[goal])
                    copy.wait_recv()
                    total = p_ref[goal].astype(f32) + held[way, goal].astype(f32)
                    staged[goal] = total.astype(bf16)
                    copy.start()

        out_ref[...] = p_ref[plane]

        @pl.when(plane > 0)
        def _():
            hop(0, plane, staged.at[plane]).wait_recv()
            out_ref[...] = (out_ref[...].astype(f32) + held[0, plane].astype(f32)).astype(bf16)

        @pl.when(plane < planes - 1)
        def _():
            hop(1, plane, staged.at[plane]).wait_recv()
            out_ref[...] = (out_ref[...].astype(f32) + held[1, plane].astype(f32)).astype(bf16)

        for goal in range(planes):

            @pl.when(goal != plane)
            def _(goal=goal):
                hop(0, goal, staged.at[goal]).wait_send()

    return comm_call(
        body,
        "sum_planes",
        ident,
        [parts],
        struct((rows, cols)),
        VMEM_SPEC,
        [
            pltpu.VMEM((2, planes, rows, cols), bf16),
            pltpu.VMEM((planes, rows, cols), bf16),
            pltpu.SemaphoreType.DMA((planes,)),
            pltpu.SemaphoreType.DMA((2, planes)),
        ],
    )


def reduce_grads(count, copies, qkv, up, out_w, down, small, parts, first_grad, ident):
    planes = count // PLANE
    rows = qkv.shape[1]
    block = down.shape[0]
    arrays = [qkv, up, out_w, small]

    def body(qkv_ref, up_ref, wo_ref, small_ref, down_ref, p_ref, first_ref, *rest):
        outs, token_ref, rest = rest[:5], rest[5], rest[6:]
        qkv_in, up_in, wo_in, small_in = rest[:4]
        halves, gets = [rest[4], up_in, rest[5], rest[6], down_ref], rest[7:12]
        near, near_sum, far_in = rest[12:15]
        send, recv, send_rep, recv_rep, send_wo, recv_wo, send_near, recv_near = rest[15:]
        me = lax.axis_index("shard")
        rep = lax.axis_index("rep")
        plane = lax.div(me, PLANE)
        across = [{"rep": lax.rem(rep + step, copies)} for step in range(1, copies)]
        greet(others(me, count) + across)
        sent = []

        def push(src, dst, peer):
            index = len(sent)
            copy = remote(src, dst, send.at[index], recv.at[index], {"shard": peer})
            copy.start()
            sent.append(copy)

        pairs = [(qkv_ref, qkv_in), (small_ref, small_in)]
        passed = []
        beside, over = [{"shard": plane_peer(me, mask)} for mask in (1, 2)]
        near_copies = [
            remote(p_ref.at[plane_slot(me, 3)], near.at[0], send_near.at[0], recv_near.at[0], beside),
            remote(p_ref.at[plane_slot(me, 1)], near.at[1], send_near.at[1], recv_near.at[1], beside),
            remote(near_sum, far_in, send_near.at[2], recv_near.at[2], over),
        ]
        near_copies[0].start()
        near_copies[1].start()

        def exchange(*places):
            for index, peer in enumerate(across):
                for place in places:
                    copy = remote(
                        halves[place],
                        gets[place].at[index],
                        send_rep.at[5 * index + place],
                        recv_rep.at[5 * index + place],
                        peer,
                    )
                    copy.start()
                    passed.append(copy)

        exchange(4)
        group = lax.rem(me, PLANE)
        target, place = lax.div(me, planes), lax.rem(me, planes)
        for lane in range(1, PLANE):
            goal = lax.rem(group + lane, PLANE)
            push(up_ref.at[goal], up_in.at[group], plane * PLANE + goal)
        up_in[group] = up_ref[group]
        for src, held in pairs:
            for step in range(1, count):
                peer = lax.rem(me + step, count)
                push(src.at[peer], held.at[me], peer)
        for src, held in pairs:
            held[me] = src[me]

        def wo_copy(source, index):
            peer = group * planes + index
            return peer, remote(
                wo_ref.at[index],
                wo_in.at[plane],
                send_wo.at[index],
                recv_wo.at[source],
                {"shard": peer},
            )

        for index in range(planes):
            peer, copy = wo_copy(plane, index)
            pl.when(peer != me)(copy.start)

        @pl.when(target == group)
        def _():
            wo_in[plane] = wo_ref[place]

        near_copies[0].wait_recv()
        total = p_ref[plane_slot(me, 2)].astype(f32) + near[0].astype(f32)
        near_sum[...] = total.astype(bf16)
        near_copies[2].start()
        for copy in sent[: PLANE - 1]:
            copy.wait_recv()
        exchange(1)
        for index in range(planes):
            pl.when(PLANE * index + target != me)(wo_copy(index, index)[1].wait_recv)
        for index in range(planes):
            peer, copy = wo_copy(plane, index)
            pl.when(peer != me)(copy.wait_send)
        total = wo_in[0].astype(f32)
        for other in range(1, planes):
            total = total + wo_in[other].astype(f32)
        halves[2][...] = total.astype(bf16)
        exchange(2)
        near_copies[1].wait_recv()
        near_copies[2].wait_recv()
        total = p_ref[lax.rem(me, PLANE)].astype(f32) + near[1].astype(f32)
        total = total + far_in[...].astype(f32) + first_ref[...]
        token_ref[...] = total.astype(bf16)
        for copy in sent[PLANE - 1 :]:
            copy.wait_recv()
        for half, held in zip(halves[:1], (qkv_in,)):
            for lane in range(PLANE):
                total = held[lane].astype(f32)
                for other in range(1, planes):
                    total = total + held[other * PLANE + lane].astype(f32)
                half[lane] = total.astype(bf16)
        for half, held, number in (
            (halves[3], small_in, count),
        ):
            total = held[0].astype(f32)
            for other in range(1, number):
                total = total + held[other].astype(f32)
            half[...] = total.astype(bf16)
        exchange(0, 3)
        for copy in passed:
            copy.wait_recv()
        for out, half, got in zip(outs, halves, gets):
            total = half[...].astype(f32)
            for index in range(copies - 1):
                total = total + got[index].astype(f32)
            out[...] = total
        for copy in sent + passed + near_copies:
            copy.wait_send()

    totals = 2 * (count - 1) + PLANE - 1
    shapes = [
        (PLANE, rows, qkv.shape[2]),
        (PLANE, rows, up.shape[2]),
        (rows, D),
        small.shape[1:],
        (block, D),
    ]
    return comm_call(
        body,
        "reduce_grads",
        ident,
        arrays + [down, parts, first_grad],
        [struct(shape, f32) for shape in shapes] + [struct(parts.shape[1:])],
        [VMEM_SPEC] * 6,
        [pltpu.VMEM(item.shape, bf16) for item in arrays]
        + [pltpu.VMEM(shapes[index], bf16) for index in (0, 2, 3)]
        + [pltpu.VMEM((copies - 1,) + shape, bf16) for shape in shapes]
        + [
            pltpu.VMEM((2,) + parts.shape[1:], bf16),
            pltpu.VMEM(parts.shape[1:], bf16),
            pltpu.VMEM(parts.shape[1:], bf16),
            pltpu.SemaphoreType.DMA((totals,)),
            pltpu.SemaphoreType.DMA((totals,)),
            pltpu.SemaphoreType.DMA((5 * (copies - 1),)),
            pltpu.SemaphoreType.DMA((5 * (copies - 1),)),
            pltpu.SemaphoreType.DMA((planes,)),
            pltpu.SemaphoreType.DMA((planes,)),
            pltpu.SemaphoreType.DMA((3,)),
            pltpu.SemaphoreType.DMA((3,)),
        ],
    )


def norm_forward(value, gain, shift):
    center = value - jnp.mean(value, axis=-1, keepdims=True)
    spread = jnp.mean(center * center, axis=-1, keepdims=True)
    scale = lax.rsqrt(spread + epsilon)
    normal = center * scale
    return (normal * gain + shift, normal, scale)


def norm_backward(upstream, normal, scale, gain):
    inner = upstream * gain
    return scale * (
        inner
        - jnp.mean(inner, axis=-1, keepdims=True)
        - normal * jnp.mean(inner * normal, axis=-1, keepdims=True)
    )


def gelu_slope(hidden):
    return 0.5 * (1.0 + lax.erf(hidden * root_half)) + hidden * inv_root_tau * jnp.exp(
        -0.5 * hidden * hidden
    )


def dot(left, right):
    return jnp.dot(left, right, preferred_element_type=f32)


def dot_left(left, right):
    return lax.dot_general(left, right, (((0,), (0,)), ((), ())), preferred_element_type=f32)


def dot_right(left, right):
    return lax.dot_general(left, right, (((1,), (1,)), ((), ())), preferred_element_type=f32)


def heads_of(value):
    return value.reshape(value.shape[0], GROUP_HEADS, HEAD_DIM).transpose(1, 0, 2)


def flat_of(value):
    return value.transpose(1, 0, 2).reshape(value.shape[1], GROUP_DIM)


def attend_forward(queries, keys, values, own_codes, all_codes):
    def step(carried, pieces):
        top, total, summed = carried
        key_rows, value_rows, key_codes = pieces
        raw = jnp.einsum("hqd,khd->hqk", queries, key_rows, preferred_element_type=f32) * 0.125
        allowed = (own_codes[:, None] == key_codes[None, :])[None]
        masked = jnp.where(allowed, raw, very_low)
        new_top = jnp.maximum(top, jnp.max(masked, axis=2))
        rescale = jnp.exp(top - new_top)
        weights = jnp.where(allowed, jnp.exp(masked - new_top[:, :, None]), 0.0)
        added = jnp.einsum(
            "hqk,khd->hqd", weights.astype(bf16), value_rows, preferred_element_type=f32
        )
        return (
            new_top,
            total * rescale + jnp.sum(weights, axis=2),
            summed * rescale[:, :, None] + added,
        ), None

    rows = queries.shape[1]
    start = (
        jnp.full((GROUP_HEADS, rows), very_low, f32),
        jnp.zeros((GROUP_HEADS, rows), f32),
        jnp.zeros((GROUP_HEADS, rows, HEAD_DIM), f32),
    )
    (top, total, summed), _ = lax.scan(step, start, (keys, values, all_codes))
    return summed / total[:, :, None], top + jnp.log(total)


def attend_backward(queries, keys, values, own_codes, all_codes, logs, delta, upstream):
    def step(carried, pieces):
        key_rows, value_rows, key_codes = pieces
        raw = jnp.einsum("hqd,khd->hqk", queries, key_rows, preferred_element_type=f32) * 0.125
        allowed = (own_codes[:, None] == key_codes[None, :])[None]
        chances = jnp.where(allowed, jnp.exp(raw - logs[:, :, None]), 0.0)
        d_chance = jnp.einsum("hqd,khd->hqk", upstream, value_rows, preferred_element_type=f32)
        d_score = (chances * (d_chance - delta[:, :, None])).astype(bf16)
        carried = carried + jnp.einsum(
            "hqk,khd->hqd", d_score, key_rows, preferred_element_type=f32
        )
        d_key = jnp.einsum("hqk,hqd->khd", d_score, queries, preferred_element_type=f32) * 0.125
        d_value = jnp.einsum(
            "hqk,hqd->khd", chances.astype(bf16), upstream, preferred_element_type=f32
        )
        size = key_rows.shape[0]
        return carried, jnp.concatenate(
            [d_key.reshape(size, GROUP_DIM), d_value.reshape(size, GROUP_DIM)], axis=1
        ).astype(bf16)

    start = jnp.zeros(queries.shape, f32)
    d_query, d_pair = lax.scan(step, start, (keys, values, all_codes))
    return d_query * 0.125, d_pair


def shards(count, copies, *arrays):
    (
        tokens,
        segments,
        padding,
        query_weight,
        key_weight,
        value_weight,
        query_bias,
        value_bias,
        out_weight,
        out_bias,
        middle_gain,
        middle_shift,
        up_weight,
        up_bias,
        down_weight,
        down_bias,
        final_gain,
        final_shift,
        cotangent,
    ) = arrays
    planes = count // PLANE
    rows = query_weight.shape[0]
    block = down_weight.shape[0]
    x_own = tokens[0]
    here = x_own.shape[0]
    wide = PLANE * here
    me = lax.axis_index("shard")
    group = lax.rem(me, PLANE)
    qkv_send = jnp.concatenate(
        [
            item.astype(bf16).reshape(rows, PLANE, GROUP_DIM)
            for item in (query_weight, key_weight, value_weight)
        ],
        axis=2,
    ).transpose(1, 0, 2)
    up_send = (
        up_weight.astype(bf16)
        .reshape(rows, planes, PLANE, block)
        .transpose(2, 0, 1, 3)
        .reshape(PLANE, rows, GROUP_FF)
    )
    codes = (2 * segments[0] + padding[0]).astype(f32)
    lanes = 128 * ((max(here, block) + 127) // 128)

    def padded(value):
        return jnp.pad(value.astype(f32), (0, lanes - value.shape[0]))

    vectors = [
        query_bias,
        value_bias,
        out_bias,
        middle_gain,
        middle_shift,
        down_bias,
        final_gain,
        final_shift,
        up_bias,
        codes,
    ]
    small_send = jnp.pad(
        jnp.stack([padded(item) for item in vectors]), ((0, 6), (0, 0))
    ).astype(bf16)
    x_all, qkv_all, up_all, wo_all, small = gather_weights(
        count,
        copies,
        x_own,
        qkv_send,
        up_send,
        out_weight.astype(bf16),
        small_send,
        0,
    )
    x_plane = x_all.reshape(wide, D)
    w_qkv = qkv_all.reshape(D, 3 * GROUP_DIM)
    lines = [[start + PLANE * step for step in range(planes)] for start in range(PLANE)]
    strip = jnp.concatenate([up_all.reshape(PLANE * rows, D), down_weight.astype(bf16)], axis=0)
    w_out = wo_all.reshape(GROUP_DIM, D)
    small = small.astype(f32)
    spread = [small[:, index, :rows].reshape(D) for index in range(8)]
    b_query, b_value, b_out, gain_mid, shift_mid, b_down, gain_end, shift_end = spread
    b_up = lax.dynamic_index_in_dim(
        small[:, 8, :block].reshape(planes, PLANE, block), group, 1, keepdims=False
    ).reshape(GROUP_FF)
    all_codes = small[:, 9, :here].reshape(planes, wide)
    own_codes = lax.dynamic_index_in_dim(all_codes, lax.div(me, PLANE), 0, keepdims=False)

    def group_part(value):
        return lax.dynamic_slice(value, (group * GROUP_DIM,), (GROUP_DIM,))

    qkv_bias = jnp.concatenate(
        [group_part(b_query), jnp.zeros((GROUP_DIM,), f32), group_part(b_value)]
    )
    qkv = (dot(x_plane, w_qkv) + qkv_bias).astype(bf16)
    pairs = gather_planes(count, qkv[:, GROUP_DIM:], 1)
    strip, pairs = lax.optimization_barrier((strip, pairs))
    strips = lax.all_gather(strip, "shard", axis_index_groups=lines, axis=0)
    w_up = strips[:, : PLANE * rows].reshape(D, GROUP_FF)
    w_down = strips[:, PLANE * rows :].reshape(GROUP_FF, D)
    queries = heads_of(qkv[:, :GROUP_DIM])
    keys = pairs[:, :, :GROUP_DIM].reshape(planes, wide, GROUP_HEADS, HEAD_DIM)
    values = pairs[:, :, GROUP_DIM:].reshape(planes, wide, GROUP_HEADS, HEAD_DIM)
    context_heads, logs = attend_forward(queries, keys, values, own_codes, all_codes)
    context_low = flat_of(context_heads).astype(bf16)

    def split(value):
        return value.reshape(PLANE, here, D)

    def enter_middle(total, pieces, lines):
        rest = total + lines[0] + pieces[0]
        middle, _, _ = norm_forward(rest, lines[1], lines[2])
        return middle.astype(bf16), [rest], []

    def enter_end(total, pieces, lines):
        middle, _, _ = norm_forward(pieces[0], lines[1], lines[2])
        result, normal, scale = norm_forward(middle + (total + lines[0]), lines[3], lines[4])
        above = pieces[1]
        back = norm_backward(above, normal, scale, lines[3])
        rounded = back.astype(bf16)
        return rounded, [result, back], [above * normal, above, rounded.astype(f32)]

    def leave_middle(total, pieces, lines):
        _, normal, scale = norm_forward(pieces[0], lines[0], lines[0])
        above = total + pieces[1]
        back = norm_backward(above, normal, scale, lines[0])
        rounded = back.astype(bf16)
        return rounded, [back], [above * normal, above, rounded.astype(f32)]

    middle_all, _, rest = plane_step(
        split(dot(context_low, w_out).astype(bf16)),
        [x_own],
        [b_out, gain_mid, shift_mid],
        enter_middle,
        [f32],
        2,
    )
    middle_plane = middle_all.reshape(wide, D)
    hidden = dot(middle_plane, w_up) + b_up
    active_low = jax.nn.gelu(hidden, approximate=False).astype(bf16)
    feed_all, end_sums, result, d_second = plane_step(
        split(dot(active_low, w_down).astype(bf16)),
        [rest, cotangent[0]],
        [b_down, gain_mid, shift_mid, gain_end, shift_end],
        enter_end,
        [bf16, f32],
        3,
    )
    output = result[None]
    feed_plane = feed_all.reshape(wide, D)
    grad_down = dot_left(active_low, feed_plane).astype(bf16)
    up_low = (dot_right(feed_plane, w_down) * gelu_slope(hidden)).astype(bf16)
    grad_up = dot_left(middle_plane, up_low).astype(bf16)
    strip_grads = lax.psum_scatter(
        jnp.concatenate(
            [
                grad_up.reshape(planes, PLANE * rows, GROUP_FF),
                grad_down.reshape(planes, block, D),
            ],
            axis=1,
        ),
        "shard",
        axis_index_groups=lines,
        scatter_dimension=0,
    )
    branch_all, middle_sums, d_first = plane_step(
        split(dot_right(up_low, w_up).astype(bf16)),
        [rest, d_second],
        [gain_mid],
        leave_middle,
        [f32],
        4,
    )
    branch_plane = branch_all.reshape(wide, D)
    grad_out = dot_left(context_low, branch_plane).astype(bf16)
    d_context = heads_of(dot_right(branch_plane, w_out).astype(bf16))
    delta = jnp.sum(d_context.astype(f32) * context_heads, axis=2)
    d_query, d_pair = attend_backward(
        queries, keys, values, own_codes, all_codes, logs, delta, d_context
    )
    pair_low = sum_planes(count, d_pair, 8)
    mixer_low = jnp.concatenate([flat_of(d_query).astype(bf16), pair_low], axis=1)
    grad_qkv = dot_left(x_plane, mixer_low).astype(bf16)
    mixer_sums = jnp.sum(mixer_low.astype(f32), axis=0)

    def from_group(value):
        return lax.dynamic_update_slice(jnp.zeros((D,), f32), value, (group * GROUP_DIM,))

    sums = [
        from_group(mixer_sums[:GROUP_DIM]),
        from_group(mixer_sums[2 * GROUP_DIM :]),
        middle_sums[2],
        middle_sums[0],
        middle_sums[1],
        end_sums[2],
        end_sums[0],
        end_sums[1],
    ]
    own_lane = (jnp.arange(PLANE) == group).astype(f32)
    up_sums = jnp.sum(up_low.astype(f32), axis=0).reshape(planes, 1, block)
    up_sums = (up_sums * own_lane[None, :, None]).reshape(count, 1, block)
    sums = jnp.stack([item.reshape(count, rows) for item in sums], axis=1)
    small_grads = jnp.concatenate(
        [
            jnp.pad(sums, ((0, 0), (0, 0), (0, lanes - rows))),
            jnp.pad(up_sums, ((0, 0), (0, 7), (0, lanes - block))),
        ],
        axis=1,
    ).astype(bf16)
    qkv_total, up_total, out_total, small_total, down_total, grad_tokens = reduce_grads(
        count,
        copies,
        grad_qkv.reshape(count, rows, 3 * GROUP_DIM),
        strip_grads[: PLANE * rows].reshape(PLANE, rows, GROUP_FF),
        grad_out.reshape(planes, rows, D),
        strip_grads[PLANE * rows :],
        small_grads,
        split(dot_right(mixer_low, w_qkv).astype(bf16)),
        d_first,
        10,
    )

    def joined(value):
        return value.transpose(1, 0, 2).reshape(rows, D)

    up_grad = (
        up_total.reshape(PLANE, rows, planes, block).transpose(1, 2, 0, 3).reshape(rows, FF)
    )
    return (
        output,
        grad_tokens[None],
        joined(qkv_total[:, :, :GROUP_DIM]),
        joined(qkv_total[:, :, GROUP_DIM : 2 * GROUP_DIM]),
        joined(qkv_total[:, :, 2 * GROUP_DIM :]),
        small_total[0, :rows],
        small_total[1, :rows],
        out_total,
        small_total[2, :rows],
        small_total[3, :rows],
        small_total[4, :rows],
        up_grad,
        small_total[8, :block],
        down_total,
        small_total[5, :rows],
        small_total[6, :rows],
        small_total[7, :rows],
    )


def solution(mesh):
    sheet, line = P("shard", None), P("shard")
    batch = P("rep", "shard", None)
    in_specs = (batch, P("rep", "shard"), P("rep", "shard"), sheet, sheet, sheet, line, line)
    in_specs += (sheet, line, line, line, sheet, line, sheet, line, line, line, batch)
    out_specs = (batch, batch, sheet, sheet, sheet, line, line, sheet, line, line, line)
    out_specs += (sheet, line, sheet, line, line, line)
    body = functools.partial(shards, mesh.shape["shard"], mesh.shape["rep"])
    return jax.shard_map(
        body, mesh=mesh, in_specs=in_specs, out_specs=out_specs, check_vma=False
    )
```

```python
import functools

import jax
import jax.numpy as jnp
from jax import lax
from jax.experimental import pallas as pl
from jax.experimental.pallas import tpu as pltpu
from jax.sharding import PartitionSpec as P

D = 768
HEADS = 12
HEAD_DIM = 64
PLANE = 4
GROUP_HEADS = HEADS // PLANE
GROUP_DIM = GROUP_HEADS * HEAD_DIM
FF = 3072
GROUP_FF = FF // PLANE

epsilon = 1e-12
very_low = -1e30
root_half = 0.7071067811865476
inv_root_tau = 0.3989422804014327
bf16 = jnp.bfloat16
f32 = jnp.float32
MESH = pl.DeviceIdType.MESH
VMEM_SPEC = pl.BlockSpec(memory_space=pltpu.VMEM)
ANY_SPEC = pl.BlockSpec(memory_space=pl.ANY)
VMEM_BYTES = 60000 * 1024
MODEL_BYTES = 100_000_000


def struct(shape, dtype=bf16):
    return jax.ShapeDtypeStruct(shape, dtype)


def comm_call(body, name, ident, inputs, out_shapes, out_specs, scratch):
    return pl.pallas_call(
        body,
        name=name,
        out_shape=out_shapes,
        in_specs=[VMEM_SPEC] * len(inputs),
        out_specs=out_specs,
        scratch_shapes=scratch,
        cost_estimate=pl.CostEstimate(flops=0, bytes_accessed=MODEL_BYTES, transcendentals=0),
        compiler_params=pltpu.CompilerParams(
            collective_id=ident, has_side_effects=True, vmem_limit_bytes=VMEM_BYTES
        ),
    )(*inputs)


def greet(peers):
    barrier = pltpu.get_barrier_semaphore()
    for peer in peers:
        pl.semaphore_signal(barrier, inc=1, device_id=peer, device_id_type=MESH)
    pl.semaphore_wait(barrier, len(peers))


def remote(src, dst, send_sem, recv_sem, peer):
    return pltpu.make_async_remote_copy(
        src_ref=src,
        dst_ref=dst,
        send_sem=send_sem,
        recv_sem=recv_sem,
        device_id=peer,
        device_id_type=MESH,
    )


def plane_peer(me, mask):
    group = lax.rem(me, PLANE)
    core = lax.rem(group, 2)
    column = lax.div(group, 2)
    if mask & 1:
        core = 1 - core
    if mask & 2:
        column = 1 - column
    return me - group + 2 * column + core


def plane_slot(me, mask):
    return lax.rem(plane_peer(me, mask), PLANE)


def plane_step(parts, pieces, vectors, action, out_types, ident):
    _, rows, cols = parts.shape
    chunks = 3 if rows % 48 == 0 else 1
    size = rows // chunks
    many, few = len(pieces), len(out_types)

    def body(p_ref, *rest):
        piece_refs, vector_ref = rest[:many], rest[many]
        all_ref, sums_ref = rest[many + 1 : many + 3]
        out_refs = rest[many + 3 : many + 3 + few]
        near, held, far_in, low, send, recv = rest[many + 3 + few :]
        me = lax.axis_index("shard")
        beside, across = [{"shard": plane_peer(me, mask)} for mask in (1, 2)]
        mine, far = lax.rem(me, PLANE), plane_slot(me, 2)
        greet([beside, across])
        spans = [pl.ds(size * index, size) for index in range(chunks)]

        def copy(kind, index):
            span = spans[index]
            table = {
                0: lambda: (p_ref.at[plane_slot(me, 3), span], near.at[0, span], beside),
                1: lambda: (p_ref.at[plane_slot(me, 1), span], near.at[1, span], beside),
                2: lambda: (held.at[span], far_in.at[span], across),
                3: lambda: (low.at[span], all_ref.at[mine, span], across),
                4: lambda: (low.at[span], all_ref.at[mine, span], beside),
                5: lambda: (all_ref.at[far, span], all_ref.at[far, span], beside),
            }
            src, dst, peer = table[kind]()
            return remote(src, dst, send.at[kind, index], recv.at[kind, index], peer)

        for index in range(chunks):
            copy(0, index).start()
        for index in range(chunks):
            copy(1, index).start()
        for index in range(chunks):
            span = spans[index]
            copy(0, index).wait_recv()
            total = p_ref[plane_slot(me, 2), span].astype(f32) + near[0, span].astype(f32)
            held[span] = total.astype(bf16)
            copy(2, index).start()
        lines = [vector_ref[index : index + 1] for index in range(len(vectors))]
        sums = None
        for index in range(chunks):
            span = spans[index]
            copy(1, index).wait_recv()
            copy(2, index).wait_recv()
            total = p_ref[mine, span].astype(f32) + near[1, span].astype(f32)
            total = total + far_in[span].astype(f32)
            result, outs, terms = action(
                total, [item[span].astype(f32) for item in piece_refs], lines
            )
            low[span] = result
            copy(3, index).start()
            copy(4, index).start()
            for ref, value in zip(out_refs, outs):
                ref[span] = value.astype(ref.dtype)
            all_ref[mine, span] = result
            terms = [jnp.sum(item, axis=0, keepdims=True) for item in terms]
            sums = terms if sums is None else [x + y for x, y in zip(sums, terms)]
        sums_ref[...] = jnp.zeros(sums_ref.shape, f32)
        for place, value in enumerate(sums):
            sums_ref[place : place + 1] = value
        for index in range(chunks):
            copy(3, index).wait_recv()
            copy(5, index).start()
        for index in range(chunks):
            copy(4, index).wait_recv()
            copy(5, index).wait_recv()
        for index in range(chunks):
            for kind in range(6):
                copy(kind, index).wait_send()

    stack = jnp.stack(vectors)
    shape = (rows, cols)
    return comm_call(
        body,
        "plane_step",
        ident,
        [parts] + list(pieces) + [stack],
        [struct((PLANE, rows, cols)), struct((8, cols), f32)]
        + [struct(shape, item) for item in out_types],
        [VMEM_SPEC] * (2 + few),
        [
            pltpu.VMEM((2, rows, cols), bf16),
            pltpu.VMEM(shape, bf16),
            pltpu.VMEM(shape, bf16),
            pltpu.VMEM(shape, bf16),
            pltpu.SemaphoreType.DMA((6, chunks)),
            pltpu.SemaphoreType.DMA((6, chunks)),
        ],
    )


def others(me, count):
    return [{"shard": lax.rem(me + step, count)} for step in range(1, count)]


def gather_weights(count, copies, tokens, qkv, up, out_w, small, ident):
    planes = count // PLANE
    rows = qkv.shape[1]

    def body(x_ref, qkv_ref, up_ref, wo_ref, small_ref, *rest):
        x_out, qkv_out, up_out, wo_out, small_out = rest[:5]
        send, recv, local, send_wo, recv_wo, send_unit, recv_unit = rest[5:]
        me = lax.axis_index("shard")
        group, plane = lax.rem(me, PLANE), lax.div(me, PLANE)
        across = [
            {"rep": lax.rem(lax.axis_index("rep") + step, copies)} for step in range(1, copies)
        ]
        greet(others(me, count) + across)
        owns = [
            (x_ref, x_out.at[group]),
            (qkv_ref.at[group], qkv_out.at[me]),
            (up_ref.at[group], up_out.at[group]),
            (small_ref, small_out.at[me]),
        ]
        started = []
        for index, (src, dst) in enumerate(owns):
            copy = pltpu.make_async_copy(src, dst, local.at[index])
            copy.start()
            started.append(copy)
        sent = []

        def push(src, dst, peer):
            index = len(sent)
            copy = remote(src, dst, send.at[index], recv.at[index], {"shard": peer})
            copy.start()
            sent.append(copy)

        for mask in (2, 1):
            push(x_ref, x_out.at[group], plane_peer(me, mask))
        far = plane_slot(me, 2)
        x_relay = remote(
            x_out.at[far], x_out.at[far], send.at[2], recv.at[2], {"shard": plane_peer(me, 1)}
        )
        sent.append(x_relay)
        for step in range(1, count):
            push(small_ref, small_out.at[me], lax.rem(me + step, count))
        rep = lax.axis_index("rep")
        split = copies == 2
        units = []
        for step in range(planes):
            for lane in range(PLANE):
                if step or lane:
                    units.append((qkv_ref, qkv_out, step, lane))
        for lane in range(1, PLANE):
            units.append((up_ref, up_out, 0, lane))

        def unit_copy(index):
            src, dst, step, lane = units[index]
            goal = lax.rem(plane + step, planes)
            goal_group = lax.rem(group + lane, PLANE)
            slot = group if src is up_ref else me
            return remote(
                src.at[goal_group],
                dst.at[slot],
                send_unit.at[index],
                recv_unit.at[index],
                {"shard": goal * PLANE + goal_group},
            )

        def unit_relay(index):
            src, dst, step, lane = units[index]
            origin = lax.rem(plane + planes - step, planes)
            origin_group = lax.rem(group + PLANE - lane, PLANE)
            slot = origin_group if src is up_ref else origin * PLANE + origin_group
            return remote(
                dst.at[slot],
                dst.at[slot],
                send_unit.at[index],
                recv_unit.at[index],
                {"rep": lax.rem(rep + 1, copies)},
            )

        def carried(index, mine):
            step = units[index][2]
            if not split or step == 0:
                return None
            return (rep == step % 2) if mine else (rep != step % 2)

        def guarded(test, action):
            if test is None:
                action()
            else:
                pl.when(test)(action)

        for index in range(len(units)):
            guarded(carried(index, True), unit_copy(index).start)
        target, place = lax.div(me, planes), lax.rem(me, planes)

        def wo_copy(source, index):
            peer = PLANE * index + target
            return peer, remote(
                wo_ref, wo_out.at[place], send_wo.at[index], recv_wo.at[source], {"shard": peer}
            )

        for index in range(planes):
            peer, copy = wo_copy(place, index)
            pl.when(peer != me)(copy.start)
        keep = pltpu.make_async_copy(wo_ref, wo_out.at[place], local.at[5])
        pl.when(target == group)(keep.start)
        sent[0].wait_recv()
        x_relay.start()
        for index, (_, _, step, _) in enumerate(units):
            if split and step:

                @pl.when(rep == step % 2)
                def _(index=index):
                    unit_relay(index).wait_recv()
                    unit_copy(index).wait_send()
                    unit_relay(index).start()

            else:
                unit_copy(index).wait_recv()
                unit_copy(index).wait_send()
        for index, (_, _, step, _) in enumerate(units):
            if split and step:
                pl.when(rep != step % 2)(unit_relay(index).wait_recv)
                pl.when(rep == step % 2)(unit_relay(index).wait_send)
        for copy in sent[1:]:
            copy.wait_recv()
        for index in range(planes):
            pl.when(group * planes + index != me)(wo_copy(index, index)[1].wait_recv)
        for index in range(planes):
            peer, copy = wo_copy(place, index)
            pl.when(peer != me)(copy.wait_send)
        pl.when(target == group)(keep.wait)
        for copy in sent:
            copy.wait_send()
        for copy in started:
            copy.wait()

    total = 3 + count - 1
    number = count - 1 + PLANE - 1
    return comm_call(
        body,
        "gather_weights",
        ident,
        [tokens, qkv, up, out_w, small],
        [
            struct((PLANE,) + tokens.shape),
            struct((count, rows, qkv.shape[2])),
            struct((PLANE, rows, up.shape[2])),
            struct((planes,) + out_w.shape),
            struct((count,) + small.shape),
        ],
        [ANY_SPEC] * 5,
        [
            pltpu.SemaphoreType.DMA((total,)),
            pltpu.SemaphoreType.DMA((total,)),
            pltpu.SemaphoreType.DMA((6,)),
            pltpu.SemaphoreType.DMA((planes,)),
            pltpu.SemaphoreType.DMA((planes,)),
            pltpu.SemaphoreType.DMA((number,)),
            pltpu.SemaphoreType.DMA((number,)),
        ],
    )


def gather_planes(count, value, ident):
    planes = count // PLANE

    def body(x_ref, out_ref, send, recv, local):
        me = lax.axis_index("shard")
        plane = lax.div(me, PLANE)
        greet([{"shard": lax.rem(me + PLANE * s, count)} for s in range(1, planes)])
        own = pltpu.make_async_copy(x_ref, out_ref.at[plane], local)
        own.start()

        def hop(way, source, src):
            peer = me + PLANE if way == 0 else me - PLANE
            return remote(
                src,
                out_ref.at[source],
                send.at[way, source],
                recv.at[way, source],
                {"shard": lax.rem(peer + count, count)},
            )

        @pl.when(plane < planes - 1)
        def _():
            hop(0, plane, x_ref).start()

        @pl.when(plane > 0)
        def _():
            hop(1, plane, x_ref).start()

        for step in range(1, planes):
            for way, source in ((0, plane - step), (1, plane + step)):
                onward = plane < planes - 1 if way == 0 else plane > 0

                @pl.when((source >= 0) & (source < planes))
                def _(way=way, source=source, onward=onward):
                    copy = hop(way, source, out_ref.at[source])
                    copy.wait_recv()
                    pl.when(onward)(copy.start)

        @pl.when(plane < planes - 1)
        def _():
            hop(0, plane, x_ref).wait_send()

        @pl.when(plane > 0)
        def _():
            hop(1, plane, x_ref).wait_send()

        for step in range(1, planes):
            for way, source in ((0, plane - step), (1, plane + step)):
                onward = plane < planes - 1 if way == 0 else plane > 0

                @pl.when((source >= 0) & (source < planes) & onward)
                def _(way=way, source=source):
                    hop(way, source, out_ref.at[source]).wait_send()

        own.wait()

    return comm_call(
        body,
        "gather_planes",
        ident,
        [value],
        struct((planes,) + value.shape),
        ANY_SPEC,
        [
            pltpu.SemaphoreType.DMA((2, planes)),
            pltpu.SemaphoreType.DMA((2, planes)),
            pltpu.SemaphoreType.DMA,
        ],
    )


def reduce_grads(count, copies, qkv, up, out_w, down, small, parts, first_grad, ident):
    planes = count // PLANE
    rows = qkv.shape[1]
    block = down.shape[0]
    arrays = [qkv, up, out_w, small]

    def body(qkv_ref, up_ref, wo_ref, small_ref, down_ref, p_ref, first_ref, *rest):
        outs, token_ref, rest = rest[:5], rest[5], rest[6:]
        qkv_in, up_in, wo_in, small_in = rest[:4]
        halves, gets = [rest[4], up_in, rest[5], rest[6], down_ref], rest[7:12]
        near, near_sum, far_in = rest[12:15]
        send, recv, send_rep, recv_rep, send_wo, recv_wo, send_near, recv_near = rest[15:]
        me = lax.axis_index("shard")
        rep = lax.axis_index("rep")
        plane = lax.div(me, PLANE)
        across = [{"rep": lax.rem(rep + step, copies)} for step in range(1, copies)]
        greet(others(me, count) + across)
        sent = []

        def push(src, dst, peer):
            index = len(sent)
            copy = remote(src, dst, send.at[index], recv.at[index], {"shard": peer})
            copy.start()
            sent.append(copy)

        pairs = [(qkv_ref, qkv_in), (small_ref, small_in)]
        passed = []
        beside, over = [{"shard": plane_peer(me, mask)} for mask in (1, 2)]
        near_copies = [
            remote(p_ref.at[plane_slot(me, 3)], near.at[0], send_near.at[0], recv_near.at[0], beside),
            remote(p_ref.at[plane_slot(me, 1)], near.at[1], send_near.at[1], recv_near.at[1], beside),
            remote(near_sum, far_in, send_near.at[2], recv_near.at[2], over),
        ]
        near_copies[0].start()
        near_copies[1].start()

        def exchange(*places):
            for index, peer in enumerate(across):
                for place in places:
                    copy = remote(
                        halves[place],
                        gets[place].at[index],
                        send_rep.at[5 * index + place],
                        recv_rep.at[5 * index + place],
                        peer,
                    )
                    copy.start()
                    passed.append(copy)

        exchange(4)
        group = lax.rem(me, PLANE)
        target, place = lax.div(me, planes), lax.rem(me, planes)
        for lane in range(1, PLANE):
            goal = lax.rem(group + lane, PLANE)
            push(up_ref.at[goal], up_in.at[group], plane * PLANE + goal)
        up_in[group] = up_ref[group]
        for src, held in pairs:
            for step in range(1, count):
                peer = lax.rem(me + step, count)
                push(src.at[peer], held.at[me], peer)
        for src, held in pairs:
            held[me] = src[me]

        def wo_copy(source, index):
            peer = group * planes + index
            return peer, remote(
                wo_ref.at[index],
                wo_in.at[plane],
                send_wo.at[index],
                recv_wo.at[source],
                {"shard": peer},
            )

        for index in range(planes):
            peer, copy = wo_copy(plane, index)
            pl.when(peer != me)(copy.start)

        @pl.when(target == group)
        def _():
            wo_in[plane] = wo_ref[place]

        near_copies[0].wait_recv()
        total = p_ref[plane_slot(me, 2)].astype(f32) + near[0].astype(f32)
        near_sum[...] = total.astype(bf16)
        near_copies[2].start()
        for copy in sent[: PLANE - 1]:
            copy.wait_recv()
        exchange(1)
        for index in range(planes):
            pl.when(PLANE * index + target != me)(wo_copy(index, index)[1].wait_recv)
        for index in range(planes):
            peer, copy = wo_copy(plane, index)
            pl.when(peer != me)(copy.wait_send)
        total = wo_in[0].astype(f32)
        for other in range(1, planes):
            total = total + wo_in[other].astype(f32)
        halves[2][...] = total.astype(bf16)
        exchange(2)
        near_copies[1].wait_recv()
        near_copies[2].wait_recv()
        total = p_ref[lax.rem(me, PLANE)].astype(f32) + near[1].astype(f32)
        total = total + far_in[...].astype(f32) + first_ref[...]
        token_ref[...] = total.astype(bf16)
        for copy in sent[PLANE - 1 :]:
            copy.wait_recv()
        for half, held in zip(halves[:1], (qkv_in,)):
            for lane in range(PLANE):
                total = held[lane].astype(f32)
                for other in range(1, planes):
                    total = total + held[other * PLANE + lane].astype(f32)
                half[lane] = total.astype(bf16)
        for half, held, number in (
            (halves[3], small_in, count),
        ):
            total = held[0].astype(f32)
            for other in range(1, number):
                total = total + held[other].astype(f32)
            half[...] = total.astype(bf16)
        exchange(0, 3)
        for copy in passed:
            copy.wait_recv()
        for out, half, got in zip(outs, halves, gets):
            total = half[...].astype(f32)
            for index in range(copies - 1):
                total = total + got[index].astype(f32)
            out[...] = total
        for copy in sent + passed + near_copies:
            copy.wait_send()

    totals = 2 * (count - 1) + PLANE - 1
    shapes = [
        (PLANE, rows, qkv.shape[2]),
        (PLANE, rows, up.shape[2]),
        (rows, D),
        small.shape[1:],
        (block, D),
    ]
    return comm_call(
        body,
        "reduce_grads",
        ident,
        arrays + [down, parts, first_grad],
        [struct(shape, f32) for shape in shapes] + [struct(parts.shape[1:])],
        [VMEM_SPEC] * 6,
        [pltpu.VMEM(item.shape, bf16) for item in arrays]
        + [pltpu.VMEM(shapes[index], bf16) for index in (0, 2, 3)]
        + [pltpu.VMEM((copies - 1,) + shape, bf16) for shape in shapes]
        + [
            pltpu.VMEM((2,) + parts.shape[1:], bf16),
            pltpu.VMEM(parts.shape[1:], bf16),
            pltpu.VMEM(parts.shape[1:], bf16),
            pltpu.SemaphoreType.DMA((totals,)),
            pltpu.SemaphoreType.DMA((totals,)),
            pltpu.SemaphoreType.DMA((5 * (copies - 1),)),
            pltpu.SemaphoreType.DMA((5 * (copies - 1),)),
            pltpu.SemaphoreType.DMA((planes,)),
            pltpu.SemaphoreType.DMA((planes,)),
            pltpu.SemaphoreType.DMA((3,)),
            pltpu.SemaphoreType.DMA((3,)),
        ],
    )


def pick(plane, table):
    value = table[-1]
    for index in range(len(table) - 1):
        value = jnp.where(plane == index, table[index], value)
    return value


def attend_back(count, queries, upstream, pairs, own_row, key_cols, logs, delta, ident):
    planes, rows, cols = pairs.shape
    half = cols // 2
    size = 256 if rows % 256 == 0 else rows
    orders = []
    for plane in range(planes):
        goals = [goal for goal in range(planes) if goal != plane]
        goals.sort(key=lambda goal: (-abs(goal - plane), goal))
        orders.append(goals + [plane])

    def body(q_ref, up_ref, kv_ref, row_ref, col_ref, log_ref, delta_ref, *rest):
        dq_ref, out_ref, dq_sum, part, held, staged, send, recv = rest
        me = lax.axis_index("shard")
        plane = lax.div(me, PLANE)
        greet([{"shard": lax.rem(me + PLANE * s, count)} for s in range(1, planes)])
        dq_sum[...] = jnp.zeros(dq_sum.shape, f32)

        def hop(way, goal):
            peer = me + PLANE if way == 0 else me - PLANE
            return remote(
                staged.at[goal],
                held.at[way, goal],
                send.at[goal],
                recv.at[way, goal],
                {"shard": lax.rem(peer + count, count)},
            )

        def compute(goal):
            part[...] = jnp.zeros(part.shape, f32)
            key_codes = col_ref[goal]

            def chunk(index, carry):
                at = pl.multiple_of(index * size, size)
                span = pl.ds(at, size)
                allowed = key_codes == row_ref[0:1, span]
                for head in range(GROUP_HEADS):
                    low, high = head * HEAD_DIM, (head + 1) * HEAD_DIM
                    q = q_ref[span, low:high]
                    g = up_ref[span, low:high]
                    k = kv_ref[goal, :, low:high]
                    v = kv_ref[goal, :, half + low : half + high]
                    raw = dot_right(k, q) * 0.125
                    chances = jnp.where(
                        allowed, jnp.exp(raw - log_ref[head : head + 1, span]), 0.0
                    )
                    d_chance = dot_right(v, g)
                    d_score = (chances * (d_chance - delta_ref[head : head + 1, span])).astype(bf16)
                    dq_sum[span, low:high] += dot_left(d_score, k)
                    part[:, low:high] += dot(d_score, q) * 0.125
                    part[:, half + low : half + high] += dot(chances.astype(bf16), g)
                return carry

            lax.fori_loop(0, rows // size, chunk, 0)

        def pass_on(goal):
            for way in (0, 1):
                ahead = goal > plane if way == 0 else goal < plane
                first = plane == 0 if way == 0 else plane == planes - 1

                @pl.when(ahead & jnp.logical_not(first))
                def _(way=way):
                    copy = hop(way, goal)
                    copy.wait_recv()
                    total = staged[goal].astype(f32) + held[way, goal].astype(f32)
                    staged[goal] = total.astype(bf16)
                    copy.start()

        def begin(goal):
            for way in (0, 1):
                ahead = goal > plane if way == 0 else goal < plane
                first = plane == 0 if way == 0 else plane == planes - 1

                @pl.when(ahead & first)
                def _(way=way):
                    hop(way, goal).start()

        goals = [pick(plane, [order[i] for order in orders]) for i in range(planes)]
        for index in range(planes):
            goal = goals[index]
            compute(goal)
            if index < planes - 1:
                staged[goal] = part[...].astype(bf16)
                begin(goal)
            if index:
                pass_on(goals[index - 1])
        dq_ref[...] = (dq_sum[...] * 0.125).astype(bf16)
        for way in (0, 1):
            behind = plane > 0 if way == 0 else plane < planes - 1

            @pl.when(behind)
            def _(way=way):
                hop(way, plane).wait_recv()
                part[...] += held[way, plane].astype(f32)

        out_ref[...] = part[...].astype(bf16)
        for index in range(planes - 1):
            hop(0, goals[index]).wait_send()

    return comm_call(
        body,
        "attend_back",
        ident,
        [queries, upstream, pairs, own_row, key_cols, logs, delta],
        [struct((rows, half)), struct((rows, cols))],
        [VMEM_SPEC] * 2,
        [
            pltpu.VMEM((rows, half), f32),
            pltpu.VMEM((rows, cols), f32),
            pltpu.VMEM((2, planes, rows, cols), bf16),
            pltpu.VMEM((planes, rows, cols), bf16),
            pltpu.SemaphoreType.DMA((planes,)),
            pltpu.SemaphoreType.DMA((2, planes)),
        ],
    )


def norm_forward(value, gain, shift):
    center = value - jnp.mean(value, axis=-1, keepdims=True)
    spread = jnp.mean(center * center, axis=-1, keepdims=True)
    scale = lax.rsqrt(spread + epsilon)
    normal = center * scale
    return (normal * gain + shift, normal, scale)


def norm_backward(upstream, normal, scale, gain):
    inner = upstream * gain
    return scale * (
        inner
        - jnp.mean(inner, axis=-1, keepdims=True)
        - normal * jnp.mean(inner * normal, axis=-1, keepdims=True)
    )


def gelu_slope(hidden):
    return 0.5 * (1.0 + lax.erf(hidden * root_half)) + hidden * inv_root_tau * jnp.exp(
        -0.5 * hidden * hidden
    )


def dot(left, right):
    return jnp.dot(left, right, preferred_element_type=f32)


def dot_left(left, right):
    return lax.dot_general(left, right, (((0,), (0,)), ((), ())), preferred_element_type=f32)


def dot_right(left, right):
    return lax.dot_general(left, right, (((1,), (1,)), ((), ())), preferred_element_type=f32)


def heads_of(value):
    return value.reshape(value.shape[0], GROUP_HEADS, HEAD_DIM).transpose(1, 0, 2)


def flat_of(value):
    return value.transpose(1, 0, 2).reshape(value.shape[1], GROUP_DIM)


def attend_forward(queries, keys, values, own_codes, all_codes):
    def step(carried, pieces):
        top, total, summed = carried
        key_rows, value_rows, key_codes = pieces
        raw = jnp.einsum("hqd,khd->hqk", queries, key_rows, preferred_element_type=f32) * 0.125
        allowed = (own_codes[:, None] == key_codes[None, :])[None]
        masked = jnp.where(allowed, raw, very_low)
        new_top = jnp.maximum(top, jnp.max(masked, axis=2))
        rescale = jnp.exp(top - new_top)
        weights = jnp.where(allowed, jnp.exp(masked - new_top[:, :, None]), 0.0)
        added = jnp.einsum(
            "hqk,khd->hqd", weights.astype(bf16), value_rows, preferred_element_type=f32
        )
        return (
            new_top,
            total * rescale + jnp.sum(weights, axis=2),
            summed * rescale[:, :, None] + added,
        ), None

    rows = queries.shape[1]
    start = (
        jnp.full((GROUP_HEADS, rows), very_low, f32),
        jnp.zeros((GROUP_HEADS, rows), f32),
        jnp.zeros((GROUP_HEADS, rows, HEAD_DIM), f32),
    )
    (top, total, summed), _ = lax.scan(step, start, (keys, values, all_codes))
    return summed / total[:, :, None], top + jnp.log(total)


def shards(count, copies, *arrays):
    (
        tokens,
        segments,
        padding,
        query_weight,
        key_weight,
        value_weight,
        query_bias,
        value_bias,
        out_weight,
        out_bias,
        middle_gain,
        middle_shift,
        up_weight,
        up_bias,
        down_weight,
        down_bias,
        final_gain,
        final_shift,
        cotangent,
    ) = arrays
    planes = count // PLANE
    rows = query_weight.shape[0]
    block = down_weight.shape[0]
    x_own = tokens[0]
    here = x_own.shape[0]
    wide = PLANE * here
    me = lax.axis_index("shard")
    group = lax.rem(me, PLANE)
    qkv_send = jnp.concatenate(
        [
            item.astype(bf16).reshape(rows, PLANE, GROUP_DIM)
            for item in (query_weight, key_weight, value_weight)
        ],
        axis=2,
    ).transpose(1, 0, 2)
    up_send = (
        up_weight.astype(bf16)
        .reshape(rows, planes, PLANE, block)
        .transpose(2, 0, 1, 3)
        .reshape(PLANE, rows, GROUP_FF)
    )
    codes = (2 * segments[0] + padding[0]).astype(f32)
    lanes = 128 * ((max(here, block) + 127) // 128)

    def padded(value):
        return jnp.pad(value.astype(f32), (0, lanes - value.shape[0]))

    vectors = [
        query_bias,
        value_bias,
        out_bias,
        middle_gain,
        middle_shift,
        down_bias,
        final_gain,
        final_shift,
        up_bias,
        codes,
    ]
    small_send = jnp.pad(
        jnp.stack([padded(item) for item in vectors]), ((0, 6), (0, 0))
    ).astype(bf16)
    x_all, qkv_all, up_all, wo_all, small = gather_weights(
        count,
        copies,
        x_own,
        qkv_send,
        up_send,
        out_weight.astype(bf16),
        small_send,
        0,
    )
    x_plane = x_all.reshape(wide, D)
    w_qkv = qkv_all.reshape(D, 3 * GROUP_DIM)
    lines = [[start + PLANE * step for step in range(planes)] for start in range(PLANE)]
    strip = jnp.concatenate([up_all.reshape(PLANE * rows, D), down_weight.astype(bf16)], axis=0)
    w_out = wo_all.reshape(GROUP_DIM, D)
    small = small.astype(f32)
    spread = [small[:, index, :rows].reshape(D) for index in range(8)]
    b_query, b_value, b_out, gain_mid, shift_mid, b_down, gain_end, shift_end = spread
    b_up = lax.dynamic_index_in_dim(
        small[:, 8, :block].reshape(planes, PLANE, block), group, 1, keepdims=False
    ).reshape(GROUP_FF)
    all_codes = small[:, 9, :here].reshape(planes, wide)
    own_codes = lax.dynamic_index_in_dim(all_codes, lax.div(me, PLANE), 0, keepdims=False)

    def group_part(value):
        return lax.dynamic_slice(value, (group * GROUP_DIM,), (GROUP_DIM,))

    qkv_bias = jnp.concatenate(
        [group_part(b_query), jnp.zeros((GROUP_DIM,), f32), group_part(b_value)]
    )
    qkv = (dot(x_plane, w_qkv) + qkv_bias).astype(bf16)
    pairs = gather_planes(count, qkv[:, GROUP_DIM:], 1)
    strip, pairs = lax.optimization_barrier((strip, pairs))
    strips = lax.all_gather(strip, "shard", axis_index_groups=lines, axis=0)
    w_up = strips[:, : PLANE * rows].reshape(D, GROUP_FF)
    w_down = strips[:, PLANE * rows :].reshape(GROUP_FF, D)
    queries = heads_of(qkv[:, :GROUP_DIM])
    keys = pairs[:, :, :GROUP_DIM].reshape(planes, wide, GROUP_HEADS, HEAD_DIM)
    values = pairs[:, :, GROUP_DIM:].reshape(planes, wide, GROUP_HEADS, HEAD_DIM)
    context_heads, logs = attend_forward(queries, keys, values, own_codes, all_codes)
    context_low = flat_of(context_heads).astype(bf16)

    def split(value):
        return value.reshape(PLANE, here, D)

    def enter_middle(total, pieces, lines):
        rest = total + lines[0] + pieces[0]
        middle, _, _ = norm_forward(rest, lines[1], lines[2])
        return middle.astype(bf16), [rest], []

    def enter_end(total, pieces, lines):
        middle, _, _ = norm_forward(pieces[0], lines[1], lines[2])
        result, normal, scale = norm_forward(middle + (total + lines[0]), lines[3], lines[4])
        above = pieces[1]
        back = norm_backward(above, normal, scale, lines[3])
        rounded = back.astype(bf16)
        return rounded, [result, back], [above * normal, above, rounded.astype(f32)]

    def leave_middle(total, pieces, lines):
        _, normal, scale = norm_forward(pieces[0], lines[0], lines[0])
        above = total + pieces[1]
        back = norm_backward(above, normal, scale, lines[0])
        rounded = back.astype(bf16)
        return rounded, [back], [above * normal, above, rounded.astype(f32)]

    middle_all, _, rest = plane_step(
        split(dot(context_low, w_out).astype(bf16)),
        [x_own],
        [b_out, gain_mid, shift_mid],
        enter_middle,
        [f32],
        2,
    )
    middle_plane = middle_all.reshape(wide, D)
    hidden = dot(middle_plane, w_up) + b_up
    active_low = jax.nn.gelu(hidden, approximate=False).astype(bf16)
    feed_all, end_sums, result, d_second = plane_step(
        split(dot(active_low, w_down).astype(bf16)),
        [rest, cotangent[0]],
        [b_down, gain_mid, shift_mid, gain_end, shift_end],
        enter_end,
        [bf16, f32],
        3,
    )
    output = result[None]
    feed_plane = feed_all.reshape(wide, D)
    grad_down = dot_left(active_low, feed_plane).astype(bf16)
    up_low = (dot_right(feed_plane, w_down) * gelu_slope(hidden)).astype(bf16)
    grad_up = dot_left(middle_plane, up_low).astype(bf16)
    strip_grads = lax.psum_scatter(
        jnp.concatenate(
            [
                grad_up.reshape(planes, PLANE * rows, GROUP_FF),
                grad_down.reshape(planes, block, D),
            ],
            axis=1,
        ),
        "shard",
        axis_index_groups=lines,
        scatter_dimension=0,
    )
    branch_all, middle_sums, d_first = plane_step(
        split(dot_right(up_low, w_up).astype(bf16)),
        [rest, d_second],
        [gain_mid],
        leave_middle,
        [f32],
        4,
    )
    branch_plane = branch_all.reshape(wide, D)
    grad_out = dot_left(context_low, branch_plane).astype(bf16)
    d_context = dot_right(branch_plane, w_out).astype(bf16)
    delta = jnp.sum(heads_of(d_context).astype(f32) * context_heads, axis=2)
    query_low, pair_low = attend_back(
        count,
        qkv[:, :GROUP_DIM],
        d_context,
        pairs,
        own_codes[None],
        all_codes[:, :, None],
        logs,
        delta,
        8,
    )
    mixer_low = jnp.concatenate([query_low, pair_low], axis=1)
    grad_qkv = dot_left(x_plane, mixer_low).astype(bf16)
    mixer_sums = jnp.sum(mixer_low.astype(f32), axis=0)

    def from_group(value):
        return lax.dynamic_update_slice(jnp.zeros((D,), f32), value, (group * GROUP_DIM,))

    sums = [
        from_group(mixer_sums[:GROUP_DIM]),
        from_group(mixer_sums[2 * GROUP_DIM :]),
        middle_sums[2],
        middle_sums[0],
        middle_sums[1],
        end_sums[2],
        end_sums[0],
        end_sums[1],
    ]
    own_lane = (jnp.arange(PLANE) == group).astype(f32)
    up_sums = jnp.sum(up_low.astype(f32), axis=0).reshape(planes, 1, block)
    up_sums = (up_sums * own_lane[None, :, None]).reshape(count, 1, block)
    sums = jnp.stack([item.reshape(count, rows) for item in sums], axis=1)
    small_grads = jnp.concatenate(
        [
            jnp.pad(sums, ((0, 0), (0, 0), (0, lanes - rows))),
            jnp.pad(up_sums, ((0, 0), (0, 7), (0, lanes - block))),
        ],
        axis=1,
    ).astype(bf16)
    qkv_total, up_total, out_total, small_total, down_total, grad_tokens = reduce_grads(
        count,
        copies,
        grad_qkv.reshape(count, rows, 3 * GROUP_DIM),
        strip_grads[: PLANE * rows].reshape(PLANE, rows, GROUP_FF),
        grad_out.reshape(planes, rows, D),
        strip_grads[PLANE * rows :],
        small_grads,
        split(dot_right(mixer_low, w_qkv).astype(bf16)),
        d_first,
        10,
    )

    def joined(value):
        return value.transpose(1, 0, 2).reshape(rows, D)

    up_grad = (
        up_total.reshape(PLANE, rows, planes, block).transpose(1, 2, 0, 3).reshape(rows, FF)
    )
    return (
        output,
        grad_tokens[None],
        joined(qkv_total[:, :, :GROUP_DIM]),
        joined(qkv_total[:, :, GROUP_DIM : 2 * GROUP_DIM]),
        joined(qkv_total[:, :, 2 * GROUP_DIM :]),
        small_total[0, :rows],
        small_total[1, :rows],
        out_total,
        small_total[2, :rows],
        small_total[3, :rows],
        small_total[4, :rows],
        up_grad,
        small_total[8, :block],
        down_total,
        small_total[5, :rows],
        small_total[6, :rows],
        small_total[7, :rows],
    )


def solution(mesh):
    sheet, line = P("shard", None), P("shard")
    batch = P("rep", "shard", None)
    in_specs = (batch, P("rep", "shard"), P("rep", "shard"), sheet, sheet, sheet, line, line)
    in_specs += (sheet, line, line, line, sheet, line, sheet, line, line, line, batch)
    out_specs = (batch, batch, sheet, sheet, sheet, line, line, sheet, line, line, line)
    out_specs += (sheet, line, sheet, line, line, line)
    body = functools.partial(shards, mesh.shape["shard"], mesh.shape["rep"])
    return jax.shard_map(
        body, mesh=mesh, in_specs=in_specs, out_specs=out_specs, check_vma=False
    )
```

```python
import functools

import jax
import jax.numpy as jnp
from jax import lax
from jax.experimental import pallas as pl
from jax.experimental.pallas import tpu as pltpu
from jax.sharding import PartitionSpec as P

D = 768
HEADS = 12
HEAD_DIM = 64
PLANE = 4
GROUP_HEADS = HEADS // PLANE
GROUP_DIM = GROUP_HEADS * HEAD_DIM
FF = 3072
GROUP_FF = FF // PLANE

epsilon = 1e-12
very_low = -1e30
root_half = 0.7071067811865476
inv_root_tau = 0.3989422804014327
bf16 = jnp.bfloat16
f32 = jnp.float32
MESH = pl.DeviceIdType.MESH
VMEM_SPEC = pl.BlockSpec(memory_space=pltpu.VMEM)
ANY_SPEC = pl.BlockSpec(memory_space=pl.ANY)
VMEM_BYTES = 60000 * 1024
MODEL_BYTES = 100_000_000


def struct(shape, dtype=bf16):
    return jax.ShapeDtypeStruct(shape, dtype)


def comm_call(body, name, ident, inputs, out_shapes, out_specs, scratch):
    return pl.pallas_call(
        body,
        name=name,
        out_shape=out_shapes,
        in_specs=[VMEM_SPEC] * len(inputs),
        out_specs=out_specs,
        scratch_shapes=scratch,
        cost_estimate=pl.CostEstimate(flops=0, bytes_accessed=MODEL_BYTES, transcendentals=0),
        compiler_params=pltpu.CompilerParams(
            collective_id=ident, has_side_effects=True, vmem_limit_bytes=VMEM_BYTES
        ),
    )(*inputs)


def greet(peers):
    barrier = pltpu.get_barrier_semaphore()
    for peer in peers:
        pl.semaphore_signal(barrier, inc=1, device_id=peer, device_id_type=MESH)
    pl.semaphore_wait(barrier, len(peers))


def remote(src, dst, send_sem, recv_sem, peer):
    return pltpu.make_async_remote_copy(
        src_ref=src,
        dst_ref=dst,
        send_sem=send_sem,
        recv_sem=recv_sem,
        device_id=peer,
        device_id_type=MESH,
    )


def plane_peer(me, mask):
    group = lax.rem(me, PLANE)
    core = lax.rem(group, 2)
    column = lax.div(group, 2)
    if mask & 1:
        core = 1 - core
    if mask & 2:
        column = 1 - column
    return me - group + 2 * column + core


def plane_slot(me, mask):
    return lax.rem(plane_peer(me, mask), PLANE)


def plane_step(parts, pieces, vectors, action, out_types, ident):
    _, rows, cols = parts.shape
    chunks = 3 if rows % 48 == 0 else 1
    size = rows // chunks
    many, few = len(pieces), len(out_types)

    def body(p_ref, *rest):
        piece_refs, vector_ref = rest[:many], rest[many]
        all_ref, sums_ref = rest[many + 1 : many + 3]
        out_refs = rest[many + 3 : many + 3 + few]
        near, held, far_in, low, send, recv = rest[many + 3 + few :]
        me = lax.axis_index("shard")
        beside, across = [{"shard": plane_peer(me, mask)} for mask in (1, 2)]
        mine, far = lax.rem(me, PLANE), plane_slot(me, 2)
        greet([beside, across])
        spans = [pl.ds(size * index, size) for index in range(chunks)]

        def copy(kind, index):
            span = spans[index]
            table = {
                0: lambda: (p_ref.at[plane_slot(me, 3), span], near.at[0, span], beside),
                1: lambda: (p_ref.at[plane_slot(me, 1), span], near.at[1, span], beside),
                2: lambda: (held.at[span], far_in.at[span], across),
                3: lambda: (low.at[span], all_ref.at[mine, span], across),
                4: lambda: (low.at[span], all_ref.at[mine, span], beside),
                5: lambda: (all_ref.at[far, span], all_ref.at[far, span], beside),
            }
            src, dst, peer = table[kind]()
            return remote(src, dst, send.at[kind, index], recv.at[kind, index], peer)

        for index in range(chunks):
            copy(0, index).start()
        for index in range(chunks):
            copy(1, index).start()
        for index in range(chunks):
            span = spans[index]
            copy(0, index).wait_recv()
            total = p_ref[plane_slot(me, 2), span].astype(f32) + near[0, span].astype(f32)
            held[span] = total.astype(bf16)
            copy(2, index).start()
        lines = [vector_ref[index : index + 1] for index in range(len(vectors))]
        sums = None
        for index in range(chunks):
            span = spans[index]
            copy(1, index).wait_recv()
            copy(2, index).wait_recv()
            total = p_ref[mine, span].astype(f32) + near[1, span].astype(f32)
            total = total + far_in[span].astype(f32)
            result, outs, terms = action(
                total, [item[span].astype(f32) for item in piece_refs], lines
            )
            low[span] = result
            copy(3, index).start()
            copy(4, index).start()
            for ref, value in zip(out_refs, outs):
                ref[span] = value.astype(ref.dtype)
            all_ref[mine, span] = result
            terms = [jnp.sum(item, axis=0, keepdims=True) for item in terms]
            sums = terms if sums is None else [x + y for x, y in zip(sums, terms)]
        sums_ref[...] = jnp.zeros(sums_ref.shape, f32)
        for place, value in enumerate(sums):
            sums_ref[place : place + 1] = value
        for index in range(chunks):
            copy(3, index).wait_recv()
            copy(5, index).start()
        for index in range(chunks):
            copy(4, index).wait_recv()
            copy(5, index).wait_recv()
        for index in range(chunks):
            for kind in range(6):
                copy(kind, index).wait_send()

    stack = jnp.stack(vectors)
    shape = (rows, cols)
    return comm_call(
        body,
        "plane_step",
        ident,
        [parts] + list(pieces) + [stack],
        [struct((PLANE, rows, cols)), struct((8, cols), f32)]
        + [struct(shape, item) for item in out_types],
        [VMEM_SPEC] * (2 + few),
        [
            pltpu.VMEM((2, rows, cols), bf16),
            pltpu.VMEM(shape, bf16),
            pltpu.VMEM(shape, bf16),
            pltpu.VMEM(shape, bf16),
            pltpu.SemaphoreType.DMA((6, chunks)),
            pltpu.SemaphoreType.DMA((6, chunks)),
        ],
    )


def others(me, count):
    return [{"shard": lax.rem(me + step, count)} for step in range(1, count)]


def gather_weights(count, copies, tokens, qkv, up, out_w, small, ident):
    planes = count // PLANE
    rows = qkv.shape[1]

    def body(x_ref, qkv_ref, up_ref, wo_ref, small_ref, *rest):
        x_out, qkv_out, up_out, wo_out, small_out = rest[:5]
        send, recv, local, send_wo, recv_wo, send_unit, recv_unit = rest[5:]
        me = lax.axis_index("shard")
        group, plane = lax.rem(me, PLANE), lax.div(me, PLANE)
        across = [
            {"rep": lax.rem(lax.axis_index("rep") + step, copies)} for step in range(1, copies)
        ]
        greet(others(me, count) + across)
        owns = [
            (x_ref, x_out.at[group]),
            (qkv_ref.at[group], qkv_out.at[me]),
            (up_ref.at[group], up_out.at[group]),
            (small_ref, small_out.at[me]),
        ]
        started = []
        for index, (src, dst) in enumerate(owns):
            copy = pltpu.make_async_copy(src, dst, local.at[index])
            copy.start()
            started.append(copy)
        sent = []

        def push(src, dst, peer):
            index = len(sent)
            copy = remote(src, dst, send.at[index], recv.at[index], {"shard": peer})
            copy.start()
            sent.append(copy)

        for mask in (2, 1):
            push(x_ref, x_out.at[group], plane_peer(me, mask))
        far = plane_slot(me, 2)
        x_relay = remote(
            x_out.at[far], x_out.at[far], send.at[2], recv.at[2], {"shard": plane_peer(me, 1)}
        )
        sent.append(x_relay)
        for step in range(1, count):
            push(small_ref, small_out.at[me], lax.rem(me + step, count))
        rep = lax.axis_index("rep")
        split = copies == 2
        units = []
        for step in range(planes):
            for lane in range(PLANE):
                if step or lane:
                    units.append((qkv_ref, qkv_out, step, lane))
        for lane in range(1, PLANE):
            units.append((up_ref, up_out, 0, lane))

        def unit_copy(index):
            src, dst, step, lane = units[index]
            goal = lax.rem(plane + step, planes)
            goal_group = lax.rem(group + lane, PLANE)
            slot = group if src is up_ref else me
            return remote(
                src.at[goal_group],
                dst.at[slot],
                send_unit.at[index],
                recv_unit.at[index],
                {"shard": goal * PLANE + goal_group},
            )

        def unit_relay(index):
            src, dst, step, lane = units[index]
            origin = lax.rem(plane + planes - step, planes)
            origin_group = lax.rem(group + PLANE - lane, PLANE)
            slot = origin_group if src is up_ref else origin * PLANE + origin_group
            return remote(
                dst.at[slot],
                dst.at[slot],
                send_unit.at[index],
                recv_unit.at[index],
                {"rep": lax.rem(rep + 1, copies)},
            )

        def carried(index, mine):
            step = units[index][2]
            if not split or step == 0:
                return None
            return (rep == step % 2) if mine else (rep != step % 2)

        def guarded(test, action):
            if test is None:
                action()
            else:
                pl.when(test)(action)

        for index in range(len(units)):
            guarded(carried(index, True), unit_copy(index).start)
        target, place = lax.div(me, planes), lax.rem(me, planes)

        def wo_copy(source, index):
            peer = PLANE * index + target
            return peer, remote(
                wo_ref, wo_out.at[place], send_wo.at[index], recv_wo.at[source], {"shard": peer}
            )

        for index in range(planes):
            peer, copy = wo_copy(place, index)
            pl.when(peer != me)(copy.start)
        keep = pltpu.make_async_copy(wo_ref, wo_out.at[place], local.at[5])
        pl.when(target == group)(keep.start)
        sent[0].wait_recv()
        x_relay.start()
        for index, (_, _, step, _) in enumerate(units):
            if split and step:

                @pl.when(rep == step % 2)
                def _(index=index):
                    unit_relay(index).wait_recv()
                    unit_copy(index).wait_send()
                    unit_relay(index).start()

            else:
                unit_copy(index).wait_recv()
                unit_copy(index).wait_send()
        for index, (_, _, step, _) in enumerate(units):
            if split and step:
                pl.when(rep != step % 2)(unit_relay(index).wait_recv)
                pl.when(rep == step % 2)(unit_relay(index).wait_send)
        for copy in sent[1:]:
            copy.wait_recv()
        for index in range(planes):
            pl.when(group * planes + index != me)(wo_copy(index, index)[1].wait_recv)
        for index in range(planes):
            peer, copy = wo_copy(place, index)
            pl.when(peer != me)(copy.wait_send)
        pl.when(target == group)(keep.wait)
        for copy in sent:
            copy.wait_send()
        for copy in started:
            copy.wait()

    total = 3 + count - 1
    number = count - 1 + PLANE - 1
    return comm_call(
        body,
        "gather_weights",
        ident,
        [tokens, qkv, up, out_w, small],
        [
            struct((PLANE,) + tokens.shape),
            struct((count, rows, qkv.shape[2])),
            struct((PLANE, rows, up.shape[2])),
            struct((planes,) + out_w.shape),
            struct((count,) + small.shape),
        ],
        [ANY_SPEC] * 5,
        [
            pltpu.SemaphoreType.DMA((total,)),
            pltpu.SemaphoreType.DMA((total,)),
            pltpu.SemaphoreType.DMA((6,)),
            pltpu.SemaphoreType.DMA((planes,)),
            pltpu.SemaphoreType.DMA((planes,)),
            pltpu.SemaphoreType.DMA((number,)),
            pltpu.SemaphoreType.DMA((number,)),
        ],
    )


def reduce_grads(count, copies, qkv, up, out_w, down, small, parts, first_grad, ident):
    planes = count // PLANE
    rows = qkv.shape[1]
    block = down.shape[0]
    arrays = [qkv, up, out_w, small]

    def body(qkv_ref, up_ref, wo_ref, small_ref, down_ref, p_ref, first_ref, *rest):
        outs, token_ref, rest = rest[:5], rest[5], rest[6:]
        qkv_in, up_in, wo_in, small_in = rest[:4]
        halves, gets = [rest[4], up_in, rest[5], rest[6], down_ref], rest[7:12]
        near, near_sum, far_in = rest[12:15]
        send, recv, send_rep, recv_rep, send_wo, recv_wo, send_near, recv_near = rest[15:]
        me = lax.axis_index("shard")
        rep = lax.axis_index("rep")
        plane = lax.div(me, PLANE)
        across = [{"rep": lax.rem(rep + step, copies)} for step in range(1, copies)]
        greet(others(me, count) + across)
        sent = []

        def push(src, dst, peer):
            index = len(sent)
            copy = remote(src, dst, send.at[index], recv.at[index], {"shard": peer})
            copy.start()
            sent.append(copy)

        pairs = [(qkv_ref, qkv_in), (small_ref, small_in)]
        passed = []
        beside, over = [{"shard": plane_peer(me, mask)} for mask in (1, 2)]
        near_copies = [
            remote(p_ref.at[plane_slot(me, 3)], near.at[0], send_near.at[0], recv_near.at[0], beside),
            remote(p_ref.at[plane_slot(me, 1)], near.at[1], send_near.at[1], recv_near.at[1], beside),
            remote(near_sum, far_in, send_near.at[2], recv_near.at[2], over),
        ]
        near_copies[0].start()
        near_copies[1].start()

        def exchange(*places):
            for index, peer in enumerate(across):
                for place in places:
                    copy = remote(
                        halves[place],
                        gets[place].at[index],
                        send_rep.at[5 * index + place],
                        recv_rep.at[5 * index + place],
                        peer,
                    )
                    copy.start()
                    passed.append(copy)

        exchange(4)
        group = lax.rem(me, PLANE)
        target, place = lax.div(me, planes), lax.rem(me, planes)
        for lane in range(1, PLANE):
            goal = lax.rem(group + lane, PLANE)
            push(up_ref.at[goal], up_in.at[group], plane * PLANE + goal)
        up_in[group] = up_ref[group]
        for src, held in pairs:
            for step in range(1, count):
                peer = lax.rem(me + step, count)
                push(src.at[peer], held.at[me], peer)
        for src, held in pairs:
            held[me] = src[me]

        def wo_copy(source, index):
            peer = group * planes + index
            return peer, remote(
                wo_ref.at[index],
                wo_in.at[plane],
                send_wo.at[index],
                recv_wo.at[source],
                {"shard": peer},
            )

        for index in range(planes):
            peer, copy = wo_copy(plane, index)
            pl.when(peer != me)(copy.start)

        @pl.when(target == group)
        def _():
            wo_in[plane] = wo_ref[place]

        near_copies[0].wait_recv()
        total = p_ref[plane_slot(me, 2)].astype(f32) + near[0].astype(f32)
        near_sum[...] = total.astype(bf16)
        near_copies[2].start()
        for copy in sent[: PLANE - 1]:
            copy.wait_recv()
        exchange(1)
        for index in range(planes):
            pl.when(PLANE * index + target != me)(wo_copy(index, index)[1].wait_recv)
        for index in range(planes):
            peer, copy = wo_copy(plane, index)
            pl.when(peer != me)(copy.wait_send)
        total = wo_in[0].astype(f32)
        for other in range(1, planes):
            total = total + wo_in[other].astype(f32)
        halves[2][...] = total.astype(bf16)
        exchange(2)
        near_copies[1].wait_recv()
        near_copies[2].wait_recv()
        total = p_ref[lax.rem(me, PLANE)].astype(f32) + near[1].astype(f32)
        total = total + far_in[...].astype(f32) + first_ref[...]
        token_ref[...] = total.astype(bf16)
        for copy in sent[PLANE - 1 :]:
            copy.wait_recv()
        for half, held in zip(halves[:1], (qkv_in,)):
            for lane in range(PLANE):
                total = held[lane].astype(f32)
                for other in range(1, planes):
                    total = total + held[other * PLANE + lane].astype(f32)
                half[lane] = total.astype(bf16)
        for half, held, number in (
            (halves[3], small_in, count),
        ):
            total = held[0].astype(f32)
            for other in range(1, number):
                total = total + held[other].astype(f32)
            half[...] = total.astype(bf16)
        exchange(0, 3)
        for copy in passed:
            copy.wait_recv()
        for out, half, got in zip(outs, halves, gets):
            total = half[...].astype(f32)
            for index in range(copies - 1):
                total = total + got[index].astype(f32)
            out[...] = total
        for copy in sent + passed + near_copies:
            copy.wait_send()

    totals = 2 * (count - 1) + PLANE - 1
    shapes = [
        (PLANE, rows, qkv.shape[2]),
        (PLANE, rows, up.shape[2]),
        (rows, D),
        small.shape[1:],
        (block, D),
    ]
    return comm_call(
        body,
        "reduce_grads",
        ident,
        arrays + [down, parts, first_grad],
        [struct(shape, f32) for shape in shapes] + [struct(parts.shape[1:])],
        [VMEM_SPEC] * 6,
        [pltpu.VMEM(item.shape, bf16) for item in arrays]
        + [pltpu.VMEM(shapes[index], bf16) for index in (0, 2, 3)]
        + [pltpu.VMEM((copies - 1,) + shape, bf16) for shape in shapes]
        + [
            pltpu.VMEM((2,) + parts.shape[1:], bf16),
            pltpu.VMEM(parts.shape[1:], bf16),
            pltpu.VMEM(parts.shape[1:], bf16),
            pltpu.SemaphoreType.DMA((totals,)),
            pltpu.SemaphoreType.DMA((totals,)),
            pltpu.SemaphoreType.DMA((5 * (copies - 1),)),
            pltpu.SemaphoreType.DMA((5 * (copies - 1),)),
            pltpu.SemaphoreType.DMA((planes,)),
            pltpu.SemaphoreType.DMA((planes,)),
            pltpu.SemaphoreType.DMA((3,)),
            pltpu.SemaphoreType.DMA((3,)),
        ],
    )


def pick(plane, table):
    value = table[-1]
    for index in range(len(table) - 1):
        value = jnp.where(plane == index, table[index], value)
    return value


def attend_back(count, queries, upstream, pairs, own_row, key_cols, logs, delta, ident):
    planes, rows, cols = pairs.shape
    half = cols // 2
    size = 256 if rows % 256 == 0 else rows
    orders = []
    for plane in range(planes):
        goals = [goal for goal in range(planes) if goal != plane]
        goals.sort(key=lambda goal: (-abs(goal - plane), goal))
        orders.append(goals + [plane])

    def body(q_ref, up_ref, kv_ref, row_ref, col_ref, log_ref, delta_ref, *rest):
        dq_ref, out_ref, dq_sum, part, held, staged, send, recv = rest
        me = lax.axis_index("shard")
        plane = lax.div(me, PLANE)
        greet([{"shard": lax.rem(me + PLANE * s, count)} for s in range(1, planes)])
        dq_sum[...] = jnp.zeros(dq_sum.shape, f32)

        def hop(way, goal):
            peer = me + PLANE if way == 0 else me - PLANE
            return remote(
                staged.at[goal],
                held.at[way, goal],
                send.at[goal],
                recv.at[way, goal],
                {"shard": lax.rem(peer + count, count)},
            )

        def compute(goal):
            part[...] = jnp.zeros(part.shape, f32)
            key_codes = col_ref[goal]

            def chunk(index, carry):
                at = pl.multiple_of(index * size, size)
                span = pl.ds(at, size)
                allowed = key_codes == row_ref[0:1, span]
                for head in range(GROUP_HEADS):
                    low, high = head * HEAD_DIM, (head + 1) * HEAD_DIM
                    q = q_ref[span, low:high]
                    g = up_ref[span, low:high]
                    k = kv_ref[goal, :, low:high]
                    v = kv_ref[goal, :, half + low : half + high]
                    raw = dot_right(k, q) * 0.125
                    chances = jnp.where(
                        allowed, jnp.exp(raw - log_ref[head : head + 1, span]), 0.0
                    )
                    d_chance = dot_right(v, g)
                    d_score = (chances * (d_chance - delta_ref[head : head + 1, span])).astype(bf16)
                    dq_sum[span, low:high] += dot_left(d_score, k)
                    part[:, low:high] += dot(d_score, q) * 0.125
                    part[:, half + low : half + high] += dot(chances.astype(bf16), g)
                return carry

            lax.fori_loop(0, rows // size, chunk, 0)

        def pass_on(goal):
            for way in (0, 1):
                ahead = goal > plane if way == 0 else goal < plane
                first = plane == 0 if way == 0 else plane == planes - 1

                @pl.when(ahead & jnp.logical_not(first))
                def _(way=way):
                    copy = hop(way, goal)
                    copy.wait_recv()
                    total = staged[goal].astype(f32) + held[way, goal].astype(f32)
                    staged[goal] = total.astype(bf16)
                    copy.start()

        def begin(goal):
            for way in (0, 1):
                ahead = goal > plane if way == 0 else goal < plane
                first = plane == 0 if way == 0 else plane == planes - 1

                @pl.when(ahead & first)
                def _(way=way):
                    hop(way, goal).start()

        goals = [pick(plane, [order[i] for order in orders]) for i in range(planes)]
        for index in range(planes):
            goal = goals[index]
            compute(goal)
            if index < planes - 1:
                staged[goal] = part[...].astype(bf16)
                begin(goal)
            if index:
                pass_on(goals[index - 1])
        dq_ref[...] = (dq_sum[...] * 0.125).astype(bf16)
        for way in (0, 1):
            behind = plane > 0 if way == 0 else plane < planes - 1

            @pl.when(behind)
            def _(way=way):
                hop(way, plane).wait_recv()
                part[...] += held[way, plane].astype(f32)

        out_ref[...] = part[...].astype(bf16)
        for index in range(planes - 1):
            hop(0, goals[index]).wait_send()

    return comm_call(
        body,
        "attend_back",
        ident,
        [queries, upstream, pairs, own_row, key_cols, logs, delta],
        [struct((rows, half)), struct((rows, cols))],
        [VMEM_SPEC] * 2,
        [
            pltpu.VMEM((rows, half), f32),
            pltpu.VMEM((rows, cols), f32),
            pltpu.VMEM((2, planes, rows, cols), bf16),
            pltpu.VMEM((planes, rows, cols), bf16),
            pltpu.SemaphoreType.DMA((planes,)),
            pltpu.SemaphoreType.DMA((2, planes)),
        ],
    )


def attend_ahead(count, queries, own_pair, own_row, key_cols, ident):
    planes = count // PLANE
    rows, cols = own_pair.shape
    half = cols // 2
    size = 256 if rows % 256 == 0 else rows
    orders, flags = [], []
    for plane in range(planes):
        order = sorted(range(planes), key=lambda source: (abs(source - plane), source))
        away = [abs(source - plane) for source in order] + [-1]
        orders.append(order)
        flags.append([int(i > 0 and away[i] == away[i + 1]) for i in range(planes)])

    def body(q_ref, kv_ref, row_ref, col_ref, all_ref, ctx_ref, log_ref, *rest):
        top, total, send, recv, local = rest
        me = lax.axis_index("shard")
        plane = lax.div(me, PLANE)
        greet([{"shard": lax.rem(me + PLANE * s, count)} for s in range(1, planes)])
        own = pltpu.make_async_copy(kv_ref, all_ref.at[plane], local)
        own.start()
        up, down = plane < planes - 1, plane > 0

        def hop(way, source, src):
            peer = me + PLANE if way == 0 else me - PLANE
            return remote(
                src,
                all_ref.at[source],
                send.at[way, source],
                recv.at[way, source],
                {"shard": lax.rem(peer + count, count)},
            )

        pl.when(up)(hop(0, plane, kv_ref).start)
        pl.when(down)(hop(1, plane, kv_ref).start)
        top[...] = jnp.full(top.shape, very_low, f32)
        total[...] = jnp.zeros(total.shape, f32)
        ctx_ref[...] = jnp.zeros(ctx_ref.shape, f32)

        def take(source, test):
            for way in (0, 1):
                came = source < plane if way == 0 else source > plane
                onward = up if way == 0 else down

                @pl.when(test & came)
                def _(way=way, onward=onward):
                    copy = hop(way, source, all_ref.at[source])
                    copy.wait_recv()
                    pl.when(onward)(copy.start)

        def compute(source, block):
            key_codes = col_ref[source]

            def chunk(index, carry):
                span = pl.ds(pl.multiple_of(index * size, size), size)
                allowed = key_codes == row_ref[0:1, span]
                for head in range(GROUP_HEADS):
                    low, high = head * HEAD_DIM, (head + 1) * HEAD_DIM
                    line = slice(head, head + 1)
                    raw = dot_right(block[:, low:high], q_ref[span, low:high]) * 0.125
                    masked = jnp.where(allowed, raw, very_low)
                    before = top[line, span]
                    after = jnp.maximum(before, jnp.max(masked, axis=0, keepdims=True))
                    rescale = jnp.exp(before - after)
                    weights = jnp.where(allowed, jnp.exp(masked - after), 0.0)
                    top[line, span] = after
                    total[line, span] = total[line, span] * rescale + jnp.sum(
                        weights, axis=0, keepdims=True
                    )
                    added = dot_left(block[:, half + low : half + high], weights.astype(bf16))
                    ctx_ref[low:high, span] = ctx_ref[low:high, span] * rescale + added
                return carry

            lax.fori_loop(0, rows // size, chunk, 0)

        compute(plane, kv_ref)
        sources = [pick(plane, [order[i] for order in orders]) for i in range(planes)]
        early = [pick(plane, [flag[i] for flag in flags]) == 1 for i in range(planes)]
        for index in range(1, planes):
            test = jnp.logical_not(early[index - 1])
            take(sources[index], test)
            if index + 1 < planes:
                take(sources[index + 1], early[index])
            compute(sources[index], all_ref.at[sources[index]])
        log_ref[...] = top[...] + jnp.log(total[...])
        for head in range(GROUP_HEADS):
            low, high = head * HEAD_DIM, (head + 1) * HEAD_DIM
            ctx_ref[low:high] = ctx_ref[low:high] / total[head : head + 1]
        pl.when(up)(hop(0, plane, kv_ref).wait_send)
        pl.when(down)(hop(1, plane, kv_ref).wait_send)
        for index in range(1, planes):
            source = sources[index]
            pl.when((source < plane) & up)(hop(0, source, all_ref.at[source]).wait_send)
            pl.when((source > plane) & down)(hop(1, source, all_ref.at[source]).wait_send)
        own.wait()

    return comm_call(
        body,
        "attend_ahead",
        ident,
        [queries, own_pair, own_row, key_cols],
        [
            struct((planes, rows, cols)),
            struct((half, rows), f32),
            struct((GROUP_HEADS, rows), f32),
        ],
        [VMEM_SPEC] * 3,
        [
            pltpu.VMEM((GROUP_HEADS, rows), f32),
            pltpu.VMEM((GROUP_HEADS, rows), f32),
            pltpu.SemaphoreType.DMA((2, planes)),
            pltpu.SemaphoreType.DMA((2, planes)),
            pltpu.SemaphoreType.DMA,
        ],
    )


def norm_forward(value, gain, shift):
    center = value - jnp.mean(value, axis=-1, keepdims=True)
    spread = jnp.mean(center * center, axis=-1, keepdims=True)
    scale = lax.rsqrt(spread + epsilon)
    normal = center * scale
    return (normal * gain + shift, normal, scale)


def norm_backward(upstream, normal, scale, gain):
    inner = upstream * gain
    return scale * (
        inner
        - jnp.mean(inner, axis=-1, keepdims=True)
        - normal * jnp.mean(inner * normal, axis=-1, keepdims=True)
    )


def gelu_slope(hidden):
    return 0.5 * (1.0 + lax.erf(hidden * root_half)) + hidden * inv_root_tau * jnp.exp(
        -0.5 * hidden * hidden
    )


def dot(left, right):
    return jnp.dot(left, right, preferred_element_type=f32)


def dot_left(left, right):
    return lax.dot_general(left, right, (((0,), (0,)), ((), ())), preferred_element_type=f32)


def dot_right(left, right):
    return lax.dot_general(left, right, (((1,), (1,)), ((), ())), preferred_element_type=f32)


def shards(count, copies, *arrays):
    (
        tokens,
        segments,
        padding,
        query_weight,
        key_weight,
        value_weight,
        query_bias,
        value_bias,
        out_weight,
        out_bias,
        middle_gain,
        middle_shift,
        up_weight,
        up_bias,
        down_weight,
        down_bias,
        final_gain,
        final_shift,
        cotangent,
    ) = arrays
    planes = count // PLANE
    rows = query_weight.shape[0]
    block = down_weight.shape[0]
    x_own = tokens[0]
    here = x_own.shape[0]
    wide = PLANE * here
    me = lax.axis_index("shard")
    group = lax.rem(me, PLANE)
    qkv_send = jnp.concatenate(
        [
            item.astype(bf16).reshape(rows, PLANE, GROUP_DIM)
            for item in (query_weight, key_weight, value_weight)
        ],
        axis=2,
    ).transpose(1, 0, 2)
    up_send = (
        up_weight.astype(bf16)
        .reshape(rows, planes, PLANE, block)
        .transpose(2, 0, 1, 3)
        .reshape(PLANE, rows, GROUP_FF)
    )
    codes = (2 * segments[0] + padding[0]).astype(f32)
    lanes = 128 * ((max(here, block) + 127) // 128)

    def padded(value):
        return jnp.pad(value.astype(f32), (0, lanes - value.shape[0]))

    vectors = [
        query_bias,
        value_bias,
        out_bias,
        middle_gain,
        middle_shift,
        down_bias,
        final_gain,
        final_shift,
        up_bias,
        codes,
    ]
    small_send = jnp.pad(
        jnp.stack([padded(item) for item in vectors]), ((0, 6), (0, 0))
    ).astype(bf16)
    x_all, qkv_all, up_all, wo_all, small = gather_weights(
        count,
        copies,
        x_own,
        qkv_send,
        up_send,
        out_weight.astype(bf16),
        small_send,
        0,
    )
    x_plane = x_all.reshape(wide, D)
    w_qkv = qkv_all.reshape(D, 3 * GROUP_DIM)
    lines = [[start + PLANE * step for step in range(planes)] for start in range(PLANE)]
    strip = jnp.concatenate([up_all.reshape(PLANE * rows, D), down_weight.astype(bf16)], axis=0)
    w_out = wo_all.reshape(GROUP_DIM, D)
    small = small.astype(f32)
    spread = [small[:, index, :rows].reshape(D) for index in range(8)]
    b_query, b_value, b_out, gain_mid, shift_mid, b_down, gain_end, shift_end = spread
    b_up = lax.dynamic_index_in_dim(
        small[:, 8, :block].reshape(planes, PLANE, block), group, 1, keepdims=False
    ).reshape(GROUP_FF)
    all_codes = small[:, 9, :here].reshape(planes, wide)
    own_codes = lax.dynamic_index_in_dim(all_codes, lax.div(me, PLANE), 0, keepdims=False)

    def group_part(value):
        return lax.dynamic_slice(value, (group * GROUP_DIM,), (GROUP_DIM,))

    qkv_bias = jnp.concatenate(
        [group_part(b_query), jnp.zeros((GROUP_DIM,), f32), group_part(b_value)]
    )
    qkv = (dot(x_plane, w_qkv) + qkv_bias).astype(bf16)
    queries = qkv[:, :GROUP_DIM]
    own_row, key_cols = own_codes[None], all_codes[:, :, None]
    pairs, context, logs = attend_ahead(
        count, queries, qkv[:, GROUP_DIM:], own_row, key_cols, 1
    )
    strip, pairs = lax.optimization_barrier((strip, pairs))
    strips = lax.all_gather(strip, "shard", axis_index_groups=lines, axis=0)
    w_up = strips[:, : PLANE * rows].reshape(D, GROUP_FF)
    w_down = strips[:, PLANE * rows :].reshape(GROUP_FF, D)
    context_low = context.astype(bf16)

    def split(value):
        return value.reshape(PLANE, here, D)

    def enter_middle(total, pieces, lines):
        rest = total + lines[0] + pieces[0]
        middle, _, _ = norm_forward(rest, lines[1], lines[2])
        return middle.astype(bf16), [rest], []

    def enter_end(total, pieces, lines):
        middle, _, _ = norm_forward(pieces[0], lines[1], lines[2])
        result, normal, scale = norm_forward(middle + (total + lines[0]), lines[3], lines[4])
        above = pieces[1]
        back = norm_backward(above, normal, scale, lines[3])
        rounded = back.astype(bf16)
        return rounded, [result, back], [above * normal, above, rounded.astype(f32)]

    def leave_middle(total, pieces, lines):
        _, normal, scale = norm_forward(pieces[0], lines[0], lines[0])
        above = total + pieces[1]
        back = norm_backward(above, normal, scale, lines[0])
        rounded = back.astype(bf16)
        return rounded, [back], [above * normal, above, rounded.astype(f32)]

    middle_all, _, rest = plane_step(
        split(dot_left(context_low, w_out).astype(bf16)),
        [x_own],
        [b_out, gain_mid, shift_mid],
        enter_middle,
        [f32],
        2,
    )
    middle_plane = middle_all.reshape(wide, D)
    hidden = dot(middle_plane, w_up) + b_up
    active_low = jax.nn.gelu(hidden, approximate=False).astype(bf16)
    feed_all, end_sums, result, d_second = plane_step(
        split(dot(active_low, w_down).astype(bf16)),
        [rest, cotangent[0]],
        [b_down, gain_mid, shift_mid, gain_end, shift_end],
        enter_end,
        [bf16, f32],
        3,
    )
    output = result[None]
    feed_plane = feed_all.reshape(wide, D)
    grad_down = dot_left(active_low, feed_plane).astype(bf16)
    up_low = (dot_right(feed_plane, w_down) * gelu_slope(hidden)).astype(bf16)
    grad_up = dot_left(middle_plane, up_low).astype(bf16)
    strip_grads = lax.psum_scatter(
        jnp.concatenate(
            [
                grad_up.reshape(planes, PLANE * rows, GROUP_FF),
                grad_down.reshape(planes, block, D),
            ],
            axis=1,
        ),
        "shard",
        axis_index_groups=lines,
        scatter_dimension=0,
    )
    branch_all, middle_sums, d_first = plane_step(
        split(dot_right(up_low, w_up).astype(bf16)),
        [rest, d_second],
        [gain_mid],
        leave_middle,
        [f32],
        4,
    )
    branch_plane = branch_all.reshape(wide, D)
    grad_out = dot(context_low, branch_plane).astype(bf16)
    d_context = dot_right(branch_plane, w_out).astype(bf16)
    delta = jnp.sum(
        (d_context.astype(f32).T * context).reshape(GROUP_HEADS, HEAD_DIM, wide), axis=1
    )
    query_low, pair_low = attend_back(
        count,
        queries,
        d_context,
        pairs,
        own_row,
        key_cols,
        logs,
        delta,
        8,
    )
    mixer_low = jnp.concatenate([query_low, pair_low], axis=1)
    grad_qkv = dot_left(x_plane, mixer_low).astype(bf16)
    mixer_sums = jnp.sum(mixer_low.astype(f32), axis=0)

    def from_group(value):
        return lax.dynamic_update_slice(jnp.zeros((D,), f32), value, (group * GROUP_DIM,))

    sums = [
        from_group(mixer_sums[:GROUP_DIM]),
        from_group(mixer_sums[2 * GROUP_DIM :]),
        middle_sums[2],
        middle_sums[0],
        middle_sums[1],
        end_sums[2],
        end_sums[0],
        end_sums[1],
    ]
    own_lane = (jnp.arange(PLANE) == group).astype(f32)
    up_sums = jnp.sum(up_low.astype(f32), axis=0).reshape(planes, 1, block)
    up_sums = (up_sums * own_lane[None, :, None]).reshape(count, 1, block)
    sums = jnp.stack([item.reshape(count, rows) for item in sums], axis=1)
    small_grads = jnp.concatenate(
        [
            jnp.pad(sums, ((0, 0), (0, 0), (0, lanes - rows))),
            jnp.pad(up_sums, ((0, 0), (0, 7), (0, lanes - block))),
        ],
        axis=1,
    ).astype(bf16)
    qkv_total, up_total, out_total, small_total, down_total, grad_tokens = reduce_grads(
        count,
        copies,
        grad_qkv.reshape(count, rows, 3 * GROUP_DIM),
        strip_grads[: PLANE * rows].reshape(PLANE, rows, GROUP_FF),
        grad_out.reshape(planes, rows, D),
        strip_grads[PLANE * rows :],
        small_grads,
        split(dot_right(mixer_low, w_qkv).astype(bf16)),
        d_first,
        10,
    )

    def joined(value):
        return value.transpose(1, 0, 2).reshape(rows, D)

    up_grad = (
        up_total.reshape(PLANE, rows, planes, block).transpose(1, 2, 0, 3).reshape(rows, FF)
    )
    return (
        output,
        grad_tokens[None],
        joined(qkv_total[:, :, :GROUP_DIM]),
        joined(qkv_total[:, :, GROUP_DIM : 2 * GROUP_DIM]),
        joined(qkv_total[:, :, 2 * GROUP_DIM :]),
        small_total[0, :rows],
        small_total[1, :rows],
        out_total,
        small_total[2, :rows],
        small_total[3, :rows],
        small_total[4, :rows],
        up_grad,
        small_total[8, :block],
        down_total,
        small_total[5, :rows],
        small_total[6, :rows],
        small_total[7, :rows],
    )


def solution(mesh):
    sheet, line = P("shard", None), P("shard")
    batch = P("rep", "shard", None)
    in_specs = (batch, P("rep", "shard"), P("rep", "shard"), sheet, sheet, sheet, line, line)
    in_specs += (sheet, line, line, line, sheet, line, sheet, line, line, line, batch)
    out_specs = (batch, batch, sheet, sheet, sheet, line, line, sheet, line, line, line)
    out_specs += (sheet, line, sheet, line, line, line)
    body = functools.partial(shards, mesh.shape["shard"], mesh.shape["rep"])
    return jax.shard_map(
        body, mesh=mesh, in_specs=in_specs, out_specs=out_specs, check_vma=False
    )
```

```python
import functools

import jax
import jax.numpy as jnp
from jax import lax
from jax.experimental import pallas as pl
from jax.experimental.pallas import tpu as pltpu
from jax.sharding import PartitionSpec as P

D = 768
HEADS = 12
HEAD_DIM = 64
PLANE = 4
GROUP_HEADS = HEADS // PLANE
GROUP_DIM = GROUP_HEADS * HEAD_DIM
FF = 3072
GROUP_FF = FF // PLANE

epsilon = 1e-12
very_low = -1e30
root_half = 0.7071067811865476
inv_root_tau = 0.3989422804014327
bf16 = jnp.bfloat16
f32 = jnp.float32
MESH = pl.DeviceIdType.MESH
VMEM_SPEC = pl.BlockSpec(memory_space=pltpu.VMEM)
ANY_SPEC = pl.BlockSpec(memory_space=pl.ANY)
VMEM_BYTES = 60000 * 1024
MODEL_BYTES = 100_000_000


def struct(shape, dtype=bf16):
    return jax.ShapeDtypeStruct(shape, dtype)


def comm_call(body, name, ident, inputs, out_shapes, out_specs, scratch):
    return pl.pallas_call(
        body,
        name=name,
        out_shape=out_shapes,
        in_specs=[VMEM_SPEC] * len(inputs),
        out_specs=out_specs,
        scratch_shapes=scratch,
        cost_estimate=pl.CostEstimate(flops=0, bytes_accessed=MODEL_BYTES, transcendentals=0),
        compiler_params=pltpu.CompilerParams(
            collective_id=ident, has_side_effects=True, vmem_limit_bytes=VMEM_BYTES
        ),
    )(*inputs)


def greet(peers):
    barrier = pltpu.get_barrier_semaphore()
    for peer in peers:
        pl.semaphore_signal(barrier, inc=1, device_id=peer, device_id_type=MESH)
    pl.semaphore_wait(barrier, len(peers))


def remote(src, dst, send_sem, recv_sem, peer):
    return pltpu.make_async_remote_copy(
        src_ref=src,
        dst_ref=dst,
        send_sem=send_sem,
        recv_sem=recv_sem,
        device_id=peer,
        device_id_type=MESH,
    )


def plane_peer(me, mask):
    group = lax.rem(me, PLANE)
    core = lax.rem(group, 2)
    column = lax.div(group, 2)
    if mask & 1:
        core = 1 - core
    if mask & 2:
        column = 1 - column
    return me - group + 2 * column + core


def plane_slot(me, mask):
    return lax.rem(plane_peer(me, mask), PLANE)


def plane_step(parts, pieces, vectors, action, out_types, ident):
    _, rows, cols = parts.shape
    chunks = 3 if rows % 48 == 0 else 1
    size = rows // chunks
    many, few = len(pieces), len(out_types)

    def body(p_ref, *rest):
        piece_refs, vector_ref = rest[:many], rest[many]
        all_ref, sums_ref = rest[many + 1 : many + 3]
        out_refs = rest[many + 3 : many + 3 + few]
        near, held, far_in, low, send, recv = rest[many + 3 + few :]
        me = lax.axis_index("shard")
        beside, across = [{"shard": plane_peer(me, mask)} for mask in (1, 2)]
        mine, far = lax.rem(me, PLANE), plane_slot(me, 2)
        greet([beside, across])
        spans = [pl.ds(size * index, size) for index in range(chunks)]

        def copy(kind, index):
            span = spans[index]
            table = {
                0: lambda: (p_ref.at[plane_slot(me, 3), span], near.at[0, span], beside),
                1: lambda: (p_ref.at[plane_slot(me, 1), span], near.at[1, span], beside),
                2: lambda: (held.at[span], far_in.at[span], across),
                3: lambda: (low.at[span], all_ref.at[mine, span], across),
                4: lambda: (low.at[span], all_ref.at[mine, span], beside),
                5: lambda: (all_ref.at[far, span], all_ref.at[far, span], beside),
            }
            src, dst, peer = table[kind]()
            return remote(src, dst, send.at[kind, index], recv.at[kind, index], peer)

        for index in range(chunks):
            copy(0, index).start()
        for index in range(chunks):
            copy(1, index).start()
        for index in range(chunks):
            span = spans[index]
            copy(0, index).wait_recv()
            total = p_ref[plane_slot(me, 2), span].astype(f32) + near[0, span].astype(f32)
            held[span] = total.astype(bf16)
            copy(2, index).start()
        lines = [vector_ref[index : index + 1] for index in range(len(vectors))]
        sums = None
        for index in range(chunks):
            span = spans[index]
            copy(1, index).wait_recv()
            copy(2, index).wait_recv()
            total = p_ref[mine, span].astype(f32) + near[1, span].astype(f32)
            total = total + far_in[span].astype(f32)
            result, outs, terms = action(
                total, [item[span].astype(f32) for item in piece_refs], lines
            )
            low[span] = result
            copy(3, index).start()
            copy(4, index).start()
            for ref, value in zip(out_refs, outs):
                ref[span] = value.astype(ref.dtype)
            all_ref[mine, span] = result
            terms = [jnp.sum(item, axis=0, keepdims=True) for item in terms]
            sums = terms if sums is None else [x + y for x, y in zip(sums, terms)]
        sums_ref[...] = jnp.zeros(sums_ref.shape, f32)
        for place, value in enumerate(sums):
            sums_ref[place : place + 1] = value
        for index in range(chunks):
            copy(3, index).wait_recv()
            copy(5, index).start()
        for index in range(chunks):
            copy(4, index).wait_recv()
            copy(5, index).wait_recv()
        for index in range(chunks):
            for kind in range(6):
                copy(kind, index).wait_send()

    stack = jnp.stack(vectors)
    shape = (rows, cols)
    return comm_call(
        body,
        "plane_step",
        ident,
        [parts] + list(pieces) + [stack],
        [struct((PLANE, rows, cols)), struct((8, cols), f32)]
        + [struct(shape, item) for item in out_types],
        [VMEM_SPEC] * (2 + few),
        [
            pltpu.VMEM((2, rows, cols), bf16),
            pltpu.VMEM(shape, bf16),
            pltpu.VMEM(shape, bf16),
            pltpu.VMEM(shape, bf16),
            pltpu.SemaphoreType.DMA((6, chunks)),
            pltpu.SemaphoreType.DMA((6, chunks)),
        ],
    )


def others(me, count):
    return [{"shard": lax.rem(me + step, count)} for step in range(1, count)]


def gather_weights(count, copies, tokens, qkv, up, out_w, small, ident):
    planes = count // PLANE
    rows = qkv.shape[1]

    def body(x_ref, qkv_ref, up_ref, wo_ref, small_ref, *rest):
        x_out, qkv_out, up_out, wo_out, small_out = rest[:5]
        send, recv, local, send_wo, recv_wo, send_unit, recv_unit = rest[5:]
        me = lax.axis_index("shard")
        group, plane = lax.rem(me, PLANE), lax.div(me, PLANE)
        across = [
            {"rep": lax.rem(lax.axis_index("rep") + step, copies)} for step in range(1, copies)
        ]
        greet(others(me, count) + across)
        owns = [
            (x_ref, x_out.at[group]),
            (qkv_ref.at[group], qkv_out.at[me]),
            (up_ref.at[group], up_out.at[group]),
            (small_ref, small_out.at[me]),
        ]
        started = []
        for index, (src, dst) in enumerate(owns):
            copy = pltpu.make_async_copy(src, dst, local.at[index])
            copy.start()
            started.append(copy)
        sent = []

        def push(src, dst, peer):
            index = len(sent)
            copy = remote(src, dst, send.at[index], recv.at[index], {"shard": peer})
            copy.start()
            sent.append(copy)

        for mask in (2, 1):
            push(x_ref, x_out.at[group], plane_peer(me, mask))
        far = plane_slot(me, 2)
        x_relay = remote(
            x_out.at[far], x_out.at[far], send.at[2], recv.at[2], {"shard": plane_peer(me, 1)}
        )
        sent.append(x_relay)
        for step in range(1, count):
            push(small_ref, small_out.at[me], lax.rem(me + step, count))
        rep = lax.axis_index("rep")
        split = copies == 2
        units = []
        for step in range(planes):
            for lane in range(PLANE):
                if step or lane:
                    units.append((qkv_ref, qkv_out, step, lane))
        for lane in range(1, PLANE):
            units.append((up_ref, up_out, 0, lane))

        def unit_copy(index):
            src, dst, step, lane = units[index]
            goal = lax.rem(plane + step, planes)
            goal_group = lax.rem(group + lane, PLANE)
            slot = group if src is up_ref else me
            return remote(
                src.at[goal_group],
                dst.at[slot],
                send_unit.at[index],
                recv_unit.at[index],
                {"shard": goal * PLANE + goal_group},
            )

        def unit_relay(index):
            src, dst, step, lane = units[index]
            origin = lax.rem(plane + planes - step, planes)
            origin_group = lax.rem(group + PLANE - lane, PLANE)
            slot = origin_group if src is up_ref else origin * PLANE + origin_group
            return remote(
                dst.at[slot],
                dst.at[slot],
                send_unit.at[index],
                recv_unit.at[index],
                {"rep": lax.rem(rep + 1, copies)},
            )

        def carried(index, mine):
            step = units[index][2]
            if not split or step == 0:
                return None
            return (rep == step % 2) if mine else (rep != step % 2)

        def guarded(test, action):
            if test is None:
                action()
            else:
                pl.when(test)(action)

        for index in range(len(units)):
            guarded(carried(index, True), unit_copy(index).start)
        target, place = lax.div(me, planes), lax.rem(me, planes)

        def wo_copy(source, index):
            peer = PLANE * index + target
            return peer, remote(
                wo_ref, wo_out.at[place], send_wo.at[index], recv_wo.at[source], {"shard": peer}
            )

        for index in range(planes):
            peer, copy = wo_copy(place, index)
            pl.when(peer != me)(copy.start)
        keep = pltpu.make_async_copy(wo_ref, wo_out.at[place], local.at[5])
        pl.when(target == group)(keep.start)
        sent[0].wait_recv()
        x_relay.start()
        for index, (_, _, step, _) in enumerate(units):
            if split and step:

                @pl.when(rep == step % 2)
                def _(index=index):
                    unit_relay(index).wait_recv()
                    unit_copy(index).wait_send()
                    unit_relay(index).start()

            else:
                unit_copy(index).wait_recv()
                unit_copy(index).wait_send()
        for index, (_, _, step, _) in enumerate(units):
            if split and step:
                pl.when(rep != step % 2)(unit_relay(index).wait_recv)
                pl.when(rep == step % 2)(unit_relay(index).wait_send)
        for copy in sent[1:]:
            copy.wait_recv()
        for index in range(planes):
            pl.when(group * planes + index != me)(wo_copy(index, index)[1].wait_recv)
        for index in range(planes):
            peer, copy = wo_copy(place, index)
            pl.when(peer != me)(copy.wait_send)
        pl.when(target == group)(keep.wait)
        for copy in sent:
            copy.wait_send()
        for copy in started:
            copy.wait()

    total = 3 + count - 1
    number = count - 1 + PLANE - 1
    return comm_call(
        body,
        "gather_weights",
        ident,
        [tokens, qkv, up, out_w, small],
        [
            struct((PLANE,) + tokens.shape),
            struct((count, rows, qkv.shape[2])),
            struct((PLANE, rows, up.shape[2])),
            struct((planes,) + out_w.shape),
            struct((count,) + small.shape),
        ],
        [ANY_SPEC] * 5,
        [
            pltpu.SemaphoreType.DMA((total,)),
            pltpu.SemaphoreType.DMA((total,)),
            pltpu.SemaphoreType.DMA((6,)),
            pltpu.SemaphoreType.DMA((planes,)),
            pltpu.SemaphoreType.DMA((planes,)),
            pltpu.SemaphoreType.DMA((number,)),
            pltpu.SemaphoreType.DMA((number,)),
        ],
    )


def reduce_grads(count, copies, qkv, up, out_w, down, small, parts, first_grad, ident):
    planes = count // PLANE
    rows = qkv.shape[1]
    block = down.shape[0]
    arrays = [qkv, up, out_w, small]

    def body(qkv_ref, up_ref, wo_ref, small_ref, down_ref, p_ref, first_ref, *rest):
        outs, token_ref, rest = rest[:5], rest[5], rest[6:]
        qkv_in, up_in, wo_in, small_in = rest[:4]
        halves, gets = [rest[4], up_in, rest[5], rest[6], down_ref], rest[7:12]
        near, near_sum, far_in = rest[12:15]
        send, recv, send_rep, recv_rep, send_wo, recv_wo, send_near, recv_near = rest[15:]
        me = lax.axis_index("shard")
        rep = lax.axis_index("rep")
        plane = lax.div(me, PLANE)
        across = [{"rep": lax.rem(rep + step, copies)} for step in range(1, copies)]
        greet(others(me, count) + across)
        sent = []

        def push(src, dst, peer):
            index = len(sent)
            copy = remote(src, dst, send.at[index], recv.at[index], {"shard": peer})
            copy.start()
            sent.append(copy)

        pairs = [(qkv_ref, qkv_in), (small_ref, small_in)]
        passed = []
        beside, over = [{"shard": plane_peer(me, mask)} for mask in (1, 2)]
        near_copies = [
            remote(p_ref.at[plane_slot(me, 3)], near.at[0], send_near.at[0], recv_near.at[0], beside),
            remote(p_ref.at[plane_slot(me, 1)], near.at[1], send_near.at[1], recv_near.at[1], beside),
            remote(near_sum, far_in, send_near.at[2], recv_near.at[2], over),
        ]
        near_copies[0].start()
        near_copies[1].start()

        def exchange(*places):
            for index, peer in enumerate(across):
                for place in places:
                    copy = remote(
                        halves[place],
                        gets[place].at[index],
                        send_rep.at[5 * index + place],
                        recv_rep.at[5 * index + place],
                        peer,
                    )
                    copy.start()
                    passed.append(copy)

        exchange(4)
        group = lax.rem(me, PLANE)
        target, place = lax.div(me, planes), lax.rem(me, planes)
        for lane in range(1, PLANE):
            goal = lax.rem(group + lane, PLANE)
            push(up_ref.at[goal], up_in.at[group], plane * PLANE + goal)
        up_in[group] = up_ref[group]
        for src, held in pairs:
            for step in range(1, count):
                peer = lax.rem(me + step, count)
                push(src.at[peer], held.at[me], peer)
        for src, held in pairs:
            held[me] = src[me]

        def wo_copy(source, index):
            peer = group * planes + index
            return peer, remote(
                wo_ref.at[index],
                wo_in.at[plane],
                send_wo.at[index],
                recv_wo.at[source],
                {"shard": peer},
            )

        for index in range(planes):
            peer, copy = wo_copy(plane, index)
            pl.when(peer != me)(copy.start)

        @pl.when(target == group)
        def _():
            wo_in[plane] = wo_ref[place]

        near_copies[0].wait_recv()
        total = p_ref[plane_slot(me, 2)].astype(f32) + near[0].astype(f32)
        near_sum[...] = total.astype(bf16)
        near_copies[2].start()
        for copy in sent[: PLANE - 1]:
            copy.wait_recv()
        exchange(1)
        for index in range(planes):
            pl.when(PLANE * index + target != me)(wo_copy(index, index)[1].wait_recv)
        for index in range(planes):
            peer, copy = wo_copy(plane, index)
            pl.when(peer != me)(copy.wait_send)
        total = wo_in[0].astype(f32)
        for other in range(1, planes):
            total = total + wo_in[other].astype(f32)
        halves[2][...] = total.astype(bf16)
        exchange(2)
        near_copies[1].wait_recv()
        near_copies[2].wait_recv()
        total = p_ref[lax.rem(me, PLANE)].astype(f32) + near[1].astype(f32)
        total = total + far_in[...].astype(f32) + first_ref[...]
        token_ref[...] = total.astype(bf16)
        for copy in sent[PLANE - 1 :]:
            copy.wait_recv()
        for half, held in zip(halves[:1], (qkv_in,)):
            for lane in range(PLANE):
                total = held[lane].astype(f32)
                for other in range(1, planes):
                    total = total + held[other * PLANE + lane].astype(f32)
                half[lane] = total.astype(bf16)
        for half, held, number in (
            (halves[3], small_in, count),
        ):
            total = held[0].astype(f32)
            for other in range(1, number):
                total = total + held[other].astype(f32)
            half[...] = total.astype(bf16)
        exchange(0, 3)
        for copy in passed:
            copy.wait_recv()
        for out, half, got in zip(outs, halves, gets):
            total = half[...].astype(f32)
            for index in range(copies - 1):
                total = total + got[index].astype(f32)
            out[...] = total
        for copy in sent + passed + near_copies:
            copy.wait_send()

    totals = 2 * (count - 1) + PLANE - 1
    shapes = [
        (PLANE, rows, qkv.shape[2]),
        (PLANE, rows, up.shape[2]),
        (rows, D),
        small.shape[1:],
        (block, D),
    ]
    return comm_call(
        body,
        "reduce_grads",
        ident,
        arrays + [down, parts, first_grad],
        [struct(shape, f32) for shape in shapes] + [struct(parts.shape[1:])],
        [VMEM_SPEC] * 6,
        [pltpu.VMEM(item.shape, bf16) for item in arrays]
        + [pltpu.VMEM(shapes[index], bf16) for index in (0, 2, 3)]
        + [pltpu.VMEM((copies - 1,) + shape, bf16) for shape in shapes]
        + [
            pltpu.VMEM((2,) + parts.shape[1:], bf16),
            pltpu.VMEM(parts.shape[1:], bf16),
            pltpu.VMEM(parts.shape[1:], bf16),
            pltpu.SemaphoreType.DMA((totals,)),
            pltpu.SemaphoreType.DMA((totals,)),
            pltpu.SemaphoreType.DMA((5 * (copies - 1),)),
            pltpu.SemaphoreType.DMA((5 * (copies - 1),)),
            pltpu.SemaphoreType.DMA((planes,)),
            pltpu.SemaphoreType.DMA((planes,)),
            pltpu.SemaphoreType.DMA((3,)),
            pltpu.SemaphoreType.DMA((3,)),
        ],
    )


def pick(plane, table):
    value = table[-1]
    for index in range(len(table) - 1):
        value = jnp.where(plane == index, table[index], value)
    return value


def attend_back(count, queries, upstream, pairs, own_row, key_cols, logs, delta, ident):
    planes, rows, cols = pairs.shape
    half = cols // 2
    size = 256 if rows % 256 == 0 else rows
    orders = []
    for plane in range(planes):
        goals = [goal for goal in range(planes) if goal != plane]
        goals.sort(key=lambda goal: (-abs(goal - plane), goal))
        orders.append(goals + [plane])

    def body(q_ref, up_ref, kv_ref, row_ref, col_ref, log_ref, delta_ref, *rest):
        dq_ref, out_ref, dq_sum, part, held, staged, send, recv = rest
        me = lax.axis_index("shard")
        plane = lax.div(me, PLANE)
        greet([{"shard": lax.rem(me + PLANE * s, count)} for s in range(1, planes)])
        dq_sum[...] = jnp.zeros(dq_sum.shape, f32)

        def hop(way, goal):
            peer = me + PLANE if way == 0 else me - PLANE
            return remote(
                staged.at[goal],
                held.at[way, goal],
                send.at[goal],
                recv.at[way, goal],
                {"shard": lax.rem(peer + count, count)},
            )

        def compute(goal):
            part[...] = jnp.zeros(part.shape, f32)
            key_codes = col_ref[goal]

            def chunk(index, carry):
                at = pl.multiple_of(index * size, size)
                span = pl.ds(at, size)
                allowed = key_codes == row_ref[0:1, span]
                for head in range(GROUP_HEADS):
                    low, high = head * HEAD_DIM, (head + 1) * HEAD_DIM
                    q = q_ref[span, low:high]
                    g = up_ref[span, low:high]
                    k = kv_ref[goal, :, low:high]
                    v = kv_ref[goal, :, half + low : half + high]
                    raw = dot_right(k, q) * 0.125
                    chances = jnp.where(
                        allowed, jnp.exp(raw - log_ref[head : head + 1, span]), 0.0
                    )
                    d_chance = dot_right(v, g)
                    d_score = (chances * (d_chance - delta_ref[head : head + 1, span])).astype(bf16)
                    dq_sum[span, low:high] += dot_left(d_score, k)
                    part[:, low:high] += dot(d_score, q) * 0.125
                    part[:, half + low : half + high] += dot(chances.astype(bf16), g)
                return carry

            lax.fori_loop(0, rows // size, chunk, 0)

        def pass_on(goal):
            for way in (0, 1):
                ahead = goal > plane if way == 0 else goal < plane
                first = plane == 0 if way == 0 else plane == planes - 1

                @pl.when(ahead & jnp.logical_not(first))
                def _(way=way):
                    copy = hop(way, goal)
                    copy.wait_recv()
                    total = staged[goal].astype(f32) + held[way, goal].astype(f32)
                    staged[goal] = total.astype(bf16)
                    copy.start()

        def begin(goal):
            for way in (0, 1):
                ahead = goal > plane if way == 0 else goal < plane
                first = plane == 0 if way == 0 else plane == planes - 1

                @pl.when(ahead & first)
                def _(way=way):
                    hop(way, goal).start()

        goals = [pick(plane, [order[i] for order in orders]) for i in range(planes)]
        for index in range(planes):
            goal = goals[index]
            compute(goal)
            if index < planes - 1:
                staged[goal] = part[...].astype(bf16)
                begin(goal)
            if index:
                pass_on(goals[index - 1])
        dq_ref[...] = (dq_sum[...] * 0.125).astype(bf16)
        for way in (0, 1):
            behind = plane > 0 if way == 0 else plane < planes - 1

            @pl.when(behind)
            def _(way=way):
                hop(way, plane).wait_recv()
                part[...] += held[way, plane].astype(f32)

        out_ref[...] = part[...].astype(bf16)
        for index in range(planes - 1):
            hop(0, goals[index]).wait_send()

    return comm_call(
        body,
        "attend_back",
        ident,
        [queries, upstream, pairs, own_row, key_cols, logs, delta],
        [struct((rows, half)), struct((rows, cols))],
        [VMEM_SPEC] * 2,
        [
            pltpu.VMEM((rows, half), f32),
            pltpu.VMEM((rows, cols), f32),
            pltpu.VMEM((2, planes, rows, cols), bf16),
            pltpu.VMEM((planes, rows, cols), bf16),
            pltpu.SemaphoreType.DMA((planes,)),
            pltpu.SemaphoreType.DMA((2, planes)),
        ],
    )


def attend_ahead(count, queries, own_pair, own_row, key_cols, ident):
    planes = count // PLANE
    rows, cols = own_pair.shape
    half = cols // 2
    size = 256 if rows % 256 == 0 else rows
    orders, flags = [], []
    for plane in range(planes):
        order = sorted(range(planes), key=lambda source: (abs(source - plane), source))
        away = [abs(source - plane) for source in order] + [-1]
        orders.append(order)
        flags.append([int(i > 0 and away[i] == away[i + 1]) for i in range(planes)])

    def body(q_ref, kv_ref, row_ref, col_ref, all_ref, ctx_ref, log_ref, *rest):
        top, total, send, recv, local = rest
        me = lax.axis_index("shard")
        plane = lax.div(me, PLANE)
        greet([{"shard": lax.rem(me + PLANE * s, count)} for s in range(1, planes)])
        own = pltpu.make_async_copy(kv_ref, all_ref.at[plane], local)
        own.start()
        up, down = plane < planes - 1, plane > 0

        def hop(way, source, src):
            peer = me + PLANE if way == 0 else me - PLANE
            return remote(
                src,
                all_ref.at[source],
                send.at[way, source],
                recv.at[way, source],
                {"shard": lax.rem(peer + count, count)},
            )

        pl.when(up)(hop(0, plane, kv_ref).start)
        pl.when(down)(hop(1, plane, kv_ref).start)
        top[...] = jnp.full(top.shape, very_low, f32)
        total[...] = jnp.zeros(total.shape, f32)
        ctx_ref[...] = jnp.zeros(ctx_ref.shape, f32)

        def take(source, test):
            for way in (0, 1):
                came = source < plane if way == 0 else source > plane
                onward = up if way == 0 else down

                @pl.when(test & came)
                def _(way=way, onward=onward):
                    copy = hop(way, source, all_ref.at[source])
                    copy.wait_recv()
                    pl.when(onward)(copy.start)

        def compute(source, block):
            key_codes = col_ref[source]

            def chunk(index, carry):
                span = pl.ds(pl.multiple_of(index * size, size), size)
                allowed = key_codes == row_ref[0:1, span]
                for head in range(GROUP_HEADS):
                    low, high = head * HEAD_DIM, (head + 1) * HEAD_DIM
                    line = slice(head, head + 1)
                    raw = dot_right(block[:, low:high], q_ref[span, low:high]) * 0.125
                    masked = jnp.where(allowed, raw, very_low)
                    before = top[line, span]
                    after = jnp.maximum(before, jnp.max(masked, axis=0, keepdims=True))
                    rescale = jnp.exp(before - after)
                    weights = jnp.where(allowed, jnp.exp(masked - after), 0.0)
                    top[line, span] = after
                    total[line, span] = total[line, span] * rescale + jnp.sum(
                        weights, axis=0, keepdims=True
                    )
                    added = dot_left(block[:, half + low : half + high], weights.astype(bf16))
                    ctx_ref[low:high, span] = ctx_ref[low:high, span] * rescale + added
                return carry

            lax.fori_loop(0, rows // size, chunk, 0)

        compute(plane, kv_ref)
        sources = [pick(plane, [order[i] for order in orders]) for i in range(planes)]
        early = [pick(plane, [flag[i] for flag in flags]) == 1 for i in range(planes)]
        for index in range(1, planes):
            test = jnp.logical_not(early[index - 1])
            take(sources[index], test)
            if index + 1 < planes:
                take(sources[index + 1], early[index])
            compute(sources[index], all_ref.at[sources[index]])
        log_ref[...] = top[...] + jnp.log(total[...])
        for head in range(GROUP_HEADS):
            low, high = head * HEAD_DIM, (head + 1) * HEAD_DIM
            ctx_ref[low:high] = ctx_ref[low:high] / total[head : head + 1]
        pl.when(up)(hop(0, plane, kv_ref).wait_send)
        pl.when(down)(hop(1, plane, kv_ref).wait_send)
        for index in range(1, planes):
            source = sources[index]
            pl.when((source < plane) & up)(hop(0, source, all_ref.at[source]).wait_send)
            pl.when((source > plane) & down)(hop(1, source, all_ref.at[source]).wait_send)
        own.wait()

    return comm_call(
        body,
        "attend_ahead",
        ident,
        [queries, own_pair, own_row, key_cols],
        [
            struct((planes, rows, cols)),
            struct((half, rows), f32),
            struct((GROUP_HEADS, rows), f32),
        ],
        [VMEM_SPEC] * 3,
        [
            pltpu.VMEM((GROUP_HEADS, rows), f32),
            pltpu.VMEM((GROUP_HEADS, rows), f32),
            pltpu.SemaphoreType.DMA((2, planes)),
            pltpu.SemaphoreType.DMA((2, planes)),
            pltpu.SemaphoreType.DMA,
        ],
    )


def norm_forward(value, gain, shift):
    center = value - jnp.mean(value, axis=-1, keepdims=True)
    spread = jnp.mean(center * center, axis=-1, keepdims=True)
    scale = lax.rsqrt(spread + epsilon)
    normal = center * scale
    return (normal * gain + shift, normal, scale)


def norm_backward(upstream, normal, scale, gain):
    inner = upstream * gain
    return scale * (
        inner
        - jnp.mean(inner, axis=-1, keepdims=True)
        - normal * jnp.mean(inner * normal, axis=-1, keepdims=True)
    )


def gelu_slope(hidden):
    return 0.5 * (1.0 + lax.erf(hidden * root_half)) + hidden * inv_root_tau * jnp.exp(
        -0.5 * hidden * hidden
    )


def dot(left, right):
    return jnp.dot(left, right, preferred_element_type=f32)


def dot_left(left, right):
    return lax.dot_general(left, right, (((0,), (0,)), ((), ())), preferred_element_type=f32)


def dot_right(left, right):
    return lax.dot_general(left, right, (((1,), (1,)), ((), ())), preferred_element_type=f32)


def shards(count, copies, *arrays):
    (
        tokens,
        segments,
        padding,
        query_weight,
        key_weight,
        value_weight,
        query_bias,
        value_bias,
        out_weight,
        out_bias,
        middle_gain,
        middle_shift,
        up_weight,
        up_bias,
        down_weight,
        down_bias,
        final_gain,
        final_shift,
        cotangent,
    ) = arrays
    planes = count // PLANE
    rows = query_weight.shape[0]
    block = down_weight.shape[0]
    x_own = tokens[0]
    here = x_own.shape[0]
    wide = PLANE * here
    me = lax.axis_index("shard")
    group = lax.rem(me, PLANE)
    qkv_send = jnp.concatenate(
        [
            item.astype(bf16).reshape(rows, PLANE, GROUP_DIM)
            for item in (query_weight, key_weight, value_weight)
        ],
        axis=2,
    ).transpose(1, 0, 2)
    up_send = (
        up_weight.astype(bf16)
        .reshape(rows, planes, PLANE, block)
        .transpose(2, 0, 1, 3)
        .reshape(PLANE, rows, GROUP_FF)
    )
    codes = (2 * segments[0] + padding[0]).astype(f32)
    lanes = 128 * ((max(here, block) + 127) // 128)

    def padded(value):
        return jnp.pad(value.astype(f32), (0, lanes - value.shape[0]))

    vectors = [
        query_bias,
        value_bias,
        out_bias,
        middle_gain,
        middle_shift,
        down_bias,
        final_gain,
        final_shift,
        up_bias,
        codes,
    ]
    small_send = jnp.pad(
        jnp.stack([padded(item) for item in vectors]), ((0, 6), (0, 0))
    ).astype(bf16)
    lines = [[start + PLANE * step for step in range(planes)] for start in range(PLANE)]
    w_down = lax.all_gather(
        down_weight.astype(bf16), "shard", axis_index_groups=lines, axis=0
    ).reshape(GROUP_FF, D)
    x_all, qkv_all, up_all, wo_all, small = gather_weights(
        count,
        copies,
        x_own,
        qkv_send,
        up_send,
        out_weight.astype(bf16),
        small_send,
        0,
    )
    x_plane = x_all.reshape(wide, D)
    w_qkv = qkv_all.reshape(D, 3 * GROUP_DIM)
    strip = up_all.reshape(PLANE * rows, D)
    w_out = wo_all.reshape(GROUP_DIM, D)
    small = small.astype(f32)
    spread = [small[:, index, :rows].reshape(D) for index in range(8)]
    b_query, b_value, b_out, gain_mid, shift_mid, b_down, gain_end, shift_end = spread
    b_up = lax.dynamic_index_in_dim(
        small[:, 8, :block].reshape(planes, PLANE, block), group, 1, keepdims=False
    ).reshape(GROUP_FF)
    all_codes = small[:, 9, :here].reshape(planes, wide)
    own_codes = lax.dynamic_index_in_dim(all_codes, lax.div(me, PLANE), 0, keepdims=False)

    def group_part(value):
        return lax.dynamic_slice(value, (group * GROUP_DIM,), (GROUP_DIM,))

    qkv_bias = jnp.concatenate(
        [group_part(b_query), jnp.zeros((GROUP_DIM,), f32), group_part(b_value)]
    )
    qkv = (dot(x_plane, w_qkv) + qkv_bias).astype(bf16)
    w_down, qkv = lax.optimization_barrier((w_down, qkv))
    queries = qkv[:, :GROUP_DIM]
    own_row, key_cols = own_codes[None], all_codes[:, :, None]
    pairs, context, logs = attend_ahead(
        count, queries, qkv[:, GROUP_DIM:], own_row, key_cols, 1
    )
    strip, pairs = lax.optimization_barrier((strip, pairs))
    w_up = lax.all_gather(strip, "shard", axis_index_groups=lines, axis=0).reshape(D, GROUP_FF)
    context_low = context.astype(bf16)

    def split(value):
        return value.reshape(PLANE, here, D)

    def enter_middle(total, pieces, lines):
        rest = total + lines[0] + pieces[0]
        middle, _, _ = norm_forward(rest, lines[1], lines[2])
        return middle.astype(bf16), [rest], []

    def enter_end(total, pieces, lines):
        middle, _, _ = norm_forward(pieces[0], lines[1], lines[2])
        result, normal, scale = norm_forward(middle + (total + lines[0]), lines[3], lines[4])
        above = pieces[1]
        back = norm_backward(above, normal, scale, lines[3])
        rounded = back.astype(bf16)
        return rounded, [result, back], [above * normal, above, rounded.astype(f32)]

    def leave_middle(total, pieces, lines):
        _, normal, scale = norm_forward(pieces[0], lines[0], lines[0])
        above = total + pieces[1]
        back = norm_backward(above, normal, scale, lines[0])
        rounded = back.astype(bf16)
        return rounded, [back], [above * normal, above, rounded.astype(f32)]

    middle_all, _, rest = plane_step(
        split(dot_left(context_low, w_out).astype(bf16)),
        [x_own],
        [b_out, gain_mid, shift_mid],
        enter_middle,
        [f32],
        2,
    )
    middle_plane = middle_all.reshape(wide, D)
    hidden = dot(middle_plane, w_up) + b_up
    active_low = jax.nn.gelu(hidden, approximate=False).astype(bf16)
    feed_all, end_sums, result, d_second = plane_step(
        split(dot(active_low, w_down).astype(bf16)),
        [rest, cotangent[0]],
        [b_down, gain_mid, shift_mid, gain_end, shift_end],
        enter_end,
        [bf16, f32],
        3,
    )
    output = result[None]
    feed_plane = feed_all.reshape(wide, D)
    grad_down = dot_left(active_low, feed_plane).astype(bf16)
    up_low = (dot_right(feed_plane, w_down) * gelu_slope(hidden)).astype(bf16)
    grad_up = dot_left(middle_plane, up_low).astype(bf16)
    strip_grads = lax.psum_scatter(
        jnp.concatenate(
            [
                grad_up.reshape(planes, PLANE * rows, GROUP_FF),
                grad_down.reshape(planes, block, D),
            ],
            axis=1,
        ),
        "shard",
        axis_index_groups=lines,
        scatter_dimension=0,
    )
    branch_all, middle_sums, d_first = plane_step(
        split(dot_right(up_low, w_up).astype(bf16)),
        [rest, d_second],
        [gain_mid],
        leave_middle,
        [f32],
        4,
    )
    branch_plane = branch_all.reshape(wide, D)
    grad_out = dot(context_low, branch_plane).astype(bf16)
    d_context = dot_right(branch_plane, w_out).astype(bf16)
    delta = jnp.sum(
        (d_context.astype(f32).T * context).reshape(GROUP_HEADS, HEAD_DIM, wide), axis=1
    )
    query_low, pair_low = attend_back(
        count,
        queries,
        d_context,
        pairs,
        own_row,
        key_cols,
        logs,
        delta,
        8,
    )
    mixer_low = jnp.concatenate([query_low, pair_low], axis=1)
    grad_qkv = dot_left(x_plane, mixer_low).astype(bf16)
    mixer_sums = jnp.sum(mixer_low.astype(f32), axis=0)

    def from_group(value):
        return lax.dynamic_update_slice(jnp.zeros((D,), f32), value, (group * GROUP_DIM,))

    sums = [
        from_group(mixer_sums[:GROUP_DIM]),
        from_group(mixer_sums[2 * GROUP_DIM :]),
        middle_sums[2],
        middle_sums[0],
        middle_sums[1],
        end_sums[2],
        end_sums[0],
        end_sums[1],
    ]
    own_lane = (jnp.arange(PLANE) == group).astype(f32)
    up_sums = jnp.sum(up_low.astype(f32), axis=0).reshape(planes, 1, block)
    up_sums = (up_sums * own_lane[None, :, None]).reshape(count, 1, block)
    sums = jnp.stack([item.reshape(count, rows) for item in sums], axis=1)
    small_grads = jnp.concatenate(
        [
            jnp.pad(sums, ((0, 0), (0, 0), (0, lanes - rows))),
            jnp.pad(up_sums, ((0, 0), (0, 7), (0, lanes - block))),
        ],
        axis=1,
    ).astype(bf16)
    qkv_total, up_total, out_total, small_total, down_total, grad_tokens = reduce_grads(
        count,
        copies,
        grad_qkv.reshape(count, rows, 3 * GROUP_DIM),
        strip_grads[: PLANE * rows].reshape(PLANE, rows, GROUP_FF),
        grad_out.reshape(planes, rows, D),
        strip_grads[PLANE * rows :],
        small_grads,
        split(dot_right(mixer_low, w_qkv).astype(bf16)),
        d_first,
        10,
    )

    def joined(value):
        return value.transpose(1, 0, 2).reshape(rows, D)

    up_grad = (
        up_total.reshape(PLANE, rows, planes, block).transpose(1, 2, 0, 3).reshape(rows, FF)
    )
    return (
        output,
        grad_tokens[None],
        joined(qkv_total[:, :, :GROUP_DIM]),
        joined(qkv_total[:, :, GROUP_DIM : 2 * GROUP_DIM]),
        joined(qkv_total[:, :, 2 * GROUP_DIM :]),
        small_total[0, :rows],
        small_total[1, :rows],
        out_total,
        small_total[2, :rows],
        small_total[3, :rows],
        small_total[4, :rows],
        up_grad,
        small_total[8, :block],
        down_total,
        small_total[5, :rows],
        small_total[6, :rows],
        small_total[7, :rows],
    )


def solution(mesh):
    sheet, line = P("shard", None), P("shard")
    batch = P("rep", "shard", None)
    in_specs = (batch, P("rep", "shard"), P("rep", "shard"), sheet, sheet, sheet, line, line)
    in_specs += (sheet, line, line, line, sheet, line, sheet, line, line, line, batch)
    out_specs = (batch, batch, sheet, sheet, sheet, line, line, sheet, line, line, line)
    out_specs += (sheet, line, sheet, line, line, line)
    body = functools.partial(shards, mesh.shape["shard"], mesh.shape["rep"])
    return jax.shard_map(
        body, mesh=mesh, in_specs=in_specs, out_specs=out_specs, check_vma=False
    )
```

```python
import functools

import jax
import jax.numpy as jnp
from jax import lax
from jax.experimental import pallas as pl
from jax.experimental.pallas import tpu as pltpu
from jax.sharding import PartitionSpec as P

D = 768
HEADS = 12
HEAD_DIM = 64
PLANE = 4
GROUP_HEADS = HEADS // PLANE
GROUP_DIM = GROUP_HEADS * HEAD_DIM
FF = 3072
GROUP_FF = FF // PLANE

epsilon = 1e-12
very_low = -1e30
root_half = 0.7071067811865476
inv_root_tau = 0.3989422804014327
bf16 = jnp.bfloat16
f32 = jnp.float32
MESH = pl.DeviceIdType.MESH
VMEM_SPEC = pl.BlockSpec(memory_space=pltpu.VMEM)
ANY_SPEC = pl.BlockSpec(memory_space=pl.ANY)
VMEM_BYTES = 60000 * 1024
MODEL_BYTES = 100_000_000


def struct(shape, dtype=bf16):
    return jax.ShapeDtypeStruct(shape, dtype)


def comm_call(body, name, ident, inputs, out_shapes, out_specs, scratch):
    return pl.pallas_call(
        body,
        name=name,
        out_shape=out_shapes,
        in_specs=[VMEM_SPEC] * len(inputs),
        out_specs=out_specs,
        scratch_shapes=scratch,
        cost_estimate=pl.CostEstimate(flops=0, bytes_accessed=MODEL_BYTES, transcendentals=0),
        compiler_params=pltpu.CompilerParams(
            collective_id=ident, has_side_effects=True, vmem_limit_bytes=VMEM_BYTES
        ),
    )(*inputs)


def greet(peers):
    barrier = pltpu.get_barrier_semaphore()
    for peer in peers:
        pl.semaphore_signal(barrier, inc=1, device_id=peer, device_id_type=MESH)
    pl.semaphore_wait(barrier, len(peers))


def remote(src, dst, send_sem, recv_sem, peer):
    return pltpu.make_async_remote_copy(
        src_ref=src,
        dst_ref=dst,
        send_sem=send_sem,
        recv_sem=recv_sem,
        device_id=peer,
        device_id_type=MESH,
    )


def plane_peer(me, mask):
    group = lax.rem(me, PLANE)
    core = lax.rem(group, 2)
    column = lax.div(group, 2)
    if mask & 1:
        core = 1 - core
    if mask & 2:
        column = 1 - column
    return me - group + 2 * column + core


def plane_slot(me, mask):
    return lax.rem(plane_peer(me, mask), PLANE)


def plane_step(parts, pieces, vectors, action, out_types, ident):
    _, rows, cols = parts.shape
    chunks = 3 if rows % 48 == 0 else 1
    size = rows // chunks
    many, few = len(pieces), len(out_types)

    def body(p_ref, *rest):
        piece_refs, vector_ref = rest[:many], rest[many]
        all_ref, sums_ref = rest[many + 1 : many + 3]
        out_refs = rest[many + 3 : many + 3 + few]
        near, held, far_in, low, send, recv = rest[many + 3 + few :]
        me = lax.axis_index("shard")
        beside, across = [{"shard": plane_peer(me, mask)} for mask in (1, 2)]
        mine, far = lax.rem(me, PLANE), plane_slot(me, 2)
        greet([beside, across])
        spans = [pl.ds(size * index, size) for index in range(chunks)]

        def copy(kind, index):
            span = spans[index]
            table = {
                0: lambda: (p_ref.at[plane_slot(me, 3), span], near.at[0, span], beside),
                1: lambda: (p_ref.at[plane_slot(me, 1), span], near.at[1, span], beside),
                2: lambda: (held.at[span], far_in.at[span], across),
                3: lambda: (low.at[span], all_ref.at[mine, span], across),
                4: lambda: (low.at[span], all_ref.at[mine, span], beside),
                5: lambda: (all_ref.at[far, span], all_ref.at[far, span], beside),
            }
            src, dst, peer = table[kind]()
            return remote(src, dst, send.at[kind, index], recv.at[kind, index], peer)

        for index in range(chunks):
            copy(0, index).start()
        for index in range(chunks):
            copy(1, index).start()
        for index in range(chunks):
            span = spans[index]
            copy(0, index).wait_recv()
            total = p_ref[plane_slot(me, 2), span].astype(f32) + near[0, span].astype(f32)
            held[span] = total.astype(bf16)
            copy(2, index).start()
        lines = [vector_ref[index : index + 1] for index in range(len(vectors))]
        sums = None
        for index in range(chunks):
            span = spans[index]
            copy(1, index).wait_recv()
            copy(2, index).wait_recv()
            total = p_ref[mine, span].astype(f32) + near[1, span].astype(f32)
            total = total + far_in[span].astype(f32)
            result, outs, terms = action(
                total, [item[span].astype(f32) for item in piece_refs], lines
            )
            low[span] = result
            copy(3, index).start()
            copy(4, index).start()
            for ref, value in zip(out_refs, outs):
                ref[span] = value.astype(ref.dtype)
            all_ref[mine, span] = result
            terms = [jnp.sum(item, axis=0, keepdims=True) for item in terms]
            sums = terms if sums is None else [x + y for x, y in zip(sums, terms)]
        sums_ref[...] = jnp.zeros(sums_ref.shape, f32)
        for place, value in enumerate(sums):
            sums_ref[place : place + 1] = value
        for index in range(chunks):
            copy(3, index).wait_recv()
            copy(5, index).start()
        for index in range(chunks):
            copy(4, index).wait_recv()
            copy(5, index).wait_recv()
        for index in range(chunks):
            for kind in range(6):
                copy(kind, index).wait_send()

    stack = jnp.stack(vectors)
    shape = (rows, cols)
    return comm_call(
        body,
        "plane_step",
        ident,
        [parts] + list(pieces) + [stack],
        [struct((PLANE, rows, cols)), struct((8, cols), f32)]
        + [struct(shape, item) for item in out_types],
        [VMEM_SPEC] * (2 + few),
        [
            pltpu.VMEM((2, rows, cols), bf16),
            pltpu.VMEM(shape, bf16),
            pltpu.VMEM(shape, bf16),
            pltpu.VMEM(shape, bf16),
            pltpu.SemaphoreType.DMA((6, chunks)),
            pltpu.SemaphoreType.DMA((6, chunks)),
        ],
    )


def others(me, count):
    return [{"shard": lax.rem(me + step, count)} for step in range(1, count)]


def gather_weights(count, copies, tokens, qkv, up, out_w, small, ident):
    planes = count // PLANE
    rows = qkv.shape[1]

    def body(x_ref, qkv_ref, up_ref, wo_ref, small_ref, *rest):
        x_out, qkv_out, up_out, wo_out, small_out = rest[:5]
        send, recv, local, send_wo, recv_wo, send_unit, recv_unit = rest[5:]
        me = lax.axis_index("shard")
        group, plane = lax.rem(me, PLANE), lax.div(me, PLANE)
        across = [
            {"rep": lax.rem(lax.axis_index("rep") + step, copies)} for step in range(1, copies)
        ]
        greet(others(me, count) + across)
        owns = [
            (x_ref, x_out.at[group]),
            (qkv_ref.at[group], qkv_out.at[me]),
            (up_ref.at[group], up_out.at[group]),
            (small_ref, small_out.at[me]),
        ]
        started = []
        for index, (src, dst) in enumerate(owns):
            copy = pltpu.make_async_copy(src, dst, local.at[index])
            copy.start()
            started.append(copy)
        sent = []

        def push(src, dst, peer):
            index = len(sent)
            copy = remote(src, dst, send.at[index], recv.at[index], {"shard": peer})
            copy.start()
            sent.append(copy)

        for mask in (2, 1):
            push(x_ref, x_out.at[group], plane_peer(me, mask))
        far = plane_slot(me, 2)
        x_relay = remote(
            x_out.at[far], x_out.at[far], send.at[2], recv.at[2], {"shard": plane_peer(me, 1)}
        )
        sent.append(x_relay)
        for step in range(1, count):
            push(small_ref, small_out.at[me], lax.rem(me + step, count))
        rep = lax.axis_index("rep")
        split = copies == 2
        units = []
        for step in range(planes):
            for lane in range(PLANE):
                if step or lane:
                    units.append((qkv_ref, qkv_out, step, lane))
        for lane in range(1, PLANE):
            units.append((up_ref, up_out, 0, lane))

        def unit_copy(index):
            src, dst, step, lane = units[index]
            goal = lax.rem(plane + step, planes)
            goal_group = lax.rem(group + lane, PLANE)
            slot = group if src is up_ref else me
            return remote(
                src.at[goal_group],
                dst.at[slot],
                send_unit.at[index],
                recv_unit.at[index],
                {"shard": goal * PLANE + goal_group},
            )

        def unit_relay(index):
            src, dst, step, lane = units[index]
            origin = lax.rem(plane + planes - step, planes)
            origin_group = lax.rem(group + PLANE - lane, PLANE)
            slot = origin_group if src is up_ref else origin * PLANE + origin_group
            return remote(
                dst.at[slot],
                dst.at[slot],
                send_unit.at[index],
                recv_unit.at[index],
                {"rep": lax.rem(rep + 1, copies)},
            )

        def carried(index, mine):
            step = units[index][2]
            if not split or step == 0:
                return None
            return (rep == step % 2) if mine else (rep != step % 2)

        def guarded(test, action):
            if test is None:
                action()
            else:
                pl.when(test)(action)

        for index in range(len(units)):
            guarded(carried(index, True), unit_copy(index).start)
        target, place = lax.div(me, planes), lax.rem(me, planes)

        def wo_copy(source, index):
            peer = PLANE * index + target
            return peer, remote(
                wo_ref, wo_out.at[place], send_wo.at[index], recv_wo.at[source], {"shard": peer}
            )

        for index in range(planes):
            peer, copy = wo_copy(place, index)
            pl.when(peer != me)(copy.start)
        keep = pltpu.make_async_copy(wo_ref, wo_out.at[place], local.at[5])
        pl.when(target == group)(keep.start)
        sent[0].wait_recv()
        x_relay.start()
        for index, (_, _, step, _) in enumerate(units):
            if split and step:

                @pl.when(rep == step % 2)
                def _(index=index):
                    unit_relay(index).wait_recv()
                    unit_copy(index).wait_send()
                    unit_relay(index).start()

            else:
                unit_copy(index).wait_recv()
                unit_copy(index).wait_send()
        for index, (_, _, step, _) in enumerate(units):
            if split and step:
                pl.when(rep != step % 2)(unit_relay(index).wait_recv)
                pl.when(rep == step % 2)(unit_relay(index).wait_send)
        for copy in sent[1:]:
            copy.wait_recv()
        for index in range(planes):
            pl.when(group * planes + index != me)(wo_copy(index, index)[1].wait_recv)
        for index in range(planes):
            peer, copy = wo_copy(place, index)
            pl.when(peer != me)(copy.wait_send)
        pl.when(target == group)(keep.wait)
        for copy in sent:
            copy.wait_send()
        for copy in started:
            copy.wait()

    total = 3 + count - 1
    number = count - 1 + PLANE - 1
    return comm_call(
        body,
        "gather_weights",
        ident,
        [tokens, qkv, up, out_w, small],
        [
            struct((PLANE,) + tokens.shape),
            struct((count, rows, qkv.shape[2])),
            struct((PLANE, rows, up.shape[2])),
            struct((planes,) + out_w.shape),
            struct((count,) + small.shape),
        ],
        [ANY_SPEC] * 5,
        [
            pltpu.SemaphoreType.DMA((total,)),
            pltpu.SemaphoreType.DMA((total,)),
            pltpu.SemaphoreType.DMA((6,)),
            pltpu.SemaphoreType.DMA((planes,)),
            pltpu.SemaphoreType.DMA((planes,)),
            pltpu.SemaphoreType.DMA((number,)),
            pltpu.SemaphoreType.DMA((number,)),
        ],
    )


def reduce_grads(count, copies, qkv, up, out_w, down, small, parts, first_grad, ident):
    planes = count // PLANE
    rows = qkv.shape[1]
    block = down.shape[0]
    arrays = [qkv, up, out_w, small]

    def body(qkv_ref, up_ref, wo_ref, small_ref, down_ref, p_ref, first_ref, *rest):
        mixer_refs, outs, token_ref, rest = rest[:3], rest[3:7], rest[7], rest[8:]
        wide_ref, outs = outs[0], outs[1:]
        qkv_in, up_in, wo_in, small_in = rest[:4]
        halves, gets = [rest[4], up_in, rest[5], rest[6], down_ref], rest[7:12]
        near, near_sum, far_in = rest[12:15]
        send, recv, send_rep, recv_rep, send_wo, recv_wo, send_near, recv_near = rest[15:]
        me = lax.axis_index("shard")
        rep = lax.axis_index("rep")
        plane = lax.div(me, PLANE)
        across = [{"rep": lax.rem(rep + step, copies)} for step in range(1, copies)]
        greet(others(me, count) + across)
        sent = []

        def push(src, dst, peer):
            index = len(sent)
            copy = remote(src, dst, send.at[index], recv.at[index], {"shard": peer})
            copy.start()
            sent.append(copy)

        pairs = [(qkv_ref, qkv_in), (small_ref, small_in)]
        passed = []
        beside, over = [{"shard": plane_peer(me, mask)} for mask in (1, 2)]
        near_copies = [
            remote(p_ref.at[plane_slot(me, 3)], near.at[0], send_near.at[0], recv_near.at[0], beside),
            remote(p_ref.at[plane_slot(me, 1)], near.at[1], send_near.at[1], recv_near.at[1], beside),
            remote(near_sum, far_in, send_near.at[2], recv_near.at[2], over),
        ]
        near_copies[0].start()
        near_copies[1].start()

        def exchange(*places):
            for index, peer in enumerate(across):
                for place in places:
                    copy = remote(
                        halves[place],
                        gets[place].at[index],
                        send_rep.at[5 * index + place],
                        recv_rep.at[5 * index + place],
                        peer,
                    )
                    copy.start()
                    passed.append(copy)

        exchange(4)
        group = lax.rem(me, PLANE)
        target, place = lax.div(me, planes), lax.rem(me, planes)
        for lane in range(1, PLANE):
            goal = lax.rem(group + lane, PLANE)
            push(up_ref.at[goal], up_in.at[group], plane * PLANE + goal)
        up_in[group] = up_ref[group]
        for src, held in pairs:
            for step in range(1, count):
                peer = lax.rem(me + step, count)
                push(src.at[peer], held.at[me], peer)
        for src, held in pairs:
            held[me] = src[me]

        def wo_copy(source, index):
            peer = group * planes + index
            return peer, remote(
                wo_ref.at[index],
                wo_in.at[plane],
                send_wo.at[index],
                recv_wo.at[source],
                {"shard": peer},
            )

        for index in range(planes):
            peer, copy = wo_copy(plane, index)
            pl.when(peer != me)(copy.start)

        @pl.when(target == group)
        def _():
            wo_in[plane] = wo_ref[place]

        near_copies[0].wait_recv()
        total = p_ref[plane_slot(me, 2)].astype(f32) + near[0].astype(f32)
        near_sum[...] = total.astype(bf16)
        near_copies[2].start()
        for copy in sent[: PLANE - 1]:
            copy.wait_recv()
        exchange(1)
        for index in range(planes):
            pl.when(PLANE * index + target != me)(wo_copy(index, index)[1].wait_recv)
        for index in range(planes):
            peer, copy = wo_copy(plane, index)
            pl.when(peer != me)(copy.wait_send)
        total = wo_in[0].astype(f32)
        for other in range(1, planes):
            total = total + wo_in[other].astype(f32)
        halves[2][...] = total.astype(bf16)
        exchange(2)
        near_copies[1].wait_recv()
        near_copies[2].wait_recv()
        total = p_ref[lax.rem(me, PLANE)].astype(f32) + near[1].astype(f32)
        total = total + far_in[...].astype(f32) + first_ref[...]
        token_ref[...] = total.astype(bf16)
        for copy in sent[PLANE - 1 :]:
            copy.wait_recv()
        for half, held in zip(halves[:1], (qkv_in,)):
            for lane in range(PLANE):
                total = held[lane].astype(f32)
                for other in range(1, planes):
                    total = total + held[other * PLANE + lane].astype(f32)
                half[lane] = total.astype(bf16)
        for half, held, number in (
            (halves[3], small_in, count),
        ):
            total = held[0].astype(f32)
            for other in range(1, number):
                total = total + held[other].astype(f32)
            half[...] = total.astype(bf16)
        exchange(0, 3)
        for copy in passed:
            copy.wait_recv()

        def full(half, got, *at):
            total = half[at].astype(f32)
            for index in range(copies - 1):
                total = total + got[(index,) + at].astype(f32)
            return total

        for lane in range(PLANE):
            total = full(halves[0], gets[0], lane)
            for place, ref in enumerate(mixer_refs):
                low = place * GROUP_DIM
                ref[:, lane * GROUP_DIM : (lane + 1) * GROUP_DIM] = total[:, low : low + GROUP_DIM]
            total = full(halves[1], gets[1], lane)
            for index in range(planes):
                low = (index * PLANE + lane) * block
                wide_ref[:, low : low + block] = total[:, index * block : (index + 1) * block]
        for out, half, got in zip(outs, halves[2:], gets[2:]):
            out[...] = full(half, got, slice(None))
        for copy in sent + passed + near_copies:
            copy.wait_send()

    totals = 2 * (count - 1) + PLANE - 1
    shapes = [
        (PLANE, rows, qkv.shape[2]),
        (PLANE, rows, up.shape[2]),
        (rows, D),
        small.shape[1:],
        (block, D),
    ]
    return comm_call(
        body,
        "reduce_grads",
        ident,
        arrays + [down, parts, first_grad],
        [struct((rows, D), f32)] * 3
        + [struct((rows, FF), f32)]
        + [struct(shape, f32) for shape in shapes[2:]]
        + [struct(parts.shape[1:])],
        [VMEM_SPEC] * 8,
        [pltpu.VMEM(item.shape, bf16) for item in arrays]
        + [pltpu.VMEM(shapes[index], bf16) for index in (0, 2, 3)]
        + [pltpu.VMEM((copies - 1,) + shape, bf16) for shape in shapes]
        + [
            pltpu.VMEM((2,) + parts.shape[1:], bf16),
            pltpu.VMEM(parts.shape[1:], bf16),
            pltpu.VMEM(parts.shape[1:], bf16),
            pltpu.SemaphoreType.DMA((totals,)),
            pltpu.SemaphoreType.DMA((totals,)),
            pltpu.SemaphoreType.DMA((5 * (copies - 1),)),
            pltpu.SemaphoreType.DMA((5 * (copies - 1),)),
            pltpu.SemaphoreType.DMA((planes,)),
            pltpu.SemaphoreType.DMA((planes,)),
            pltpu.SemaphoreType.DMA((3,)),
            pltpu.SemaphoreType.DMA((3,)),
        ],
    )


def pick(plane, table):
    value = table[-1]
    for index in range(len(table) - 1):
        value = jnp.where(plane == index, table[index], value)
    return value


def attend_back(count, queries, upstream, pairs, own_row, key_cols, logs, delta, ident):
    planes, rows, cols = pairs.shape
    half = cols // 2
    size = 256 if rows % 256 == 0 else rows
    orders = []
    for plane in range(planes):
        goals = [goal for goal in range(planes) if goal != plane]
        goals.sort(key=lambda goal: (-abs(goal - plane), goal))
        orders.append(goals + [plane])

    def body(q_ref, up_ref, kv_ref, row_ref, col_ref, log_ref, delta_ref, *rest):
        dq_ref, out_ref, dq_sum, part, held, staged, send, recv = rest
        me = lax.axis_index("shard")
        plane = lax.div(me, PLANE)
        greet([{"shard": lax.rem(me + PLANE * s, count)} for s in range(1, planes)])
        dq_sum[...] = jnp.zeros(dq_sum.shape, f32)

        def hop(way, goal):
            peer = me + PLANE if way == 0 else me - PLANE
            return remote(
                staged.at[goal],
                held.at[way, goal],
                send.at[goal],
                recv.at[way, goal],
                {"shard": lax.rem(peer + count, count)},
            )

        def compute(goal):
            part[...] = jnp.zeros(part.shape, f32)
            key_codes = col_ref[goal]

            def chunk(index, carry):
                at = pl.multiple_of(index * size, size)
                span = pl.ds(at, size)
                allowed = key_codes == row_ref[0:1, span]
                for head in range(GROUP_HEADS):
                    low, high = head * HEAD_DIM, (head + 1) * HEAD_DIM
                    q = q_ref[span, low:high]
                    g = up_ref[span, low:high]
                    k = kv_ref[goal, :, low:high]
                    v = kv_ref[goal, :, half + low : half + high]
                    raw = dot_right(k, q)
                    chances = jnp.where(
                        allowed, jnp.exp(raw - log_ref[head : head + 1, span]), 0.0
                    )
                    d_chance = dot_right(v, g)
                    d_score = (chances * (d_chance - delta_ref[head : head + 1, span])).astype(bf16)
                    dq_sum[low:high, span] += dot_left(k, d_score)
                    part[:, low:high] += dot(d_score, q)
                    part[:, half + low : half + high] += dot(chances.astype(bf16), g)
                return carry

            lax.fori_loop(0, rows // size, chunk, 0)

        def pass_on(goal):
            for way in (0, 1):
                ahead = goal > plane if way == 0 else goal < plane
                first = plane == 0 if way == 0 else plane == planes - 1

                @pl.when(ahead & jnp.logical_not(first))
                def _(way=way):
                    copy = hop(way, goal)
                    copy.wait_recv()
                    total = staged[goal].astype(f32) + held[way, goal].astype(f32)
                    staged[goal] = total.astype(bf16)
                    copy.start()

        def begin(goal):
            for way in (0, 1):
                ahead = goal > plane if way == 0 else goal < plane
                first = plane == 0 if way == 0 else plane == planes - 1

                @pl.when(ahead & first)
                def _(way=way):
                    hop(way, goal).start()

        goals = [pick(plane, [order[i] for order in orders]) for i in range(planes)]
        for index in range(planes):
            goal = goals[index]
            compute(goal)
            if index < planes - 1:
                staged[goal] = part[...].astype(bf16)
                begin(goal)
            if index:
                pass_on(goals[index - 1])
        dq_ref[...] = (dq_sum[...] * 0.125).astype(bf16)
        for way in (0, 1):
            behind = plane > 0 if way == 0 else plane < planes - 1

            @pl.when(behind)
            def _(way=way):
                hop(way, plane).wait_recv()
                part[...] += held[way, plane].astype(f32)

        out_ref[...] = part[...].astype(bf16)
        for index in range(planes - 1):
            hop(0, goals[index]).wait_send()

    return comm_call(
        body,
        "attend_back",
        ident,
        [queries, upstream, pairs, own_row, key_cols, logs, delta],
        [struct((half, rows)), struct((rows, cols))],
        [VMEM_SPEC] * 2,
        [
            pltpu.VMEM((half, rows), f32),
            pltpu.VMEM((rows, cols), f32),
            pltpu.VMEM((2, planes, rows, cols), bf16),
            pltpu.VMEM((planes, rows, cols), bf16),
            pltpu.SemaphoreType.DMA((planes,)),
            pltpu.SemaphoreType.DMA((2, planes)),
        ],
    )


def attend_ahead(count, queries, own_pair, own_row, key_cols, ident):
    planes = count // PLANE
    rows, cols = own_pair.shape
    half = cols // 2
    size = 256 if rows % 256 == 0 else rows
    orders, flags = [], []
    for plane in range(planes):
        order = sorted(range(planes), key=lambda source: (abs(source - plane), source))
        away = [abs(source - plane) for source in order] + [-1]
        orders.append(order)
        flags.append([int(i > 0 and away[i] == away[i + 1]) for i in range(planes)])

    def body(q_ref, kv_ref, row_ref, col_ref, all_ref, ctx_ref, log_ref, *rest):
        top, total, send, recv, local = rest
        me = lax.axis_index("shard")
        plane = lax.div(me, PLANE)
        greet([{"shard": lax.rem(me + PLANE * s, count)} for s in range(1, planes)])
        own = pltpu.make_async_copy(kv_ref, all_ref.at[plane], local)
        own.start()
        up, down = plane < planes - 1, plane > 0

        def hop(way, source, src):
            peer = me + PLANE if way == 0 else me - PLANE
            return remote(
                src,
                all_ref.at[source],
                send.at[way, source],
                recv.at[way, source],
                {"shard": lax.rem(peer + count, count)},
            )

        pl.when(up)(hop(0, plane, kv_ref).start)
        pl.when(down)(hop(1, plane, kv_ref).start)
        top[...] = jnp.full(top.shape, very_low, f32)
        total[...] = jnp.zeros(total.shape, f32)
        ctx_ref[...] = jnp.zeros(ctx_ref.shape, f32)

        def take(source, test):
            for way in (0, 1):
                came = source < plane if way == 0 else source > plane
                onward = up if way == 0 else down

                @pl.when(test & came)
                def _(way=way, onward=onward):
                    copy = hop(way, source, all_ref.at[source])
                    copy.wait_recv()
                    pl.when(onward)(copy.start)

        def compute(source, block):
            key_codes = col_ref[source]

            def chunk(index, carry):
                span = pl.ds(pl.multiple_of(index * size, size), size)
                allowed = key_codes == row_ref[0:1, span]
                for head in range(GROUP_HEADS):
                    low, high = head * HEAD_DIM, (head + 1) * HEAD_DIM
                    line = slice(head, head + 1)
                    raw = dot_right(block[:, low:high], q_ref[span, low:high])
                    masked = jnp.where(allowed, raw, very_low)
                    before = top[line, span]
                    after = jnp.maximum(before, jnp.max(masked, axis=0, keepdims=True))
                    rescale = jnp.exp(before - after)
                    weights = jnp.exp(masked - after)
                    top[line, span] = after
                    total[line, span] = total[line, span] * rescale + jnp.sum(
                        weights, axis=0, keepdims=True
                    )
                    added = dot_left(block[:, half + low : half + high], weights.astype(bf16))
                    ctx_ref[low:high, span] = ctx_ref[low:high, span] * rescale + added
                return carry

            lax.fori_loop(0, rows // size, chunk, 0)

        compute(plane, kv_ref)
        sources = [pick(plane, [order[i] for order in orders]) for i in range(planes)]
        early = [pick(plane, [flag[i] for flag in flags]) == 1 for i in range(planes)]
        for index in range(1, planes):
            test = jnp.logical_not(early[index - 1])
            take(sources[index], test)
            if index + 1 < planes:
                take(sources[index + 1], early[index])
            compute(sources[index], all_ref.at[sources[index]])
        log_ref[...] = top[...] + jnp.log(total[...])
        for head in range(GROUP_HEADS):
            low, high = head * HEAD_DIM, (head + 1) * HEAD_DIM
            ctx_ref[low:high] = ctx_ref[low:high] / total[head : head + 1]
        pl.when(up)(hop(0, plane, kv_ref).wait_send)
        pl.when(down)(hop(1, plane, kv_ref).wait_send)
        for index in range(1, planes):
            source = sources[index]
            pl.when((source < plane) & up)(hop(0, source, all_ref.at[source]).wait_send)
            pl.when((source > plane) & down)(hop(1, source, all_ref.at[source]).wait_send)
        own.wait()

    return comm_call(
        body,
        "attend_ahead",
        ident,
        [queries, own_pair, own_row, key_cols],
        [
            struct((planes, rows, cols)),
            struct((half, rows), f32),
            struct((GROUP_HEADS, rows), f32),
        ],
        [VMEM_SPEC] * 3,
        [
            pltpu.VMEM((GROUP_HEADS, rows), f32),
            pltpu.VMEM((GROUP_HEADS, rows), f32),
            pltpu.SemaphoreType.DMA((2, planes)),
            pltpu.SemaphoreType.DMA((2, planes)),
            pltpu.SemaphoreType.DMA,
        ],
    )


def norm_forward(value, gain, shift):
    center = value - jnp.mean(value, axis=-1, keepdims=True)
    spread = jnp.mean(center * center, axis=-1, keepdims=True)
    scale = lax.rsqrt(spread + epsilon)
    normal = center * scale
    return (normal * gain + shift, normal, scale)


def norm_backward(upstream, normal, scale, gain):
    inner = upstream * gain
    return scale * (
        inner
        - jnp.mean(inner, axis=-1, keepdims=True)
        - normal * jnp.mean(inner * normal, axis=-1, keepdims=True)
    )


def gelu_slope(hidden):
    return 0.5 * (1.0 + lax.erf(hidden * root_half)) + hidden * inv_root_tau * jnp.exp(
        -0.5 * hidden * hidden
    )


def dot(left, right):
    return jnp.dot(left, right, preferred_element_type=f32)


def dot_left(left, right):
    return lax.dot_general(left, right, (((0,), (0,)), ((), ())), preferred_element_type=f32)


def dot_right(left, right):
    return lax.dot_general(left, right, (((1,), (1,)), ((), ())), preferred_element_type=f32)


def shards(count, copies, *arrays):
    (
        tokens,
        segments,
        padding,
        query_weight,
        key_weight,
        value_weight,
        query_bias,
        value_bias,
        out_weight,
        out_bias,
        middle_gain,
        middle_shift,
        up_weight,
        up_bias,
        down_weight,
        down_bias,
        final_gain,
        final_shift,
        cotangent,
    ) = arrays
    planes = count // PLANE
    rows = query_weight.shape[0]
    block = down_weight.shape[0]
    x_own = tokens[0]
    here = x_own.shape[0]
    wide = PLANE * here
    me = lax.axis_index("shard")
    group = lax.rem(me, PLANE)
    qkv_send = jnp.concatenate(
        [
            item.astype(bf16).reshape(rows, PLANE, GROUP_DIM)
            for item in (query_weight, key_weight, value_weight)
        ],
        axis=2,
    ).transpose(1, 0, 2)
    up_send = (
        up_weight.astype(bf16)
        .reshape(rows, planes, PLANE, block)
        .transpose(2, 0, 1, 3)
        .reshape(PLANE, rows, GROUP_FF)
    )
    codes = (2 * segments[0] + padding[0]).astype(f32)
    lanes = 128 * ((max(here, block) + 127) // 128)

    def padded(value):
        return jnp.pad(value.astype(f32), (0, lanes - value.shape[0]))

    vectors = [
        query_bias,
        value_bias,
        out_bias,
        middle_gain,
        middle_shift,
        down_bias,
        final_gain,
        final_shift,
        up_bias,
        codes,
    ]
    small_send = jnp.pad(
        jnp.stack([padded(item) for item in vectors]), ((0, 6), (0, 0))
    ).astype(bf16)
    lines = [[start + PLANE * step for step in range(planes)] for start in range(PLANE)]
    w_down = lax.all_gather(
        down_weight.astype(bf16), "shard", axis_index_groups=lines, axis=0
    ).reshape(GROUP_FF, D)
    x_all, qkv_all, up_all, wo_all, small = gather_weights(
        count,
        copies,
        x_own,
        qkv_send,
        up_send,
        out_weight.astype(bf16),
        small_send,
        0,
    )
    x_plane = x_all.reshape(wide, D)
    w_qkv = qkv_all.reshape(D, 3 * GROUP_DIM)
    strip = up_all.reshape(PLANE * rows, D)
    w_out = wo_all.reshape(GROUP_DIM, D)
    small = small.astype(f32)
    spread = [small[:, index, :rows].reshape(D) for index in range(8)]
    b_query, b_value, b_out, gain_mid, shift_mid, b_down, gain_end, shift_end = spread
    b_up = lax.dynamic_index_in_dim(
        small[:, 8, :block].reshape(planes, PLANE, block), group, 1, keepdims=False
    ).reshape(GROUP_FF)
    all_codes = small[:, 9, :here].reshape(planes, wide)
    own_codes = lax.dynamic_index_in_dim(all_codes, lax.div(me, PLANE), 0, keepdims=False)

    def group_part(value):
        return lax.dynamic_slice(value, (group * GROUP_DIM,), (GROUP_DIM,))

    qkv_bias = jnp.concatenate(
        [group_part(b_query), jnp.zeros((GROUP_DIM,), f32), group_part(b_value)]
    )
    qkv = (dot(x_plane, w_qkv) + qkv_bias).astype(bf16)
    w_down, qkv = lax.optimization_barrier((w_down, qkv))
    queries = qkv[:, :GROUP_DIM] * bf16(0.125)
    own_row, key_cols = own_codes[None], all_codes[:, :, None]
    pairs, context, logs = attend_ahead(
        count, queries, qkv[:, GROUP_DIM:], own_row, key_cols, 1
    )
    strip, pairs = lax.optimization_barrier((strip, pairs))
    w_up = lax.all_gather(strip, "shard", axis_index_groups=lines, axis=0).reshape(D, GROUP_FF)
    context_low = context.astype(bf16)

    def split(value):
        return value.reshape(PLANE, here, D)

    def enter_middle(total, pieces, lines):
        rest = total + lines[0] + pieces[0]
        middle, _, _ = norm_forward(rest, lines[1], lines[2])
        return middle.astype(bf16), [rest], []

    def enter_end(total, pieces, lines):
        middle, _, _ = norm_forward(pieces[0], lines[1], lines[2])
        result, normal, scale = norm_forward(middle + (total + lines[0]), lines[3], lines[4])
        above = pieces[1]
        back = norm_backward(above, normal, scale, lines[3])
        rounded = back.astype(bf16)
        return rounded, [result, back], [above * normal, above, rounded.astype(f32)]

    def leave_middle(total, pieces, lines):
        _, normal, scale = norm_forward(pieces[0], lines[0], lines[0])
        above = total + pieces[1]
        back = norm_backward(above, normal, scale, lines[0])
        rounded = back.astype(bf16)
        return rounded, [back], [above * normal, above, rounded.astype(f32)]

    middle_all, _, rest = plane_step(
        split(dot_left(context_low, w_out).astype(bf16)),
        [x_own],
        [b_out, gain_mid, shift_mid],
        enter_middle,
        [f32],
        2,
    )
    middle_plane = middle_all.reshape(wide, D)
    hidden = dot(middle_plane, w_up) + b_up
    active_low = jax.nn.gelu(hidden, approximate=False).astype(bf16)
    feed_all, end_sums, result, d_second = plane_step(
        split(dot(active_low, w_down).astype(bf16)),
        [rest, cotangent[0]],
        [b_down, gain_mid, shift_mid, gain_end, shift_end],
        enter_end,
        [bf16, f32],
        3,
    )
    output = result[None]
    feed_plane = feed_all.reshape(wide, D)
    grad_down = dot_left(active_low, feed_plane).astype(bf16)
    up_low = (dot_right(feed_plane, w_down) * gelu_slope(hidden)).astype(bf16)
    grad_up = dot_left(middle_plane, up_low).astype(bf16)
    strip_grads = lax.psum_scatter(
        jnp.concatenate(
            [
                grad_up.reshape(planes, PLANE * rows, GROUP_FF),
                grad_down.reshape(planes, block, D),
            ],
            axis=1,
        ),
        "shard",
        axis_index_groups=lines,
        scatter_dimension=0,
    )
    branch_all, middle_sums, d_first = plane_step(
        split(dot_right(up_low, w_up).astype(bf16)),
        [rest, d_second],
        [gain_mid],
        leave_middle,
        [f32],
        4,
    )
    branch_plane = branch_all.reshape(wide, D)
    grad_out = dot(context_low, branch_plane).astype(bf16)
    d_context = dot_right(branch_plane, w_out).astype(bf16)
    delta = jnp.sum(
        (d_context.astype(f32).T * context).reshape(GROUP_HEADS, HEAD_DIM, wide), axis=1
    )
    query_low, pair_low = attend_back(
        count,
        queries,
        d_context,
        pairs,
        own_row,
        key_cols,
        logs,
        delta,
        8,
    )
    mixer_low = jnp.concatenate([query_low.T, pair_low], axis=1)
    grad_qkv = dot_left(x_plane, mixer_low).astype(bf16)
    mixer_sums = jnp.sum(mixer_low.astype(f32), axis=0)

    def from_group(value):
        return lax.dynamic_update_slice(jnp.zeros((D,), f32), value, (group * GROUP_DIM,))

    sums = [
        from_group(mixer_sums[:GROUP_DIM]),
        from_group(mixer_sums[2 * GROUP_DIM :]),
        middle_sums[2],
        middle_sums[0],
        middle_sums[1],
        end_sums[2],
        end_sums[0],
        end_sums[1],
    ]
    own_lane = (jnp.arange(PLANE) == group).astype(f32)
    up_sums = jnp.sum(up_low.astype(f32), axis=0).reshape(planes, 1, block)
    up_sums = (up_sums * own_lane[None, :, None]).reshape(count, 1, block)
    sums = jnp.stack([item.reshape(count, rows) for item in sums], axis=1)
    small_grads = jnp.concatenate(
        [
            jnp.pad(sums, ((0, 0), (0, 0), (0, lanes - rows))),
            jnp.pad(up_sums, ((0, 0), (0, 7), (0, lanes - block))),
        ],
        axis=1,
    ).astype(bf16)
    query_grad, key_grad, value_grad, up_grad, out_total, small_total, down_total, grad_tokens = reduce_grads(
        count,
        copies,
        grad_qkv.reshape(count, rows, 3 * GROUP_DIM),
        strip_grads[: PLANE * rows].reshape(PLANE, rows, GROUP_FF),
        grad_out.reshape(planes, rows, D),
        strip_grads[PLANE * rows :],
        small_grads,
        split(dot_right(mixer_low, w_qkv).astype(bf16)),
        d_first,
        10,
    )

    return (
        output,
        grad_tokens[None],
        query_grad,
        key_grad,
        value_grad,
        small_total[0, :rows],
        small_total[1, :rows],
        out_total,
        small_total[2, :rows],
        small_total[3, :rows],
        small_total[4, :rows],
        up_grad,
        small_total[8, :block],
        down_total,
        small_total[5, :rows],
        small_total[6, :rows],
        small_total[7, :rows],
    )


def solution(mesh):
    sheet, line = P("shard", None), P("shard")
    batch = P("rep", "shard", None)
    in_specs = (batch, P("rep", "shard"), P("rep", "shard"), sheet, sheet, sheet, line, line)
    in_specs += (sheet, line, line, line, sheet, line, sheet, line, line, line, batch)
    out_specs = (batch, batch, sheet, sheet, sheet, line, line, sheet, line, line, line)
    out_specs += (sheet, line, sheet, line, line, line)
    body = functools.partial(shards, mesh.shape["shard"], mesh.shape["rep"])
    return jax.shard_map(
        body, mesh=mesh, in_specs=in_specs, out_specs=out_specs, check_vma=False
    )
```

```python
import functools

import jax
import jax.numpy as jnp
from jax import lax
from jax.experimental import pallas as pl
from jax.experimental.pallas import tpu as pltpu
from jax.sharding import PartitionSpec as P

D = 768
HEADS = 12
HEAD_DIM = 64
PLANE = 4
GROUP_HEADS = HEADS // PLANE
GROUP_DIM = GROUP_HEADS * HEAD_DIM
FF = 3072
GROUP_FF = FF // PLANE

epsilon = 1e-12
very_low = -1e30
root_half = 0.7071067811865476
inv_root_tau = 0.3989422804014327
bf16 = jnp.bfloat16
f32 = jnp.float32
MESH = pl.DeviceIdType.MESH
VMEM_SPEC = pl.BlockSpec(memory_space=pltpu.VMEM)
ANY_SPEC = pl.BlockSpec(memory_space=pl.ANY)
VMEM_BYTES = 60000 * 1024
MODEL_BYTES = 100_000_000


def struct(shape, dtype=bf16):
    return jax.ShapeDtypeStruct(shape, dtype)


def comm_call(body, name, ident, inputs, out_shapes, out_specs, scratch):
    return pl.pallas_call(
        body,
        name=name,
        out_shape=out_shapes,
        in_specs=[VMEM_SPEC] * len(inputs),
        out_specs=out_specs,
        scratch_shapes=scratch,
        cost_estimate=pl.CostEstimate(flops=0, bytes_accessed=MODEL_BYTES, transcendentals=0),
        compiler_params=pltpu.CompilerParams(
            collective_id=ident, has_side_effects=True, vmem_limit_bytes=VMEM_BYTES
        ),
    )(*inputs)


def greet(peers):
    barrier = pltpu.get_barrier_semaphore()
    for peer in peers:
        pl.semaphore_signal(barrier, inc=1, device_id=peer, device_id_type=MESH)
    pl.semaphore_wait(barrier, len(peers))


def remote(src, dst, send_sem, recv_sem, peer):
    return pltpu.make_async_remote_copy(
        src_ref=src,
        dst_ref=dst,
        send_sem=send_sem,
        recv_sem=recv_sem,
        device_id=peer,
        device_id_type=MESH,
    )


def plane_peer(me, mask):
    group = lax.rem(me, PLANE)
    core = lax.rem(group, 2)
    column = lax.div(group, 2)
    if mask & 1:
        core = 1 - core
    if mask & 2:
        column = 1 - column
    return me - group + 2 * column + core


def plane_slot(me, mask):
    return lax.rem(plane_peer(me, mask), PLANE)


def plane_step(parts, pieces, vectors, action, out_types, ident):
    _, rows, cols = parts.shape
    chunks = 3 if rows % 48 == 0 else 1
    size = rows // chunks
    many, few = len(pieces), len(out_types)

    def body(p_ref, *rest):
        piece_refs, vector_ref = rest[:many], rest[many]
        all_ref, sums_ref = rest[many + 1 : many + 3]
        out_refs = rest[many + 3 : many + 3 + few]
        near, held, far_in, low, send, recv = rest[many + 3 + few :]
        me = lax.axis_index("shard")
        beside, across = [{"shard": plane_peer(me, mask)} for mask in (1, 2)]
        mine, far = lax.rem(me, PLANE), plane_slot(me, 2)
        greet([beside, across])
        spans = [pl.ds(size * index, size) for index in range(chunks)]

        def copy(kind, index):
            span = spans[index]
            table = {
                0: lambda: (p_ref.at[plane_slot(me, 3), span], near.at[0, span], beside),
                1: lambda: (p_ref.at[plane_slot(me, 1), span], near.at[1, span], beside),
                2: lambda: (held.at[span], far_in.at[span], across),
                3: lambda: (low.at[span], all_ref.at[mine, span], across),
                4: lambda: (low.at[span], all_ref.at[mine, span], beside),
                5: lambda: (all_ref.at[far, span], all_ref.at[far, span], beside),
            }
            src, dst, peer = table[kind]()
            return remote(src, dst, send.at[kind, index], recv.at[kind, index], peer)

        for index in range(chunks):
            copy(0, index).start()
        for index in range(chunks):
            copy(1, index).start()
        for index in range(chunks):
            span = spans[index]
            copy(0, index).wait_recv()
            total = p_ref[plane_slot(me, 2), span].astype(f32) + near[0, span].astype(f32)
            held[span] = total.astype(bf16)
            copy(2, index).start()
        lines = [vector_ref[index : index + 1] for index in range(len(vectors))]
        sums = None
        for index in range(chunks):
            span = spans[index]
            copy(1, index).wait_recv()
            copy(2, index).wait_recv()
            total = p_ref[mine, span].astype(f32) + near[1, span].astype(f32)
            total = total + far_in[span].astype(f32)
            result, outs, terms = action(
                total, [item[span].astype(f32) for item in piece_refs], lines
            )
            low[span] = result
            copy(3, index).start()
            copy(4, index).start()
            for ref, value in zip(out_refs, outs):
                ref[span] = value.astype(ref.dtype)
            all_ref[mine, span] = result
            terms = [jnp.sum(item, axis=0, keepdims=True) for item in terms]
            sums = terms if sums is None else [x + y for x, y in zip(sums, terms)]
        sums_ref[...] = jnp.zeros(sums_ref.shape, f32)
        for place, value in enumerate(sums):
            sums_ref[place : place + 1] = value
        for index in range(chunks):
            copy(3, index).wait_recv()
            copy(5, index).start()
        for index in range(chunks):
            copy(4, index).wait_recv()
            copy(5, index).wait_recv()
        for index in range(chunks):
            for kind in range(6):
                copy(kind, index).wait_send()

    stack = jnp.stack(vectors)
    shape = (rows, cols)
    return comm_call(
        body,
        "plane_step",
        ident,
        [parts] + list(pieces) + [stack],
        [struct((PLANE, rows, cols)), struct((8, cols), f32)]
        + [struct(shape, item) for item in out_types],
        [VMEM_SPEC] * (2 + few),
        [
            pltpu.VMEM((2, rows, cols), bf16),
            pltpu.VMEM(shape, bf16),
            pltpu.VMEM(shape, bf16),
            pltpu.VMEM(shape, bf16),
            pltpu.SemaphoreType.DMA((6, chunks)),
            pltpu.SemaphoreType.DMA((6, chunks)),
        ],
    )


def others(me, count):
    return [{"shard": lax.rem(me + step, count)} for step in range(1, count)]


def gather_weights(count, copies, tokens, qkv, up, out_w, small, ident):
    planes = count // PLANE
    rows = qkv.shape[1]

    def body(x_ref, qkv_ref, up_ref, wo_ref, small_ref, *rest):
        x_out, qkv_out, up_out, wo_out, small_out = rest[:5]
        send, recv, local, send_wo, recv_wo, send_unit, recv_unit = rest[5:]
        me = lax.axis_index("shard")
        group, plane = lax.rem(me, PLANE), lax.div(me, PLANE)
        across = [
            {"rep": lax.rem(lax.axis_index("rep") + step, copies)} for step in range(1, copies)
        ]
        greet(others(me, count) + across)
        owns = [
            (x_ref, x_out.at[group]),
            (qkv_ref.at[group], qkv_out.at[me]),
            (up_ref.at[group], up_out.at[group]),
            (small_ref, small_out.at[me]),
        ]
        started = []
        for index, (src, dst) in enumerate(owns):
            copy = pltpu.make_async_copy(src, dst, local.at[index])
            copy.start()
            started.append(copy)
        sent = []

        def push(src, dst, peer):
            index = len(sent)
            copy = remote(src, dst, send.at[index], recv.at[index], {"shard": peer})
            copy.start()
            sent.append(copy)

        for mask in (2, 1):
            push(x_ref, x_out.at[group], plane_peer(me, mask))
        far = plane_slot(me, 2)
        x_relay = remote(
            x_out.at[far], x_out.at[far], send.at[2], recv.at[2], {"shard": plane_peer(me, 1)}
        )
        sent.append(x_relay)
        for step in range(1, count):
            push(small_ref, small_out.at[me], lax.rem(me + step, count))
        rep = lax.axis_index("rep")
        split = copies == 2
        units = []
        for step in range(planes):
            for lane in range(PLANE):
                if step or lane:
                    units.append((qkv_ref, qkv_out, step, lane))
        for lane in range(1, PLANE):
            units.append((up_ref, up_out, 0, lane))

        def unit_copy(index):
            src, dst, step, lane = units[index]
            goal = lax.rem(plane + step, planes)
            goal_group = lax.rem(group + lane, PLANE)
            slot = group if src is up_ref else me
            return remote(
                src.at[goal_group],
                dst.at[slot],
                send_unit.at[index],
                recv_unit.at[index],
                {"shard": goal * PLANE + goal_group},
            )

        def unit_relay(index):
            src, dst, step, lane = units[index]
            origin = lax.rem(plane + planes - step, planes)
            origin_group = lax.rem(group + PLANE - lane, PLANE)
            slot = origin_group if src is up_ref else origin * PLANE + origin_group
            return remote(
                dst.at[slot],
                dst.at[slot],
                send_unit.at[index],
                recv_unit.at[index],
                {"rep": lax.rem(rep + 1, copies)},
            )

        def carried(index, mine):
            step = units[index][2]
            if not split or step == 0:
                return None
            return (rep == step % 2) if mine else (rep != step % 2)

        def guarded(test, action):
            if test is None:
                action()
            else:
                pl.when(test)(action)

        for index in range(len(units)):
            guarded(carried(index, True), unit_copy(index).start)
        target, place = lax.div(me, planes), lax.rem(me, planes)

        def wo_copy(source, index):
            peer = PLANE * index + target
            return peer, remote(
                wo_ref, wo_out.at[place], send_wo.at[index], recv_wo.at[source], {"shard": peer}
            )

        for index in range(planes):
            peer, copy = wo_copy(place, index)
            pl.when(peer != me)(copy.start)
        keep = pltpu.make_async_copy(wo_ref, wo_out.at[place], local.at[5])
        pl.when(target == group)(keep.start)
        sent[0].wait_recv()
        x_relay.start()
        for index, (_, _, step, _) in enumerate(units):
            if split and step:

                @pl.when(rep == step % 2)
                def _(index=index):
                    unit_relay(index).wait_recv()
                    unit_copy(index).wait_send()
                    unit_relay(index).start()

            else:
                unit_copy(index).wait_recv()
                unit_copy(index).wait_send()
        for index, (_, _, step, _) in enumerate(units):
            if split and step:
                pl.when(rep != step % 2)(unit_relay(index).wait_recv)
                pl.when(rep == step % 2)(unit_relay(index).wait_send)
        for copy in sent[1:]:
            copy.wait_recv()
        for index in range(planes):
            pl.when(group * planes + index != me)(wo_copy(index, index)[1].wait_recv)
        for index in range(planes):
            peer, copy = wo_copy(place, index)
            pl.when(peer != me)(copy.wait_send)
        pl.when(target == group)(keep.wait)
        for copy in sent:
            copy.wait_send()
        for copy in started:
            copy.wait()

    total = 3 + count - 1
    number = count - 1 + PLANE - 1
    return comm_call(
        body,
        "gather_weights",
        ident,
        [tokens, qkv, up, out_w, small],
        [
            struct((PLANE,) + tokens.shape),
            struct((count, rows, qkv.shape[2])),
            struct((PLANE, rows, up.shape[2])),
            struct((planes,) + out_w.shape),
            struct((count,) + small.shape),
        ],
        [ANY_SPEC] * 5,
        [
            pltpu.SemaphoreType.DMA((total,)),
            pltpu.SemaphoreType.DMA((total,)),
            pltpu.SemaphoreType.DMA((6,)),
            pltpu.SemaphoreType.DMA((planes,)),
            pltpu.SemaphoreType.DMA((planes,)),
            pltpu.SemaphoreType.DMA((number,)),
            pltpu.SemaphoreType.DMA((number,)),
        ],
    )


def reduce_grads(count, copies, qkv, up, out_w, down, small, parts, first_grad, ident):
    planes = count // PLANE
    rows = qkv.shape[1]
    block = down.shape[0]
    arrays = [qkv, up, out_w, small]
    split = copies == 2 and planes % 2 == 0
    pieces = planes // 2

    def body(qkv_ref, up_ref, wo_ref, small_ref, down_ref, p_ref, first_ref, *rest):
        mixer_refs, outs, token_ref, rest = rest[:3], rest[3:7], rest[7], rest[8:]
        wide_ref, outs = outs[0], outs[1:]
        qkv_in, up_in, wo_in, small_in = rest[:4]
        halves, gets = [rest[4], up_in, rest[5], rest[6], down_ref], rest[7:12]
        near, near_sum, far_in = rest[12:15]
        peer_q, sum_q, in_q = rest[15:18]
        send, recv, send_rep, recv_rep, send_wo, recv_wo, send_near, recv_near = rest[18:26]
        send_y, recv_y, send_q, recv_q = rest[26:]
        me = lax.axis_index("shard")
        rep = lax.axis_index("rep")
        plane = lax.div(me, PLANE)
        across = [{"rep": lax.rem(rep + step, copies)} for step in range(1, copies)]
        greet(others(me, count) + across)
        sent = []

        def push(src, dst, peer):
            index = len(sent)
            copy = remote(src, dst, send.at[index], recv.at[index], {"shard": peer})
            copy.start()
            sent.append(copy)

        pairs = [(small_ref, small_in)] if split else [(qkv_ref, qkv_in), (small_ref, small_in)]
        swaps = []
        if split:
            for index in range(pieces):
                goal = lax.rem(plane + 1 - rep + 2 * index, planes)
                swaps.append(
                    remote(
                        qkv_ref.at[pl.ds(goal * PLANE, PLANE)],
                        peer_q.at[index],
                        send_y.at[index],
                        recv_y.at[index],
                        across[0],
                    )
                )
            for copy in swaps[::-1]:
                copy.start()
        passed = []
        beside, over = [{"shard": plane_peer(me, mask)} for mask in (1, 2)]
        near_copies = [
            remote(p_ref.at[plane_slot(me, 3)], near.at[0], send_near.at[0], recv_near.at[0], beside),
            remote(p_ref.at[plane_slot(me, 1)], near.at[1], send_near.at[1], recv_near.at[1], beside),
            remote(near_sum, far_in, send_near.at[2], recv_near.at[2], over),
        ]
        near_copies[0].start()
        near_copies[1].start()

        def exchange(*places):
            for index, peer in enumerate(across):
                for place in places:
                    copy = remote(
                        halves[place],
                        gets[place].at[index],
                        send_rep.at[5 * index + place],
                        recv_rep.at[5 * index + place],
                        peer,
                    )
                    copy.start()
                    passed.append(copy)

        exchange(4)
        group = lax.rem(me, PLANE)
        target, place = lax.div(me, planes), lax.rem(me, planes)
        for lane in range(1, PLANE):
            goal = lax.rem(group + lane, PLANE)
            push(up_ref.at[goal], up_in.at[group], plane * PLANE + goal)
        up_in[group] = up_ref[group]
        for src, held in pairs:
            for step in range(1, count):
                peer = lax.rem(me + step, count)
                push(src.at[peer], held.at[me], peer)
        for src, held in pairs:
            held[me] = src[me]

        def wo_copy(source, index):
            peer = group * planes + index
            return peer, remote(
                wo_ref.at[index],
                wo_in.at[plane],
                send_wo.at[index],
                recv_wo.at[source],
                {"shard": peer},
            )

        for index in range(planes):
            peer, copy = wo_copy(plane, index)
            pl.when(peer != me)(copy.start)

        @pl.when(target == group)
        def _():
            wo_in[plane] = wo_ref[place]

        moved = []
        for index in reversed(range(pieces if split else 0)):
            goal = lax.rem(plane + rep + 2 * index, planes)
            swaps[index].wait_recv()
            for lane in range(PLANE):
                total = qkv_ref[goal * PLANE + lane].astype(f32) + peer_q[index, lane].astype(f32)
                sum_q[index, lane] = total.astype(bf16)
            for step in range(PLANE):
                lane = lax.rem(group + step, PLANE)
                number = index * PLANE + step
                copy = remote(
                    sum_q.at[index, lane],
                    in_q.at[index, group],
                    send_q.at[number],
                    recv_q.at[number],
                    {"shard": goal * PLANE + lane},
                )
                if number:
                    copy.start()
                else:
                    pl.when(rep != 0)(copy.start)

                    @pl.when(rep == 0)
                    def _():
                        in_q[0, group] = sum_q[0, group]

                moved.append((number, copy))
        near_copies[0].wait_recv()
        total = p_ref[plane_slot(me, 2)].astype(f32) + near[0].astype(f32)
        near_sum[...] = total.astype(bf16)
        near_copies[2].start()
        for copy in sent[: PLANE - 1]:
            copy.wait_recv()
        exchange(1)
        for index in range(planes):
            pl.when(PLANE * index + target != me)(wo_copy(index, index)[1].wait_recv)
        for index in range(planes):
            peer, copy = wo_copy(plane, index)
            pl.when(peer != me)(copy.wait_send)
        total = wo_in[0].astype(f32)
        for other in range(1, planes):
            total = total + wo_in[other].astype(f32)
        halves[2][...] = total.astype(bf16)
        exchange(2)
        near_copies[1].wait_recv()
        near_copies[2].wait_recv()
        total = p_ref[lax.rem(me, PLANE)].astype(f32) + near[1].astype(f32)
        total = total + far_in[...].astype(f32) + first_ref[...]
        token_ref[...] = total.astype(bf16)
        for copy in sent[PLANE - 1 :]:
            copy.wait_recv()
        for number, copy in moved:
            if number:
                copy.wait_recv()
            else:
                pl.when(rep != 0)(copy.wait_recv)
        for lane in range(PLANE):
            if split:
                terms = [in_q[index, lane] for index in range(pieces)]
            else:
                terms = [qkv_in[other * PLANE + lane] for other in range(planes)]
            total = terms[0].astype(f32)
            for term in terms[1:]:
                total = total + term.astype(f32)
            halves[0][lane] = total.astype(bf16)
        for half, held, number in (
            (halves[3], small_in, count),
        ):
            total = held[0].astype(f32)
            for other in range(1, number):
                total = total + held[other].astype(f32)
            half[...] = total.astype(bf16)
        exchange(0, 3)
        for copy in passed:
            copy.wait_recv()

        def full(half, got, *at):
            total = half[at].astype(f32)
            for index in range(copies - 1):
                total = total + got[(index,) + at].astype(f32)
            return total

        for lane in range(PLANE):
            total = full(halves[0], gets[0], lane)
            for place, ref in enumerate(mixer_refs):
                low = place * GROUP_DIM
                ref[:, lane * GROUP_DIM : (lane + 1) * GROUP_DIM] = total[:, low : low + GROUP_DIM]
            total = full(halves[1], gets[1], lane)
            for index in range(planes):
                low = (index * PLANE + lane) * block
                wide_ref[:, low : low + block] = total[:, index * block : (index + 1) * block]
        for out, half, got in zip(outs, halves[2:], gets[2:]):
            out[...] = full(half, got, slice(None))
        for copy in sent + passed + near_copies + swaps:
            copy.wait_send()
        for number, copy in moved:
            if number:
                copy.wait_send()
            else:
                pl.when(rep != 0)(copy.wait_send)

    totals = (1 if split else 2) * (count - 1) + PLANE - 1
    shapes = [
        (PLANE, rows, qkv.shape[2]),
        (PLANE, rows, up.shape[2]),
        (rows, D),
        small.shape[1:],
        (block, D),
    ]
    return comm_call(
        body,
        "reduce_grads",
        ident,
        arrays + [down, parts, first_grad],
        [struct((rows, D), f32)] * 3
        + [struct((rows, FF), f32)]
        + [struct(shape, f32) for shape in shapes[2:]]
        + [struct(parts.shape[1:])],
        [VMEM_SPEC] * 8,
        [pltpu.VMEM(item.shape, bf16) for item in arrays]
        + [pltpu.VMEM(shapes[index], bf16) for index in (0, 2, 3)]
        + [pltpu.VMEM((copies - 1,) + shape, bf16) for shape in shapes]
        + [
            pltpu.VMEM((2,) + parts.shape[1:], bf16),
            pltpu.VMEM(parts.shape[1:], bf16),
            pltpu.VMEM(parts.shape[1:], bf16),
            pltpu.VMEM((pieces, PLANE) + qkv.shape[1:], bf16),
            pltpu.VMEM((pieces, PLANE) + qkv.shape[1:], bf16),
            pltpu.VMEM((pieces, PLANE) + qkv.shape[1:], bf16),
            pltpu.SemaphoreType.DMA((totals,)),
            pltpu.SemaphoreType.DMA((totals,)),
            pltpu.SemaphoreType.DMA((5 * (copies - 1),)),
            pltpu.SemaphoreType.DMA((5 * (copies - 1),)),
            pltpu.SemaphoreType.DMA((planes,)),
            pltpu.SemaphoreType.DMA((planes,)),
            pltpu.SemaphoreType.DMA((3,)),
            pltpu.SemaphoreType.DMA((3,)),
            pltpu.SemaphoreType.DMA((pieces,)),
            pltpu.SemaphoreType.DMA((pieces,)),
            pltpu.SemaphoreType.DMA((pieces * PLANE,)),
            pltpu.SemaphoreType.DMA((pieces * PLANE,)),
        ],
    )


def pick(plane, table):
    value = table[-1]
    for index in range(len(table) - 1):
        value = jnp.where(plane == index, table[index], value)
    return value


def attend_back(count, queries, upstream, pairs, own_row, key_cols, logs, delta, ident):
    planes, rows, cols = pairs.shape
    half = cols // 2
    size = 256 if rows % 256 == 0 else rows
    orders = []
    for plane in range(planes):
        goals = [goal for goal in range(planes) if goal != plane]
        goals.sort(key=lambda goal: (-abs(goal - plane), goal))
        orders.append(goals + [plane])

    def body(q_ref, up_ref, kv_ref, row_ref, col_ref, log_ref, delta_ref, *rest):
        dq_ref, out_ref, dq_sum, part, held, staged, send, recv = rest
        me = lax.axis_index("shard")
        plane = lax.div(me, PLANE)
        greet([{"shard": lax.rem(me + PLANE * s, count)} for s in range(1, planes)])
        dq_sum[...] = jnp.zeros(dq_sum.shape, f32)

        def hop(way, goal):
            peer = me + PLANE if way == 0 else me - PLANE
            return remote(
                staged.at[goal],
                held.at[way, goal],
                send.at[goal],
                recv.at[way, goal],
                {"shard": lax.rem(peer + count, count)},
            )

        def compute(goal):
            part[...] = jnp.zeros(part.shape, f32)
            key_codes = col_ref[goal]

            def chunk(index, carry):
                at = pl.multiple_of(index * size, size)
                span = pl.ds(at, size)
                allowed = key_codes == row_ref[0:1, span]
                for head in range(GROUP_HEADS):
                    low, high = head * HEAD_DIM, (head + 1) * HEAD_DIM
                    q = q_ref[span, low:high]
                    g = up_ref[span, low:high]
                    k = kv_ref[goal, :, low:high]
                    v = kv_ref[goal, :, half + low : half + high]
                    raw = dot_right(k, q)
                    chances = jnp.where(
                        allowed, jnp.exp(raw - log_ref[head : head + 1, span]), 0.0
                    )
                    d_chance = dot_right(v, g)
                    d_score = (chances * (d_chance - delta_ref[head : head + 1, span])).astype(bf16)
                    dq_sum[low:high, span] += dot_left(k, d_score)
                    part[:, low:high] += dot(d_score, q)
                    part[:, half + low : half + high] += dot(chances.astype(bf16), g)
                return carry

            lax.fori_loop(0, rows // size, chunk, 0)

        def pass_on(goal):
            for way in (0, 1):
                ahead = goal > plane if way == 0 else goal < plane
                first = plane == 0 if way == 0 else plane == planes - 1

                @pl.when(ahead & jnp.logical_not(first))
                def _(way=way):
                    copy = hop(way, goal)
                    copy.wait_recv()
                    total = staged[goal].astype(f32) + held[way, goal].astype(f32)
                    staged[goal] = total.astype(bf16)
                    copy.start()

        def begin(goal):
            for way in (0, 1):
                ahead = goal > plane if way == 0 else goal < plane
                first = plane == 0 if way == 0 else plane == planes - 1

                @pl.when(ahead & first)
                def _(way=way):
                    hop(way, goal).start()

        goals = [pick(plane, [order[i] for order in orders]) for i in range(planes)]
        for index in range(planes):
            goal = goals[index]
            compute(goal)
            if index < planes - 1:
                staged[goal] = part[...].astype(bf16)
                begin(goal)
            if index:
                pass_on(goals[index - 1])
        dq_ref[...] = (dq_sum[...] * 0.125).astype(bf16)
        for way in (0, 1):
            behind = plane > 0 if way == 0 else plane < planes - 1

            @pl.when(behind)
            def _(way=way):
                hop(way, plane).wait_recv()
                part[...] += held[way, plane].astype(f32)

        out_ref[...] = part[...].astype(bf16)
        for index in range(planes - 1):
            hop(0, goals[index]).wait_send()

    return comm_call(
        body,
        "attend_back",
        ident,
        [queries, upstream, pairs, own_row, key_cols, logs, delta],
        [struct((half, rows)), struct((rows, cols))],
        [VMEM_SPEC] * 2,
        [
            pltpu.VMEM((half, rows), f32),
            pltpu.VMEM((rows, cols), f32),
            pltpu.VMEM((2, planes, rows, cols), bf16),
            pltpu.VMEM((planes, rows, cols), bf16),
            pltpu.SemaphoreType.DMA((planes,)),
            pltpu.SemaphoreType.DMA((2, planes)),
        ],
    )


def attend_ahead(count, queries, own_pair, own_row, key_cols, ident):
    planes = count // PLANE
    rows, cols = own_pair.shape
    half = cols // 2
    size = 256 if rows % 256 == 0 else rows
    orders, flags = [], []
    for plane in range(planes):
        order = sorted(range(planes), key=lambda source: (abs(source - plane), source))
        away = [abs(source - plane) for source in order] + [-1]
        orders.append(order)
        flags.append([int(i > 0 and away[i] == away[i + 1]) for i in range(planes)])

    def body(q_ref, kv_ref, row_ref, col_ref, all_ref, ctx_ref, log_ref, *rest):
        top, total, send, recv, local = rest
        me = lax.axis_index("shard")
        plane = lax.div(me, PLANE)
        greet([{"shard": lax.rem(me + PLANE * s, count)} for s in range(1, planes)])
        own = pltpu.make_async_copy(kv_ref, all_ref.at[plane], local)
        own.start()
        up, down = plane < planes - 1, plane > 0

        def hop(way, source, src):
            peer = me + PLANE if way == 0 else me - PLANE
            return remote(
                src,
                all_ref.at[source],
                send.at[way, source],
                recv.at[way, source],
                {"shard": lax.rem(peer + count, count)},
            )

        pl.when(up)(hop(0, plane, kv_ref).start)
        pl.when(down)(hop(1, plane, kv_ref).start)
        top[...] = jnp.full(top.shape, very_low, f32)
        total[...] = jnp.zeros(total.shape, f32)
        ctx_ref[...] = jnp.zeros(ctx_ref.shape, f32)

        def take(source, test):
            for way in (0, 1):
                came = source < plane if way == 0 else source > plane
                onward = up if way == 0 else down

                @pl.when(test & came)
                def _(way=way, onward=onward):
                    copy = hop(way, source, all_ref.at[source])
                    copy.wait_recv()
                    pl.when(onward)(copy.start)

        def compute(source, block):
            key_codes = col_ref[source]

            def chunk(index, carry):
                span = pl.ds(pl.multiple_of(index * size, size), size)
                allowed = key_codes == row_ref[0:1, span]
                for head in range(GROUP_HEADS):
                    low, high = head * HEAD_DIM, (head + 1) * HEAD_DIM
                    line = slice(head, head + 1)
                    raw = dot_right(block[:, low:high], q_ref[span, low:high])
                    masked = jnp.where(allowed, raw, very_low)
                    before = top[line, span]
                    after = jnp.maximum(before, jnp.max(masked, axis=0, keepdims=True))
                    rescale = jnp.exp(before - after)
                    weights = jnp.exp(masked - after)
                    top[line, span] = after
                    total[line, span] = total[line, span] * rescale + jnp.sum(
                        weights, axis=0, keepdims=True
                    )
                    added = dot_left(block[:, half + low : half + high], weights.astype(bf16))
                    ctx_ref[low:high, span] = ctx_ref[low:high, span] * rescale + added
                return carry

            lax.fori_loop(0, rows // size, chunk, 0)

        compute(plane, kv_ref)
        sources = [pick(plane, [order[i] for order in orders]) for i in range(planes)]
        early = [pick(plane, [flag[i] for flag in flags]) == 1 for i in range(planes)]
        for index in range(1, planes):
            test = jnp.logical_not(early[index - 1])
            take(sources[index], test)
            if index + 1 < planes:
                take(sources[index + 1], early[index])
            compute(sources[index], all_ref.at[sources[index]])
        log_ref[...] = top[...] + jnp.log(total[...])
        for head in range(GROUP_HEADS):
            low, high = head * HEAD_DIM, (head + 1) * HEAD_DIM
            ctx_ref[low:high] = ctx_ref[low:high] / total[head : head + 1]
        pl.when(up)(hop(0, plane, kv_ref).wait_send)
        pl.when(down)(hop(1, plane, kv_ref).wait_send)
        for index in range(1, planes):
            source = sources[index]
            pl.when((source < plane) & up)(hop(0, source, all_ref.at[source]).wait_send)
            pl.when((source > plane) & down)(hop(1, source, all_ref.at[source]).wait_send)
        own.wait()

    return comm_call(
        body,
        "attend_ahead",
        ident,
        [queries, own_pair, own_row, key_cols],
        [
            struct((planes, rows, cols)),
            struct((half, rows), f32),
            struct((GROUP_HEADS, rows), f32),
        ],
        [VMEM_SPEC] * 3,
        [
            pltpu.VMEM((GROUP_HEADS, rows), f32),
            pltpu.VMEM((GROUP_HEADS, rows), f32),
            pltpu.SemaphoreType.DMA((2, planes)),
            pltpu.SemaphoreType.DMA((2, planes)),
            pltpu.SemaphoreType.DMA,
        ],
    )


def norm_forward(value, gain, shift):
    center = value - jnp.mean(value, axis=-1, keepdims=True)
    spread = jnp.mean(center * center, axis=-1, keepdims=True)
    scale = lax.rsqrt(spread + epsilon)
    normal = center * scale
    return (normal * gain + shift, normal, scale)


def norm_backward(upstream, normal, scale, gain):
    inner = upstream * gain
    return scale * (
        inner
        - jnp.mean(inner, axis=-1, keepdims=True)
        - normal * jnp.mean(inner * normal, axis=-1, keepdims=True)
    )


def gelu_slope(hidden):
    return 0.5 * (1.0 + lax.erf(hidden * root_half)) + hidden * inv_root_tau * jnp.exp(
        -0.5 * hidden * hidden
    )


def dot(left, right):
    return jnp.dot(left, right, preferred_element_type=f32)


def dot_left(left, right):
    return lax.dot_general(left, right, (((0,), (0,)), ((), ())), preferred_element_type=f32)


def dot_right(left, right):
    return lax.dot_general(left, right, (((1,), (1,)), ((), ())), preferred_element_type=f32)


def shards(count, copies, *arrays):
    (
        tokens,
        segments,
        padding,
        query_weight,
        key_weight,
        value_weight,
        query_bias,
        value_bias,
        out_weight,
        out_bias,
        middle_gain,
        middle_shift,
        up_weight,
        up_bias,
        down_weight,
        down_bias,
        final_gain,
        final_shift,
        cotangent,
    ) = arrays
    planes = count // PLANE
    rows = query_weight.shape[0]
    block = down_weight.shape[0]
    x_own = tokens[0]
    here = x_own.shape[0]
    wide = PLANE * here
    me = lax.axis_index("shard")
    group = lax.rem(me, PLANE)
    qkv_send = jnp.concatenate(
        [
            item.astype(bf16).reshape(rows, PLANE, GROUP_DIM)
            for item in (query_weight, key_weight, value_weight)
        ],
        axis=2,
    ).transpose(1, 0, 2)
    up_send = (
        up_weight.astype(bf16)
        .reshape(rows, planes, PLANE, block)
        .transpose(2, 0, 1, 3)
        .reshape(PLANE, rows, GROUP_FF)
    )
    codes = (2 * segments[0] + padding[0]).astype(f32)
    lanes = 128 * ((max(here, block) + 127) // 128)

    def padded(value):
        return jnp.pad(value.astype(f32), (0, lanes - value.shape[0]))

    vectors = [
        query_bias,
        value_bias,
        out_bias,
        middle_gain,
        middle_shift,
        down_bias,
        final_gain,
        final_shift,
        up_bias,
        codes,
    ]
    small_send = jnp.pad(
        jnp.stack([padded(item) for item in vectors]), ((0, 6), (0, 0))
    ).astype(bf16)
    lines = [[start + PLANE * step for step in range(planes)] for start in range(PLANE)]
    w_down = lax.all_gather(
        down_weight.astype(bf16), "shard", axis_index_groups=lines, axis=0
    ).reshape(GROUP_FF, D)
    x_all, qkv_all, up_all, wo_all, small = gather_weights(
        count,
        copies,
        x_own,
        qkv_send,
        up_send,
        out_weight.astype(bf16),
        small_send,
        0,
    )
    x_plane = x_all.reshape(wide, D)
    w_qkv = qkv_all.reshape(D, 3 * GROUP_DIM)
    strip = up_all.reshape(PLANE * rows, D)
    w_out = wo_all.reshape(GROUP_DIM, D)
    small = small.astype(f32)
    spread = [small[:, index, :rows].reshape(D) for index in range(8)]
    b_query, b_value, b_out, gain_mid, shift_mid, b_down, gain_end, shift_end = spread
    b_up = lax.dynamic_index_in_dim(
        small[:, 8, :block].reshape(planes, PLANE, block), group, 1, keepdims=False
    ).reshape(GROUP_FF)
    all_codes = small[:, 9, :here].reshape(planes, wide)
    own_codes = lax.dynamic_index_in_dim(all_codes, lax.div(me, PLANE), 0, keepdims=False)

    def group_part(value):
        return lax.dynamic_slice(value, (group * GROUP_DIM,), (GROUP_DIM,))

    qkv_bias = jnp.concatenate(
        [group_part(b_query), jnp.zeros((GROUP_DIM,), f32), group_part(b_value)]
    )
    qkv = (dot(x_plane, w_qkv) + qkv_bias).astype(bf16)
    w_down, qkv = lax.optimization_barrier((w_down, qkv))
    queries = qkv[:, :GROUP_DIM] * bf16(0.125)
    own_row, key_cols = own_codes[None], all_codes[:, :, None]
    pairs, context, logs = attend_ahead(
        count, queries, qkv[:, GROUP_DIM:], own_row, key_cols, 1
    )
    strip, pairs = lax.optimization_barrier((strip, pairs))
    w_up = lax.all_gather(strip, "shard", axis_index_groups=lines, axis=0).reshape(D, GROUP_FF)
    context_low = context.astype(bf16)

    def split(value):
        return value.reshape(PLANE, here, D)

    def enter_middle(total, pieces, lines):
        rest = total + lines[0] + pieces[0]
        middle, _, _ = norm_forward(rest, lines[1], lines[2])
        return middle.astype(bf16), [rest], []

    def enter_end(total, pieces, lines):
        middle, _, _ = norm_forward(pieces[0], lines[1], lines[2])
        result, normal, scale = norm_forward(middle + (total + lines[0]), lines[3], lines[4])
        above = pieces[1]
        back = norm_backward(above, normal, scale, lines[3])
        rounded = back.astype(bf16)
        return rounded, [result, back], [above * normal, above, rounded.astype(f32)]

    def leave_middle(total, pieces, lines):
        _, normal, scale = norm_forward(pieces[0], lines[0], lines[0])
        above = total + pieces[1]
        back = norm_backward(above, normal, scale, lines[0])
        rounded = back.astype(bf16)
        return rounded, [back], [above * normal, above, rounded.astype(f32)]

    middle_all, _, rest = plane_step(
        split(dot_left(context_low, w_out).astype(bf16)),
        [x_own],
        [b_out, gain_mid, shift_mid],
        enter_middle,
        [f32],
        2,
    )
    middle_plane = middle_all.reshape(wide, D)
    hidden = dot(middle_plane, w_up) + b_up
    active_low = jax.nn.gelu(hidden, approximate=False).astype(bf16)
    feed_all, end_sums, result, d_second = plane_step(
        split(dot(active_low, w_down).astype(bf16)),
        [rest, cotangent[0]],
        [b_down, gain_mid, shift_mid, gain_end, shift_end],
        enter_end,
        [bf16, f32],
        3,
    )
    output = result[None]
    feed_plane = feed_all.reshape(wide, D)
    grad_down = dot_left(active_low, feed_plane).astype(bf16)
    up_low = (dot_right(feed_plane, w_down) * gelu_slope(hidden)).astype(bf16)
    grad_up = dot_left(middle_plane, up_low).astype(bf16)
    strip_grads = lax.psum_scatter(
        jnp.concatenate(
            [
                grad_up.reshape(planes, PLANE * rows, GROUP_FF),
                grad_down.reshape(planes, block, D),
            ],
            axis=1,
        ),
        "shard",
        axis_index_groups=lines,
        scatter_dimension=0,
    )
    branch_all, middle_sums, d_first = plane_step(
        split(dot_right(up_low, w_up).astype(bf16)),
        [rest, d_second],
        [gain_mid],
        leave_middle,
        [f32],
        4,
    )
    branch_plane = branch_all.reshape(wide, D)
    grad_out = dot(context_low, branch_plane).astype(bf16)
    d_context = dot_right(branch_plane, w_out).astype(bf16)
    delta = jnp.sum(
        (d_context.astype(f32).T * context).reshape(GROUP_HEADS, HEAD_DIM, wide), axis=1
    )
    query_low, pair_low = attend_back(
        count,
        queries,
        d_context,
        pairs,
        own_row,
        key_cols,
        logs,
        delta,
        8,
    )
    mixer_low = jnp.concatenate([query_low.T, pair_low], axis=1)
    grad_qkv = dot_left(x_plane, mixer_low).astype(bf16)
    mixer_sums = jnp.sum(mixer_low.astype(f32), axis=0)

    def from_group(value):
        return lax.dynamic_update_slice(jnp.zeros((D,), f32), value, (group * GROUP_DIM,))

    sums = [
        from_group(mixer_sums[:GROUP_DIM]),
        from_group(mixer_sums[2 * GROUP_DIM :]),
        middle_sums[2],
        middle_sums[0],
        middle_sums[1],
        end_sums[2],
        end_sums[0],
        end_sums[1],
    ]
    own_lane = (jnp.arange(PLANE) == group).astype(f32)
    up_sums = jnp.sum(up_low.astype(f32), axis=0).reshape(planes, 1, block)
    up_sums = (up_sums * own_lane[None, :, None]).reshape(count, 1, block)
    sums = jnp.stack([item.reshape(count, rows) for item in sums], axis=1)
    small_grads = jnp.concatenate(
        [
            jnp.pad(sums, ((0, 0), (0, 0), (0, lanes - rows))),
            jnp.pad(up_sums, ((0, 0), (0, 7), (0, lanes - block))),
        ],
        axis=1,
    ).astype(bf16)
    query_grad, key_grad, value_grad, up_grad, out_total, small_total, down_total, grad_tokens = reduce_grads(
        count,
        copies,
        grad_qkv.reshape(count, rows, 3 * GROUP_DIM),
        strip_grads[: PLANE * rows].reshape(PLANE, rows, GROUP_FF),
        grad_out.reshape(planes, rows, D),
        strip_grads[PLANE * rows :],
        small_grads,
        split(dot_right(mixer_low, w_qkv).astype(bf16)),
        d_first,
        10,
    )

    return (
        output,
        grad_tokens[None],
        query_grad,
        key_grad,
        value_grad,
        small_total[0, :rows],
        small_total[1, :rows],
        out_total,
        small_total[2, :rows],
        small_total[3, :rows],
        small_total[4, :rows],
        up_grad,
        small_total[8, :block],
        down_total,
        small_total[5, :rows],
        small_total[6, :rows],
        small_total[7, :rows],
    )


def solution(mesh):
    sheet, line = P("shard", None), P("shard")
    batch = P("rep", "shard", None)
    in_specs = (batch, P("rep", "shard"), P("rep", "shard"), sheet, sheet, sheet, line, line)
    in_specs += (sheet, line, line, line, sheet, line, sheet, line, line, line, batch)
    out_specs = (batch, batch, sheet, sheet, sheet, line, line, sheet, line, line, line)
    out_specs += (sheet, line, sheet, line, line, line)
    body = functools.partial(shards, mesh.shape["shard"], mesh.shape["rep"])
    return jax.shard_map(
        body, mesh=mesh, in_specs=in_specs, out_specs=out_specs, check_vma=False
    )
```

```python
import functools

import jax
import jax.numpy as jnp
from jax import lax
from jax.experimental import pallas as pl
from jax.experimental.pallas import tpu as pltpu
from jax.sharding import PartitionSpec as P

D = 768
HEADS = 12
HEAD_DIM = 64
PLANE = 4
GROUP_HEADS = HEADS // PLANE
GROUP_DIM = GROUP_HEADS * HEAD_DIM
FF = 3072
GROUP_FF = FF // PLANE

epsilon = 1e-12
very_low = -1e30
root_half = 0.7071067811865476
inv_root_tau = 0.3989422804014327
bf16 = jnp.bfloat16
f32 = jnp.float32
MESH = pl.DeviceIdType.MESH
VMEM_SPEC = pl.BlockSpec(memory_space=pltpu.VMEM)
ANY_SPEC = pl.BlockSpec(memory_space=pl.ANY)
VMEM_BYTES = 60000 * 1024
MODEL_BYTES = 100_000_000


def struct(shape, dtype=bf16):
    return jax.ShapeDtypeStruct(shape, dtype)


def comm_call(body, name, ident, inputs, out_shapes, out_specs, scratch):
    return pl.pallas_call(
        body,
        name=name,
        out_shape=out_shapes,
        in_specs=[VMEM_SPEC] * len(inputs),
        out_specs=out_specs,
        scratch_shapes=scratch,
        cost_estimate=pl.CostEstimate(flops=0, bytes_accessed=MODEL_BYTES, transcendentals=0),
        compiler_params=pltpu.CompilerParams(
            collective_id=ident, has_side_effects=True, vmem_limit_bytes=VMEM_BYTES
        ),
    )(*inputs)


def greet(peers):
    barrier = pltpu.get_barrier_semaphore()
    for peer in peers:
        pl.semaphore_signal(barrier, inc=1, device_id=peer, device_id_type=MESH)
    pl.semaphore_wait(barrier, len(peers))


def remote(src, dst, send_sem, recv_sem, peer):
    return pltpu.make_async_remote_copy(
        src_ref=src,
        dst_ref=dst,
        send_sem=send_sem,
        recv_sem=recv_sem,
        device_id=peer,
        device_id_type=MESH,
    )


def plane_peer(me, mask):
    group = lax.rem(me, PLANE)
    core = lax.rem(group, 2)
    column = lax.div(group, 2)
    if mask & 1:
        core = 1 - core
    if mask & 2:
        column = 1 - column
    return me - group + 2 * column + core


def plane_slot(me, mask):
    return lax.rem(plane_peer(me, mask), PLANE)


def plane_step(parts, pieces, vectors, action, out_types, ident):
    _, rows, cols = parts.shape
    chunks = 3 if rows % 48 == 0 else 1
    size = rows // chunks
    many, few = len(pieces), len(out_types)

    def body(p_ref, *rest):
        piece_refs, vector_ref = rest[:many], rest[many]
        all_ref, sums_ref = rest[many + 1 : many + 3]
        out_refs = rest[many + 3 : many + 3 + few]
        near, held, far_in, low, send, recv = rest[many + 3 + few :]
        me = lax.axis_index("shard")
        beside, across = [{"shard": plane_peer(me, mask)} for mask in (1, 2)]
        mine, far = lax.rem(me, PLANE), plane_slot(me, 2)
        greet([beside, across])
        spans = [pl.ds(size * index, size) for index in range(chunks)]

        def copy(kind, index):
            span = spans[index]
            table = {
                0: lambda: (p_ref.at[plane_slot(me, 3), span], near.at[0, span], beside),
                1: lambda: (p_ref.at[plane_slot(me, 1), span], near.at[1, span], beside),
                2: lambda: (held.at[span], far_in.at[span], across),
                3: lambda: (low.at[span], all_ref.at[mine, span], across),
                4: lambda: (low.at[span], all_ref.at[mine, span], beside),
                5: lambda: (all_ref.at[far, span], all_ref.at[far, span], beside),
            }
            src, dst, peer = table[kind]()
            return remote(src, dst, send.at[kind, index], recv.at[kind, index], peer)

        for index in range(chunks):
            copy(0, index).start()
        for index in range(chunks):
            copy(1, index).start()
        for index in range(chunks):
            span = spans[index]
            copy(0, index).wait_recv()
            total = p_ref[plane_slot(me, 2), span].astype(f32) + near[0, span].astype(f32)
            held[span] = total.astype(bf16)
            copy(2, index).start()
        lines = [vector_ref[index : index + 1] for index in range(len(vectors))]
        sums = None
        for index in range(chunks):
            span = spans[index]
            copy(1, index).wait_recv()
            copy(2, index).wait_recv()
            total = p_ref[mine, span].astype(f32) + near[1, span].astype(f32)
            total = total + far_in[span].astype(f32)
            result, outs, terms = action(
                total, [item[span].astype(f32) for item in piece_refs], lines
            )
            low[span] = result
            copy(3, index).start()
            copy(4, index).start()
            for ref, value in zip(out_refs, outs):
                ref[span] = value.astype(ref.dtype)
            all_ref[mine, span] = result
            terms = [jnp.sum(item, axis=0, keepdims=True) for item in terms]
            sums = terms if sums is None else [x + y for x, y in zip(sums, terms)]
        sums_ref[...] = jnp.zeros(sums_ref.shape, f32)
        for place, value in enumerate(sums):
            sums_ref[place : place + 1] = value
        for index in range(chunks):
            copy(3, index).wait_recv()
            copy(5, index).start()
        for index in range(chunks):
            copy(4, index).wait_recv()
            copy(5, index).wait_recv()
        for index in range(chunks):
            for kind in range(6):
                copy(kind, index).wait_send()

    stack = jnp.stack(vectors)
    shape = (rows, cols)
    return comm_call(
        body,
        "plane_step",
        ident,
        [parts] + list(pieces) + [stack],
        [struct((PLANE, rows, cols)), struct((8, cols), f32)]
        + [struct(shape, item) for item in out_types],
        [VMEM_SPEC] * (2 + few),
        [
            pltpu.VMEM((2, rows, cols), bf16),
            pltpu.VMEM(shape, bf16),
            pltpu.VMEM(shape, bf16),
            pltpu.VMEM(shape, bf16),
            pltpu.SemaphoreType.DMA((6, chunks)),
            pltpu.SemaphoreType.DMA((6, chunks)),
        ],
    )


def others(me, count):
    return [{"shard": lax.rem(me + step, count)} for step in range(1, count)]


def gather_weights(count, copies, tokens, qkv, up, out_w, small, ident):
    planes = count // PLANE
    rows = qkv.shape[1]

    def body(x_ref, qkv_ref, up_ref, wo_ref, small_ref, *rest):
        x_out, qkv_out, up_out, wo_out, small_out = rest[:5]
        send, recv, local, send_wo, recv_wo, send_unit, recv_unit = rest[5:]
        me = lax.axis_index("shard")
        group, plane = lax.rem(me, PLANE), lax.div(me, PLANE)
        across = [
            {"rep": lax.rem(lax.axis_index("rep") + step, copies)} for step in range(1, copies)
        ]
        greet(others(me, count) + across)
        owns = [
            (x_ref, x_out.at[group]),
            (qkv_ref.at[group], qkv_out.at[me]),
            (up_ref.at[group], up_out.at[group]),
            (small_ref, small_out.at[me]),
        ]
        started = []
        for index, (src, dst) in enumerate(owns):
            copy = pltpu.make_async_copy(src, dst, local.at[index])
            copy.start()
            started.append(copy)
        sent = []

        def push(src, dst, peer):
            index = len(sent)
            copy = remote(src, dst, send.at[index], recv.at[index], {"shard": peer})
            copy.start()
            sent.append(copy)

        for mask in (2, 1):
            push(x_ref, x_out.at[group], plane_peer(me, mask))
        far = plane_slot(me, 2)
        x_relay = remote(
            x_out.at[far], x_out.at[far], send.at[2], recv.at[2], {"shard": plane_peer(me, 1)}
        )
        sent.append(x_relay)
        for step in range(1, count):
            push(small_ref, small_out.at[me], lax.rem(me + step, count))
        rep = lax.axis_index("rep")
        split = copies == 2
        units = []
        for step in range(planes):
            for lane in range(PLANE):
                if step or lane:
                    units.append((qkv_ref, qkv_out, step, lane))
        for lane in range(1, PLANE):
            units.append((up_ref, up_out, 0, lane))

        def unit_copy(index):
            src, dst, step, lane = units[index]
            goal = lax.rem(plane + step, planes)
            goal_group = lax.rem(group + lane, PLANE)
            slot = group if src is up_ref else me
            return remote(
                src.at[goal_group],
                dst.at[slot],
                send_unit.at[index],
                recv_unit.at[index],
                {"shard": goal * PLANE + goal_group},
            )

        def unit_relay(index):
            src, dst, step, lane = units[index]
            origin = lax.rem(plane + planes - step, planes)
            origin_group = lax.rem(group + PLANE - lane, PLANE)
            slot = origin_group if src is up_ref else origin * PLANE + origin_group
            return remote(
                dst.at[slot],
                dst.at[slot],
                send_unit.at[index],
                recv_unit.at[index],
                {"rep": lax.rem(rep + 1, copies)},
            )

        def carried(index, mine):
            step = units[index][2]
            if not split or step == 0:
                return None
            return (rep == step % 2) if mine else (rep != step % 2)

        def guarded(test, action):
            if test is None:
                action()
            else:
                pl.when(test)(action)

        for index in range(len(units)):
            guarded(carried(index, True), unit_copy(index).start)
        target, place = lax.div(me, planes), lax.rem(me, planes)

        def wo_copy(source, index):
            peer = PLANE * index + target
            return peer, remote(
                wo_ref, wo_out.at[place], send_wo.at[index], recv_wo.at[source], {"shard": peer}
            )

        for index in range(planes):
            peer, copy = wo_copy(place, index)
            pl.when(peer != me)(copy.start)
        keep = pltpu.make_async_copy(wo_ref, wo_out.at[place], local.at[5])
        pl.when(target == group)(keep.start)
        sent[0].wait_recv()
        x_relay.start()
        for index, (_, _, step, _) in enumerate(units):
            if split and step:

                @pl.when(rep == step % 2)
                def _(index=index):
                    unit_relay(index).wait_recv()
                    unit_copy(index).wait_send()
                    unit_relay(index).start()

            else:
                unit_copy(index).wait_recv()
                unit_copy(index).wait_send()
        for index, (_, _, step, _) in enumerate(units):
            if split and step:
                pl.when(rep != step % 2)(unit_relay(index).wait_recv)
                pl.when(rep == step % 2)(unit_relay(index).wait_send)
        for copy in sent[1:]:
            copy.wait_recv()
        for index in range(planes):
            pl.when(group * planes + index != me)(wo_copy(index, index)[1].wait_recv)
        for index in range(planes):
            peer, copy = wo_copy(place, index)
            pl.when(peer != me)(copy.wait_send)
        pl.when(target == group)(keep.wait)
        for copy in sent:
            copy.wait_send()
        for copy in started:
            copy.wait()

    total = 3 + count - 1
    number = count - 1 + PLANE - 1
    return comm_call(
        body,
        "gather_weights",
        ident,
        [tokens, qkv, up, out_w, small],
        [
            struct((PLANE,) + tokens.shape),
            struct((count, rows, qkv.shape[2])),
            struct((PLANE, rows, up.shape[2])),
            struct((planes,) + out_w.shape),
            struct((count,) + small.shape),
        ],
        [ANY_SPEC] * 5,
        [
            pltpu.SemaphoreType.DMA((total,)),
            pltpu.SemaphoreType.DMA((total,)),
            pltpu.SemaphoreType.DMA((6,)),
            pltpu.SemaphoreType.DMA((planes,)),
            pltpu.SemaphoreType.DMA((planes,)),
            pltpu.SemaphoreType.DMA((number,)),
            pltpu.SemaphoreType.DMA((number,)),
        ],
    )


def reduce_grads(count, copies, qkv, up, out_w, down, small, parts, ident):
    planes = count // PLANE
    rows = qkv.shape[1]
    block = down.shape[0]
    arrays = [qkv, up, out_w, small]
    split = copies == 2 and planes % 2 == 0
    pieces = planes // 2

    def body(qkv_ref, up_ref, wo_ref, small_ref, down_ref, p_ref, *rest):
        outs, token_ref, rest = rest[:5], rest[5], rest[6:]
        mix_ref, wide_ref = outs[:2]
        qkv_in, up_in, wo_in, small_in = rest[:4]
        halves = [ref.at[0] for ref in outs[:4]] + [down_ref]
        near, near_sum, far_in = rest[4:7]
        peer_q, sum_q, in_q = rest[7:10]
        send, recv, send_rep, recv_rep, send_wo, recv_wo, send_near, recv_near = rest[10:18]
        send_y, recv_y, send_q, recv_q = rest[18:]
        me = lax.axis_index("shard")
        rep = lax.axis_index("rep")
        plane = lax.div(me, PLANE)
        across = [{"rep": lax.rem(rep + step, copies)} for step in range(1, copies)]
        greet(others(me, count) + across)
        sent = []

        def push(src, dst, peer):
            index = len(sent)
            copy = remote(src, dst, send.at[index], recv.at[index], {"shard": peer})
            copy.start()
            sent.append(copy)

        pairs = [(small_ref, small_in)] if split else [(qkv_ref, qkv_in), (small_ref, small_in)]
        swaps = []
        if split:
            for index in range(pieces):
                goal = lax.rem(plane + 1 - rep + 2 * index, planes)
                swaps.append(
                    remote(
                        qkv_ref.at[pl.ds(goal * PLANE, PLANE)],
                        peer_q.at[index],
                        send_y.at[index],
                        recv_y.at[index],
                        across[0],
                    )
                )
            for copy in swaps[::-1]:
                copy.start()
        passed = []
        beside, over = [{"shard": plane_peer(me, mask)} for mask in (1, 2)]
        near_copies = [
            remote(p_ref.at[plane_slot(me, 3)], near.at[0], send_near.at[0], recv_near.at[0], beside),
            remote(p_ref.at[plane_slot(me, 1)], near.at[1], send_near.at[1], recv_near.at[1], beside),
            remote(near_sum, far_in, send_near.at[2], recv_near.at[2], over),
        ]
        near_copies[0].start()
        near_copies[1].start()

        def exchange(*places):
            for index, peer in enumerate(across):
                for place in places:
                    copy = remote(
                        halves[place],
                        outs[place].at[index if place == 4 else index + 1],
                        send_rep.at[5 * index + place],
                        recv_rep.at[5 * index + place],
                        peer,
                    )
                    copy.start()
                    passed.append(copy)

        exchange(4)
        group = lax.rem(me, PLANE)
        target, place = lax.div(me, planes), lax.rem(me, planes)
        for lane in range(1, PLANE):
            goal = lax.rem(group + lane, PLANE)
            push(up_ref.at[goal], up_in.at[group], plane * PLANE + goal)
        up_in[group] = up_ref[group]
        for src, held in pairs:
            for step in range(1, count):
                peer = lax.rem(me + step, count)
                push(src.at[peer], held.at[me], peer)
        for src, held in pairs:
            held[me] = src[me]

        def wo_copy(source, index):
            peer = group * planes + index
            return peer, remote(
                wo_ref.at[index],
                wo_in.at[plane],
                send_wo.at[index],
                recv_wo.at[source],
                {"shard": peer},
            )

        for index in range(planes):
            peer, copy = wo_copy(plane, index)
            pl.when(peer != me)(copy.start)

        @pl.when(target == group)
        def _():
            wo_in[plane] = wo_ref[place]

        moved = []
        for index in reversed(range(pieces if split else 0)):
            goal = lax.rem(plane + rep + 2 * index, planes)
            swaps[index].wait_recv()
            for lane in range(PLANE):
                total = qkv_ref[goal * PLANE + lane].astype(f32) + peer_q[index, lane].astype(f32)
                sum_q[index, lane] = total.astype(bf16)
            for step in range(PLANE):
                lane = lax.rem(group + step, PLANE)
                number = index * PLANE + step
                copy = remote(
                    sum_q.at[index, lane],
                    in_q.at[index, group],
                    send_q.at[number],
                    recv_q.at[number],
                    {"shard": goal * PLANE + lane},
                )
                if number:
                    copy.start()
                else:
                    pl.when(rep != 0)(copy.start)

                    @pl.when(rep == 0)
                    def _():
                        in_q[0, group] = sum_q[0, group]

                moved.append((number, copy))
        near_copies[0].wait_recv()
        total = p_ref[plane_slot(me, 2)].astype(f32) + near[0].astype(f32)
        near_sum[...] = total.astype(bf16)
        near_copies[2].start()
        for copy in sent[: PLANE - 1]:
            copy.wait_recv()
        for lane in range(PLANE):
            value = up_in[lane]
            for index in range(planes):
                low = (index * PLANE + lane) * block
                wide_ref[0, :, low : low + block] = value[:, index * block : (index + 1) * block]
        exchange(1)
        for index in range(planes):
            pl.when(PLANE * index + target != me)(wo_copy(index, index)[1].wait_recv)
        for index in range(planes):
            peer, copy = wo_copy(plane, index)
            pl.when(peer != me)(copy.wait_send)
        total = wo_in[0].astype(f32)
        for other in range(1, planes):
            total = total + wo_in[other].astype(f32)
        halves[2][...] = total.astype(bf16)
        exchange(2)
        near_copies[1].wait_recv()
        near_copies[2].wait_recv()
        total = p_ref[lax.rem(me, PLANE)].astype(f32) + near[1].astype(f32)
        token_ref[...] = total + far_in[...].astype(f32)
        for copy in sent[PLANE - 1 :]:
            copy.wait_recv()
        for number, copy in moved:
            if number:
                copy.wait_recv()
            else:
                pl.when(rep != 0)(copy.wait_recv)
        for lane in range(PLANE):
            if split:
                terms = [in_q[index, lane] for index in range(pieces)]
            else:
                terms = [qkv_in[other * PLANE + lane] for other in range(planes)]
            total = terms[0].astype(f32)
            for term in terms[1:]:
                total = total + term.astype(f32)
            total = total.astype(bf16)
            for place in range(3):
                low = place * GROUP_DIM
                mix_ref[0, place, :, lane * GROUP_DIM : (lane + 1) * GROUP_DIM] = total[
                    :, low : low + GROUP_DIM
                ]
        for half, held, number in (
            (halves[3], small_in, count),
        ):
            total = held[0].astype(f32)
            for other in range(1, number):
                total = total + held[other].astype(f32)
            half[...] = total.astype(bf16)
        exchange(0, 3)
        for copy in passed:
            copy.wait_recv()
        for copy in sent + passed + near_copies + swaps:
            copy.wait_send()
        for number, copy in moved:
            if number:
                copy.wait_send()
            else:
                pl.when(rep != 0)(copy.wait_send)

    totals = (1 if split else 2) * (count - 1) + PLANE - 1
    shapes = [
        (copies, 3, rows, D),
        (copies, rows, FF),
        (copies, rows, D),
        (copies,) + small.shape[1:],
        (copies - 1, block, D),
    ]
    return comm_call(
        body,
        "reduce_grads",
        ident,
        arrays + [down, parts],
        [struct(shape) for shape in shapes] + [struct(parts.shape[1:], f32)],
        [VMEM_SPEC] * 6,
        [pltpu.VMEM(item.shape, bf16) for item in arrays]
        + [
            pltpu.VMEM((2,) + parts.shape[1:], bf16),
            pltpu.VMEM(parts.shape[1:], bf16),
            pltpu.VMEM(parts.shape[1:], bf16),
            pltpu.VMEM((pieces, PLANE) + qkv.shape[1:], bf16),
            pltpu.VMEM((pieces, PLANE) + qkv.shape[1:], bf16),
            pltpu.VMEM((pieces, PLANE) + qkv.shape[1:], bf16),
            pltpu.SemaphoreType.DMA((totals,)),
            pltpu.SemaphoreType.DMA((totals,)),
            pltpu.SemaphoreType.DMA((5 * (copies - 1),)),
            pltpu.SemaphoreType.DMA((5 * (copies - 1),)),
            pltpu.SemaphoreType.DMA((planes,)),
            pltpu.SemaphoreType.DMA((planes,)),
            pltpu.SemaphoreType.DMA((3,)),
            pltpu.SemaphoreType.DMA((3,)),
            pltpu.SemaphoreType.DMA((pieces,)),
            pltpu.SemaphoreType.DMA((pieces,)),
            pltpu.SemaphoreType.DMA((pieces * PLANE,)),
            pltpu.SemaphoreType.DMA((pieces * PLANE,)),
        ],
    )


def pick(plane, table):
    value = table[-1]
    for index in range(len(table) - 1):
        value = jnp.where(plane == index, table[index], value)
    return value


def columns(code_ref, col_ref):
    for index in range(code_ref.shape[0]):
        line = jnp.broadcast_to(code_ref[index : index + 1], (8, code_ref.shape[1]))
        col_ref[index] = line.T[:, 0:1]


def attend_back(count, queries, upstream, pairs, own_row, codes, logs, delta, ident):
    planes, rows, cols = pairs.shape
    half = cols // 2
    size = 256 if rows % 256 == 0 else rows
    orders = []
    for plane in range(planes):
        goals = [goal for goal in range(planes) if goal != plane]
        goals.sort(key=lambda goal: (-abs(goal - plane), goal))
        orders.append(goals + [plane])

    def body(q_ref, up_ref, kv_ref, row_ref, code_ref, log_ref, delta_ref, *rest):
        dq_ref, out_ref, dq_sum, part, held, staged, col_ref, send, recv = rest
        me = lax.axis_index("shard")
        plane = lax.div(me, PLANE)
        greet([{"shard": lax.rem(me + PLANE * s, count)} for s in range(1, planes)])
        columns(code_ref, col_ref)
        dq_sum[...] = jnp.zeros(dq_sum.shape, f32)

        def hop(way, goal):
            peer = me + PLANE if way == 0 else me - PLANE
            return remote(
                staged.at[goal],
                held.at[way, goal],
                send.at[goal],
                recv.at[way, goal],
                {"shard": lax.rem(peer + count, count)},
            )

        def compute(goal):
            part[...] = jnp.zeros(part.shape, f32)
            key_codes = col_ref[goal]

            def chunk(index, carry):
                at = pl.multiple_of(index * size, size)
                span = pl.ds(at, size)
                allowed = key_codes == row_ref[0:1, span]
                for head in range(GROUP_HEADS):
                    low, high = head * HEAD_DIM, (head + 1) * HEAD_DIM
                    q = q_ref[span, low:high]
                    g = up_ref[span, low:high]
                    k = kv_ref[goal, :, low:high]
                    v = kv_ref[goal, :, half + low : half + high]
                    raw = dot_right(k, q)
                    chances = jnp.where(
                        allowed, jnp.exp(raw - log_ref[head : head + 1, span]), 0.0
                    )
                    d_chance = dot_right(v, g)
                    d_score = (chances * (d_chance - delta_ref[head : head + 1, span])).astype(bf16)
                    dq_sum[low:high, span] += dot_left(k, d_score)
                    part[:, low:high] += dot(d_score, q)
                    part[:, half + low : half + high] += dot(chances.astype(bf16), g)
                return carry

            lax.fori_loop(0, rows // size, chunk, 0)

        def pass_on(goal):
            for way in (0, 1):
                ahead = goal > plane if way == 0 else goal < plane
                first = plane == 0 if way == 0 else plane == planes - 1

                @pl.when(ahead & jnp.logical_not(first))
                def _(way=way):
                    copy = hop(way, goal)
                    copy.wait_recv()
                    total = staged[goal].astype(f32) + held[way, goal].astype(f32)
                    staged[goal] = total.astype(bf16)
                    copy.start()

        def begin(goal):
            for way in (0, 1):
                ahead = goal > plane if way == 0 else goal < plane
                first = plane == 0 if way == 0 else plane == planes - 1

                @pl.when(ahead & first)
                def _(way=way):
                    hop(way, goal).start()

        goals = [pick(plane, [order[i] for order in orders]) for i in range(planes)]
        for index in range(planes):
            goal = goals[index]
            compute(goal)
            if index < planes - 1:
                staged[goal] = part[...].astype(bf16)
                begin(goal)
            if index:
                pass_on(goals[index - 1])
        dq_ref[...] = (dq_sum[...] * 0.125).astype(bf16)
        for way in (0, 1):
            behind = plane > 0 if way == 0 else plane < planes - 1

            @pl.when(behind)
            def _(way=way):
                hop(way, plane).wait_recv()
                part[...] += held[way, plane].astype(f32)

        out_ref[...] = part[...].astype(bf16)
        for index in range(planes - 1):
            hop(0, goals[index]).wait_send()

    return comm_call(
        body,
        "attend_back",
        ident,
        [queries, upstream, pairs, own_row, codes, logs, delta],
        [struct((half, rows)), struct((rows, cols))],
        [VMEM_SPEC] * 2,
        [
            pltpu.VMEM((half, rows), f32),
            pltpu.VMEM((rows, cols), f32),
            pltpu.VMEM((2, planes, rows, cols), bf16),
            pltpu.VMEM((planes, rows, cols), bf16),
            pltpu.VMEM((planes, rows, 1), f32),
            pltpu.SemaphoreType.DMA((planes,)),
            pltpu.SemaphoreType.DMA((2, planes)),
        ],
    )


def attend_ahead(count, queries, own_pair, own_row, codes, ident):
    planes = count // PLANE
    rows, cols = own_pair.shape
    half = cols // 2
    size = 256 if rows % 256 == 0 else rows
    orders, flags = [], []
    for plane in range(planes):
        order = sorted(range(planes), key=lambda source: (abs(source - plane), source))
        away = [abs(source - plane) for source in order] + [-1]
        orders.append(order)
        flags.append([int(i > 0 and away[i] == away[i + 1]) for i in range(planes)])

    def body(q_ref, kv_ref, row_ref, code_ref, all_ref, ctx_ref, log_ref, *rest):
        top, total, col_ref, send, recv, local = rest
        me = lax.axis_index("shard")
        plane = lax.div(me, PLANE)
        greet([{"shard": lax.rem(me + PLANE * s, count)} for s in range(1, planes)])
        own = pltpu.make_async_copy(kv_ref, all_ref.at[plane], local)
        own.start()
        up, down = plane < planes - 1, plane > 0

        def hop(way, source, src):
            peer = me + PLANE if way == 0 else me - PLANE
            return remote(
                src,
                all_ref.at[source],
                send.at[way, source],
                recv.at[way, source],
                {"shard": lax.rem(peer + count, count)},
            )

        pl.when(up)(hop(0, plane, kv_ref).start)
        pl.when(down)(hop(1, plane, kv_ref).start)
        columns(code_ref, col_ref)
        top[...] = jnp.full(top.shape, very_low, f32)
        total[...] = jnp.zeros(total.shape, f32)
        ctx_ref[...] = jnp.zeros(ctx_ref.shape, f32)

        def take(source, test):
            for way in (0, 1):
                came = source < plane if way == 0 else source > plane
                onward = up if way == 0 else down

                @pl.when(test & came)
                def _(way=way, onward=onward):
                    copy = hop(way, source, all_ref.at[source])
                    copy.wait_recv()
                    pl.when(onward)(copy.start)

        def compute(source, block):
            key_codes = col_ref[source]

            def chunk(index, carry):
                span = pl.ds(pl.multiple_of(index * size, size), size)
                allowed = key_codes == row_ref[0:1, span]
                for head in range(GROUP_HEADS):
                    low, high = head * HEAD_DIM, (head + 1) * HEAD_DIM
                    line = slice(head, head + 1)
                    raw = dot_right(block[:, low:high], q_ref[span, low:high])
                    masked = jnp.where(allowed, raw, very_low)
                    before = top[line, span]
                    after = jnp.maximum(before, jnp.max(masked, axis=0, keepdims=True))
                    rescale = jnp.exp(before - after)
                    weights = jnp.exp(masked - after)
                    top[line, span] = after
                    total[line, span] = total[line, span] * rescale + jnp.sum(
                        weights, axis=0, keepdims=True
                    )
                    added = dot_left(block[:, half + low : half + high], weights.astype(bf16))
                    ctx_ref[low:high, span] = ctx_ref[low:high, span] * rescale + added
                return carry

            lax.fori_loop(0, rows // size, chunk, 0)

        compute(plane, kv_ref)
        sources = [pick(plane, [order[i] for order in orders]) for i in range(planes)]
        early = [pick(plane, [flag[i] for flag in flags]) == 1 for i in range(planes)]
        for index in range(1, planes):
            test = jnp.logical_not(early[index - 1])
            take(sources[index], test)
            if index + 1 < planes:
                take(sources[index + 1], early[index])
            compute(sources[index], all_ref.at[sources[index]])
        log_ref[...] = top[...] + jnp.log(total[...])
        for head in range(GROUP_HEADS):
            low, high = head * HEAD_DIM, (head + 1) * HEAD_DIM
            ctx_ref[low:high] = ctx_ref[low:high] / total[head : head + 1]
        pl.when(up)(hop(0, plane, kv_ref).wait_send)
        pl.when(down)(hop(1, plane, kv_ref).wait_send)
        for index in range(1, planes):
            source = sources[index]
            pl.when((source < plane) & up)(hop(0, source, all_ref.at[source]).wait_send)
            pl.when((source > plane) & down)(hop(1, source, all_ref.at[source]).wait_send)
        own.wait()

    return comm_call(
        body,
        "attend_ahead",
        ident,
        [queries, own_pair, own_row, codes],
        [
            struct((planes, rows, cols)),
            struct((half, rows), f32),
            struct((GROUP_HEADS, rows), f32),
        ],
        [VMEM_SPEC] * 3,
        [
            pltpu.VMEM((GROUP_HEADS, rows), f32),
            pltpu.VMEM((GROUP_HEADS, rows), f32),
            pltpu.VMEM((planes, rows, 1), f32),
            pltpu.SemaphoreType.DMA((2, planes)),
            pltpu.SemaphoreType.DMA((2, planes)),
            pltpu.SemaphoreType.DMA,
        ],
    )


def norm_forward(value, gain, shift):
    center = value - jnp.mean(value, axis=-1, keepdims=True)
    spread = jnp.mean(center * center, axis=-1, keepdims=True)
    scale = lax.rsqrt(spread + epsilon)
    normal = center * scale
    return (normal * gain + shift, normal, scale)


def norm_backward(upstream, normal, scale, gain):
    inner = upstream * gain
    return scale * (
        inner
        - jnp.mean(inner, axis=-1, keepdims=True)
        - normal * jnp.mean(inner * normal, axis=-1, keepdims=True)
    )


def gelu_slope(hidden):
    return 0.5 * (1.0 + lax.erf(hidden * root_half)) + hidden * inv_root_tau * jnp.exp(
        -0.5 * hidden * hidden
    )


def dot(left, right):
    return jnp.dot(left, right, preferred_element_type=f32)


def dot_left(left, right):
    return lax.dot_general(left, right, (((0,), (0,)), ((), ())), preferred_element_type=f32)


def dot_right(left, right):
    return lax.dot_general(left, right, (((1,), (1,)), ((), ())), preferred_element_type=f32)


def shards(count, copies, *arrays):
    (
        tokens,
        segments,
        padding,
        query_weight,
        key_weight,
        value_weight,
        query_bias,
        value_bias,
        out_weight,
        out_bias,
        middle_gain,
        middle_shift,
        up_weight,
        up_bias,
        down_weight,
        down_bias,
        final_gain,
        final_shift,
        cotangent,
    ) = arrays
    planes = count // PLANE
    rows = query_weight.shape[0]
    block = down_weight.shape[0]
    x_own = tokens[0]
    here = x_own.shape[0]
    wide = PLANE * here
    me = lax.axis_index("shard")
    group = lax.rem(me, PLANE)
    qkv_send = jnp.concatenate(
        [
            item.astype(bf16).reshape(rows, PLANE, GROUP_DIM)
            for item in (query_weight, key_weight, value_weight)
        ],
        axis=2,
    ).transpose(1, 0, 2)
    up_send = (
        up_weight.astype(bf16)
        .reshape(rows, planes, PLANE, block)
        .transpose(2, 0, 1, 3)
        .reshape(PLANE, rows, GROUP_FF)
    )
    codes = (2 * segments[0] + padding[0]).astype(f32)
    lanes = 128 * ((max(here, block) + 127) // 128)

    def padded(value):
        return jnp.pad(value.astype(f32), (0, lanes - value.shape[0]))

    vectors = [
        query_bias,
        value_bias,
        out_bias,
        middle_gain,
        middle_shift,
        down_bias,
        final_gain,
        final_shift,
        up_bias,
        codes,
    ]
    small_send = jnp.pad(
        jnp.stack([padded(item) for item in vectors]), ((0, 6), (0, 0))
    ).astype(bf16)
    lines = [[start + PLANE * step for step in range(planes)] for start in range(PLANE)]
    w_down = lax.all_gather(
        down_weight.astype(bf16), "shard", axis_index_groups=lines, axis=0
    ).reshape(GROUP_FF, D)
    x_all, qkv_all, up_all, wo_all, small = gather_weights(
        count,
        copies,
        x_own,
        qkv_send,
        up_send,
        out_weight.astype(bf16),
        small_send,
        0,
    )
    x_plane = x_all.reshape(wide, D)
    w_qkv = qkv_all.reshape(D, 3 * GROUP_DIM)
    strip = up_all.reshape(PLANE * rows, D)
    w_out = wo_all.reshape(GROUP_DIM, D)
    small = small.astype(f32)
    spread = [small[:, index, :rows].reshape(D) for index in range(8)]
    b_query, b_value, b_out, gain_mid, shift_mid, b_down, gain_end, shift_end = spread
    b_up = lax.dynamic_index_in_dim(
        small[:, 8, :block].reshape(planes, PLANE, block), group, 1, keepdims=False
    ).reshape(GROUP_FF)
    all_codes = small[:, 9, :here].reshape(planes, wide)
    own_codes = lax.dynamic_index_in_dim(all_codes, lax.div(me, PLANE), 0, keepdims=False)

    def group_part(value):
        return lax.dynamic_slice(value, (group * GROUP_DIM,), (GROUP_DIM,))

    qkv_bias = jnp.concatenate(
        [group_part(b_query), jnp.zeros((GROUP_DIM,), f32), group_part(b_value)]
    )
    qkv = (dot(x_plane, w_qkv) + qkv_bias).astype(bf16)
    w_down, qkv = lax.optimization_barrier((w_down, qkv))
    queries = qkv[:, :GROUP_DIM] * bf16(0.125)
    own_row = own_codes[None]
    pairs, context, logs = attend_ahead(
        count, queries, qkv[:, GROUP_DIM:], own_row, all_codes, 1
    )
    strip, pairs = lax.optimization_barrier((strip, pairs))
    w_up = lax.all_gather(strip, "shard", axis_index_groups=lines, axis=0).reshape(D, GROUP_FF)
    context_low = context.astype(bf16)

    def split(value):
        return value.reshape(PLANE, here, D)

    def enter_middle(total, pieces, lines):
        rest = total + lines[0] + pieces[0]
        middle, _, _ = norm_forward(rest, lines[1], lines[2])
        return middle.astype(bf16), [rest], []

    def enter_end(total, pieces, lines):
        middle, _, _ = norm_forward(pieces[0], lines[1], lines[2])
        result, normal, scale = norm_forward(middle + (total + lines[0]), lines[3], lines[4])
        above = pieces[1]
        back = norm_backward(above, normal, scale, lines[3])
        rounded = back.astype(bf16)
        return rounded, [result, back], [above * normal, above, rounded.astype(f32)]

    def leave_middle(total, pieces, lines):
        _, normal, scale = norm_forward(pieces[0], lines[0], lines[0])
        above = total + pieces[1]
        back = norm_backward(above, normal, scale, lines[0])
        rounded = back.astype(bf16)
        return rounded, [back], [above * normal, above, rounded.astype(f32)]

    middle_all, _, rest = plane_step(
        split(dot_left(context_low, w_out).astype(bf16)),
        [x_own],
        [b_out, gain_mid, shift_mid],
        enter_middle,
        [f32],
        2,
    )
    middle_plane = middle_all.reshape(wide, D)
    hidden = dot(middle_plane, w_up) + b_up
    active_low = jax.nn.gelu(hidden, approximate=False).astype(bf16)
    feed_all, end_sums, result, d_second = plane_step(
        split(dot(active_low, w_down).astype(bf16)),
        [rest, cotangent[0]],
        [b_down, gain_mid, shift_mid, gain_end, shift_end],
        enter_end,
        [bf16, f32],
        3,
    )
    output = result[None]
    feed_plane = feed_all.reshape(wide, D)
    grad_down = dot_left(active_low, feed_plane).astype(bf16)
    up_low = (dot_right(feed_plane, w_down) * gelu_slope(hidden)).astype(bf16)
    grad_up = dot_left(middle_plane, up_low).astype(bf16)
    strip_grads = lax.psum_scatter(
        jnp.concatenate(
            [
                grad_up.reshape(planes, PLANE * rows, GROUP_FF),
                grad_down.reshape(planes, block, D),
            ],
            axis=1,
        ),
        "shard",
        axis_index_groups=lines,
        scatter_dimension=0,
    )
    branch_all, middle_sums, d_first = plane_step(
        split(dot_right(up_low, w_up).astype(bf16)),
        [rest, d_second],
        [gain_mid],
        leave_middle,
        [f32],
        4,
    )
    branch_plane = branch_all.reshape(wide, D)
    grad_out = dot(context_low, branch_plane).astype(bf16)
    d_context = dot_right(branch_plane, w_out).astype(bf16)
    delta = jnp.sum(
        (d_context.astype(f32).T * context).reshape(GROUP_HEADS, HEAD_DIM, wide), axis=1
    )
    query_low, pair_low = attend_back(
        count,
        queries,
        d_context,
        pairs,
        own_row,
        all_codes,
        logs,
        delta,
        8,
    )
    mixer_low = jnp.concatenate([query_low.T, pair_low], axis=1)
    grad_qkv = dot_left(x_plane, mixer_low).astype(bf16)
    mixer_sums = jnp.sum(mixer_low.astype(f32), axis=0)

    def from_group(value):
        return lax.dynamic_update_slice(jnp.zeros((D,), f32), value, (group * GROUP_DIM,))

    sums = [
        from_group(mixer_sums[:GROUP_DIM]),
        from_group(mixer_sums[2 * GROUP_DIM :]),
        middle_sums[2],
        middle_sums[0],
        middle_sums[1],
        end_sums[2],
        end_sums[0],
        end_sums[1],
    ]
    own_lane = (jnp.arange(PLANE) == group).astype(f32)
    up_sums = jnp.sum(up_low.astype(f32), axis=0).reshape(planes, 1, block)
    up_sums = (up_sums * own_lane[None, :, None]).reshape(count, 1, block)
    sums = jnp.stack([item.reshape(count, rows) for item in sums], axis=1)
    small_grads = jnp.concatenate(
        [
            jnp.pad(sums, ((0, 0), (0, 0), (0, lanes - rows))),
            jnp.pad(up_sums, ((0, 0), (0, 7), (0, lanes - block))),
        ],
        axis=1,
    ).astype(bf16)
    down_half = strip_grads[PLANE * rows :]
    mixed, wide_sums, out_sums, small_sums, down_sums, input_sums = reduce_grads(
        count,
        copies,
        grad_qkv.reshape(count, rows, 3 * GROUP_DIM),
        strip_grads[: PLANE * rows].reshape(PLANE, rows, GROUP_FF),
        grad_out.reshape(planes, rows, D),
        down_half,
        small_grads,
        split(dot_right(mixer_low, w_qkv).astype(bf16)),
        10,
    )


    def added(value):
        return jnp.sum(value.astype(f32), axis=0)

    query_grad, key_grad, value_grad = [added(mixed[:, place]) for place in range(3)]
    up_grad, out_total, small_total = added(wide_sums), added(out_sums), added(small_sums)
    down_total = added(down_sums) + down_half.astype(f32)
    grad_tokens = (input_sums + d_first).astype(bf16)
    return (
        output,
        grad_tokens[None],
        query_grad,
        key_grad,
        value_grad,
        small_total[0, :rows],
        small_total[1, :rows],
        out_total,
        small_total[2, :rows],
        small_total[3, :rows],
        small_total[4, :rows],
        up_grad,
        small_total[8, :block],
        down_total,
        small_total[5, :rows],
        small_total[6, :rows],
        small_total[7, :rows],
    )


def solution(mesh):
    sheet, line = P("shard", None), P("shard")
    batch = P("rep", "shard", None)
    in_specs = (batch, P("rep", "shard"), P("rep", "shard"), sheet, sheet, sheet, line, line)
    in_specs += (sheet, line, line, line, sheet, line, sheet, line, line, line, batch)
    out_specs = (batch, batch, sheet, sheet, sheet, line, line, sheet, line, line, line)
    out_specs += (sheet, line, sheet, line, line, line)
    body = functools.partial(shards, mesh.shape["shard"], mesh.shape["rep"])
    return jax.shard_map(
        body, mesh=mesh, in_specs=in_specs, out_specs=out_specs, check_vma=False
    )
```

```python
import functools

import jax
import jax.numpy as jnp
from jax import lax
from jax.experimental import pallas as pl
from jax.experimental.pallas import tpu as pltpu
from jax.sharding import PartitionSpec as P

D = 768
HEADS = 12
HEAD_DIM = 64
PLANE = 4
GROUP_HEADS = HEADS // PLANE
GROUP_DIM = GROUP_HEADS * HEAD_DIM
FF = 3072
GROUP_FF = FF // PLANE

epsilon = 1e-12
very_low = -1e30
root_half = 0.7071067811865476
inv_root_tau = 0.3989422804014327
bf16 = jnp.bfloat16
f32 = jnp.float32
MESH = pl.DeviceIdType.MESH
VMEM_SPEC = pl.BlockSpec(memory_space=pltpu.VMEM)
ANY_SPEC = pl.BlockSpec(memory_space=pl.ANY)
VMEM_BYTES = 60000 * 1024
MODEL_BYTES = 100_000_000


def struct(shape, dtype=bf16):
    return jax.ShapeDtypeStruct(shape, dtype)


def comm_call(body, name, ident, inputs, out_shapes, out_specs, scratch):
    return pl.pallas_call(
        body,
        name=name,
        out_shape=out_shapes,
        in_specs=[VMEM_SPEC] * len(inputs),
        out_specs=out_specs,
        scratch_shapes=scratch,
        cost_estimate=pl.CostEstimate(flops=0, bytes_accessed=MODEL_BYTES, transcendentals=0),
        compiler_params=pltpu.CompilerParams(
            collective_id=ident, has_side_effects=True, vmem_limit_bytes=VMEM_BYTES
        ),
    )(*inputs)


def greet(peers):
    barrier = pltpu.get_barrier_semaphore()
    for peer in peers:
        pl.semaphore_signal(barrier, inc=1, device_id=peer, device_id_type=MESH)
    pl.semaphore_wait(barrier, len(peers))


def remote(src, dst, send_sem, recv_sem, peer):
    return pltpu.make_async_remote_copy(
        src_ref=src,
        dst_ref=dst,
        send_sem=send_sem,
        recv_sem=recv_sem,
        device_id=peer,
        device_id_type=MESH,
    )


def plane_peer(me, mask):
    group = lax.rem(me, PLANE)
    core = lax.rem(group, 2)
    column = lax.div(group, 2)
    if mask & 1:
        core = 1 - core
    if mask & 2:
        column = 1 - column
    return me - group + 2 * column + core


def plane_slot(me, mask):
    return lax.rem(plane_peer(me, mask), PLANE)


def plane_step(parts, pieces, vectors, action, out_types, ident):
    _, rows, cols = parts.shape
    chunks = 3 if rows % 48 == 0 else 1
    size = rows // chunks
    many, few = len(pieces), len(out_types)

    def body(p_ref, *rest):
        piece_refs, vector_ref = rest[:many], rest[many]
        all_ref, sums_ref = rest[many + 1 : many + 3]
        out_refs = rest[many + 3 : many + 3 + few]
        near, held, far_in, low, send, recv = rest[many + 3 + few :]
        me = lax.axis_index("shard")
        beside, across = [{"shard": plane_peer(me, mask)} for mask in (1, 2)]
        mine, far = lax.rem(me, PLANE), plane_slot(me, 2)
        greet([beside, across])
        spans = [pl.ds(size * index, size) for index in range(chunks)]

        def copy(kind, index):
            span = spans[index]
            table = {
                0: lambda: (p_ref.at[plane_slot(me, 3), span], near.at[0, span], beside),
                1: lambda: (p_ref.at[plane_slot(me, 1), span], near.at[1, span], beside),
                2: lambda: (held.at[span], far_in.at[span], across),
                3: lambda: (low.at[span], all_ref.at[mine, span], across),
                4: lambda: (low.at[span], all_ref.at[mine, span], beside),
                5: lambda: (all_ref.at[far, span], all_ref.at[far, span], beside),
            }
            src, dst, peer = table[kind]()
            return remote(src, dst, send.at[kind, index], recv.at[kind, index], peer)

        for index in range(chunks):
            copy(0, index).start()
        for index in range(chunks):
            copy(1, index).start()
        for index in range(chunks):
            span = spans[index]
            copy(0, index).wait_recv()
            total = p_ref[plane_slot(me, 2), span].astype(f32) + near[0, span].astype(f32)
            held[span] = total.astype(bf16)
            copy(2, index).start()
        lines = [vector_ref[index : index + 1] for index in range(len(vectors))]
        sums = None
        for index in range(chunks):
            span = spans[index]
            copy(1, index).wait_recv()
            copy(2, index).wait_recv()
            total = p_ref[mine, span].astype(f32) + near[1, span].astype(f32)
            total = total + far_in[span].astype(f32)
            result, outs, terms = action(
                total, [item[span].astype(f32) for item in piece_refs], lines
            )
            low[span] = result
            copy(3, index).start()
            copy(4, index).start()
            for ref, value in zip(out_refs, outs):
                ref[span] = value.astype(ref.dtype)
            all_ref[mine, span] = result
            terms = [jnp.sum(item, axis=0, keepdims=True) for item in terms]
            sums = terms if sums is None else [x + y for x, y in zip(sums, terms)]
        sums_ref[...] = jnp.zeros(sums_ref.shape, f32)
        for place, value in enumerate(sums):
            sums_ref[place : place + 1] = value
        for index in range(chunks):
            copy(3, index).wait_recv()
            copy(5, index).start()
        for index in range(chunks):
            copy(4, index).wait_recv()
            copy(5, index).wait_recv()
        for index in range(chunks):
            for kind in range(6):
                copy(kind, index).wait_send()

    stack = jnp.stack(vectors)
    shape = (rows, cols)
    return comm_call(
        body,
        "plane_step",
        ident,
        [parts] + list(pieces) + [stack],
        [struct((PLANE, rows, cols)), struct((8, cols), f32)]
        + [struct(shape, item) for item in out_types],
        [VMEM_SPEC] * (2 + few),
        [
            pltpu.VMEM((2, rows, cols), bf16),
            pltpu.VMEM(shape, bf16),
            pltpu.VMEM(shape, bf16),
            pltpu.VMEM(shape, bf16),
            pltpu.SemaphoreType.DMA((6, chunks)),
            pltpu.SemaphoreType.DMA((6, chunks)),
        ],
    )


def others(me, count):
    return [{"shard": lax.rem(me + step, count)} for step in range(1, count)]


def gather_weights(count, copies, tokens, qkv, up, out_w, small, ident):
    planes = count // PLANE
    rows = qkv.shape[1]

    def body(x_ref, qkv_ref, up_ref, wo_ref, small_ref, *rest):
        x_out, qkv_out, up_out, wo_out, small_out = rest[:5]
        send, recv, local, send_wo, recv_wo, send_unit, recv_unit = rest[5:]
        me = lax.axis_index("shard")
        group, plane = lax.rem(me, PLANE), lax.div(me, PLANE)
        across = [
            {"rep": lax.rem(lax.axis_index("rep") + step, copies)} for step in range(1, copies)
        ]
        greet(others(me, count) + across)
        owns = [
            (x_ref, x_out.at[group]),
            (qkv_ref.at[group], qkv_out.at[me]),
            (up_ref.at[group], up_out.at[group]),
            (small_ref, small_out.at[me]),
        ]
        started = []
        for index, (src, dst) in enumerate(owns):
            copy = pltpu.make_async_copy(src, dst, local.at[index])
            copy.start()
            started.append(copy)
        sent = []

        def push(src, dst, peer):
            index = len(sent)
            copy = remote(src, dst, send.at[index], recv.at[index], {"shard": peer})
            copy.start()
            sent.append(copy)

        for mask in (2, 1):
            push(x_ref, x_out.at[group], plane_peer(me, mask))
        far = plane_slot(me, 2)
        x_relay = remote(
            x_out.at[far], x_out.at[far], send.at[2], recv.at[2], {"shard": plane_peer(me, 1)}
        )
        sent.append(x_relay)
        for step in range(1, count):
            push(small_ref, small_out.at[me], lax.rem(me + step, count))
        rep = lax.axis_index("rep")
        split = copies == 2
        units = []
        for step in range(planes):
            for lane in range(PLANE):
                if step or lane:
                    units.append((qkv_ref, qkv_out, step, lane))
        for lane in range(1, PLANE):
            units.append((up_ref, up_out, 0, lane))

        def unit_copy(index):
            src, dst, step, lane = units[index]
            goal = lax.rem(plane + step, planes)
            goal_group = lax.rem(group + lane, PLANE)
            slot = group if src is up_ref else me
            return remote(
                src.at[goal_group],
                dst.at[slot],
                send_unit.at[index],
                recv_unit.at[index],
                {"shard": goal * PLANE + goal_group},
            )

        def unit_relay(index):
            src, dst, step, lane = units[index]
            origin = lax.rem(plane + planes - step, planes)
            origin_group = lax.rem(group + PLANE - lane, PLANE)
            slot = origin_group if src is up_ref else origin * PLANE + origin_group
            return remote(
                dst.at[slot],
                dst.at[slot],
                send_unit.at[index],
                recv_unit.at[index],
                {"rep": lax.rem(rep + 1, copies)},
            )

        def carried(index, mine):
            step = units[index][2]
            if not split or step == 0:
                return None
            return (rep == step % 2) if mine else (rep != step % 2)

        def guarded(test, action):
            if test is None:
                action()
            else:
                pl.when(test)(action)

        for index in range(len(units)):
            guarded(carried(index, True), unit_copy(index).start)
        target, place = lax.div(me, planes), lax.rem(me, planes)

        def wo_copy(source, index):
            peer = PLANE * index + target
            return peer, remote(
                wo_ref, wo_out.at[place], send_wo.at[index], recv_wo.at[source], {"shard": peer}
            )

        for index in range(planes):
            peer, copy = wo_copy(place, index)
            pl.when(peer != me)(copy.start)
        keep = pltpu.make_async_copy(wo_ref, wo_out.at[place], local.at[5])
        pl.when(target == group)(keep.start)
        sent[0].wait_recv()
        x_relay.start()
        for index, (_, _, step, _) in enumerate(units):
            if split and step:

                @pl.when(rep == step % 2)
                def _(index=index):
                    unit_relay(index).wait_recv()
                    unit_copy(index).wait_send()
                    unit_relay(index).start()

            else:
                unit_copy(index).wait_recv()
                unit_copy(index).wait_send()
        for index, (_, _, step, _) in enumerate(units):
            if split and step:
                pl.when(rep != step % 2)(unit_relay(index).wait_recv)
                pl.when(rep == step % 2)(unit_relay(index).wait_send)
        for copy in sent[1:]:
            copy.wait_recv()
        for index in range(planes):
            pl.when(group * planes + index != me)(wo_copy(index, index)[1].wait_recv)
        for index in range(planes):
            peer, copy = wo_copy(place, index)
            pl.when(peer != me)(copy.wait_send)
        pl.when(target == group)(keep.wait)
        for copy in sent:
            copy.wait_send()
        for copy in started:
            copy.wait()

    total = 3 + count - 1
    number = count - 1 + PLANE - 1
    return comm_call(
        body,
        "gather_weights",
        ident,
        [tokens, qkv, up, out_w, small],
        [
            struct((PLANE,) + tokens.shape),
            struct((count, rows, qkv.shape[2])),
            struct((PLANE, rows, up.shape[2])),
            struct((planes,) + out_w.shape),
            struct((count,) + small.shape),
        ],
        [ANY_SPEC] * 5,
        [
            pltpu.SemaphoreType.DMA((total,)),
            pltpu.SemaphoreType.DMA((total,)),
            pltpu.SemaphoreType.DMA((6,)),
            pltpu.SemaphoreType.DMA((planes,)),
            pltpu.SemaphoreType.DMA((planes,)),
            pltpu.SemaphoreType.DMA((number,)),
            pltpu.SemaphoreType.DMA((number,)),
        ],
    )


def reduce_grads(count, copies, qkv, up, out_w, down, small, parts, ident):
    planes = count // PLANE
    rows = qkv.shape[1]
    block = down.shape[0]
    arrays = [qkv, up, out_w, small]
    split = copies == 2 and planes % 2 == 0
    pieces = planes // 2

    def body(qkv_ref, up_ref, wo_ref, small_ref, down_ref, p_ref, *rest):
        outs, token_ref, rest = rest[:5], rest[5], rest[6:]
        mix_ref, wide_ref = outs[:2]
        qkv_in, up_in, wo_in, small_in = rest[:4]
        halves = [ref.at[0] for ref in outs[:4]] + [down_ref]
        near, near_sum, far_in = rest[4:7]
        peer_q, sum_q, in_q = rest[7:10]
        send, recv, send_rep, recv_rep, send_wo, recv_wo, send_near, recv_near = rest[10:18]
        send_y, recv_y, send_q, recv_q = rest[18:]
        me = lax.axis_index("shard")
        rep = lax.axis_index("rep")
        plane = lax.div(me, PLANE)
        across = [{"rep": lax.rem(rep + step, copies)} for step in range(1, copies)]
        greet(others(me, count) + across)
        sent = []

        def push(src, dst, peer):
            index = len(sent)
            copy = remote(src, dst, send.at[index], recv.at[index], {"shard": peer})
            copy.start()
            sent.append(copy)

        pairs = [(small_ref, small_in)] if split else [(qkv_ref, qkv_in), (small_ref, small_in)]
        swaps = []
        if split:
            for index in range(pieces):
                goal = lax.rem(plane + 1 - rep + 2 * index, planes)
                swaps.append(
                    remote(
                        qkv_ref.at[pl.ds(goal * PLANE, PLANE)],
                        peer_q.at[index],
                        send_y.at[index],
                        recv_y.at[index],
                        across[0],
                    )
                )
            for copy in swaps[::-1]:
                copy.start()
        passed = []
        beside, over = [{"shard": plane_peer(me, mask)} for mask in (1, 2)]
        near_copies = [
            remote(p_ref.at[plane_slot(me, 3)], near.at[0], send_near.at[0], recv_near.at[0], beside),
            remote(p_ref.at[plane_slot(me, 1)], near.at[1], send_near.at[1], recv_near.at[1], beside),
            remote(near_sum, far_in, send_near.at[2], recv_near.at[2], over),
        ]
        near_copies[0].start()
        near_copies[1].start()

        def exchange(*places):
            for index, peer in enumerate(across):
                for place in places:
                    copy = remote(
                        halves[place],
                        outs[place].at[index if place == 4 else index + 1],
                        send_rep.at[5 * index + place],
                        recv_rep.at[5 * index + place],
                        peer,
                    )
                    copy.start()
                    passed.append(copy)

        exchange(4)
        group = lax.rem(me, PLANE)
        target, place = lax.div(me, planes), lax.rem(me, planes)
        for lane in range(1, PLANE):
            goal = lax.rem(group + lane, PLANE)
            push(up_ref.at[goal], up_in.at[group], plane * PLANE + goal)
        up_in[group] = up_ref[group]
        for src, held in pairs:
            for step in range(1, count):
                peer = lax.rem(me + step, count)
                push(src.at[peer], held.at[me], peer)
        for src, held in pairs:
            held[me] = src[me]

        def wo_copy(source, index):
            peer = group * planes + index
            return peer, remote(
                wo_ref.at[index],
                wo_in.at[plane],
                send_wo.at[index],
                recv_wo.at[source],
                {"shard": peer},
            )

        for index in range(planes):
            peer, copy = wo_copy(plane, index)
            pl.when(peer != me)(copy.start)

        @pl.when(target == group)
        def _():
            wo_in[plane] = wo_ref[place]

        moved = []
        for index in reversed(range(pieces if split else 0)):
            goal = lax.rem(plane + rep + 2 * index, planes)
            swaps[index].wait_recv()
            for lane in range(PLANE):
                total = qkv_ref[goal * PLANE + lane].astype(f32) + peer_q[index, lane].astype(f32)
                sum_q[index, lane] = total.astype(bf16)
            for step in range(PLANE):
                lane = lax.rem(group + step, PLANE)
                number = index * PLANE + step
                copy = remote(
                    sum_q.at[index, lane],
                    in_q.at[index, group],
                    send_q.at[number],
                    recv_q.at[number],
                    {"shard": goal * PLANE + lane},
                )
                if number:
                    copy.start()
                else:
                    pl.when(rep != 0)(copy.start)

                    @pl.when(rep == 0)
                    def _():
                        in_q[0, group] = sum_q[0, group]

                moved.append((number, copy))
        near_copies[0].wait_recv()
        total = p_ref[plane_slot(me, 2)].astype(f32) + near[0].astype(f32)
        near_sum[...] = total.astype(bf16)
        near_copies[2].start()
        for copy in sent[: PLANE - 1]:
            copy.wait_recv()
        for lane in range(PLANE):
            value = up_in[lane]
            for index in range(planes):
                low = (index * PLANE + lane) * block
                wide_ref[0, :, low : low + block] = value[:, index * block : (index + 1) * block]
        exchange(1)
        for index in range(planes):
            pl.when(PLANE * index + target != me)(wo_copy(index, index)[1].wait_recv)
        for index in range(planes):
            peer, copy = wo_copy(plane, index)
            pl.when(peer != me)(copy.wait_send)
        total = wo_in[0].astype(f32)
        for other in range(1, planes):
            total = total + wo_in[other].astype(f32)
        halves[2][...] = total.astype(bf16)
        exchange(2)
        near_copies[1].wait_recv()
        near_copies[2].wait_recv()
        total = p_ref[lax.rem(me, PLANE)].astype(f32) + near[1].astype(f32)
        token_ref[...] = total + far_in[...].astype(f32)
        for copy in sent[PLANE - 1 :]:
            copy.wait_recv()
        for number, copy in moved:
            if number:
                copy.wait_recv()
            else:
                pl.when(rep != 0)(copy.wait_recv)
        for lane in range(PLANE):
            if split:
                terms = [in_q[index, lane] for index in range(pieces)]
            else:
                terms = [qkv_in[other * PLANE + lane] for other in range(planes)]
            total = terms[0].astype(f32)
            for term in terms[1:]:
                total = total + term.astype(f32)
            total = total.astype(bf16)
            for place in range(3):
                low = place * GROUP_DIM
                mix_ref[0, place, :, lane * GROUP_DIM : (lane + 1) * GROUP_DIM] = total[
                    :, low : low + GROUP_DIM
                ]
        for half, held, number in (
            (halves[3], small_in, count),
        ):
            total = held[0].astype(f32)
            for other in range(1, number):
                total = total + held[other].astype(f32)
            half[...] = total.astype(bf16)
        exchange(0, 3)
        for copy in passed:
            copy.wait_recv()
        for copy in sent + passed + near_copies + swaps:
            copy.wait_send()
        for number, copy in moved:
            if number:
                copy.wait_send()
            else:
                pl.when(rep != 0)(copy.wait_send)

    totals = (1 if split else 2) * (count - 1) + PLANE - 1
    shapes = [
        (copies, 3, rows, D),
        (copies, rows, FF),
        (copies, rows, D),
        (copies,) + small.shape[1:],
        (copies - 1, block, D),
    ]
    return comm_call(
        body,
        "reduce_grads",
        ident,
        arrays + [down, parts],
        [struct(shape) for shape in shapes] + [struct(parts.shape[1:], f32)],
        [VMEM_SPEC] * 6,
        [pltpu.VMEM(item.shape, bf16) for item in arrays]
        + [
            pltpu.VMEM((2,) + parts.shape[1:], bf16),
            pltpu.VMEM(parts.shape[1:], bf16),
            pltpu.VMEM(parts.shape[1:], bf16),
            pltpu.VMEM((pieces, PLANE) + qkv.shape[1:], bf16),
            pltpu.VMEM((pieces, PLANE) + qkv.shape[1:], bf16),
            pltpu.VMEM((pieces, PLANE) + qkv.shape[1:], bf16),
            pltpu.SemaphoreType.DMA((totals,)),
            pltpu.SemaphoreType.DMA((totals,)),
            pltpu.SemaphoreType.DMA((5 * (copies - 1),)),
            pltpu.SemaphoreType.DMA((5 * (copies - 1),)),
            pltpu.SemaphoreType.DMA((planes,)),
            pltpu.SemaphoreType.DMA((planes,)),
            pltpu.SemaphoreType.DMA((3,)),
            pltpu.SemaphoreType.DMA((3,)),
            pltpu.SemaphoreType.DMA((pieces,)),
            pltpu.SemaphoreType.DMA((pieces,)),
            pltpu.SemaphoreType.DMA((pieces * PLANE,)),
            pltpu.SemaphoreType.DMA((pieces * PLANE,)),
        ],
    )


def pick(plane, table):
    value = table[-1]
    for index in range(len(table) - 1):
        value = jnp.where(plane == index, table[index], value)
    return value


def columns(code_ref, col_ref):
    for index in range(code_ref.shape[0]):
        line = jnp.broadcast_to(code_ref[index : index + 1], (8, code_ref.shape[1]))
        col_ref[index] = line.T[:, 0:1]


def attend_back(count, queries, upstream, pairs, own_row, codes, logs, delta, ident):
    planes, rows, cols = pairs.shape
    half = cols // 2
    size = 256 if rows % 256 == 0 else rows
    orders = []
    for plane in range(planes):
        goals = [goal for goal in range(planes) if goal != plane]
        goals.sort(key=lambda goal: (-abs(goal - plane), goal))
        orders.append(goals + [plane])

    def body(q_ref, up_ref, kv_ref, row_ref, code_ref, log_ref, delta_ref, *rest):
        dq_ref, out_ref, dq_sum, part, held, staged, col_ref, send, recv = rest
        me = lax.axis_index("shard")
        plane = lax.div(me, PLANE)
        greet([{"shard": lax.rem(me + PLANE * s, count)} for s in range(1, planes)])
        columns(code_ref, col_ref)
        dq_sum[...] = jnp.zeros(dq_sum.shape, f32)

        def hop(way, goal):
            peer = me + PLANE if way == 0 else me - PLANE
            return remote(
                staged.at[goal],
                held.at[way, goal],
                send.at[goal],
                recv.at[way, goal],
                {"shard": lax.rem(peer + count, count)},
            )

        def compute(goal):
            part[...] = jnp.zeros(part.shape, f32)
            key_codes = col_ref[goal]

            def chunk(index, carry):
                at = pl.multiple_of(index * size, size)
                span = pl.ds(at, size)
                allowed = key_codes == row_ref[0:1, span]
                for head in range(GROUP_HEADS):
                    low, high = head * HEAD_DIM, (head + 1) * HEAD_DIM
                    q = q_ref[span, low:high]
                    g = up_ref[span, low:high]
                    k = kv_ref[goal, :, low:high]
                    v = kv_ref[goal, :, half + low : half + high]
                    raw = dot_right(k, q)
                    chances = jnp.where(
                        allowed, jnp.exp(raw - log_ref[head : head + 1, span]), 0.0
                    )
                    d_chance = dot_right(v, g)
                    d_score = (chances * (d_chance - delta_ref[head : head + 1, span])).astype(bf16)
                    dq_sum[low:high, span] += dot_left(k, d_score)
                    part[:, low:high] += dot(d_score, q)
                    part[:, half + low : half + high] += dot(chances.astype(bf16), g)
                return carry

            lax.fori_loop(0, rows // size, chunk, 0)

        def pass_on(goal):
            for way in (0, 1):
                ahead = goal > plane if way == 0 else goal < plane
                first = plane == 0 if way == 0 else plane == planes - 1

                @pl.when(ahead & jnp.logical_not(first))
                def _(way=way):
                    copy = hop(way, goal)
                    copy.wait_recv()
                    total = staged[goal].astype(f32) + held[way, goal].astype(f32)
                    staged[goal] = total.astype(bf16)
                    copy.start()

        def begin(goal):
            for way in (0, 1):
                ahead = goal > plane if way == 0 else goal < plane
                first = plane == 0 if way == 0 else plane == planes - 1

                @pl.when(ahead & first)
                def _(way=way):
                    hop(way, goal).start()

        goals = [pick(plane, [order[i] for order in orders]) for i in range(planes)]
        for index in range(planes):
            goal = goals[index]
            compute(goal)
            if index < planes - 1:
                staged[goal] = part[...].astype(bf16)
                begin(goal)
            if index:
                pass_on(goals[index - 1])
        dq_ref[...] = (dq_sum[...] * 0.125).astype(bf16)
        for way in (0, 1):
            behind = plane > 0 if way == 0 else plane < planes - 1

            @pl.when(behind)
            def _(way=way):
                hop(way, plane).wait_recv()
                part[...] += held[way, plane].astype(f32)

        out_ref[...] = part[...].astype(bf16)
        for index in range(planes - 1):
            hop(0, goals[index]).wait_send()

    return comm_call(
        body,
        "attend_back",
        ident,
        [queries, upstream, pairs, own_row, codes, logs, delta],
        [struct((half, rows)), struct((rows, cols))],
        [VMEM_SPEC] * 2,
        [
            pltpu.VMEM((half, rows), f32),
            pltpu.VMEM((rows, cols), f32),
            pltpu.VMEM((2, planes, rows, cols), bf16),
            pltpu.VMEM((planes, rows, cols), bf16),
            pltpu.VMEM((planes, rows, 1), f32),
            pltpu.SemaphoreType.DMA((planes,)),
            pltpu.SemaphoreType.DMA((2, planes)),
        ],
    )


def attend_ahead(count, queries, own_pair, own_row, codes, ident):
    planes = count // PLANE
    rows, cols = own_pair.shape
    half = cols // 2
    size = 256 if rows % 256 == 0 else rows
    orders, flags = [], []
    for plane in range(planes):
        order = sorted(range(planes), key=lambda source: (abs(source - plane), source))
        away = [abs(source - plane) for source in order] + [-1]
        orders.append(order)
        flags.append([int(i > 0 and away[i] == away[i + 1]) for i in range(planes)])

    def body(q_ref, kv_ref, row_ref, code_ref, all_ref, ctx_ref, log_ref, *rest):
        top, total, col_ref, send, recv, local = rest
        me = lax.axis_index("shard")
        plane = lax.div(me, PLANE)
        greet([{"shard": lax.rem(me + PLANE * s, count)} for s in range(1, planes)])
        own = pltpu.make_async_copy(kv_ref, all_ref.at[plane], local)
        own.start()
        up, down = plane < planes - 1, plane > 0

        def hop(way, source, src):
            peer = me + PLANE if way == 0 else me - PLANE
            return remote(
                src,
                all_ref.at[source],
                send.at[way, source],
                recv.at[way, source],
                {"shard": lax.rem(peer + count, count)},
            )

        pl.when(up)(hop(0, plane, kv_ref).start)
        pl.when(down)(hop(1, plane, kv_ref).start)
        columns(code_ref, col_ref)
        top[...] = jnp.full(top.shape, very_low, f32)
        total[...] = jnp.zeros(total.shape, f32)
        ctx_ref[...] = jnp.zeros(ctx_ref.shape, f32)

        def take(source, test):
            for way in (0, 1):
                came = source < plane if way == 0 else source > plane
                onward = up if way == 0 else down

                @pl.when(test & came)
                def _(way=way, onward=onward):
                    copy = hop(way, source, all_ref.at[source])
                    copy.wait_recv()
                    pl.when(onward)(copy.start)

        def compute(source, block):
            key_codes = col_ref[source]

            def chunk(index, carry):
                span = pl.ds(pl.multiple_of(index * size, size), size)
                allowed = key_codes == row_ref[0:1, span]
                for head in range(GROUP_HEADS):
                    low, high = head * HEAD_DIM, (head + 1) * HEAD_DIM
                    line = slice(head, head + 1)
                    raw = dot_right(block[:, low:high], q_ref[span, low:high])
                    masked = jnp.where(allowed, raw, very_low)
                    before = top[line, span]
                    after = jnp.maximum(before, jnp.max(masked, axis=0, keepdims=True))
                    rescale = jnp.exp(before - after)
                    weights = jnp.exp(masked - after)
                    top[line, span] = after
                    total[line, span] = total[line, span] * rescale + jnp.sum(
                        weights, axis=0, keepdims=True
                    )
                    added = dot_left(block[:, half + low : half + high], weights.astype(bf16))
                    ctx_ref[low:high, span] = ctx_ref[low:high, span] * rescale + added
                return carry

            lax.fori_loop(0, rows // size, chunk, 0)

        compute(plane, kv_ref)
        sources = [pick(plane, [order[i] for order in orders]) for i in range(planes)]
        early = [pick(plane, [flag[i] for flag in flags]) == 1 for i in range(planes)]
        for index in range(1, planes):
            test = jnp.logical_not(early[index - 1])
            take(sources[index], test)
            if index + 1 < planes:
                take(sources[index + 1], early[index])
            compute(sources[index], all_ref.at[sources[index]])
        log_ref[...] = top[...] + jnp.log(total[...])
        for head in range(GROUP_HEADS):
            low, high = head * HEAD_DIM, (head + 1) * HEAD_DIM
            ctx_ref[low:high] = ctx_ref[low:high] / total[head : head + 1]
        pl.when(up)(hop(0, plane, kv_ref).wait_send)
        pl.when(down)(hop(1, plane, kv_ref).wait_send)
        for index in range(1, planes):
            source = sources[index]
            pl.when((source < plane) & up)(hop(0, source, all_ref.at[source]).wait_send)
            pl.when((source > plane) & down)(hop(1, source, all_ref.at[source]).wait_send)
        own.wait()

    return comm_call(
        body,
        "attend_ahead",
        ident,
        [queries, own_pair, own_row, codes],
        [
            struct((planes, rows, cols)),
            struct((half, rows), f32),
            struct((GROUP_HEADS, rows), f32),
        ],
        [VMEM_SPEC] * 3,
        [
            pltpu.VMEM((GROUP_HEADS, rows), f32),
            pltpu.VMEM((GROUP_HEADS, rows), f32),
            pltpu.VMEM((planes, rows, 1), f32),
            pltpu.SemaphoreType.DMA((2, planes)),
            pltpu.SemaphoreType.DMA((2, planes)),
            pltpu.SemaphoreType.DMA,
        ],
    )


def norm_forward(value, gain, shift):
    center = value - jnp.mean(value, axis=-1, keepdims=True)
    spread = jnp.mean(center * center, axis=-1, keepdims=True)
    scale = lax.rsqrt(spread + epsilon)
    normal = center * scale
    return (normal * gain + shift, normal, scale)


def norm_backward(upstream, normal, scale, gain):
    inner = upstream * gain
    return scale * (
        inner
        - jnp.mean(inner, axis=-1, keepdims=True)
        - normal * jnp.mean(inner * normal, axis=-1, keepdims=True)
    )


def gelu_slope(hidden):
    return 0.5 * (1.0 + lax.erf(hidden * root_half)) + hidden * inv_root_tau * jnp.exp(
        -0.5 * hidden * hidden
    )


def dot(left, right):
    return jnp.dot(left, right, preferred_element_type=f32)


def dot_left(left, right):
    return lax.dot_general(left, right, (((0,), (0,)), ((), ())), preferred_element_type=f32)


def dot_right(left, right):
    return lax.dot_general(left, right, (((1,), (1,)), ((), ())), preferred_element_type=f32)


def shards(count, copies, *arrays):
    (
        tokens,
        segments,
        padding,
        query_weight,
        key_weight,
        value_weight,
        query_bias,
        value_bias,
        out_weight,
        out_bias,
        middle_gain,
        middle_shift,
        up_weight,
        up_bias,
        down_weight,
        down_bias,
        final_gain,
        final_shift,
        cotangent,
    ) = arrays
    planes = count // PLANE
    rows = query_weight.shape[0]
    block = down_weight.shape[0]
    x_own = tokens[0]
    here = x_own.shape[0]
    wide = PLANE * here
    me = lax.axis_index("shard")
    group = lax.rem(me, PLANE)
    qkv_send = jnp.concatenate(
        [
            item.astype(bf16).reshape(rows, PLANE, GROUP_DIM)
            for item in (query_weight, key_weight, value_weight)
        ],
        axis=2,
    ).transpose(1, 0, 2)
    up_send = (
        up_weight.astype(bf16)
        .reshape(rows, planes, PLANE, block)
        .transpose(2, 0, 1, 3)
        .reshape(PLANE, rows, GROUP_FF)
    )
    codes = (2 * segments[0] + padding[0]).astype(f32)
    lanes = 128 * ((max(here, block) + 127) // 128)

    def padded(value):
        return jnp.pad(value.astype(f32), (0, lanes - value.shape[0]))

    vectors = [
        query_bias,
        value_bias,
        out_bias,
        middle_gain,
        middle_shift,
        down_bias,
        final_gain,
        final_shift,
        up_bias,
        codes,
    ]
    small_send = jnp.pad(
        jnp.stack([padded(item) for item in vectors]), ((0, 6), (0, 0))
    ).astype(bf16)
    lines = [[start + PLANE * step for step in range(planes)] for start in range(PLANE)]
    w_down = lax.all_gather(
        down_weight.astype(bf16), "shard", axis_index_groups=lines, axis=0
    ).reshape(GROUP_FF, D)
    x_all, qkv_all, up_all, wo_all, small = gather_weights(
        count,
        copies,
        x_own,
        qkv_send,
        up_send,
        out_weight.astype(bf16),
        small_send,
        0,
    )
    x_plane = x_all.reshape(wide, D)
    w_qkv = qkv_all.reshape(D, 3 * GROUP_DIM)
    strip = up_all.reshape(PLANE * rows, D)
    w_out = wo_all.reshape(GROUP_DIM, D)
    small = small.astype(f32)
    spread = [small[:, index, :rows].reshape(D) for index in range(8)]
    b_query, b_value, b_out, gain_mid, shift_mid, b_down, gain_end, shift_end = spread
    b_up = lax.dynamic_index_in_dim(
        small[:, 8, :block].reshape(planes, PLANE, block), group, 1, keepdims=False
    ).reshape(GROUP_FF)
    all_codes = small[:, 9, :here].reshape(planes, wide)
    own_codes = lax.dynamic_index_in_dim(all_codes, lax.div(me, PLANE), 0, keepdims=False)

    def group_part(value):
        return lax.dynamic_slice(value, (group * GROUP_DIM,), (GROUP_DIM,))

    qkv_bias = jnp.concatenate(
        [group_part(b_query), jnp.zeros((GROUP_DIM,), f32), group_part(b_value)]
    )
    qkv = (dot(x_plane, w_qkv) + qkv_bias).astype(bf16)
    w_down, qkv = lax.optimization_barrier((w_down, qkv))
    queries = qkv[:, :GROUP_DIM] * bf16(0.125)
    own_row = own_codes[None]
    pairs, context, logs = attend_ahead(
        count, queries, qkv[:, GROUP_DIM:], own_row, all_codes, 1
    )
    strip, pairs = lax.optimization_barrier((strip, pairs))
    w_up = lax.all_gather(strip, "shard", axis_index_groups=lines, axis=0).reshape(D, GROUP_FF)
    context_low = context.astype(bf16)

    def split(value):
        return value.reshape(PLANE, here, D)

    def enter_middle(total, pieces, lines):
        rest = total + lines[0] + pieces[0]
        middle, _, _ = norm_forward(rest, lines[1], lines[2])
        return middle.astype(bf16), [rest], []

    def enter_end(total, pieces, lines):
        middle, _, _ = norm_forward(pieces[0], lines[1], lines[2])
        result, normal, scale = norm_forward(middle + (total + lines[0]), lines[3], lines[4])
        above = pieces[1]
        back = norm_backward(above, normal, scale, lines[3])
        rounded = back.astype(bf16)
        return rounded, [result, back], [above * normal, above, rounded.astype(f32)]

    def leave_middle(total, pieces, lines):
        _, normal, scale = norm_forward(pieces[0], lines[0], lines[0])
        above = total + pieces[1]
        back = norm_backward(above, normal, scale, lines[0])
        rounded = back.astype(bf16)
        return rounded, [back], [above * normal, above, rounded.astype(f32)]

    middle_all, _, rest = plane_step(
        split(dot_left(context_low, w_out).astype(bf16)),
        [x_own],
        [b_out, gain_mid, shift_mid],
        enter_middle,
        [f32],
        2,
    )
    middle_plane = middle_all.reshape(wide, D)
    hidden = dot(middle_plane, w_up) + b_up
    active_low = (hidden * (0.5 * (1.0 + lax.erf(hidden * root_half)))).astype(bf16)
    feed_all, end_sums, result, d_second = plane_step(
        split(dot(active_low, w_down).astype(bf16)),
        [rest, cotangent[0]],
        [b_down, gain_mid, shift_mid, gain_end, shift_end],
        enter_end,
        [bf16, f32],
        3,
    )
    output = result[None]
    feed_plane = feed_all.reshape(wide, D)
    grad_down = dot_left(active_low, feed_plane).astype(bf16)
    up_low = (dot_right(feed_plane, w_down) * gelu_slope(hidden)).astype(bf16)
    grad_up = dot_left(middle_plane, up_low).astype(bf16)
    strip_grads = lax.psum_scatter(
        jnp.concatenate(
            [
                grad_up.reshape(planes, PLANE * rows, GROUP_FF),
                grad_down.reshape(planes, block, D),
            ],
            axis=1,
        ),
        "shard",
        axis_index_groups=lines,
        scatter_dimension=0,
    )
    branch_all, middle_sums, d_first = plane_step(
        split(dot_right(up_low, w_up).astype(bf16)),
        [rest, d_second],
        [gain_mid],
        leave_middle,
        [f32],
        4,
    )
    branch_plane = branch_all.reshape(wide, D)
    grad_out = dot(context_low, branch_plane).astype(bf16)
    d_context = dot_right(branch_plane, w_out).astype(bf16)
    delta = jnp.sum(
        (d_context.astype(f32).T * context).reshape(GROUP_HEADS, HEAD_DIM, wide), axis=1
    )
    query_low, pair_low = attend_back(
        count,
        queries,
        d_context,
        pairs,
        own_row,
        all_codes,
        logs,
        delta,
        8,
    )
    mixer_low = jnp.concatenate([query_low.T, pair_low], axis=1)
    grad_qkv = dot_left(x_plane, mixer_low).astype(bf16)
    mixer_sums = jnp.sum(mixer_low.astype(f32), axis=0)

    def from_group(value):
        return lax.dynamic_update_slice(jnp.zeros((D,), f32), value, (group * GROUP_DIM,))

    sums = [
        from_group(mixer_sums[:GROUP_DIM]),
        from_group(mixer_sums[2 * GROUP_DIM :]),
        middle_sums[2],
        middle_sums[0],
        middle_sums[1],
        end_sums[2],
        end_sums[0],
        end_sums[1],
    ]
    own_lane = (jnp.arange(PLANE) == group).astype(f32)
    up_sums = jnp.sum(up_low.astype(f32), axis=0).reshape(planes, 1, block)
    up_sums = (up_sums * own_lane[None, :, None]).reshape(count, 1, block)
    sums = jnp.stack([item.reshape(count, rows) for item in sums], axis=1)
    small_grads = jnp.concatenate(
        [
            jnp.pad(sums, ((0, 0), (0, 0), (0, lanes - rows))),
            jnp.pad(up_sums, ((0, 0), (0, 7), (0, lanes - block))),
        ],
        axis=1,
    ).astype(bf16)
    down_half = strip_grads[PLANE * rows :]
    mixed, wide_sums, out_sums, small_sums, down_sums, input_sums = reduce_grads(
        count,
        copies,
        grad_qkv.reshape(count, rows, 3 * GROUP_DIM),
        strip_grads[: PLANE * rows].reshape(PLANE, rows, GROUP_FF),
        grad_out.reshape(planes, rows, D),
        down_half,
        small_grads,
        split(dot_right(mixer_low, w_qkv).astype(bf16)),
        10,
    )


    def added(value):
        return jnp.sum(value.astype(f32), axis=0)

    query_grad, key_grad, value_grad = [added(mixed[:, place]) for place in range(3)]
    up_grad, out_total, small_total = added(wide_sums), added(out_sums), added(small_sums)
    down_total = added(down_sums) + down_half.astype(f32)
    grad_tokens = (input_sums + d_first).astype(bf16)
    return (
        output,
        grad_tokens[None],
        query_grad,
        key_grad,
        value_grad,
        small_total[0, :rows],
        small_total[1, :rows],
        out_total,
        small_total[2, :rows],
        small_total[3, :rows],
        small_total[4, :rows],
        up_grad,
        small_total[8, :block],
        down_total,
        small_total[5, :rows],
        small_total[6, :rows],
        small_total[7, :rows],
    )


def solution(mesh):
    sheet, line = P("shard", None), P("shard")
    batch = P("rep", "shard", None)
    in_specs = (batch, P("rep", "shard"), P("rep", "shard"), sheet, sheet, sheet, line, line)
    in_specs += (sheet, line, line, line, sheet, line, sheet, line, line, line, batch)
    out_specs = (batch, batch, sheet, sheet, sheet, line, line, sheet, line, line, line)
    out_specs += (sheet, line, sheet, line, line, line)
    body = functools.partial(shards, mesh.shape["shard"], mesh.shape["rep"])
    return jax.shard_map(
        body, mesh=mesh, in_specs=in_specs, out_specs=out_specs, check_vma=False
    )
```
